8 devices in a mesh: rep: 1 (over z), yz: 2 (over y), x: 4 (over x, core).
Axes of the slice: x: 2, y: 2, z: 1, core: 2. Of those that a mesh axis runs over, the one named last changes fastest.
Arguments:
- hidden: bfloat16 [256, 1536], P('rep', ('x', 'yz'))
- norm_gain: bfloat16 [2, 1536], P(None, 'x')
- w_attn: bfloat16 [2, 1536, 2048], P(None, 'x', 'yz')
- w_mlp: bfloat16 [2, 1536, 2, 8960], P(None, 'x', None, 'yz')
- w_out: bfloat16 [2, 1536, 1536], P(None, 'yz', 'x')
- w_down: bfloat16 [2, 8960, 1536], P(None, 'yz', 'x')
- k_cache: bfloat16 [2, 256, 2, 1024, 128], P(None, ('rep', 'x', 'yz'))
- v_cache: bfloat16 [2, 256, 2, 1024, 128], P(None, ('rep', 'x', 'yz'))
- lengths: int32 [256], P(('rep', 'x', 'yz'))
Outputs:
- output 1: bfloat16 [256, 1536], P('rep', ('x', 'yz'))
- output 2: bfloat16 [2, 256, 2, 1024, 128], P(None, ('rep', 'x', 'yz'))
- output 3: bfloat16 [2, 256, 2, 1024, 128], P(None, ('rep', 'x', 'yz'))
All inputs are finite; a program needn't handle non-finite values.
Results may differ from the reference program's by a relative error of at most 0.0192237.
Values are sent between devices in bfloat16 or wider.
A program may use at most 1 GiB of HBM per device.

```python
import math
import jax
import jax.numpy as jnp
from jax import lax

MODEL_DIM = 1536
NUM_HEADS = 12
KV_HEADS = 2
HEAD_DIM = 128
MLP_DIM = 8960
LAYERS = 2
CACHE_LEN = 1024
NUM_SEQS = 256
GROUP_SIZE = NUM_HEADS // KV_HEADS
ATTN_COLS = (NUM_HEADS + 2 * KV_HEADS) * HEAD_DIM
NORM_EPS = 1e-5


def setup_inputs(seed: int = 0, part: int = 0) -> dict:
    shared_keys = jax.random.split(jax.random.key(seed), 5)
    own_keys = jax.random.split(jax.random.fold_in(jax.random.key(seed + 1), part), 4)
    col_scale = 0.4 + 1.2 * jnp.arange(MODEL_DIM, dtype=jnp.float32) / MODEL_DIM
    hidden = (jax.random.normal(own_keys[0], (NUM_SEQS, MODEL_DIM), jnp.float32) * col_scale).astype(jnp.bfloat16)
    norm_gain = jax.random.uniform(shared_keys[0], (LAYERS, MODEL_DIM), jnp.float32, 0.5, 1.5).astype(jnp.bfloat16)
    w_attn = (jax.random.normal(shared_keys[1], (LAYERS, MODEL_DIM, ATTN_COLS), jnp.float32) * MODEL_DIM ** -0.5).astype(jnp.bfloat16)
    w_mlp = (jax.random.normal(shared_keys[2], (LAYERS, MODEL_DIM, 2, MLP_DIM), jnp.float32) * MODEL_DIM ** -0.5).astype(jnp.bfloat16)
    w_out = (jax.random.normal(shared_keys[3], (LAYERS, NUM_HEADS * HEAD_DIM, MODEL_DIM), jnp.float32) * (NUM_HEADS * HEAD_DIM) ** -0.5).astype(jnp.bfloat16)
    w_down = (jax.random.normal(shared_keys[4], (LAYERS, MLP_DIM, MODEL_DIM), jnp.float32) * MLP_DIM ** -0.5).astype(jnp.bfloat16)
    key_scale = math.sqrt(math.log(CACHE_LEN / 4.0))
    cache_shape = (LAYERS, NUM_SEQS, KV_HEADS, CACHE_LEN, HEAD_DIM)
    k_cache = (jax.random.normal(own_keys[1], cache_shape, jnp.float32) * key_scale).astype(jnp.bfloat16)
    v_cache = jax.random.normal(own_keys[2], cache_shape, jnp.float32).astype(jnp.bfloat16)
    drawn = jax.random.randint(own_keys[3], (NUM_SEQS,), 1, CACHE_LEN, jnp.int32)
    lengths = drawn.at[0].set(CACHE_LEN - 1).at[1].set(1)
    return {'hidden': hidden, 'norm_gain': norm_gain, 'w_attn': w_attn, 'w_mlp': w_mlp, 'w_out': w_out, 'w_down': w_down, 'k_cache': k_cache, 'v_cache': v_cache, 'lengths': lengths}


def reference(hidden, norm_gain, w_attn, w_mlp, w_out, w_down, k_cache, v_cache, lengths):
    positions = jnp.arange(CACHE_LEN)
    slot_hit = (positions[None, :] == lengths[:, None])[:, None, :, None]
    visible = (positions[None, :] <= lengths[:, None])[:, None, None, :]

    def decode_layer(current, params):
        gain_l, attn_l, mlp_l, out_l, down_l, keys_l, vals_l = params
        current_f = current.astype(jnp.float32)
        inv_rms = lax.rsqrt(jnp.mean(current_f * current_f, axis=1, keepdims=True) + NORM_EPS)
        normed = (current_f * inv_rms * gain_l.astype(jnp.float32)).astype(jnp.bfloat16)
        attn_z = jnp.dot(normed, attn_l, preferred_element_type=jnp.float32).astype(jnp.bfloat16)
        mlp_z = jnp.dot(normed, mlp_l.reshape(MODEL_DIM, 2 * MLP_DIM), preferred_element_type=jnp.float32).astype(jnp.bfloat16)
        qkv_rows = attn_z.reshape(NUM_SEQS, KV_HEADS, GROUP_SIZE + 2, HEAD_DIM)
        queries = qkv_rows[:, :, :GROUP_SIZE]
        key_new = qkv_rows[:, :, GROUP_SIZE]
        val_new = qkv_rows[:, :, GROUP_SIZE + 1]
        keys_upd = jnp.where(slot_hit, key_new[:, :, None, :], keys_l)
        vals_upd = jnp.where(slot_hit, val_new[:, :, None, :], vals_l)
        scores = jnp.einsum('bgqd,bgsd->bgqs', queries.astype(jnp.float32), keys_upd.astype(jnp.float32)) * HEAD_DIM ** -0.5
        scores = jnp.where(visible, scores, -1e30)
        probs = jax.nn.softmax(scores, axis=-1).astype(jnp.bfloat16)
        attn_o = jnp.einsum('bgqs,bgsd->bgqd', probs.astype(jnp.float32), vals_upd.astype(jnp.float32)).astype(jnp.bfloat16)
        gate_up = mlp_z.reshape(NUM_SEQS, 2, MLP_DIM).astype(jnp.float32)
        mixed = (jax.nn.silu(gate_up[:, 0]) * gate_up[:, 1]).astype(jnp.bfloat16)
        update = jnp.dot(attn_o.reshape(NUM_SEQS, NUM_HEADS * HEAD_DIM), out_l, preferred_element_type=jnp.float32) + jnp.dot(mixed, down_l, preferred_element_type=jnp.float32)
        return (current_f + update).astype(jnp.bfloat16), (keys_upd, vals_upd)

    hidden_out, cache_pair = lax.scan(decode_layer, hidden, (norm_gain, w_attn, w_mlp, w_out, w_down, k_cache, v_cache))
    return hidden_out, cache_pair[0], cache_pair[1]
```

```python
import functools

import jax
import jax.numpy as jnp
from jax import lax
from jax.experimental import pallas as pl
from jax.experimental.pallas import tpu as pltpu
from jax.sharding import PartitionSpec as P

NORM_EPS = 1e-5
MESH = pl.DeviceIdType.MESH
BF16 = jnp.bfloat16
F32 = jnp.float32

CHUNKS = 5
EARLY = 1
VMEM_LIMITS = (62 * 2 ** 20, 58 * 2 ** 20, 58 * 2 ** 20)


def dot(a, b):
    return jnp.dot(a, b, preferred_element_type=F32)


class Links:
    def __init__(self, send_sems, recv_sems, local_sems):
        self.send_sems, self.recv_sems, self.local_sems = send_sems, recv_sems, local_sems
        self.sent, self.used, self.local_used = [], 0, 0
        x, y = lax.axis_index('x'), lax.axis_index('yz')
        self.x, self.y = x, y
        core = lax.rem(x, 2)
        self.along_x = (3 - x, x + 1 - 2 * core, lax.rem(x + 2, 4))
        self.blocks = self.along_x + (x,)
        self.targets = tuple({'x': p, 'yz': y} for p in self.along_x) + ({'x': x, 'yz': 1 - y},)

    def barrier(self):
        sem = pltpu.get_barrier_semaphore()
        for target in self.targets:
            pl.semaphore_signal(sem, inc=1, device_id=target, device_id_type=MESH)
        pl.semaphore_wait(sem, len(self.targets))

    def push(self, src, dst, to):
        k = self.used
        self.used += 1
        copy = pltpu.make_async_remote_copy(
            src_ref=src, dst_ref=dst, send_sem=self.send_sems.at[k], recv_sem=self.recv_sems.at[k],
            device_id=self.targets[to], device_id_type=MESH)
        copy.start()
        self.sent.append(copy)
        return copy

    def copy(self, src, dst):
        k = self.local_used
        self.local_used += 1
        copy = pltpu.make_async_copy(src, dst, self.local_sems.at[k])
        copy.start()
        return copy

    def drain(self):
        for copy in self.sent:
            copy.wait_send()


DIAG, PARTNER, ACROSS, YZ = 0, 1, 2, 3


def spread_matrices(depth):
    row = lax.broadcasted_iota(jnp.int32, (depth, 2 * depth), 0)
    col = lax.broadcasted_iota(jnp.int32, (depth, 2 * depth), 1)
    one, zero = jnp.ones((), F32), jnp.zeros((), F32)
    return (jnp.where(col == 2 * row, one, zero).astype(BF16), jnp.where(col == 2 * row + 1, one, zero).astype(BF16))


def front(links, layer, h_t, model_dim, gain_ref, wa, wm, qkv_out, zsend_out, zmine_out, s):
    depth, rows = h_t.shape
    shard = rows // 4
    chunks, _, cols = s['z_recv'].shape
    x, y = links.x, links.y
    s['sq_send'][...] = jnp.broadcast_to(jnp.sum(h_t * h_t, axis=0, keepdims=True), s['sq_send'].shape)
    sq_copies = [links.push(s['sq_send'], s['sq_recv'].at[k], k) for k in (DIAG, ACROSS, PARTNER)]
    gain = jnp.broadcast_to(gain_ref[layer:layer + 1, :].astype(F32), (128, depth)).T
    gain = jnp.concatenate([gain] * (rows // 128), axis=1)
    even, odd = spread_matrices(depth)
    for c in sq_copies:
        c.wait_recv()
    total = s['sq_send'][...] + s['sq_recv'][PARTNER] + (s['sq_recv'][ACROSS] + s['sq_recv'][DIAG])
    inv_rms = lax.rsqrt(total[:1] / model_dim + NORM_EPS)
    s['u'][...] = (h_t * inv_rms * gain).T.astype(BF16)
    u = jnp.concatenate([s['u'][pl.ds(pl.multiple_of(b * shard, shard), shard), :] for b in links.blocks], axis=0)
    wa.wait()
    s['a_part'][...] = dot(u, s['wa'][...]).astype(BF16)
    half = rows // 2
    a_core = links.push(s['a_part'].at[pl.ds(0, half)], s['a_core'], PARTNER)
    u_gate, u_up = dot(u, even).astype(BF16), dot(u, odd).astype(BF16)
    for k in range(4):
        s['u2'][pl.ds(2 * k * shard, shard), :] = u_gate[k * shard:(k + 1) * shard]
        s['u2'][pl.ds((2 * k + 1) * shard, shard), :] = u_up[k * shard:(k + 1) * shard]

    z_copies, early, outs = {}, {}, []

    def project(j):
        wm[j].wait()
        s['z_part'][j] = dot(s['u2'][...], s['wm'][j].reshape(2 * depth, cols)).astype(BF16)
        z_copies[j] = links.push(s['z_part'].at[j, pl.ds(0, rows)], s['z_recv'].at[j], PARTNER)

    def combine(j):
        z_copies[j].wait_recv()
        half_z = 2 * shard
        s['z_x'][j] = (s['z_part'][j, rows:rows + half_z].astype(F32) + s['z_recv'][j, :half_z].astype(F32)).astype(BF16)
        if j < EARLY:
            early[j] = links.push(s['z_x'].at[j], s['z_early'].at[j], ACROSS)
        else:
            outs.append(links.copy(s['z_x'].at[j], zsend_out.at[j - EARLY]))
        s['z_mine'][j] = (s['z_part'][j, rows + half_z:].astype(F32) + s['z_recv'][j, half_z:].astype(F32)).astype(BF16)
        if j >= EARLY:
            outs.append(links.copy(s['z_mine'].at[j], zmine_out.at[j]))

    project(0)
    a_core.wait_recv()
    s['a_sum'][...] = (s['a_part'][half:].astype(F32) + s['a_core'][...].astype(F32)).astype(BF16)
    a_across = links.push(s['a_sum'].at[pl.ds(0, shard)], s['a_across'], ACROSS)
    project(1)
    combine(0)
    project(2)
    a_across.wait_recv()
    s['a_full'][...] = (s['a_sum'][shard:].astype(F32) + s['a_across'][...].astype(F32)).astype(BF16)
    seqs = shard // 2
    a_yz = links.push(s['a_full'].at[pl.ds(pl.multiple_of((1 - y) * seqs, seqs), seqs)], s['a_yz'], YZ)
    qkv_out[y] = s['a_full'][pl.ds(pl.multiple_of(y * seqs, seqs), seqs), :]
    combine(1)
    for j in range(3, chunks):
        project(j)
        combine(j - 1)
    combine(chunks - 1)
    for j in range(EARLY):
        early[j].wait_recv()
        s['z_mine'][j] = (s['z_mine'][j].astype(F32) + s['z_early'][j].astype(F32)).astype(BF16)
        outs.append(links.copy(s['z_mine'].at[j], zmine_out.at[j]))
    a_yz.wait_recv()
    qkv_out[1 - y] = s['a_yz'][...]
    for c in outs:
        c.wait()


def back(links, o_ref, zgot_ref, z_loads, wd, wo, s, whole):
    chunks, rows, cols = s['m'].shape
    shard = rows // 4
    seqs = shard // 2
    x, y = links.x, links.y
    own_rows = pl.ds(pl.multiple_of(y * seqs, seqs), seqs)
    o_yz = links.push(o_ref.at[1 - y], s['o'].at[pl.ds(3 * shard + pl.multiple_of(y * seqs, seqs), seqs)], YZ)
    s['o'][pl.ds(3 * shard + pl.multiple_of(y * seqs, seqs), seqs), :] = o_ref[y]
    across, partner, diag = {}, {}, {}

    def block(j, k):
        return s['m'].at[j, pl.ds(k * shard, shard)]

    def mix(j):
        z_loads[j].wait()
        z = s['z_in'][j].astype(F32)
        if j >= EARLY:
            z = (z + zgot_ref[j - EARLY].astype(F32)).astype(BF16).astype(F32)
        gate, up = z[:shard], z[shard:]
        s['m'][j, 3 * shard:] = (gate * jax.nn.sigmoid(gate) * up).astype(BF16)
        across[j] = links.push(block(j, 3), block(j, 2), ACROSS)
        partner[j] = links.push(block(j, 3), block(j, 1), PARTNER)

    def forward(j):
        across[j].wait_recv()
        diag[j] = links.push(block(j, 2), block(j, 0), PARTNER)

    def o_block(k):
        return s['o'].at[pl.ds(k * shard, shard)]

    mix(0)
    mix(1)
    o_yz.wait_recv()
    o_across = links.push(o_block(3), o_block(2), ACROSS)
    o_partner = links.push(o_block(3), o_block(1), PARTNER)
    for j in range(2, chunks):
        mix(j)
    acc = None
    o_diag = None
    for j in range(chunks):
        forward(j)
        if j == 1:
            o_across.wait_recv()
            o_diag = links.push(o_block(2), o_block(0), PARTNER)
        if j >= 1:
            acc = down(links, j - 1, partner, diag, wd, s, acc)
        if j == 2:
            o_partner.wait_recv()
            o_diag.wait_recv()
            wo.wait()
            s['acc'][...] += dot(s['o'][...], s['wo'][...])
    down(links, chunks - 1, partner, diag, wd, s, acc)
    for k in range(4):
        s['update'][pl.ds(pl.multiple_of(links.blocks[k] * shard, shard), shard), :] = s['acc'][k * shard:(k + 1) * shard, :]
    s['up_part'][...] = s['update'][...].T.astype(BF16)
    if whole:
        up = links.push(s['up_part'], s['up_recv'], YZ)
        up.wait_recv()
        return s['up_part'][...].astype(F32) + s['up_recv'][...].astype(F32)
    part = s['up_recv'].shape[0]
    up = links.push(s['up_part'].at[pl.ds(pl.multiple_of((1 - y) * part, part), part)], s['up_recv'], YZ)
    up.wait_recv()
    own = s['up_part'][pl.ds(pl.multiple_of(y * part, part), part), :]
    return own.astype(F32) + s['up_recv'][...].astype(F32)


def down(links, j, partner, diag, wd, s, acc):
    partner[j].wait_recv()
    diag[j].wait_recv()
    wd[j].wait()
    part = dot(s['m'][j], s['wd'][j])
    if acc is None:
        s['acc'][...] = part
    else:
        s['acc'][...] += part
    return True


def load_front(links, layer, wa_hbm, wm_hbm, s):
    cols = s['wm'].shape[-1]
    wa = links.copy(wa_hbm.at[layer], s['wa'])
    wm = [links.copy(wm_hbm.at[layer, :, :, pl.ds(j * cols, cols)], s['wm'].at[j]) for j in range(s['wm'].shape[0])]
    return wa, wm


def load_back(links, layer, zmine_hbm, wd_hbm, wo_hbm, s):
    chunks, cols, _ = s['wd'].shape
    z_loads = [links.copy(zmine_hbm.at[j], s['z_in'].at[j]) for j in range(chunks)]
    wd = [links.copy(wd_hbm.at[layer, pl.ds(j * cols, cols)], s['wd'].at[j]) for j in range(chunks)]
    wo = links.copy(wo_hbm.at[layer], s['wo'])
    return z_loads, wd, wo


def start_kernel(names, model_dim, h_ref, gain_ref, wa_hbm, wm_hbm, qkv_out, zsend_out, zmine_out, h_out, *scratch):
    s = dict(zip(names, scratch))
    links = Links(s['send'], s['recv'], s['local'])
    wa, wm = load_front(links, 0, wa_hbm, wm_hbm, s)
    links.barrier()
    part = h_ref.shape[0]
    mine = pl.ds(pl.multiple_of(links.y * part, part), part)
    h_yz = links.push(h_ref, s['h'].at[mine], YZ)
    s['h'][mine, :] = h_ref[...]
    h_yz.wait_recv()
    h_out[...] = s['h'][...]
    front(links, 0, s['h'][...].astype(F32), model_dim, gain_ref, wa, wm, qkv_out, zsend_out, zmine_out, s)
    links.drain()


def middle_kernel(names, model_dim, h_ref, o_ref, gain_ref, zmine_hbm, zgot_ref, wd_hbm, wo_hbm, wa_hbm, wm_hbm, qkv_out, zsend_out,
                  zmine_out, h_out, *scratch):
    s = dict(zip(names, scratch))
    links = Links(s['send'], s['recv'], s['local'])
    z_loads, wd, wo = load_back(links, 0, zmine_hbm, wd_hbm, wo_hbm, s)
    wa, wm = load_front(links, 1, wa_hbm, wm_hbm, s)
    links.barrier()
    update = back(links, o_ref, zgot_ref, z_loads, wd, wo, s, True)
    h_new = (h_ref[...].astype(F32) + update).astype(BF16)
    h_out[...] = h_new
    front(links, 1, h_new.astype(F32), model_dim, gain_ref, wa, wm, qkv_out, zsend_out, zmine_out, s)
    links.drain()


def end_kernel(names, h_ref, o_ref, zmine_hbm, zgot_ref, wd_hbm, wo_hbm, h_out, *scratch):
    s = dict(zip(names, scratch))
    links = Links(s['send'], s['recv'], s['local'])
    z_loads, wd, wo = load_back(links, 1, zmine_hbm, wd_hbm, wo_hbm, s)
    links.barrier()
    update = back(links, o_ref, zgot_ref, z_loads, wd, wo, s, False)
    part = h_out.shape[0]
    own = h_ref[pl.ds(pl.multiple_of(links.y * part, part), part), :]
    h_out[...] = (own.astype(F32) + update).astype(BF16)
    links.drain()


def attention_kernel(layer, per_step, len_ref, qkv_ref, k_hbm, v_hbm, *rest):
    k_out, v_out, o_ref, kbuf, vbuf, q_scr, o_scr, in_sem, out_sem = rest[-9:]
    num_seqs, kv_heads, cache_len, head_dim = kbuf.shape
    slots = qkv_ref.shape[2] // head_dim
    rows = kv_heads * slots
    scale = head_dim ** -0.5

    def load(i):
        return (pltpu.make_async_copy(k_hbm.at[layer, i], kbuf.at[i], in_sem.at[0, i]),
                pltpu.make_async_copy(v_hbm.at[layer, i], vbuf.at[i], in_sem.at[1, i]))

    def store(i):
        return (pltpu.make_async_copy(kbuf.at[i], k_out.at[layer, i], out_sem.at[0, i]),
                pltpu.make_async_copy(vbuf.at[i], v_out.at[layer, i], out_sem.at[1, i]))

    @pl.loop(0, num_seqs)
    def _(i):
        for c in load(i):
            c.start()

    for head in range(kv_heads):
        for j in range(slots):
            q_scr[pl.ds(head * slots + j, num_seqs, stride=rows), :] = (
                qkv_ref[head, :, j * head_dim:(j + 1) * head_dim].astype(F32))

    tile_row = lax.broadcasted_iota(jnp.int32, (16, head_dim), 0)
    position = lax.broadcasted_iota(jnp.int32, (rows, cache_len), 1)

    @pl.loop(0, num_seqs // per_step)
    def _(step):
        group = [step * per_step + sub for sub in range(per_step)]
        for i in group:
            for c in load(i):
                c.wait()
            length = len_ref[i]
            base = pl.multiple_of((length // 16) * 16, 16)
            hit = tile_row == length - base
            for head in range(kv_heads):
                for buf, j in ((kbuf, slots - 2), (vbuf, slots - 1)):
                    new = q_scr[pl.ds(i * rows + head * slots + j, 1), :]
                    old = buf[i, head, pl.ds(base, 16), :].astype(F32)
                    buf[i, head, pl.ds(base, 16), :] = jnp.where(hit, new, old).astype(buf.dtype)
            for c in store(i):
                c.start()
        scores, probs = [], []
        for i in group:
            q = q_scr[pl.ds(pl.multiple_of(i * rows, rows), rows), :].astype(BF16)
            by_head = [lax.dot_general(q, kbuf[i, head], (((1,), (1,)), ((), ())), preferred_element_type=F32)
                       for head in range(kv_heads)]
            scores.append(jnp.concatenate([by_head[head][head * slots:(head + 1) * slots] for head in range(kv_heads)], axis=0))
        for i, score in zip(group, scores):
            score = jnp.where(position <= len_ref[i], score * scale, -1e30)
            e = jnp.exp(score - jnp.max(score, axis=1, keepdims=True))
            probs.append((e / jnp.sum(e, axis=1, keepdims=True)).astype(BF16))
        for i, p in zip(group, probs):
            by_head = [dot(p, vbuf[i, head]) for head in range(kv_heads)]
            o_scr[pl.ds(pl.multiple_of(i * rows, rows), rows), :] = jnp.concatenate(
                [by_head[head][head * slots:(head + 1) * slots] for head in range(kv_heads)], axis=0)

    for head in range(kv_heads):
        for j in range(slots - 2):
            o_ref[head, :, j * head_dim:(j + 1) * head_dim] = (
                o_scr[pl.ds(head * slots + j, num_seqs, stride=rows), :].astype(o_ref.dtype))

    @pl.loop(0, num_seqs)
    def _(i):
        for c in store(i):
            c.wait()


ANY = pl.BlockSpec(memory_space=pl.ANY)
VMEM = pl.BlockSpec(memory_space=pltpu.VMEM)


def attention(layer, lengths, qkv, k_cache, v_cache, outs):
    layers, num_seqs, kv_heads, cache_len, head_dim = k_cache.shape
    slots = qkv.shape[2] // head_dim
    rows = kv_heads * slots
    return pl.pallas_call(
        functools.partial(attention_kernel, layer, 2),
        out_shape=(jax.ShapeDtypeStruct(k_cache.shape, k_cache.dtype), jax.ShapeDtypeStruct(v_cache.shape, v_cache.dtype),
                   jax.ShapeDtypeStruct((kv_heads, num_seqs, (slots - 2) * head_dim), BF16)),
        in_specs=[pl.BlockSpec(memory_space=pltpu.SMEM), VMEM, ANY, ANY] + [ANY] * len(outs),
        out_specs=(ANY, ANY, VMEM),
        scratch_shapes=[pltpu.VMEM((num_seqs, kv_heads, cache_len, head_dim), BF16)] * 2
        + [pltpu.VMEM((num_seqs * rows, head_dim), F32)] * 2 + [pltpu.SemaphoreType.DMA((2, num_seqs))] * 2,
        input_output_aliases={4: 0, 5: 1} if outs else {},
        compiler_params=pltpu.CompilerParams(vmem_limit_bytes=44 * 2 ** 20),
        cost_estimate=pl.CostEstimate(flops=10 ** 10, bytes_accessed=8 * num_seqs * kv_heads * cache_len * head_dim, transcendentals=0),
        name=f'attention_{layer}',
    )(lengths, qkv, k_cache, v_cache, *outs)


def solution(mesh):
    seq_axes = ('rep', 'x', 'yz')
    hidden_spec = P('rep', ('x', 'yz'))
    cache_spec = P(None, seq_axes, None, None, None)
    in_specs = (hidden_spec, P(None, 'x'), P(None, 'x', 'yz'), P(None, 'x', None, 'yz'), P(None, 'yz', 'x'), P(None, 'yz', 'x'), cache_spec, cache_spec, P(seq_axes))
    out_specs = (hidden_spec, cache_spec, cache_spec)
    swap = [(0, 2), (2, 0), (1, 3), (3, 1)]

    def device_step(hidden, norm_gain, w_attn, w_mlp, w_out, w_down, k_cache, v_cache, lengths):
        rows, part = hidden.shape
        depth, attn_cols = w_attn.shape[1:]
        model_dim = depth * mesh.shape['x']
        mlp_cols = w_mlp.shape[3]
        out_depth = w_out.shape[1]
        shard, half = rows // 4, rows // 2
        seqs = shard // 2
        cols = mlp_cols // CHUNKS
        late = CHUNKS - EARLY
        sq = (8, rows)
        common = {
            'send': pltpu.SemaphoreType.DMA((40,)), 'recv': pltpu.SemaphoreType.DMA((40,)), 'local': pltpu.SemaphoreType.DMA((40,)),
        }
        front_scratch = {
            'sq_send': pltpu.VMEM(sq, F32), 'sq_recv': pltpu.VMEM((3,) + sq, F32), 'u': pltpu.VMEM((rows, depth), BF16),
            'wa': pltpu.VMEM((depth, attn_cols), BF16), 'wm': pltpu.VMEM((CHUNKS, depth, 2, cols), BF16),
            'a_part': pltpu.VMEM((rows, attn_cols), BF16), 'a_core': pltpu.VMEM((half, attn_cols), BF16),
            'a_sum': pltpu.VMEM((half, attn_cols), BF16), 'a_across': pltpu.VMEM((shard, attn_cols), BF16),
            'a_full': pltpu.VMEM((shard, attn_cols), BF16), 'a_yz': pltpu.VMEM((seqs, attn_cols), BF16),
            'u2': pltpu.VMEM((2 * rows, 2 * depth), BF16), 'z_part': pltpu.VMEM((CHUNKS, 2 * rows, cols), BF16),
            'z_recv': pltpu.VMEM((CHUNKS, rows, cols), BF16), 'z_x': pltpu.VMEM((CHUNKS, half, cols), BF16),
            'z_mine': pltpu.VMEM((CHUNKS, half, cols), BF16), 'z_early': pltpu.VMEM((EARLY, half, cols), BF16),
        }

        def back_scratch(whole):
            return {
                'o': pltpu.VMEM((rows, out_depth), BF16), 'm': pltpu.VMEM((CHUNKS, rows, cols), BF16),
                'z_in': pltpu.VMEM((CHUNKS, half, cols), BF16),
                'wd': pltpu.VMEM((CHUNKS, cols, depth), BF16), 'wo': pltpu.VMEM((out_depth, depth), BF16),
                'acc': pltpu.VMEM((rows, depth), F32), 'update': pltpu.VMEM((rows, depth), F32),
                'up_part': pltpu.VMEM((depth, rows), BF16), 'up_recv': pltpu.VMEM((depth if whole else part, rows), BF16),
            }

        front_shapes = (
            jax.ShapeDtypeStruct((2, seqs, attn_cols), BF16), jax.ShapeDtypeStruct((late, half, cols), BF16),
            jax.ShapeDtypeStruct((CHUNKS, half, cols), BF16), jax.ShapeDtypeStruct((depth, rows), BF16))
        front_specs = (VMEM, ANY, ANY, VMEM)

        def call(kernel, name, collective_id, scratch, in_specs, out_shape, out_specs, *args):
            return pl.pallas_call(
                functools.partial(kernel, tuple(scratch)), out_shape=out_shape, in_specs=list(in_specs), out_specs=out_specs,
                scratch_shapes=list(scratch.values()), name=name,
                compiler_params=pltpu.CompilerParams(collective_id=collective_id, has_side_effects=True, vmem_limit_bytes=VMEM_LIMITS[collective_id]),
            )(*args)

        def start(names, *refs):
            start_kernel(names, model_dim, *refs)

        def middle(names, *refs):
            middle_kernel(names, model_dim, *refs)

        qkv, zsend, zmine, h_block = call(
            start, 'start', 0, {**common, **front_scratch, 'h': pltpu.VMEM((depth, rows), BF16)}, (VMEM, VMEM, ANY, ANY),
            front_shapes, front_specs, hidden.T, norm_gain, w_attn, w_mlp)
        zgot = lax.ppermute(zsend, 'x', swap)
        k_new, v_new, o = attention(0, lengths, qkv, k_cache, v_cache, ())
        qkv, zsend, zmine, h_block = call(
            middle, 'middle', 1, {**common, **front_scratch, **back_scratch(True)}, (VMEM, VMEM, VMEM, ANY, VMEM) + (ANY,) * 4,
            front_shapes, front_specs, h_block, o, norm_gain, zmine, zgot, w_down, w_out, w_attn, w_mlp)
        zgot = lax.ppermute(zsend, 'x', swap)
        k_new, v_new, o = attention(1, lengths, qkv, k_cache, v_cache, (k_new, v_new))
        h_out = call(
            end_kernel, 'end', 2, {**common, **back_scratch(False)}, (VMEM, VMEM, ANY, VMEM) + (ANY,) * 2,
            jax.ShapeDtypeStruct((part, rows), BF16), VMEM, h_block, o, zmine, zgot, w_down, w_out)
        return h_out.T, k_new, v_new

    return jax.shard_map(device_step, mesh=mesh, in_specs=in_specs, out_specs=out_specs, check_vma=False)
```

```python
import functools

import jax
import jax.numpy as jnp
from jax import lax
from jax.experimental import pallas as pl
from jax.experimental.pallas import tpu as pltpu
from jax.sharding import PartitionSpec as P

NORM_EPS = 1e-5
MESH = pl.DeviceIdType.MESH
BF16 = jnp.bfloat16
F32 = jnp.float32

CHUNKS = 5
EARLY = 2
VMEM_LIMIT = 62 * 2 ** 20


def dot(a, b):
    return jnp.dot(a, b, preferred_element_type=F32)


class Links:
    def __init__(self, send_sems, recv_sems, local_sems, everyone):
        self.send_sems, self.recv_sems, self.local_sems = send_sems, recv_sems, local_sems
        self.sent, self.used, self.local_used = [], 0, 0
        x, y = lax.axis_index('x'), lax.axis_index('yz')
        self.x, self.y = x, y
        core = lax.rem(x, 2)
        self.along_x = (3 - x, x + 1 - 2 * core, lax.rem(x + 2, 4))
        self.blocks = self.along_x + (x,)
        self.targets = tuple({'x': p, 'yz': y} for p in self.blocks) + ({'x': x, 'yz': 1 - y},) + tuple(
            {'x': p, 'yz': 1 - y} for p in self.along_x)
        self.peers = [k for k in range(8 if everyone else 5) if k != OWN]
        self.barrier = pltpu.get_barrier_semaphore()
        for k in self.peers:
            pl.semaphore_signal(self.barrier, inc=1, device_id=self.targets[k], device_id_type=MESH)

    def meet(self):
        pl.semaphore_wait(self.barrier, len(self.peers))

    def push(self, src, dst, to):
        k = self.used
        self.used += 1
        copy = pltpu.make_async_remote_copy(
            src_ref=src, dst_ref=dst, send_sem=self.send_sems.at[k], recv_sem=self.recv_sems.at[k],
            device_id=self.targets[to], device_id_type=MESH)
        copy.start()
        self.sent.append(copy)
        return copy

    def copy(self, src, dst):
        k = self.local_used
        self.local_used += 1
        copy = pltpu.make_async_copy(src, dst, self.local_sems.at[k])
        copy.start()
        return copy

    def drain(self):
        for copy in self.sent:
            copy.wait_send()


DIAG, PARTNER, ACROSS, OWN, YZ = 0, 1, 2, 3, 4
PARTS = 2


def spread_matrices(depth):
    row = lax.broadcasted_iota(jnp.int32, (depth, 2 * depth), 0)
    col = lax.broadcasted_iota(jnp.int32, (depth, 2 * depth), 1)
    one, zero = jnp.ones((), F32), jnp.zeros((), F32)
    return (jnp.where(col == 2 * row, one, zero).astype(BF16), jnp.where(col == 2 * row + 1, one, zero).astype(BF16))


def part_order(rows, inverse):
    i = lax.broadcasted_iota(jnp.int32, (rows, rows), 0)
    j = lax.broadcasted_iota(jnp.int32, (rows, rows), 1)
    src, dst = (j, i) if inverse else (i, j)
    run = rows // (8 * PARTS)
    piece = src // run
    place = lax.rem(piece, PARTS) * (8 * run) + (piece // PARTS) * run + lax.rem(src, run)
    return jnp.where(dst == place, jnp.ones((), F32), jnp.zeros((), F32)).astype(BF16)


class Front:
    def __init__(self, links, layer, gain_hbm, wa_hbm, wm_hbm, model_dim, outs, s):
        self.links, self.s, self.layer, self.model_dim = links, s, layer, model_dim
        self.gain_copy = links.copy(gain_hbm, s['gain_in'])
        self.qkv_out, self.zsend_out, self.zmine_out = outs
        self.chunks, self.depth, _, self.cols = s['wm'].shape
        self.wa = links.copy(wa_hbm.at[layer], s['wa'])
        self.wm = [links.copy(wm_hbm.at[layer, :, :, pl.ds(j * self.cols, self.cols)], s['wm'].at[j]) for j in range(self.chunks)]
        self.wa_ready, self.wm_ready = False, [False] * self.chunks
        self.a_core, self.a_across, self.a_yz, self.z_core, self.early, self.out_copies = {}, {}, {}, {}, {}, []
        self.sq = {}

    def constants(self):
        lanes = self.s['u'].shape[1]
        self.gain_copy.wait()
        gain = jnp.broadcast_to(self.s['gain_in'][self.layer:self.layer + 1, :].astype(F32), (lanes, self.depth)).T
        self.s['gain'][...] = gain
        self.s['even'][...], self.s['odd'][...] = spread_matrices(self.depth)

    def send_squares(self, p, h_t, to):
        s = self.s
        s['sq_send'][p] = jnp.broadcast_to(jnp.sum(h_t * h_t, axis=0, keepdims=True), s['sq_send'].shape[1:])
        self.sq[p] = [self.links.push(s['sq_send'].at[p], s['sq_recv'].at[p, k], k) for k in to]

    def normalize(self, p, h_t, to):
        s, links = self.s, self.links
        for c in self.sq[p]:
            c.wait_recv()
        total = s['sq_send'][p]
        for k in sorted(to):
            total = total + s['sq_recv'][p, k]
        inv_rms = lax.rsqrt(total[:1] / self.model_dim + NORM_EPS)
        s['u'][p] = (h_t * inv_rms * s['gain'][...]).T.astype(BF16)
        shard = s['u'].shape[1] // 4
        u = jnp.concatenate([s['u'][p, pl.ds(pl.multiple_of(b * shard, shard), shard), :] for b in links.blocks], axis=0)
        s['u_rel'][p] = u
        if not self.wa_ready:
            self.wa.wait()
            self.wa_ready = True
        s['a_part'][p] = dot(u, s['wa'][...]).astype(BF16)
        self.a_core[p] = links.push(s['a_part'].at[p, pl.ds(0, 2 * shard)], s['a_core'].at[p], PARTNER)

    def spread(self, p):
        s = self.s
        u = s['u_rel'][p]
        gate, up = dot(u, s['even'][...]).astype(BF16), dot(u, s['odd'][...]).astype(BF16)
        shard = u.shape[0] // 4
        for k in range(4):
            s['u2'][p, 2 * k * shard:(2 * k + 1) * shard] = gate[k * shard:(k + 1) * shard]
            s['u2'][p, (2 * k + 1) * shard:(2 * k + 2) * shard] = up[k * shard:(k + 1) * shard]

    def attend_core(self, p):
        s = self.s
        half = s['a_core'].shape[1]
        self.a_core[p].wait_recv()
        s['a_sum'][p] = (s['a_part'][p, half:].astype(F32) + s['a_core'][p].astype(F32)).astype(BF16)
        self.a_across[p] = self.links.push(s['a_sum'].at[p, pl.ds(0, half // 2)], s['a_across'].at[p], ACROSS)

    def attend_across(self, p):
        s, y = self.s, self.links.y
        shard, seqs = s['a_across'].shape[1], s['a_yz'].shape[1]
        self.a_across[p].wait_recv()
        s['a_full'][p] = (s['a_sum'][p, shard:].astype(F32) + s['a_across'][p].astype(F32)).astype(BF16)
        self.a_yz[p] = self.links.push(s['a_full'].at[p, pl.ds(pl.multiple_of((1 - y) * seqs, seqs), seqs)], s['a_yz'].at[p], YZ)
        self.out_copies.append(self.links.copy(
            s['a_full'].at[p, pl.ds(pl.multiple_of(y * seqs, seqs), seqs)], self.qkv_out.at[y, pl.ds(p * seqs, seqs)]))

    def attend_yz(self, p):
        s, y = self.s, self.links.y
        seqs = s['a_yz'].shape[1]
        self.a_yz[p].wait_recv()
        self.out_copies.append(self.links.copy(s['a_yz'].at[p], self.qkv_out.at[1 - y, pl.ds(p * seqs, seqs)]))

    def project(self, p, j):
        s = self.s
        if not self.wm_ready[j]:
            self.wm[j].wait()
            self.wm_ready[j] = True
        s['z_part'][p, j] = dot(s['u2'][p], s['wm'][j].reshape(2 * self.depth, self.cols)).astype(BF16)
        half = s['z_recv'].shape[2]
        self.z_core[p, j] = self.links.push(s['z_part'].at[p, j, pl.ds(0, half)], s['z_recv'].at[p, j], PARTNER)

    def combine(self, p, j):
        s, unit = self.s, p * self.chunks + j
        half = s['z_recv'].shape[2]
        shard2 = half // 2
        self.z_core[p, j].wait_recv()
        s['z_x'][unit] = (s['z_part'][p, j, half:half + shard2].astype(F32) + s['z_recv'][p, j, :shard2].astype(F32)).astype(BF16)
        if unit < EARLY:
            self.early[unit] = self.links.push(s['z_x'].at[unit], s['z_early'].at[unit], ACROSS)
        else:
            self.out_copies.append(self.links.copy(s['z_x'].at[unit], self.zsend_out.at[unit - EARLY]))
        s['z_mine'][unit] = (s['z_part'][p, j, half + shard2:].astype(F32) + s['z_recv'][p, j, shard2:].astype(F32)).astype(BF16)
        if unit >= EARLY:
            self.out_copies.append(self.links.copy(s['z_mine'].at[unit], self.zmine_out.at[unit]))

    def finish(self):
        s = self.s
        for unit in range(EARLY):
            self.early[unit].wait_recv()
            s['z_mine'][unit] = (s['z_mine'][unit].astype(F32) + s['z_early'][unit].astype(F32)).astype(BF16)
            self.out_copies.append(self.links.copy(s['z_mine'].at[unit], self.zmine_out.at[unit]))
        for p in range(PARTS):
            self.attend_yz(p)
        for c in self.out_copies:
            c.wait()

    def run(self, steps):
        for name, *args in steps:
            getattr(self, name)(*args)


class Back:
    def __init__(self, links, layer, h_hbm, o_hbm, zgot_hbm, zmine_hbm, wd_hbm, wo_hbm, whole, s):
        self.links, self.s, self.whole = links, s, whole
        self.chunks, cols, _ = s['wd'].shape
        self.z = []
        for unit in range(PARTS * self.chunks):
            self.z.append([links.copy(zmine_hbm.at[unit], s['z_in'].at[unit])])
            if unit >= EARLY:
                self.z[-1].append(links.copy(zgot_hbm.at[unit - EARLY], s['z_got'].at[unit - EARLY]))
            if unit == 0:
                self.o_copy = links.copy(o_hbm, s['o_in'])
                self.h_copy = links.copy(h_hbm, s['h_in'])
        self.wd = [links.copy(wd_hbm.at[layer, pl.ds(j * cols, cols)], s['wd'].at[j]) for j in range(self.chunks)]
        self.wo = links.copy(wo_hbm.at[layer], s['wo'])
        self.wo_ready, self.wd_ready = False, [False] * self.chunks
        self.across, self.partner, self.diag = {}, {}, {}
        self.o_across, self.o_partner, self.o_diag = {}, {}, {}
        self.up = {}

    def mix(self, p, j):
        s, unit = self.s, p * self.chunks + j
        for c in self.z[unit]:
            c.wait()
        z = s['z_in'][unit].astype(F32)
        if unit >= EARLY:
            z = (z + s['z_got'][unit - EARLY].astype(F32)).astype(BF16).astype(F32)
        shard = z.shape[0] // 2
        gate, up = z[:shard], z[shard:]
        s['m'][p, j, OWN * shard:] = (gate * jax.nn.sigmoid(gate) * up).astype(BF16)

    def block(self, p, j, k):
        shard = self.s['m'].shape[2] // 4
        return self.s['m'].at[p, j, pl.ds(k * shard, shard)]

    def send(self, p, j):
        self.across[p, j] = self.links.push(self.block(p, j, OWN), self.block(p, j, ACROSS), ACROSS)
        self.partner[p, j] = self.links.push(self.block(p, j, OWN), self.block(p, j, PARTNER), PARTNER)

    def forward(self, p, j):
        self.across[p, j].wait_recv()
        self.diag[p, j] = self.links.push(self.block(p, j, ACROSS), self.block(p, j, DIAG), PARTNER)

    def send_o_yz(self):
        y, s = self.links.y, self.s
        self.o_copy.wait()
        self.o_yz = self.links.push(s['o_in'].at[1 - y], s['o_yz'], YZ)

    def o_block(self, p, k):
        shard = self.s['o'].shape[1] // 4
        return self.s['o'].at[p, pl.ds(k * shard, shard)]

    def send_o(self):
        y, s = self.links.y, self.s
        self.o_yz.wait_recv()
        shard = s['o'].shape[1] // 4
        seqs = shard // 2
        for p in range(PARTS):
            s['o'][p, pl.ds(OWN * shard + pl.multiple_of(y * seqs, seqs), seqs), :] = s['o_in'][y, p * seqs:(p + 1) * seqs]
            s['o'][p, pl.ds(OWN * shard + pl.multiple_of((1 - y) * seqs, seqs), seqs), :] = s['o_yz'][p * seqs:(p + 1) * seqs]
            self.o_across[p] = self.links.push(self.o_block(p, OWN), self.o_block(p, ACROSS), ACROSS)
            self.o_partner[p] = self.links.push(self.o_block(p, OWN), self.o_block(p, PARTNER), PARTNER)

    def forward_o(self, p):
        self.o_across[p].wait_recv()
        self.o_diag[p] = self.links.push(self.o_block(p, ACROSS), self.o_block(p, DIAG), PARTNER)

    def project_o(self, p):
        s = self.s
        self.o_partner[p].wait_recv()
        self.o_diag[p].wait_recv()
        if not self.wo_ready:
            self.wo.wait()
            self.wo_ready = True
        s['acc'][p] += dot(s['o'][p], s['wo'][...])

    def down(self, p, j):
        s = self.s
        self.partner[p, j].wait_recv()
        self.diag[p, j].wait_recv()
        if not self.wd_ready[j]:
            self.wd[j].wait()
            self.wd_ready[j] = True
        part = dot(s['m'][p, j], s['wd'][j])
        if j == 0:
            s['acc'][p] = part
        else:
            s['acc'][p] += part

    def send_update(self, p):
        s, links = self.s, self.links
        shard = s['acc'].shape[1] // 4
        for k in range(4):
            s['update'][p, pl.ds(pl.multiple_of(links.blocks[k] * shard, shard), shard), :] = s['acc'][p, k * shard:(k + 1) * shard, :]
        s['up_part'][p] = s['update'][p].T.astype(BF16)
        if self.whole:
            src = s['up_part'].at[p]
        else:
            part = s['up_recv'].shape[1]
            src = s['up_part'].at[p, pl.ds(pl.multiple_of((1 - links.y) * part, part), part)]
        self.up[p] = links.push(src, s['up_recv'].at[p], YZ)

    def update(self, p):
        s, links = self.s, self.links
        self.up[p].wait_recv()
        if self.whole:
            own = s['up_part'][p]
        else:
            part = s['up_recv'].shape[1]
            own = s['up_part'][p, pl.ds(pl.multiple_of(links.y * part, part), part), :]
        return own.astype(F32) + s['up_recv'][p].astype(F32)

    def open(self):
        links, chunks = self.links, self.chunks
        self.mix(0, 0)
        links.meet()
        self.send_o_yz()
        self.send(0, 0)
        for j in range(1, chunks):
            self.mix(0, j)
            self.send(0, j)
            if j == 2:
                self.send_o()
        if chunks < 3:
            self.send_o()
        for j in range(chunks):
            self.mix(1, j)
            self.send(1, j)


def start_kernel(names, model_dim, h_hbm, gain_hbm, wa_hbm, wm_hbm, qkv_out, zsend_out, zmine_out, h_out, *scratch):
    s = dict(zip(names, scratch))
    links = Links(s['send'], s['recv'], s['local'], True)
    h_copy = links.copy(h_hbm, s['h_in'])
    f = Front(links, 0, gain_hbm, wa_hbm, wm_hbm, model_dim, (qkv_out, zsend_out, zmine_out), s)
    part, rows = h_hbm.shape
    lanes = rows // PARTS
    mine = pl.ds(pl.multiple_of(links.y * part, part), part)
    order = part_order(rows, False)
    h_copy.wait()
    own = dot(s['h_in'][...], order)
    for p in range(PARTS):
        s['h'][p, mine, :] = own[:, p * lanes:(p + 1) * lanes].astype(BF16)
    links.meet()
    h_yz = [links.push(s['h'].at[p, mine], s['h'].at[p, mine], YZ) for p in range(PARTS)]
    to = [k for k in range(8) if k != OWN]
    for p in range(PARTS):
        f.send_squares(p, own[:, p * lanes:(p + 1) * lanes], to)
    f.constants()
    for p in range(PARTS):
        h_yz[p].wait_recv()
        f.out_copies.append(links.copy(s['h'].at[p], h_out.at[p]))
        f.normalize(p, s['h'][p].astype(F32), to)
    f.spread(0)
    f.project(0, 0)
    f.attend_core(0)
    f.attend_core(1)
    f.spread(1)
    finish_front(f)
    links.drain()


def finish_front(f, begun=1):
    units = [(p, j) for p in range(PARTS) for j in range(f.chunks)]
    for n in range(begun, len(units)):
        f.project(*units[n])
        f.combine(*units[n - 1])
        if n == 5:
            f.attend_across(0)
        if n == 7:
            f.attend_across(1)
    f.combine(*units[-1])
    f.finish()


def middle_kernel(names, model_dim, h_hbm, o_hbm, gain_hbm, zmine_hbm, zgot_hbm, wd_hbm, wo_hbm, wa_hbm, wm_hbm, qkv_out, zsend_out,
                  zmine_out, h_out, *scratch):
    s = dict(zip(names, scratch))
    links = Links(s['send'], s['recv'], s['local'], False)
    b = Back(links, 0, h_hbm, o_hbm, zgot_hbm, zmine_hbm, wd_hbm, wo_hbm, True, s)
    f = Front(links, 1, gain_hbm, wa_hbm, wm_hbm, model_dim, (qkv_out, zsend_out, zmine_out), s)
    to = (DIAG, PARTNER, ACROSS)
    b.open()
    f.constants()
    b.h_copy.wait()

    def new_h(p):
        h = (s['h_in'][p].astype(F32) + b.update(p)).astype(BF16)
        s['h'][p] = h
        f.out_copies.append(links.copy(s['h'].at[p], h_out.at[p]))
        f.send_squares(p, h.astype(F32), to)

    first_part(b)
    second_part(b, lambda: new_h(0), lambda: f.normalize(0, s['h'][0].astype(F32), to))
    f.spread(0)
    f.attend_core(0)
    f.project(0, 0)
    new_h(1)
    f.project(0, 1)
    f.combine(0, 0)
    f.project(0, 2)
    f.combine(0, 1)
    f.normalize(1, s['h'][1].astype(F32), to)
    f.spread(1)
    f.project(0, 3)
    f.combine(0, 2)
    f.attend_core(1)
    finish_front(f, 4)
    links.drain()


def first_part(b):
    for j in range(b.chunks):
        b.forward(0, j)
        if j == 2:
            b.forward_o(0)
            b.forward_o(1)
        if j >= 1:
            b.down(0, j - 1)
    b.forward(1, 0)
    b.down(0, b.chunks - 1)
    b.project_o(0)
    b.send_update(0)


def second_part(b, when_updated, when_squared):
    for j in range(1, b.chunks):
        b.forward(1, j)
        b.down(1, j - 1)
        if j == 1:
            b.project_o(1)
        if j == b.chunks - 2:
            when_updated()
    b.down(1, b.chunks - 1)
    b.send_update(1)
    when_squared()


def end_kernel(names, h_hbm, o_hbm, zmine_hbm, zgot_hbm, wd_hbm, wo_hbm, h_out, *scratch):
    s = dict(zip(names, scratch))
    links = Links(s['send'], s['recv'], s['local'], False)
    b = Back(links, 1, h_hbm, o_hbm, zgot_hbm, zmine_hbm, wd_hbm, wo_hbm, False, s)
    part, rows = h_out.shape
    own_rows = pl.ds(pl.multiple_of(links.y * part, part), part)
    b.open()
    b.h_copy.wait()

    def new_h(p):
        return (s['h_in'][p, own_rows, :].astype(F32) + b.update(p)).astype(BF16)

    first_part(b)
    kept = []
    second_part(b, lambda: kept.append(new_h(0)), lambda: None)
    order = part_order(rows, True)
    h_new = jnp.concatenate(kept + [new_h(1)], axis=1)
    h_out[...] = dot(h_new, order).astype(BF16)
    links.drain()


def attention_kernel(layer, per_step, len_hbm, qkv_hbm, k_hbm, v_hbm, *rest):
    k_out, v_out, o_hbm, kbuf, vbuf, q_scr, o_scr, qkv_ref, o_ref, len_ref, in_sem, out_sem, small_sem = rest[-13:]
    num_seqs, kv_heads, cache_len, head_dim = kbuf.shape
    slots = qkv_ref.shape[2] // head_dim
    rows = kv_heads * slots
    scale = head_dim ** -0.5

    def load(i):
        return (pltpu.make_async_copy(k_hbm.at[layer, i], kbuf.at[i], in_sem.at[0, i]),
                pltpu.make_async_copy(v_hbm.at[layer, i], vbuf.at[i], in_sem.at[1, i]))

    def store(i):
        return (pltpu.make_async_copy(kbuf.at[i], k_out.at[layer, i], out_sem.at[0, i]),
                pltpu.make_async_copy(vbuf.at[i], v_out.at[layer, i], out_sem.at[1, i]))

    qkv_copy = pltpu.make_async_copy(qkv_hbm, qkv_ref, small_sem.at[0])
    len_copy = pltpu.make_async_copy(len_hbm, len_ref, small_sem.at[1])
    qkv_copy.start()
    len_copy.start()

    @pl.loop(0, num_seqs)
    def _(i):
        for c in load(i):
            c.start()

    qkv_copy.wait()
    len_copy.wait()
    for head in range(kv_heads):
        for j in range(slots):
            q_scr[pl.ds(head * slots + j, num_seqs, stride=rows), :] = (
                qkv_ref[head, :, j * head_dim:(j + 1) * head_dim].astype(F32))

    tile_row = lax.broadcasted_iota(jnp.int32, (16, head_dim), 0)
    position = lax.broadcasted_iota(jnp.int32, (rows, cache_len), 1)

    @pl.loop(0, num_seqs // per_step)
    def _(step):
        group = [step * per_step + sub for sub in range(per_step)]
        for i in group:
            for c in load(i):
                c.wait()
            length = len_ref[i]
            base = pl.multiple_of((length // 16) * 16, 16)
            hit = tile_row == length - base
            for head in range(kv_heads):
                for buf, j in ((kbuf, slots - 2), (vbuf, slots - 1)):
                    new = q_scr[pl.ds(i * rows + head * slots + j, 1), :]
                    old = buf[i, head, pl.ds(base, 16), :].astype(F32)
                    buf[i, head, pl.ds(base, 16), :] = jnp.where(hit, new, old).astype(buf.dtype)
            for c in store(i):
                c.start()
        scores, probs = [], []
        for i in group:
            q = q_scr[pl.ds(pl.multiple_of(i * rows, rows), rows), :].astype(BF16)
            by_head = [lax.dot_general(q, kbuf[i, head], (((1,), (1,)), ((), ())), preferred_element_type=F32)
                       for head in range(kv_heads)]
            scores.append(jnp.concatenate([by_head[head][head * slots:(head + 1) * slots] for head in range(kv_heads)], axis=0))
        for i, score in zip(group, scores):
            score = jnp.where(position <= len_ref[i], score * scale, -1e30)
            e = jnp.exp(score - jnp.max(score, axis=1, keepdims=True))
            probs.append((e / jnp.sum(e, axis=1, keepdims=True)).astype(BF16))
        for i, p in zip(group, probs):
            by_head = [dot(p, vbuf[i, head]) for head in range(kv_heads)]
            o_scr[pl.ds(pl.multiple_of(i * rows, rows), rows), :] = jnp.concatenate(
                [by_head[head][head * slots:(head + 1) * slots] for head in range(kv_heads)], axis=0)

    for head in range(kv_heads):
        for j in range(slots - 2):
            o_ref[head, :, j * head_dim:(j + 1) * head_dim] = (
                o_scr[pl.ds(head * slots + j, num_seqs, stride=rows), :].astype(o_ref.dtype))
    o_copy = pltpu.make_async_copy(o_ref, o_hbm, small_sem.at[2])
    o_copy.start()

    @pl.loop(0, num_seqs)
    def _(i):
        for c in store(i):
            c.wait()

    o_copy.wait()


VMEM = pl.BlockSpec(memory_space=pltpu.VMEM)
HBM = pl.BlockSpec(memory_space=pltpu.HBM)


def attention(layer, lengths, qkv, k_cache, v_cache, outs):
    layers, num_seqs, kv_heads, cache_len, head_dim = k_cache.shape
    slots = qkv.shape[2] // head_dim
    rows = kv_heads * slots
    return pl.pallas_call(
        functools.partial(attention_kernel, layer, 2),
        out_shape=(jax.ShapeDtypeStruct(k_cache.shape, k_cache.dtype), jax.ShapeDtypeStruct(v_cache.shape, v_cache.dtype),
                   jax.ShapeDtypeStruct((kv_heads, num_seqs, (slots - 2) * head_dim), BF16)),
        in_specs=[HBM] * (4 + len(outs)),
        out_specs=(HBM, HBM, HBM),
        scratch_shapes=[pltpu.VMEM((num_seqs, kv_heads, cache_len, head_dim), BF16)] * 2
        + [pltpu.VMEM((num_seqs * rows, head_dim), F32)] * 2 + [
            pltpu.VMEM(qkv.shape, BF16), pltpu.VMEM((kv_heads, num_seqs, (slots - 2) * head_dim), BF16),
            pltpu.SMEM((num_seqs,), jnp.int32)]
        + [pltpu.SemaphoreType.DMA((2, num_seqs))] * 2 + [pltpu.SemaphoreType.DMA((3,))],
        input_output_aliases={4: 0, 5: 1} if outs else {},
        compiler_params=pltpu.CompilerParams(vmem_limit_bytes=VMEM_LIMIT),
        cost_estimate=pl.CostEstimate(flops=10 ** 10, bytes_accessed=8 * num_seqs * kv_heads * cache_len * head_dim, transcendentals=0),
        name=f'attention_{layer}',
    )(lengths, qkv, k_cache, v_cache, *outs)


def solution(mesh):
    seq_axes = ('rep', 'x', 'yz')
    hidden_spec = P('rep', ('x', 'yz'))
    cache_spec = P(None, seq_axes, None, None, None)
    in_specs = (hidden_spec, P(None, 'x'), P(None, 'x', 'yz'), P(None, 'x', None, 'yz'), P(None, 'yz', 'x'), P(None, 'yz', 'x'), cache_spec, cache_spec, P(seq_axes))
    out_specs = (hidden_spec, cache_spec, cache_spec)
    swap = [(0, 2), (2, 0), (1, 3), (3, 1)]

    def device_step(hidden, norm_gain, w_attn, w_mlp, w_out, w_down, k_cache, v_cache, lengths):
        rows, part = hidden.shape
        depth, attn_cols = w_attn.shape[1:]
        model_dim = depth * mesh.shape['x']
        mlp_cols = w_mlp.shape[3]
        out_depth = w_out.shape[1]
        cols = mlp_cols // CHUNKS
        units = CHUNKS * PARTS
        lanes = rows // PARTS
        half, shard = lanes // 2, lanes // 4
        seqs = shard // 2
        num_seqs = PARTS * seqs
        sems = pltpu.SemaphoreType.DMA((80,))
        common = {'send': sems, 'recv': sems, 'local': sems}
        front_scratch = {
            'sq_send': pltpu.VMEM((PARTS, 8, lanes), F32), 'sq_recv': pltpu.VMEM((PARTS, 8, 8, lanes), F32),
            'h': pltpu.VMEM((PARTS, depth, lanes), BF16), 'gain_in': pltpu.VMEM(norm_gain.shape, BF16), 'gain': pltpu.VMEM((depth, lanes), F32),
            'even': pltpu.VMEM((depth, 2 * depth), BF16), 'odd': pltpu.VMEM((depth, 2 * depth), BF16),
            'u': pltpu.VMEM((PARTS, lanes, depth), BF16), 'u_rel': pltpu.VMEM((PARTS, lanes, depth), BF16),
            'wa': pltpu.VMEM((depth, attn_cols), BF16), 'wm': pltpu.VMEM((CHUNKS, depth, 2, cols), BF16),
            'a_part': pltpu.VMEM((PARTS, lanes, attn_cols), BF16), 'a_core': pltpu.VMEM((PARTS, half, attn_cols), BF16),
            'a_sum': pltpu.VMEM((PARTS, half, attn_cols), BF16), 'a_across': pltpu.VMEM((PARTS, shard, attn_cols), BF16),
            'a_full': pltpu.VMEM((PARTS, shard, attn_cols), BF16), 'a_yz': pltpu.VMEM((PARTS, seqs, attn_cols), BF16),
            'u2': pltpu.VMEM((PARTS, 2 * lanes, 2 * depth), BF16), 'z_part': pltpu.VMEM((PARTS, CHUNKS, 2 * lanes, cols), BF16),
            'z_recv': pltpu.VMEM((PARTS, CHUNKS, lanes, cols), BF16), 'z_x': pltpu.VMEM((units, half, cols), BF16),
            'z_mine': pltpu.VMEM((units, half, cols), BF16), 'z_early': pltpu.VMEM((EARLY, half, cols), BF16),
        }

        def back_scratch(whole):
            return {
                'o_yz': pltpu.VMEM((num_seqs, out_depth), BF16), 'o': pltpu.VMEM((PARTS, lanes, out_depth), BF16),
                'm': pltpu.VMEM((PARTS, CHUNKS, lanes, cols), BF16), 'z_in': pltpu.VMEM((units, half, cols), BF16),
                'z_got': pltpu.VMEM((units - EARLY, half, cols), BF16), 'o_in': pltpu.VMEM((2, num_seqs, out_depth), BF16),
                'h_in': pltpu.VMEM((PARTS, depth, lanes), BF16),
                'wd': pltpu.VMEM((CHUNKS, cols, depth), BF16), 'wo': pltpu.VMEM((out_depth, depth), BF16),
                'acc': pltpu.VMEM((PARTS, lanes, depth), F32), 'update': pltpu.VMEM((PARTS, lanes, depth), F32),
                'up_part': pltpu.VMEM((PARTS, depth, lanes), BF16),
                'up_recv': pltpu.VMEM((PARTS, depth if whole else part, lanes), BF16),
            }

        front_shapes = (
            jax.ShapeDtypeStruct((2, num_seqs, attn_cols), BF16), jax.ShapeDtypeStruct((units - EARLY, half, cols), BF16),
            jax.ShapeDtypeStruct((units, half, cols), BF16), jax.ShapeDtypeStruct((PARTS, depth, lanes), BF16))
        front_specs = (HBM,) * 4

        def call(kernel, name, collective_id, scratch, in_specs, out_shape, out_specs, *args):
            return pl.pallas_call(
                functools.partial(kernel, tuple(scratch)), out_shape=out_shape, in_specs=list(in_specs), out_specs=out_specs,
                scratch_shapes=list(scratch.values()), name=name,
                compiler_params=pltpu.CompilerParams(collective_id=collective_id, has_side_effects=True, vmem_limit_bytes=VMEM_LIMIT),
            )(*args)

        def start(names, *refs):
            start_kernel(names, model_dim, *refs)

        def middle(names, *refs):
            middle_kernel(names, model_dim, *refs)

        qkv, zsend, zmine, h_block = call(
            start, 'start', 0, {**common, **front_scratch, 'h_in': pltpu.VMEM((part, rows), BF16)}, (HBM,) * 4,
            front_shapes, front_specs, hidden.T, norm_gain, w_attn, w_mlp)
        zgot = lax.ppermute(zsend, 'x', swap)
        k_new, v_new, o = attention(0, lengths, qkv, k_cache, v_cache, ())
        qkv, zsend, zmine, h_block = call(
            middle, 'middle', 1, {**common, **front_scratch, **back_scratch(True)}, (HBM,) * 9,
            front_shapes, front_specs, h_block, o, norm_gain, zmine, zgot, w_down, w_out, w_attn, w_mlp)
        zgot = lax.ppermute(zsend, 'x', swap)
        k_new, v_new, o = attention(1, lengths, qkv, k_cache, v_cache, (k_new, v_new))
        h_out = call(
            end_kernel, 'end', 2, {**common, **back_scratch(False)}, (HBM,) * 6,
            jax.ShapeDtypeStruct((part, rows), BF16), VMEM, h_block, o, zmine, zgot, w_down, w_out)
        return h_out.T, k_new, v_new

    return jax.shard_map(device_step, mesh=mesh, in_specs=in_specs, out_specs=out_specs, check_vma=False)
```

```python
import functools

import jax
import jax.numpy as jnp
from jax import lax
from jax.experimental import pallas as pl
from jax.experimental.pallas import tpu as pltpu
from jax.sharding import PartitionSpec as P

NORM_EPS = 1e-5
MESH = pl.DeviceIdType.MESH
BF16 = jnp.bfloat16
F32 = jnp.float32

CHUNKS = 5
EARLY = 1
LAG = 2
VMEM_LIMIT = 67043328


def dot(a, b):
    return jnp.dot(a, b, preferred_element_type=F32)


class Links:
    def __init__(self, send_sems, recv_sems, local_sems, everyone):
        self.send_sems, self.recv_sems, self.local_sems = send_sems, recv_sems, local_sems
        self.groups, self.used, self.local_groups, self.local_used = {}, 0, {}, 0
        x, y = lax.axis_index('x'), lax.axis_index('yz')
        self.x, self.y = x, y
        core = lax.rem(x, 2)
        self.along_x = (3 - x, x + 1 - 2 * core, lax.rem(x + 2, 4))
        self.blocks = self.along_x + (x,)
        self.targets = tuple({'x': p, 'yz': y} for p in self.blocks) + ({'x': x, 'yz': 1 - y},) + tuple(
            {'x': p, 'yz': 1 - y} for p in self.along_x)
        self.peers = [k for k in range(8) if k != OWN] if everyone else [DIAG, PARTNER, ACROSS, YZ, ACROSS_YZ]
        self.barrier = pltpu.get_barrier_semaphore()
        for k in self.peers:
            pl.semaphore_signal(self.barrier, inc=1, device_id=self.targets[k], device_id_type=MESH)

    def meet(self):
        pl.semaphore_wait(self.barrier, len(self.peers))

    def push(self, src, dst, to, group):
        k = self.used
        self.used += 1
        g = self.groups.setdefault(group, len(self.groups))
        copy = pltpu.make_async_remote_copy(
            src_ref=src, dst_ref=dst, send_sem=self.send_sems.at[g], recv_sem=self.recv_sems.at[k],
            device_id=self.targets[to], device_id_type=MESH)
        copy.start()
        return copy

    def copy(self, src, dst, group=None):
        if group is None or group not in self.local_groups:
            k = self.local_used
            self.local_used += 1
            if group is not None:
                self.local_groups[group] = k
        else:
            k = self.local_groups[group]
        copy = pltpu.make_async_copy(src, dst, self.local_sems.at[k])
        copy.start()
        return copy

    def drain(self, sent, stored):
        for group, g in self.groups.items():
            pltpu.make_async_copy(sent[group], sent[group], self.send_sems.at[g]).wait()
        for group, k in self.local_groups.items():
            pltpu.make_async_copy(stored[group], stored[group], self.local_sems.at[k]).wait()


DIAG, PARTNER, ACROSS, OWN, YZ, ACROSS_YZ = 0, 1, 2, 3, 4, 7
PARTS = 2


def spread_matrices(depth):
    row = lax.broadcasted_iota(jnp.int32, (depth, 2 * depth), 0)
    col = lax.broadcasted_iota(jnp.int32, (depth, 2 * depth), 1)
    one, zero = jnp.ones((), F32), jnp.zeros((), F32)
    return (jnp.where(col == 2 * row, one, zero).astype(BF16), jnp.where(col == 2 * row + 1, one, zero).astype(BF16))


def part_order(rows, inverse):
    i = lax.broadcasted_iota(jnp.int32, (rows, rows), 0)
    j = lax.broadcasted_iota(jnp.int32, (rows, rows), 1)
    src, dst = (j, i) if inverse else (i, j)
    run = rows // (8 * PARTS)
    piece = src // run
    place = lax.rem(piece, PARTS) * (8 * run) + (piece // PARTS) * run + lax.rem(src, run)
    return jnp.where(dst == place, jnp.ones((), F32), jnp.zeros((), F32)).astype(BF16)


class Front:
    def __init__(self, links, layer, gain_hbm, wa_hbm, wm_hbm, model_dim, outs, s):
        self.links, self.s, self.layer, self.model_dim = links, s, layer, model_dim
        self.gain_copy = links.copy(gain_hbm, s['gain_in'])
        self.qkv_out, self.zsend_out, self.zmine_out = outs
        self.chunks, self.depth, _, self.cols = s['wm'].shape
        self.wa = links.copy(wa_hbm.at[layer], s['wa'])
        self.wm = [links.copy(wm_hbm.at[layer, :, :, pl.ds(j * self.cols, self.cols)], s['wm'].at[j]) for j in range(self.chunks)]
        self.wa_ready, self.wm_ready = False, [False] * self.chunks
        self.a_core, self.a_got, self.z_core, self.early = {}, {}, {}, {}
        self.sq = {}

    def constants(self):
        lanes = self.s['u'].shape[1]
        self.gain_copy.wait()
        gain = jnp.broadcast_to(self.s['gain_in'][self.layer:self.layer + 1, :].astype(F32), (lanes, self.depth)).T
        self.s['gain'][...] = gain
        self.s['even'][...], self.s['odd'][...] = spread_matrices(self.depth)

    def send_squares(self, p, h_t, to):
        s = self.s
        s['sq_send'][p] = jnp.broadcast_to(jnp.sum(h_t * h_t, axis=0, keepdims=True), s['sq_send'].shape[1:])
        self.sq[p] = [self.links.push(s['sq_send'].at[p], s['sq_recv'].at[p, k], k, 'sq') for k in to]

    def normalize(self, p, h_t, to):
        s, links = self.s, self.links
        for c in self.sq[p]:
            c.wait_recv()
        total = s['sq_send'][p]
        for k in sorted(to):
            total = total + s['sq_recv'][p, k]
        inv_rms = lax.rsqrt(total[:1] / self.model_dim + NORM_EPS)
        s['u'][p] = (h_t * inv_rms * s['gain'][...]).T.astype(BF16)
        shard = s['u'].shape[1] // 4
        u = jnp.concatenate([s['u'][p, pl.ds(pl.multiple_of(b * shard, shard), shard), :] for b in links.blocks], axis=0)
        s['u_rel'][p] = u
        if not self.wa_ready:
            self.wa.wait()
            self.wa_ready = True
        s['a_part'][p] = dot(u, s['wa'][...]).astype(BF16)
        self.a_core[p] = links.push(s['a_part'].at[p, pl.ds(0, 2 * shard)], s['a_core'].at[p], PARTNER, 'a_core')

    def spread(self, p):
        s = self.s
        u = s['u_rel'][p]
        gate, up = dot(u, s['even'][...]).astype(BF16), dot(u, s['odd'][...]).astype(BF16)
        shard = u.shape[0] // 4
        for k in range(4):
            s['u2'][p, 2 * k * shard:(2 * k + 1) * shard] = gate[k * shard:(k + 1) * shard]
            s['u2'][p, (2 * k + 1) * shard:(2 * k + 2) * shard] = up[k * shard:(k + 1) * shard]

    def attend_core(self, p):
        s = self.s
        half = s['a_core'].shape[1]
        self.a_core[p].wait_recv()
        s['a_sum'][p] = (s['a_part'][p, half:].astype(F32) + s['a_core'][p].astype(F32)).astype(BF16)
        shard, seqs = half // 2, s['a_got'].shape[2]
        y = self.links.y
        here, there = pl.multiple_of(y * seqs, seqs), pl.multiple_of((1 - y) * seqs, seqs)
        self.a_got[p] = [
            self.links.push(s['a_sum'].at[p, pl.ds(there, seqs)], s['a_got'].at[p, 2], ACROSS_YZ, 'a_got'),
            self.links.push(s['a_sum'].at[p, pl.ds(here, seqs)], s['a_got'].at[p, 0], ACROSS, 'a_got'),
            self.links.push(s['a_sum'].at[p, pl.ds(shard + there, seqs)], s['a_got'].at[p, 1], YZ, 'a_got')]

    def attend_ends(self, p):
        s, y = self.s, self.links.y
        shard, seqs = s['a_sum'].shape[1] // 2, s['a_got'].shape[2]
        for c in self.a_got[p]:
            c.wait_recv()
        own = s['a_sum'][p, pl.ds(shard + pl.multiple_of(y * seqs, seqs), seqs), :]
        s['a_full'][p, 0] = (own.astype(F32) + s['a_got'][p, 0].astype(F32)).astype(BF16)
        s['a_full'][p, 1] = (s['a_got'][p, 1].astype(F32) + s['a_got'][p, 2].astype(F32)).astype(BF16)
        for k, head in enumerate((y, 1 - y)):
            self.links.copy(s['a_full'].at[p, k], self.qkv_out.at[head, pl.ds(p * seqs, seqs)], 'qkv')

    def project(self, p, j):
        s = self.s
        if not self.wm_ready[j]:
            self.wm[j].wait()
            self.wm_ready[j] = True
        s['z_part'][p, j] = dot(s['u2'][p], s['wm'][j].reshape(2 * self.depth, self.cols)).astype(BF16)
        half = s['z_recv'].shape[2]
        self.z_core[p, j] = self.links.push(s['z_part'].at[p, j, pl.ds(0, half)], s['z_recv'].at[p, j], PARTNER, 'z')

    def combine(self, p, j):
        s, unit = self.s, p * self.chunks + j
        half = s['z_recv'].shape[2]
        shard2 = half // 2
        self.z_core[p, j].wait_recv()
        s['z_x'][unit] = (s['z_part'][p, j, half:half + shard2].astype(F32) + s['z_recv'][p, j, :shard2].astype(F32)).astype(BF16)
        if unit < EARLY:
            self.early[unit] = self.links.push(s['z_x'].at[unit], s['z_early'].at[unit], ACROSS, 'early')
        else:
            self.links.copy(s['z_x'].at[unit], self.zsend_out.at[unit - EARLY], 'z_x')
        s['z_mine'][unit] = (s['z_part'][p, j, half + shard2:].astype(F32) + s['z_recv'][p, j, shard2:].astype(F32)).astype(BF16)
        if unit >= EARLY:
            self.links.copy(s['z_mine'].at[unit], self.zmine_out.at[unit], 'z_mine')

    def finish(self):
        s = self.s
        for unit in range(EARLY):
            self.early[unit].wait_recv()
            s['z_mine'][unit] = (s['z_mine'][unit].astype(F32) + s['z_early'][unit].astype(F32)).astype(BF16)
            self.links.copy(s['z_mine'].at[unit], self.zmine_out.at[unit], 'z_mine')

    def sizes(self):
        s = self.s
        return ({'a_core': s['a_core'], 'a_got': s['a_got'], 'z': s['z_recv'], 'early': s['z_early']},
                {'z_x': s['z_x'].at[pl.ds(EARLY, s['z_x'].shape[0] - EARLY)], 'z_mine': s['z_mine'], 'qkv': s['a_full'], 'h': s['h']})


class Back:
    def __init__(self, links, layer, h_hbm, o_hbm, zgot_hbm, zmine_hbm, wd_hbm, wo_hbm, whole, s):
        self.links, self.s, self.whole = links, s, whole
        self.chunks, cols, _ = s['wd'].shape
        self.z = []
        for unit in range(PARTS * self.chunks):
            self.z.append([links.copy(zmine_hbm.at[unit], s['z_in'].at[unit])])
            if unit >= EARLY:
                self.z[-1].append(links.copy(zgot_hbm.at[unit - EARLY], s['z_got'].at[unit - EARLY]))
            if unit == 0:
                self.o_copy = links.copy(o_hbm, s['o_in'])
                self.h_copy = links.copy(h_hbm, s['h_in'])
        self.wd = [links.copy(wd_hbm.at[layer, pl.ds(j * cols, cols)], s['wd'].at[j]) for j in range(self.chunks)]
        self.wo = links.copy(wo_hbm.at[layer], s['wo'])
        self.wo_ready, self.wd_ready = False, [False] * self.chunks
        self.across, self.partner, self.diag = {}, {}, {}
        self.o_across, self.o_partner, self.o_diag = {}, {}, {}
        self.up = {}

    def mix(self, p, j):
        s, unit = self.s, p * self.chunks + j
        for c in self.z[unit]:
            c.wait()
        z = s['z_in'][unit].astype(F32)
        if unit >= EARLY:
            z = (z + s['z_got'][unit - EARLY].astype(F32)).astype(BF16).astype(F32)
        shard = z.shape[0] // 2
        gate, up = z[:shard], z[shard:]
        s['m'][p, j, OWN * shard:] = (gate * jax.nn.sigmoid(gate) * up).astype(BF16)

    def block(self, p, j, k):
        shard = self.s['m'].shape[2] // 4
        return self.s['m'].at[p, j, pl.ds(k * shard, shard)]

    def send(self, p, j):
        self.across[p, j] = self.links.push(self.block(p, j, OWN), self.block(p, j, ACROSS), ACROSS, 'm')
        self.partner[p, j] = self.links.push(self.block(p, j, OWN), self.block(p, j, PARTNER), PARTNER, 'm')

    def forward(self, p, j):
        self.across[p, j].wait_recv()
        self.diag[p, j] = self.links.push(self.block(p, j, ACROSS), self.block(p, j, DIAG), PARTNER, 'm')

    def send_o_yz(self):
        y, s = self.links.y, self.s
        self.o_copy.wait()
        self.o_yz = self.links.push(s['o_in'].at[1 - y], s['o_yz'], YZ, 'o_yz')

    def o_block(self, p, k):
        shard = self.s['o'].shape[1] // 4
        return self.s['o'].at[p, pl.ds(k * shard, shard)]

    def send_o(self):
        y, s = self.links.y, self.s
        self.o_yz.wait_recv()
        shard = s['o'].shape[1] // 4
        seqs = shard // 2
        for p in range(PARTS):
            s['o'][p, pl.ds(OWN * shard + pl.multiple_of(y * seqs, seqs), seqs), :] = s['o_in'][y, p * seqs:(p + 1) * seqs]
            s['o'][p, pl.ds(OWN * shard + pl.multiple_of((1 - y) * seqs, seqs), seqs), :] = s['o_yz'][p * seqs:(p + 1) * seqs]
            self.o_across[p] = self.links.push(self.o_block(p, OWN), self.o_block(p, ACROSS), ACROSS, 'o')
            self.o_partner[p] = self.links.push(self.o_block(p, OWN), self.o_block(p, PARTNER), PARTNER, 'o')

    def forward_o(self, p):
        self.o_across[p].wait_recv()
        self.o_diag[p] = self.links.push(self.o_block(p, ACROSS), self.o_block(p, DIAG), PARTNER, 'o')

    def project_o(self, p):
        s = self.s
        self.o_partner[p].wait_recv()
        self.o_diag[p].wait_recv()
        if not self.wo_ready:
            self.wo.wait()
            self.wo_ready = True
        s['acc'][p] += dot(s['o'][p], s['wo'][...])

    def down(self, p, j):
        s = self.s
        self.partner[p, j].wait_recv()
        self.diag[p, j].wait_recv()
        if not self.wd_ready[j]:
            self.wd[j].wait()
            self.wd_ready[j] = True
        part = dot(s['m'][p, j], s['wd'][j])
        if j == 0:
            s['acc'][p] = part
        else:
            s['acc'][p] += part

    def send_update(self, p):
        s, links = self.s, self.links
        shard = s['acc'].shape[1] // 4
        for k in range(4):
            s['update'][p, pl.ds(pl.multiple_of(links.blocks[k] * shard, shard), shard), :] = s['acc'][p, k * shard:(k + 1) * shard, :]
        s['up_part'][p] = s['update'][p].T.astype(BF16)
        if self.whole:
            src = s['up_part'].at[p]
        else:
            part = s['up_recv'].shape[1]
            src = s['up_part'].at[p, pl.ds(pl.multiple_of((1 - links.y) * part, part), part)]
        self.up[p] = links.push(src, s['up_recv'].at[p], YZ, 'up')

    def update(self, p):
        s, links = self.s, self.links
        self.up[p].wait_recv()
        if self.whole:
            own = s['up_part'][p]
        else:
            part = s['up_recv'].shape[1]
            own = s['up_part'][p, pl.ds(pl.multiple_of(links.y * part, part), part), :]
        return own.astype(F32) + s['up_recv'][p].astype(F32)

    def sizes(self):
        s = self.s
        sent = 3 * s['m'].shape[2] // 4
        return {'m': s['m'].at[:, :, pl.ds(0, sent)], 'o': s['o'].at[:, pl.ds(0, sent)], 'o_yz': s['o_yz'], 'up': s['up_recv']}

    def open(self):
        links, chunks = self.links, self.chunks
        self.mix(0, 0)
        links.meet()
        self.send_o_yz()
        self.send(0, 0)
        for j in range(1, chunks):
            self.mix(0, j)
            self.send(0, j)
            if j == 2:
                self.send_o()
        if chunks < 3:
            self.send_o()
        for j in range(chunks):
            self.mix(1, j)
            self.send(1, j)


def start_kernel(names, model_dim, h_hbm, gain_hbm, wa_hbm, wm_hbm, qkv_out, zsend_out, zmine_out, h_out, *scratch):
    s = dict(zip(names, scratch))
    links = Links(s['send'], s['recv'], s['local'], True)
    h_copy = links.copy(h_hbm, s['h_in'])
    f = Front(links, 0, gain_hbm, wa_hbm, wm_hbm, model_dim, (qkv_out, zsend_out, zmine_out), s)
    part, rows = h_hbm.shape
    lanes = rows // PARTS
    mine = pl.ds(pl.multiple_of(links.y * part, part), part)
    order = part_order(rows, False)
    h_copy.wait()
    own = dot(s['h_in'][...], order)
    for p in range(PARTS):
        s['h'][p, mine, :] = own[:, p * lanes:(p + 1) * lanes].astype(BF16)
    links.meet()
    h_yz = [links.push(s['h'].at[p, mine], s['h'].at[p, mine], YZ, 'h') for p in range(PARTS)]
    to = [k for k in range(8) if k != OWN]
    for p in range(PARTS):
        f.send_squares(p, own[:, p * lanes:(p + 1) * lanes], to)
    f.constants()
    for p in range(PARTS):
        h_yz[p].wait_recv()
        links.copy(s['h'].at[p], h_out.at[p], 'h')
        f.normalize(p, s['h'][p].astype(F32), to)
    f.spread(0)
    f.attend_core(0)
    f.spread(1)
    f.attend_core(1)
    finish_front(f, 0, {6: 0, 8: 1})
    sent, stored = f.sizes()
    links.drain({**sent, 'sq': s['sq_recv'].at[:, pl.ds(0, len(to))], 'h': s['h'].at[:, mine]}, stored)


def finish_front(f, begun, exchanges):
    units = [(p, j) for p in range(PARTS) for j in range(f.chunks)]
    for n in range(begun, len(units)):
        f.project(*units[n])
        if n >= LAG:
            f.combine(*units[n - LAG])
        if n in exchanges:
            f.attend_ends(exchanges[n])
    for n in range(len(units) - LAG, len(units)):
        f.combine(*units[n])
    f.finish()


def middle_kernel(names, model_dim, h_hbm, o_hbm, gain_hbm, zmine_hbm, zgot_hbm, wd_hbm, wo_hbm, wa_hbm, wm_hbm, qkv_out, zsend_out,
                  zmine_out, h_out, *scratch):
    s = dict(zip(names, scratch))
    links = Links(s['send'], s['recv'], s['local'], False)
    b = Back(links, 0, h_hbm, o_hbm, zgot_hbm, zmine_hbm, wd_hbm, wo_hbm, True, s)
    f = Front(links, 1, gain_hbm, wa_hbm, wm_hbm, model_dim, (qkv_out, zsend_out, zmine_out), s)
    to = (DIAG, PARTNER, ACROSS)
    b.open()
    f.constants()
    b.h_copy.wait()

    def new_h(p):
        h = (s['h_in'][p].astype(F32) + b.update(p)).astype(BF16)
        s['h'][p] = h
        links.copy(s['h'].at[p], h_out.at[p], 'h')
        f.send_squares(p, h.astype(F32), to)

    first_part(b)
    second_part(b, lambda: new_h(0), lambda: f.normalize(0, s['h'][0].astype(F32), to))
    f.spread(0)
    f.attend_core(0)
    f.project(0, 0)
    new_h(1)
    f.project(0, 1)
    f.project(0, 2)
    f.combine(0, 0)
    f.project(0, 3)
    f.combine(0, 1)
    f.normalize(1, s['h'][1].astype(F32), to)
    f.spread(1)
    f.project(0, 4)
    f.attend_core(1)
    f.attend_ends(0)
    f.combine(0, 2)
    finish_front(f, 5, {9: 1})
    sent, stored = f.sizes()
    links.drain({**sent, **b.sizes(), 'sq': s['sq_recv'].at[:, pl.ds(0, len(to))]}, stored)


def first_part(b):
    for j in range(b.chunks):
        b.forward(0, j)
        if j == 2:
            b.forward_o(0)
            b.forward_o(1)
        if j >= 1:
            b.down(0, j - 1)
    b.project_o(0)
    b.down(0, b.chunks - 1)
    b.send_update(0)
    b.forward(1, 0)


def second_part(b, when_updated, when_squared):
    for j in range(1, b.chunks):
        b.forward(1, j)
        b.down(1, j - 1)
        if j == 1:
            b.project_o(1)
        if j == b.chunks - 2:
            when_updated()
    b.down(1, b.chunks - 1)
    b.send_update(1)
    when_squared()


def end_kernel(names, h_hbm, o_hbm, zmine_hbm, zgot_hbm, wd_hbm, wo_hbm, h_out, *scratch):
    s = dict(zip(names, scratch))
    links = Links(s['send'], s['recv'], s['local'], False)
    b = Back(links, 1, h_hbm, o_hbm, zgot_hbm, zmine_hbm, wd_hbm, wo_hbm, False, s)
    part, rows = h_out.shape
    own_rows = pl.ds(pl.multiple_of(links.y * part, part), part)
    b.open()
    b.h_copy.wait()

    def new_h(p):
        return (s['h_in'][p, own_rows, :].astype(F32) + b.update(p)).astype(BF16)

    first_part(b)
    kept = []
    second_part(b, lambda: kept.append(new_h(0)), lambda: None)
    order = part_order(rows, True)
    h_new = jnp.concatenate(kept + [new_h(1)], axis=1)
    h_out[...] = dot(h_new, order).astype(BF16)
    links.drain(b.sizes(), {})


def attention_kernel(layer, per_step, len_hbm, qkv_hbm, k_hbm, v_hbm, *rest):
    k_out, v_out, o_hbm, kbuf, vbuf, q_scr, o_scr, qkv_ref, o_ref, len_ref, in_sem, out_sem, small_sem = rest[-13:]
    num_seqs, kv_heads, cache_len, head_dim = kbuf.shape
    slots = qkv_ref.shape[2] // head_dim
    rows = kv_heads * slots
    scale = head_dim ** -0.5

    def load(i):
        return (pltpu.make_async_copy(k_hbm.at[layer, i], kbuf.at[i], in_sem.at[0, i]),
                pltpu.make_async_copy(v_hbm.at[layer, i], vbuf.at[i], in_sem.at[1, i]))

    def store(i):
        return (pltpu.make_async_copy(kbuf.at[i], k_out.at[layer, i], out_sem.at[0, i]),
                pltpu.make_async_copy(vbuf.at[i], v_out.at[layer, i], out_sem.at[1, i]))

    qkv_copy = pltpu.make_async_copy(qkv_hbm, qkv_ref, small_sem.at[0])
    len_copy = pltpu.make_async_copy(len_hbm, len_ref, small_sem.at[1])
    qkv_copy.start()
    len_copy.start()

    @pl.loop(0, num_seqs)
    def _(i):
        for c in load(i):
            c.start()

    qkv_copy.wait()
    len_copy.wait()
    for head in range(kv_heads):
        for j in range(slots):
            q_scr[pl.ds(head * slots + j, num_seqs, stride=rows), :] = (
                qkv_ref[head, :, j * head_dim:(j + 1) * head_dim].astype(F32))

    tile_row = lax.broadcasted_iota(jnp.int32, (16, head_dim), 0)
    position = lax.broadcasted_iota(jnp.int32, (rows, cache_len), 1)

    @pl.loop(0, num_seqs // per_step)
    def _(step):
        group = [step * per_step + sub for sub in range(per_step)]
        for i in group:
            for c in load(i):
                c.wait()
            length = len_ref[i]
            base = pl.multiple_of((length // 16) * 16, 16)
            hit = tile_row == length - base
            for head in range(kv_heads):
                for buf, j in ((kbuf, slots - 2), (vbuf, slots - 1)):
                    new = q_scr[pl.ds(i * rows + head * slots + j, 1), :]
                    old = buf[i, head, pl.ds(base, 16), :].astype(F32)
                    buf[i, head, pl.ds(base, 16), :] = jnp.where(hit, new, old).astype(buf.dtype)
            for c in store(i):
                c.start()
        scores, probs = [], []
        for i in group:
            q = q_scr[pl.ds(pl.multiple_of(i * rows, rows), rows), :].astype(BF16)
            by_head = [lax.dot_general(q, kbuf[i, head], (((1,), (1,)), ((), ())), preferred_element_type=F32)
                       for head in range(kv_heads)]
            scores.append(jnp.concatenate([by_head[head][head * slots:(head + 1) * slots] for head in range(kv_heads)], axis=0))
        for i, score in zip(group, scores):
            score = jnp.where(position <= len_ref[i], score * scale, -1e30)
            e = jnp.exp(score - jnp.max(score, axis=1, keepdims=True))
            probs.append((e / jnp.sum(e, axis=1, keepdims=True)).astype(BF16))
        for i, p in zip(group, probs):
            by_head = [dot(p, vbuf[i, head]) for head in range(kv_heads)]
            o_scr[pl.ds(pl.multiple_of(i * rows, rows), rows), :] = jnp.concatenate(
                [by_head[head][head * slots:(head + 1) * slots] for head in range(kv_heads)], axis=0)

    for head in range(kv_heads):
        for j in range(slots - 2):
            o_ref[head, :, j * head_dim:(j + 1) * head_dim] = (
                o_scr[pl.ds(head * slots + j, num_seqs, stride=rows), :].astype(o_ref.dtype))
    o_copy = pltpu.make_async_copy(o_ref, o_hbm, small_sem.at[2])
    o_copy.start()

    @pl.loop(0, num_seqs)
    def _(i):
        for c in store(i):
            c.wait()

    o_copy.wait()


VMEM = pl.BlockSpec(memory_space=pltpu.VMEM)
HBM = pl.BlockSpec(memory_space=pltpu.HBM)


def attention(layer, lengths, qkv, k_cache, v_cache, outs):
    layers, num_seqs, kv_heads, cache_len, head_dim = k_cache.shape
    slots = qkv.shape[2] // head_dim
    rows = kv_heads * slots
    return pl.pallas_call(
        functools.partial(attention_kernel, layer, 2),
        out_shape=(jax.ShapeDtypeStruct(k_cache.shape, k_cache.dtype), jax.ShapeDtypeStruct(v_cache.shape, v_cache.dtype),
                   jax.ShapeDtypeStruct((kv_heads, num_seqs, (slots - 2) * head_dim), BF16)),
        in_specs=[HBM] * (4 + len(outs)),
        out_specs=(HBM, HBM, HBM),
        scratch_shapes=[pltpu.VMEM((num_seqs, kv_heads, cache_len, head_dim), BF16)] * 2
        + [pltpu.VMEM((num_seqs * rows, head_dim), F32)] * 2 + [
            pltpu.VMEM(qkv.shape, BF16), pltpu.VMEM((kv_heads, num_seqs, (slots - 2) * head_dim), BF16),
            pltpu.SMEM((num_seqs,), jnp.int32)]
        + [pltpu.SemaphoreType.DMA((2, num_seqs))] * 2 + [pltpu.SemaphoreType.DMA((3,))],
        input_output_aliases={4: 0, 5: 1} if outs else {},
        compiler_params=pltpu.CompilerParams(vmem_limit_bytes=VMEM_LIMIT),
        cost_estimate=pl.CostEstimate(flops=10 ** 10, bytes_accessed=8 * num_seqs * kv_heads * cache_len * head_dim, transcendentals=0),
        name=f'attention_{layer}',
    )(lengths, qkv, k_cache, v_cache, *outs)


def solution(mesh):
    seq_axes = ('rep', 'x', 'yz')
    hidden_spec = P('rep', ('x', 'yz'))
    cache_spec = P(None, seq_axes, None, None, None)
    in_specs = (hidden_spec, P(None, 'x'), P(None, 'x', 'yz'), P(None, 'x', None, 'yz'), P(None, 'yz', 'x'), P(None, 'yz', 'x'), cache_spec, cache_spec, P(seq_axes))
    out_specs = (hidden_spec, cache_spec, cache_spec)
    swap = [(0, 2), (2, 0), (1, 3), (3, 1)]

    def device_step(hidden, norm_gain, w_attn, w_mlp, w_out, w_down, k_cache, v_cache, lengths):
        rows, part = hidden.shape
        depth, attn_cols = w_attn.shape[1:]
        model_dim = depth * mesh.shape['x']
        mlp_cols = w_mlp.shape[3]
        out_depth = w_out.shape[1]
        cols = mlp_cols // CHUNKS
        units = CHUNKS * PARTS
        lanes = rows // PARTS
        half, shard = lanes // 2, lanes // 4
        seqs = shard // 2
        num_seqs = PARTS * seqs

        def semaphores(groups, remote, local):
            return {'send': pltpu.SemaphoreType.DMA((groups,)), 'recv': pltpu.SemaphoreType.DMA((remote,)),
                    'local': pltpu.SemaphoreType.DMA((local,))}

        front_scratch = {
            'sq_send': pltpu.VMEM((PARTS, 8, lanes), F32), 'sq_recv': pltpu.VMEM((PARTS, 8, 8, lanes), F32),
            'h': pltpu.VMEM((PARTS, depth, lanes), BF16), 'gain_in': pltpu.VMEM(norm_gain.shape, BF16), 'gain': pltpu.VMEM((depth, lanes), F32),
            'even': pltpu.VMEM((depth, 2 * depth), BF16), 'odd': pltpu.VMEM((depth, 2 * depth), BF16),
            'u': pltpu.VMEM((PARTS, lanes, depth), BF16), 'u_rel': pltpu.VMEM((PARTS, lanes, depth), BF16),
            'wa': pltpu.VMEM((depth, attn_cols), BF16), 'wm': pltpu.VMEM((CHUNKS, depth, 2, cols), BF16),
            'a_part': pltpu.VMEM((PARTS, lanes, attn_cols), BF16), 'a_core': pltpu.VMEM((PARTS, half, attn_cols), BF16),
            'a_sum': pltpu.VMEM((PARTS, half, attn_cols), BF16), 'a_got': pltpu.VMEM((PARTS, 3, seqs, attn_cols), BF16),
            'a_full': pltpu.VMEM((PARTS, 2, seqs, attn_cols), BF16),
            'u2': pltpu.VMEM((PARTS, 2 * lanes, 2 * depth), BF16), 'z_part': pltpu.VMEM((PARTS, CHUNKS, 2 * lanes, cols), BF16),
            'z_recv': pltpu.VMEM((PARTS, CHUNKS, lanes, cols), BF16), 'z_x': pltpu.VMEM((units, half, cols), BF16),
            'z_mine': pltpu.VMEM((units, half, cols), BF16), 'z_early': pltpu.VMEM((EARLY, half, cols), BF16),
        }

        def back_scratch(whole):
            return {
                'o_yz': pltpu.VMEM((num_seqs, out_depth), BF16), 'o': pltpu.VMEM((PARTS, lanes, out_depth), BF16),
                'm': pltpu.VMEM((PARTS, CHUNKS, lanes, cols), BF16), 'z_in': pltpu.VMEM((units, half, cols), BF16),
                'z_got': pltpu.VMEM((units - EARLY, half, cols), BF16), 'o_in': pltpu.VMEM((2, num_seqs, out_depth), BF16),
                'h_in': pltpu.VMEM((PARTS, depth, lanes), BF16),
                'wd': pltpu.VMEM((CHUNKS, cols, depth), BF16), 'wo': pltpu.VMEM((out_depth, depth), BF16),
                'acc': pltpu.VMEM((PARTS, lanes, depth), F32), 'update': pltpu.VMEM((PARTS, lanes, depth), F32),
                'up_part': pltpu.VMEM((PARTS, depth, lanes), BF16),
                'up_recv': pltpu.VMEM((PARTS, depth if whole else part, lanes), BF16),
            }

        front_shapes = (
            jax.ShapeDtypeStruct((2, num_seqs, attn_cols), BF16), jax.ShapeDtypeStruct((units - EARLY, half, cols), BF16),
            jax.ShapeDtypeStruct((units, half, cols), BF16), jax.ShapeDtypeStruct((PARTS, depth, lanes), BF16))
        front_specs = (HBM,) * 4

        def call(kernel, name, collective_id, scratch, in_specs, out_shape, out_specs, *args):
            return pl.pallas_call(
                functools.partial(kernel, tuple(scratch)), out_shape=out_shape, in_specs=list(in_specs), out_specs=out_specs,
                scratch_shapes=list(scratch.values()), name=name,
                compiler_params=pltpu.CompilerParams(collective_id=collective_id, has_side_effects=True, vmem_limit_bytes=VMEM_LIMIT),
            )(*args)

        def start(names, *refs):
            start_kernel(names, model_dim, *refs)

        def middle(names, *refs):
            middle_kernel(names, model_dim, *refs)

        qkv, zsend, zmine, h_block = call(
            start, 'start', 0, {**semaphores(6, 35, 12), **front_scratch, 'h_in': pltpu.VMEM((part, rows), BF16)}, (HBM,) * 4,
            front_shapes, front_specs, hidden.T, norm_gain, w_attn, w_mlp)
        zgot = lax.ppermute(zsend, 'x', swap)
        k_new, v_new, o = attention(0, lengths, qkv, k_cache, v_cache, ())
        qkv, zsend, zmine, h_block = call(
            middle, 'middle', 1, {**semaphores(9, 64, 38), **front_scratch, **back_scratch(True)}, (HBM,) * 9,
            front_shapes, front_specs, h_block, o, norm_gain, zmine, zgot, w_down, w_out, w_attn, w_mlp)
        zgot = lax.ppermute(zsend, 'x', swap)
        k_new, v_new, o = attention(1, lengths, qkv, k_cache, v_cache, (k_new, v_new))
        h_out = call(
            end_kernel, 'end', 2, {**semaphores(4, 39, 27), **back_scratch(False)}, (HBM,) * 6,
            jax.ShapeDtypeStruct((part, rows), BF16), VMEM, h_block, o, zmine, zgot, w_down, w_out)
        return h_out.T, k_new, v_new

    return jax.shard_map(device_step, mesh=mesh, in_specs=in_specs, out_specs=out_specs, check_vma=False)
```

```python
import functools

import jax
import jax.numpy as jnp
from jax import lax
from jax.experimental import pallas as pl
from jax.experimental.pallas import tpu as pltpu
from jax.sharding import PartitionSpec as P

NORM_EPS = 1e-5
MESH = pl.DeviceIdType.MESH
BF16 = jnp.bfloat16
F32 = jnp.float32

CHUNKS = 5
EARLY = 1
LAG = 2
END_VMEM_LIMIT = 56393728
VMEM_LIMIT = 67043328


def dot(a, b):
    return jnp.dot(a, b, preferred_element_type=F32)


class Links:
    def __init__(self, send_sems, recv_sems, local_sems, peers):
        self.send_sems, self.recv_sems, self.local_sems = send_sems, recv_sems, local_sems
        self.groups, self.used, self.local_groups, self.local_used = {}, 0, {}, 0
        x, y = lax.axis_index('x'), lax.axis_index('yz')
        self.x, self.y = x, y
        core = lax.rem(x, 2)
        self.along_x = (3 - x, x + 1 - 2 * core, lax.rem(x + 2, 4))
        self.blocks = self.along_x + (x,)
        self.targets = tuple({'x': p, 'yz': y} for p in self.blocks) + ({'x': x, 'yz': 1 - y},) + tuple(
            {'x': p, 'yz': 1 - y} for p in self.along_x)
        self.peers = peers
        self.barrier = pltpu.get_barrier_semaphore()
        for k in self.peers:
            pl.semaphore_signal(self.barrier, inc=1, device_id=self.targets[k], device_id_type=MESH)

    def meet(self):
        pl.semaphore_wait(self.barrier, len(self.peers))

    def push(self, src, dst, to, group):
        k = self.used
        self.used += 1
        g = self.groups.setdefault(group, len(self.groups))
        copy = pltpu.make_async_remote_copy(
            src_ref=src, dst_ref=dst, send_sem=self.send_sems.at[g], recv_sem=self.recv_sems.at[k],
            device_id=self.targets[to], device_id_type=MESH)
        copy.start()
        return copy

    def copy(self, src, dst, group=None):
        if group is None or group not in self.local_groups:
            k = self.local_used
            self.local_used += 1
            if group is not None:
                self.local_groups[group] = k
        else:
            k = self.local_groups[group]
        copy = pltpu.make_async_copy(src, dst, self.local_sems.at[k])
        copy.start()
        return copy

    def drain(self, sent, stored):
        for group, g in self.groups.items():
            pltpu.make_async_copy(sent[group], sent[group], self.send_sems.at[g]).wait()
        for group, k in self.local_groups.items():
            pltpu.make_async_copy(stored[group], stored[group], self.local_sems.at[k]).wait()


DIAG, PARTNER, ACROSS, OWN, YZ, ACROSS_YZ = 0, 1, 2, 3, 4, 7
EVERYONE = [k for k in range(8) if k != OWN]
PARTS = 2


def spread_matrices(depth):
    row = lax.broadcasted_iota(jnp.int32, (depth, 2 * depth), 0)
    col = lax.broadcasted_iota(jnp.int32, (depth, 2 * depth), 1)
    one, zero = jnp.ones((), F32), jnp.zeros((), F32)
    return (jnp.where(col == 2 * row, one, zero).astype(BF16), jnp.where(col == 2 * row + 1, one, zero).astype(BF16))


def part_order(rows, inverse):
    i = lax.broadcasted_iota(jnp.int32, (rows, rows), 0)
    j = lax.broadcasted_iota(jnp.int32, (rows, rows), 1)
    src, dst = (j, i) if inverse else (i, j)
    run = rows // (8 * PARTS)
    piece = src // run
    place = lax.rem(piece, PARTS) * (8 * run) + (piece // PARTS) * run + lax.rem(src, run)
    return jnp.where(dst == place, jnp.ones((), F32), jnp.zeros((), F32)).astype(BF16)


class Front:
    def __init__(self, links, layer, gain_hbm, wa_hbm, wm_hbm, model_dim, outs, s):
        self.links, self.s, self.layer, self.model_dim = links, s, layer, model_dim
        self.gain_copy = links.copy(gain_hbm, s['gain_in'])
        self.qkv_out, self.zsend_out, self.zmine_out, self.h_out = outs
        self.chunks, self.cols = s['z_recv'].shape[1], s['z_recv'].shape[3]
        self.depth = s['wa'].shape[0]
        self.wa = links.copy(wa_hbm.at[layer], s['wa'])
        self.wm = links.copy(wm_hbm.at[layer], s['wm'])
        self.wa_ready, self.wm_ready = False, False
        part = self.depth // 2
        self.mine = pl.ds(pl.multiple_of(links.y * part, part), part)
        self.h_yz = {}
        self.a_core, self.a_got, self.z_core, self.early = {}, {}, {}, {}
        self.sq = {}

    def constants(self):
        lanes = self.s['u'].shape[1]
        self.gain_copy.wait()
        gain = jnp.broadcast_to(self.s['gain_in'][self.layer:self.layer + 1, :].astype(F32), (lanes, self.depth)).T
        self.s['gain'][...] = gain
        self.s['even'][...], self.s['odd'][...] = spread_matrices(self.depth)

    def squares(self, p, h_t):
        s = self.s
        s['h'][p, self.mine, :] = h_t.astype(BF16)
        s['sq_send'][p] = jnp.broadcast_to(jnp.sum(h_t * h_t, axis=0, keepdims=True), s['sq_send'].shape[1:])

    def send_h(self, p):
        s, links = self.s, self.links
        self.sq[p] = [links.push(s['sq_send'].at[p], s['sq_recv'].at[p, k], k, 'sq') for k in EVERYONE]
        self.h_yz[p] = links.push(s['h'].at[p, self.mine], s['h'].at[p, self.mine], YZ, 'h')
        links.copy(s['h'].at[p, self.mine], self.h_out.at[p], 'h')

    def normalize(self, p):
        s, links = self.s, self.links
        for c in self.sq[p]:
            c.wait_recv()
        total = s['sq_send'][p]
        for k in EVERYONE:
            total = total + s['sq_recv'][p, k]
        self.h_yz[p].wait_recv()
        h_t = s['h'][p].astype(F32)
        inv_rms = lax.rsqrt(total[:1] / self.model_dim + NORM_EPS)
        s['u'][p] = (h_t * inv_rms * s['gain'][...]).T.astype(BF16)
        shard = s['u'].shape[1] // 4
        u = jnp.concatenate([s['u'][p, pl.ds(pl.multiple_of(b * shard, shard), shard), :] for b in links.blocks], axis=0)
        s['u_rel'][p] = u
        if not self.wa_ready:
            self.wa.wait()
            self.wa_ready = True
        s['a_part'][p] = dot(u, s['wa'][...]).astype(BF16)
        self.a_core[p] = links.push(s['a_part'].at[p, pl.ds(0, 2 * shard)], s['a_core'].at[p], PARTNER, 'a_core')

    def spread(self, p):
        s = self.s
        u = s['u_rel'][p]
        gate, up = dot(u, s['even'][...]).astype(BF16), dot(u, s['odd'][...]).astype(BF16)
        shard = u.shape[0] // 4
        for k in range(4):
            s['u2'][p, 2 * k * shard:(2 * k + 1) * shard] = gate[k * shard:(k + 1) * shard]
            s['u2'][p, (2 * k + 1) * shard:(2 * k + 2) * shard] = up[k * shard:(k + 1) * shard]

    def attend_core(self, p):
        s = self.s
        half = s['a_core'].shape[1]
        self.a_core[p].wait_recv()
        s['a_sum'][p] = (s['a_part'][p, half:].astype(F32) + s['a_core'][p].astype(F32)).astype(BF16)
        shard, seqs = half // 2, s['a_got'].shape[2]
        y = self.links.y
        here, there = pl.multiple_of(y * seqs, seqs), pl.multiple_of((1 - y) * seqs, seqs)
        self.a_got[p] = [
            self.links.push(s['a_sum'].at[p, pl.ds(there, seqs)], s['a_got'].at[p, 2], ACROSS_YZ, 'a_got'),
            self.links.push(s['a_sum'].at[p, pl.ds(here, seqs)], s['a_got'].at[p, 0], ACROSS, 'a_got'),
            self.links.push(s['a_sum'].at[p, pl.ds(shard + there, seqs)], s['a_got'].at[p, 1], YZ, 'a_got')]

    def attend_ends(self, p):
        s, y = self.s, self.links.y
        shard, seqs = s['a_sum'].shape[1] // 2, s['a_got'].shape[2]
        for c in self.a_got[p]:
            c.wait_recv()
        own = s['a_sum'][p, pl.ds(shard + pl.multiple_of(y * seqs, seqs), seqs), :]
        s['a_full'][p, 0] = (own.astype(F32) + s['a_got'][p, 0].astype(F32)).astype(BF16)
        s['a_full'][p, 1] = (s['a_got'][p, 1].astype(F32) + s['a_got'][p, 2].astype(F32)).astype(BF16)
        for k, head in enumerate((y, 1 - y)):
            self.links.copy(s['a_full'].at[p, k], self.qkv_out.at[head, pl.ds(p * seqs, seqs)], 'qkv')

    def project(self, p, j):
        s = self.s
        if not self.wm_ready:
            self.wm.wait()
            self.wm_ready = True
        w = s['wm'][:, :, j * self.cols:(j + 1) * self.cols].reshape(2 * self.depth, self.cols)
        s['z_part'][p, j] = dot(s['u2'][p], w).astype(BF16)
        half = s['z_recv'].shape[2]
        self.z_core[p, j] = self.links.push(s['z_part'].at[p, j, pl.ds(0, half)], s['z_recv'].at[p, j], PARTNER, 'z')

    def combine(self, p, j):
        s, unit = self.s, p * self.chunks + j
        half = s['z_recv'].shape[2]
        shard2 = half // 2
        self.z_core[p, j].wait_recv()
        s['z_x'][unit] = (s['z_part'][p, j, half:half + shard2].astype(F32) + s['z_recv'][p, j, :shard2].astype(F32)).astype(BF16)
        if unit < EARLY:
            self.early[unit] = self.links.push(s['z_x'].at[unit], s['z_early'].at[unit], ACROSS, 'early')
        else:
            self.links.copy(s['z_x'].at[unit], self.zsend_out.at[unit - EARLY], 'z_x')
        s['z_mine'][unit] = (s['z_part'][p, j, half + shard2:].astype(F32) + s['z_recv'][p, j, shard2:].astype(F32)).astype(BF16)
        if unit >= EARLY:
            self.links.copy(s['z_mine'].at[unit], self.zmine_out.at[unit], 'z_mine')

    def finish(self):
        s = self.s
        for unit in range(EARLY):
            self.early[unit].wait_recv()
            s['z_mine'][unit] = (s['z_mine'][unit].astype(F32) + s['z_early'][unit].astype(F32)).astype(BF16)
            self.links.copy(s['z_mine'].at[unit], self.zmine_out.at[unit], 'z_mine')

    def sizes(self):
        s = self.s
        return ({'a_core': s['a_core'], 'a_got': s['a_got'], 'z': s['z_recv'], 'early': s['z_early'],
                 'sq': s['sq_recv'].at[:, pl.ds(0, len(EVERYONE))], 'h': s['h'].at[:, self.mine]},
                {'z_x': s['z_x'].at[pl.ds(EARLY, s['z_x'].shape[0] - EARLY)], 'z_mine': s['z_mine'], 'qkv': s['a_full'], 'h': s['h'].at[:, self.mine]})


class Back:
    def __init__(self, links, layer, h_hbm, o_hbm, zgot_hbm, zmine_hbm, wd_hbm, wo_hbm, s):
        self.links, self.s = links, s
        self.chunks, self.cols = s['m'].shape[1], s['m'].shape[3]
        units = PARTS * self.chunks
        self.z = []
        for first, last in ((0, 1), (1, self.chunks), (self.chunks, units)):
            run = pl.ds(first, last - first)
            self.z.append((first, links.copy(zmine_hbm.at[run], s['z_in'].at[run])))
            start = max(first, EARLY)
            if start < last:
                run = pl.ds(start - EARLY, last - start)
                self.z.append((start, links.copy(zgot_hbm.at[run], s['z_got'].at[run])))
            if first == 0:
                self.o_copy = links.copy(o_hbm, s['o_in'])
                self.h_copy = links.copy(h_hbm, s['h_in'])
        self.wd = links.copy(wd_hbm.at[layer], s['wd'])
        self.wo = links.copy(wo_hbm.at[layer], s['wo'])
        self.wo_ready, self.wd_ready = False, False
        self.across, self.partner, self.diag = {}, {}, {}
        self.o_across, self.o_partner, self.o_diag = {}, {}, {}
        self.up = {}

    def mix(self, p, j):
        s, unit = self.s, p * self.chunks + j
        while self.z and self.z[0][0] <= unit:
            self.z.pop(0)[1].wait()
        z = s['z_in'][unit].astype(F32)
        if unit >= EARLY:
            z = (z + s['z_got'][unit - EARLY].astype(F32)).astype(BF16).astype(F32)
        shard = z.shape[0] // 2
        gate, up = z[:shard], z[shard:]
        s['m'][p, j, OWN * shard:] = (gate * jax.nn.sigmoid(gate) * up).astype(BF16)

    def block(self, p, j, k):
        shard = self.s['m'].shape[2] // 4
        return self.s['m'].at[p, j, pl.ds(k * shard, shard)]

    def send(self, p, j):
        self.across[p, j] = self.links.push(self.block(p, j, OWN), self.block(p, j, ACROSS), ACROSS, 'm')

    def send_partner(self, p):
        m = self.s['m']
        shard = m.shape[2] // 4
        self.partner[p] = self.links.push(m.at[p, :, pl.ds(OWN * shard, shard)], m.at[p, :, pl.ds(PARTNER * shard, shard)], PARTNER, 'm')

    def forward(self, p, j):
        self.across[p, j].wait_recv()
        self.diag[p, j] = self.links.push(self.block(p, j, ACROSS), self.block(p, j, DIAG), PARTNER, 'm')

    def send_o_yz(self):
        y, s = self.links.y, self.s
        self.o_copy.wait()
        self.o_yz = self.links.push(s['o_in'].at[1 - y], s['o_yz'], YZ, 'o_yz')

    def o_block(self, p, k):
        shard = self.s['o'].shape[1] // 4
        return self.s['o'].at[p, pl.ds(k * shard, shard)]

    def send_o(self):
        y, s = self.links.y, self.s
        self.o_yz.wait_recv()
        shard = s['o'].shape[1] // 4
        seqs = shard // 2
        for p in range(PARTS):
            s['o'][p, pl.ds(OWN * shard + pl.multiple_of(y * seqs, seqs), seqs), :] = s['o_in'][y, p * seqs:(p + 1) * seqs]
            s['o'][p, pl.ds(OWN * shard + pl.multiple_of((1 - y) * seqs, seqs), seqs), :] = s['o_yz'][p * seqs:(p + 1) * seqs]
            self.o_across[p] = self.links.push(self.o_block(p, OWN), self.o_block(p, ACROSS), ACROSS, 'o')
            self.o_partner[p] = self.links.push(self.o_block(p, OWN), self.o_block(p, PARTNER), PARTNER, 'o')

    def forward_o(self, p):
        self.o_across[p].wait_recv()
        self.o_diag[p] = self.links.push(self.o_block(p, ACROSS), self.o_block(p, DIAG), PARTNER, 'o')

    def project_o(self, p):
        s = self.s
        self.o_partner[p].wait_recv()
        self.o_diag[p].wait_recv()
        if not self.wo_ready:
            self.wo.wait()
            self.wo_ready = True
        s['acc'][p] += dot(s['o'][p], s['wo'][...])

    def down(self, p, j):
        s = self.s
        if j == 0:
            self.partner[p].wait_recv()
        self.diag[p, j].wait_recv()
        if not self.wd_ready:
            self.wd.wait()
            self.wd_ready = True
        part = dot(s['m'][p, j], s['wd'][j * self.cols:(j + 1) * self.cols])
        if j == 0:
            s['acc'][p] = part
        else:
            s['acc'][p] += part

    def send_update(self, p):
        s, links = self.s, self.links
        shard = s['acc'].shape[1] // 4
        for k in range(4):
            s['update'][p, pl.ds(pl.multiple_of(links.blocks[k] * shard, shard), shard), :] = s['acc'][p, k * shard:(k + 1) * shard, :]
        s['up_part'][p] = s['update'][p].T.astype(BF16)
        part = s['up_recv'].shape[1]
        src = s['up_part'].at[p, pl.ds(pl.multiple_of((1 - links.y) * part, part), part)]
        self.up[p] = links.push(src, s['up_recv'].at[p], YZ, 'up')

    def new_h(self, p):
        s, links = self.s, self.links
        self.up[p].wait_recv()
        part = s['up_recv'].shape[1]
        own = s['up_part'][p, pl.ds(pl.multiple_of(links.y * part, part), part), :]
        return (s['h_in'][p].astype(F32) + (own.astype(F32) + s['up_recv'][p].astype(F32))).astype(BF16)

    def sizes(self):
        s = self.s
        sent = 3 * s['m'].shape[2] // 4
        return {'m': s['m'].at[:, :, pl.ds(0, sent)], 'o': s['o'].at[:, pl.ds(0, sent)], 'o_yz': s['o_yz'], 'up': s['up_recv']}

    def open(self):
        links, chunks = self.links, self.chunks
        self.mix(0, 0)
        links.meet()
        self.send(0, 0)
        self.send_o_yz()
        for j in range(1, chunks):
            self.mix(0, j)
            self.send(0, j)
            if j == 2:
                self.send_o()
        self.send_partner(0)
        for j in range(chunks):
            self.mix(1, j)
            self.send(1, j)
        self.send_partner(1)
        self.h_copy.wait()


def start_kernel(names, model_dim, h_hbm, gain_hbm, wa_hbm, wm_hbm, qkv_out, zsend_out, zmine_out, h_out, *scratch):
    s = dict(zip(names, scratch))
    links = Links(s['send'], s['recv'], s['local'], EVERYONE)
    h_copy = links.copy(h_hbm, s['h_in'])
    f = Front(links, 0, gain_hbm, wa_hbm, wm_hbm, model_dim, (qkv_out, zsend_out, zmine_out, h_out), s)
    rows = h_hbm.shape[1]
    lanes = rows // PARTS
    order = part_order(rows, False)
    h_copy.wait()
    own = dot(s['h_in'][...], order)
    for p in range(PARTS):
        f.squares(p, own[:, p * lanes:(p + 1) * lanes])
    f.constants()
    links.meet()
    for p in range(PARTS):
        f.send_h(p)
    for p in range(PARTS):
        f.normalize(p)
    f.spread(0)
    f.attend_core(0)
    f.spread(1)
    f.attend_core(1)
    finish_front(f, 0, {6: 0, 8: 1})
    links.drain(*f.sizes())


def finish_front(f, begun, exchanges):
    units = [(p, j) for p in range(PARTS) for j in range(f.chunks)]
    for n in range(begun, len(units)):
        f.project(*units[n])
        if n >= LAG:
            f.combine(*units[n - LAG])
        if n in exchanges:
            f.attend_ends(exchanges[n])
    for n in range(len(units) - LAG, len(units)):
        f.combine(*units[n])
    f.finish()


def middle_kernel(names, model_dim, h_hbm, o_hbm, gain_hbm, zmine_hbm, zgot_hbm, wd_hbm, wo_hbm, wa_hbm, wm_hbm, qkv_out, zsend_out,
                  zmine_out, h_out, *scratch):
    s = dict(zip(names, scratch))
    links = Links(s['send'], s['recv'], s['local'], EVERYONE)
    b = Back(links, 0, h_hbm, o_hbm, zgot_hbm, zmine_hbm, wd_hbm, wo_hbm, s)
    f = Front(links, 1, gain_hbm, wa_hbm, wm_hbm, model_dim, (qkv_out, zsend_out, zmine_out, h_out), s)
    b.open()
    f.constants()

    def pass_h(p):
        f.squares(p, b.new_h(p).astype(F32))
        f.send_h(p)

    first_part(b)
    second_part(b, lambda: pass_h(0))
    f.normalize(0)
    pass_h(1)
    f.spread(0)
    f.attend_core(0)
    f.project(0, 0)
    f.project(0, 1)
    f.project(0, 2)
    f.combine(0, 0)
    f.project(0, 3)
    f.combine(0, 1)
    f.normalize(1)
    f.project(0, 4)
    f.attend_ends(0)
    f.combine(0, 2)
    f.spread(1)
    f.attend_core(1)
    finish_front(f, 5, {9: 1})
    sent, stored = f.sizes()
    links.drain({**sent, **b.sizes()}, stored)


def first_part(b):
    for j in range(b.chunks):
        b.forward(0, j)
        if j == 2:
            b.forward_o(0)
            b.forward_o(1)
        if j >= 1:
            b.down(0, j - 1)
    b.project_o(0)
    b.down(0, b.chunks - 1)
    b.send_update(0)
    b.forward(1, 0)


def second_part(b, when_updated):
    for j in range(1, b.chunks):
        b.forward(1, j)
        b.down(1, j - 1)
        if j == 1:
            b.project_o(1)
        if j == b.chunks - 2:
            when_updated()
    b.down(1, b.chunks - 1)
    b.send_update(1)


def end_kernel(names, h_hbm, o_hbm, zmine_hbm, zgot_hbm, wd_hbm, wo_hbm, h_out, *scratch):
    s = dict(zip(names, scratch))
    links = Links(s['send'], s['recv'], s['local'], [PARTNER, ACROSS, YZ])
    b = Back(links, 1, h_hbm, o_hbm, zgot_hbm, zmine_hbm, wd_hbm, wo_hbm, s)
    b.open()
    first_part(b)
    h_new = []
    second_part(b, lambda: h_new.append(b.new_h(0)))
    order = part_order(h_out.shape[1], True)
    h_new.append(b.new_h(1))
    h_out[...] = dot(jnp.concatenate(h_new, axis=1), order).astype(BF16)
    links.drain(b.sizes(), {})


def attention_kernel(layer, per_step, len_hbm, qkv_hbm, k_hbm, v_hbm, *rest):
    k_out, v_out, o_hbm, kbuf, vbuf, q_scr, o_scr, qkv_ref, o_ref, len_ref, in_sem, out_sem, small_sem = rest[-13:]
    num_seqs, kv_heads, cache_len, head_dim = kbuf.shape
    slots = qkv_ref.shape[2] // head_dim
    rows = kv_heads * slots
    scale = head_dim ** -0.5

    def load(i):
        return (pltpu.make_async_copy(k_hbm.at[layer, i], kbuf.at[i], in_sem.at[0, i]),
                pltpu.make_async_copy(v_hbm.at[layer, i], vbuf.at[i], in_sem.at[1, i]))

    def store(i):
        return (pltpu.make_async_copy(kbuf.at[i], k_out.at[layer, i], out_sem.at[0, i]),
                pltpu.make_async_copy(vbuf.at[i], v_out.at[layer, i], out_sem.at[1, i]))

    qkv_copy = pltpu.make_async_copy(qkv_hbm, qkv_ref, small_sem.at[0])
    len_copy = pltpu.make_async_copy(len_hbm, len_ref, small_sem.at[1])
    qkv_copy.start()
    len_copy.start()

    @pl.loop(0, num_seqs)
    def _(i):
        for c in load(i):
            c.start()

    qkv_copy.wait()
    len_copy.wait()
    for head in range(kv_heads):
        for j in range(slots):
            q_scr[pl.ds(head * slots + j, num_seqs, stride=rows), :] = (
                qkv_ref[head, :, j * head_dim:(j + 1) * head_dim].astype(F32))

    tile_row = lax.broadcasted_iota(jnp.int32, (16, head_dim), 0)
    position = lax.broadcasted_iota(jnp.int32, (rows, cache_len), 1)

    @pl.loop(0, num_seqs // per_step)
    def _(step):
        group = [step * per_step + sub for sub in range(per_step)]
        for i in group:
            for c in load(i):
                c.wait()
            length = len_ref[i]
            base = pl.multiple_of((length // 16) * 16, 16)
            hit = tile_row == length - base
            for head in range(kv_heads):
                for buf, j in ((kbuf, slots - 2), (vbuf, slots - 1)):
                    new = q_scr[pl.ds(i * rows + head * slots + j, 1), :]
                    old = buf[i, head, pl.ds(base, 16), :].astype(F32)
                    buf[i, head, pl.ds(base, 16), :] = jnp.where(hit, new, old).astype(buf.dtype)
            for c in store(i):
                c.start()
        scores, probs = [], []
        for i in group:
            q = q_scr[pl.ds(pl.multiple_of(i * rows, rows), rows), :].astype(BF16)
            by_head = [lax.dot_general(q, kbuf[i, head], (((1,), (1,)), ((), ())), preferred_element_type=F32)
                       for head in range(kv_heads)]
            scores.append(jnp.concatenate([by_head[head][head * slots:(head + 1) * slots] for head in range(kv_heads)], axis=0))
        for i, score in zip(group, scores):
            score = jnp.where(position <= len_ref[i], score * scale, -1e30)
            e = jnp.exp(score - jnp.max(score, axis=1, keepdims=True))
            probs.append((e / jnp.sum(e, axis=1, keepdims=True)).astype(BF16))
        for i, p in zip(group, probs):
            by_head = [dot(p, vbuf[i, head]) for head in range(kv_heads)]
            o_scr[pl.ds(pl.multiple_of(i * rows, rows), rows), :] = jnp.concatenate(
                [by_head[head][head * slots:(head + 1) * slots] for head in range(kv_heads)], axis=0)

    for head in range(kv_heads):
        for j in range(slots - 2):
            o_ref[head, :, j * head_dim:(j + 1) * head_dim] = (
                o_scr[pl.ds(head * slots + j, num_seqs, stride=rows), :].astype(o_ref.dtype))
    o_copy = pltpu.make_async_copy(o_ref, o_hbm, small_sem.at[2])
    o_copy.start()

    @pl.loop(0, num_seqs)
    def _(i):
        for c in store(i):
            c.wait()

    o_copy.wait()


VMEM = pl.BlockSpec(memory_space=pltpu.VMEM)
HBM = pl.BlockSpec(memory_space=pltpu.HBM)


def attention(layer, lengths, qkv, k_cache, v_cache, outs):
    layers, num_seqs, kv_heads, cache_len, head_dim = k_cache.shape
    slots = qkv.shape[2] // head_dim
    rows = kv_heads * slots
    return pl.pallas_call(
        functools.partial(attention_kernel, layer, 2),
        out_shape=(jax.ShapeDtypeStruct(k_cache.shape, k_cache.dtype), jax.ShapeDtypeStruct(v_cache.shape, v_cache.dtype),
                   jax.ShapeDtypeStruct((kv_heads, num_seqs, (slots - 2) * head_dim), BF16)),
        in_specs=[HBM] * (4 + len(outs)),
        out_specs=(HBM, HBM, HBM),
        scratch_shapes=[pltpu.VMEM((num_seqs, kv_heads, cache_len, head_dim), BF16)] * 2
        + [pltpu.VMEM((num_seqs * rows, head_dim), F32)] * 2 + [
            pltpu.VMEM(qkv.shape, BF16), pltpu.VMEM((kv_heads, num_seqs, (slots - 2) * head_dim), BF16),
            pltpu.SMEM((num_seqs,), jnp.int32)]
        + [pltpu.SemaphoreType.DMA((2, num_seqs))] * 2 + [pltpu.SemaphoreType.DMA((3,))],
        input_output_aliases={4: 0, 5: 1} if outs else {},
        compiler_params=pltpu.CompilerParams(vmem_limit_bytes=VMEM_LIMIT),
        cost_estimate=pl.CostEstimate(flops=10 ** 10, bytes_accessed=8 * num_seqs * kv_heads * cache_len * head_dim, transcendentals=0),
        name=f'attention_{layer}',
    )(lengths, qkv, k_cache, v_cache, *outs)


def solution(mesh):
    seq_axes = ('rep', 'x', 'yz')
    hidden_spec = P('rep', ('x', 'yz'))
    cache_spec = P(None, seq_axes, None, None, None)
    in_specs = (hidden_spec, P(None, 'x'), P(None, 'x', 'yz'), P(None, 'x', None, 'yz'), P(None, 'yz', 'x'), P(None, 'yz', 'x'), cache_spec, cache_spec, P(seq_axes))
    out_specs = (hidden_spec, cache_spec, cache_spec)
    swap = [(0, 2), (2, 0), (1, 3), (3, 1)]

    def device_step(hidden, norm_gain, w_attn, w_mlp, w_out, w_down, k_cache, v_cache, lengths):
        rows, part = hidden.shape
        depth, attn_cols = w_attn.shape[1:]
        model_dim = depth * mesh.shape['x']
        mlp_cols = w_mlp.shape[3]
        out_depth = w_out.shape[1]
        cols = mlp_cols // CHUNKS
        units = CHUNKS * PARTS
        lanes = rows // PARTS
        half, shard = lanes // 2, lanes // 4
        seqs = shard // 2
        num_seqs = PARTS * seqs

        def semaphores(groups, remote, local):
            return {'send': pltpu.SemaphoreType.DMA((groups,)), 'recv': pltpu.SemaphoreType.DMA((remote,)),
                    'local': pltpu.SemaphoreType.DMA((local,))}

        front_scratch = {
            'sq_send': pltpu.VMEM((PARTS, 8, lanes), F32), 'sq_recv': pltpu.VMEM((PARTS, 8, 8, lanes), F32),
            'h': pltpu.VMEM((PARTS, depth, lanes), BF16), 'gain_in': pltpu.VMEM(norm_gain.shape, BF16), 'gain': pltpu.VMEM((depth, lanes), F32),
            'even': pltpu.VMEM((depth, 2 * depth), BF16), 'odd': pltpu.VMEM((depth, 2 * depth), BF16),
            'u': pltpu.VMEM((PARTS, lanes, depth), BF16), 'u_rel': pltpu.VMEM((PARTS, lanes, depth), BF16),
            'wa': pltpu.VMEM((depth, attn_cols), BF16), 'wm': pltpu.VMEM((depth, 2, mlp_cols), BF16),
            'a_part': pltpu.VMEM((PARTS, lanes, attn_cols), BF16), 'a_core': pltpu.VMEM((PARTS, half, attn_cols), BF16),
            'a_sum': pltpu.VMEM((PARTS, half, attn_cols), BF16), 'a_got': pltpu.VMEM((PARTS, 3, seqs, attn_cols), BF16),
            'a_full': pltpu.VMEM((PARTS, 2, seqs, attn_cols), BF16),
            'u2': pltpu.VMEM((PARTS, 2 * lanes, 2 * depth), BF16), 'z_part': pltpu.VMEM((PARTS, CHUNKS, 2 * lanes, cols), BF16),
            'z_recv': pltpu.VMEM((PARTS, CHUNKS, lanes, cols), BF16), 'z_x': pltpu.VMEM((units, half, cols), BF16),
            'z_mine': pltpu.VMEM((units, half, cols), BF16), 'z_early': pltpu.VMEM((EARLY, half, cols), BF16),
        }

        back_scratch = {
            'o_yz': pltpu.VMEM((num_seqs, out_depth), BF16), 'o': pltpu.VMEM((PARTS, lanes, out_depth), BF16),
            'm': pltpu.VMEM((PARTS, CHUNKS, lanes, cols), BF16), 'z_in': pltpu.VMEM((units, half, cols), BF16),
            'z_got': pltpu.VMEM((units - EARLY, half, cols), BF16), 'o_in': pltpu.VMEM((2, num_seqs, out_depth), BF16),
            'h_in': pltpu.VMEM((PARTS, part, lanes), BF16),
            'wd': pltpu.VMEM((mlp_cols, depth), BF16), 'wo': pltpu.VMEM((out_depth, depth), BF16),
            'acc': pltpu.VMEM((PARTS, lanes, depth), F32), 'update': pltpu.VMEM((PARTS, lanes, depth), F32),
            'up_part': pltpu.VMEM((PARTS, depth, lanes), BF16), 'up_recv': pltpu.VMEM((PARTS, part, lanes), BF16),
        }

        front_shapes = (
            jax.ShapeDtypeStruct((2, num_seqs, attn_cols), BF16), jax.ShapeDtypeStruct((units - EARLY, half, cols), BF16),
            jax.ShapeDtypeStruct((units, half, cols), BF16), jax.ShapeDtypeStruct((PARTS, part, lanes), BF16))
        front_specs = (HBM,) * 4

        def call(kernel, name, collective_id, scratch, in_specs, out_shape, out_specs, *args):
            return pl.pallas_call(
                functools.partial(kernel, tuple(scratch)), out_shape=out_shape, in_specs=list(in_specs), out_specs=out_specs,
                scratch_shapes=list(scratch.values()), name=name,
                compiler_params=pltpu.CompilerParams(collective_id=collective_id, has_side_effects=True, vmem_limit_bytes=END_VMEM_LIMIT if kernel is end_kernel else VMEM_LIMIT),
            )(*args)

        def start(names, *refs):
            start_kernel(names, model_dim, *refs)

        def middle(names, *refs):
            middle_kernel(names, model_dim, *refs)

        qkv, zsend, zmine, h_block = call(
            start, 'start', 0, {**semaphores(6, 35, 8), **front_scratch, 'h_in': pltpu.VMEM((part, rows), BF16)}, (HBM,) * 4,
            front_shapes, front_specs, hidden.T, norm_gain, w_attn, w_mlp)
        zgot = lax.ppermute(zsend, 'x', swap)
        k_new, v_new, o = attention(0, lengths, qkv, k_cache, v_cache, ())
        qkv, zsend, zmine, h_block = call(
            middle, 'middle', 1, {**semaphores(10, 66, 16), **front_scratch, **back_scratch}, (HBM,) * 9,
            front_shapes, front_specs, h_block, o, norm_gain, zmine, zgot, w_down, w_out, w_attn, w_mlp)
        zgot = lax.ppermute(zsend, 'x', swap)
        k_new, v_new, o = attention(1, lengths, qkv, k_cache, v_cache, (k_new, v_new))
        h_out = call(
            end_kernel, 'end', 2, {**semaphores(4, 31, 9), **back_scratch}, (HBM,) * 6,
            jax.ShapeDtypeStruct((part, rows), BF16), VMEM, h_block, o, zmine, zgot, w_down, w_out)
        return h_out.T, k_new, v_new

    return jax.shard_map(device_step, mesh=mesh, in_specs=in_specs, out_specs=out_specs, check_vma=False)
```

```python
import functools

import jax
import jax.numpy as jnp
from jax import lax
from jax.experimental import pallas as pl
from jax.experimental.pallas import tpu as pltpu
from jax.sharding import PartitionSpec as P

NORM_EPS = 1e-5
MESH = pl.DeviceIdType.MESH
BF16 = jnp.bfloat16
F32 = jnp.float32

CHUNKS = 5
EARLY = 1
LAG = 2
END_VMEM_LIMIT = 56393728
VMEM_LIMIT = 67043328


def dot(a, b):
    return jnp.dot(a, b, preferred_element_type=F32)


class Links:
    def __init__(self, send_sems, recv_sems, local_sems, peers):
        self.send_sems, self.recv_sems, self.local_sems = send_sems, recv_sems, local_sems
        self.groups, self.used, self.local_groups, self.local_used = {}, 0, {}, 0
        x, y = lax.axis_index('x'), lax.axis_index('yz')
        self.x, self.y = x, y
        core = lax.rem(x, 2)
        self.along_x = (3 - x, x + 1 - 2 * core, lax.rem(x + 2, 4))
        self.blocks = self.along_x + (x,)
        self.targets = tuple({'x': p, 'yz': y} for p in self.blocks) + ({'x': x, 'yz': 1 - y},) + tuple(
            {'x': p, 'yz': 1 - y} for p in self.along_x)
        self.peers = peers
        self.barrier = pltpu.get_barrier_semaphore()
        for k in self.peers:
            pl.semaphore_signal(self.barrier, inc=1, device_id=self.targets[k], device_id_type=MESH)

    def meet(self):
        pl.semaphore_wait(self.barrier, len(self.peers))

    def push(self, src, dst, to, group):
        k = self.used
        self.used += 1
        g = self.groups.setdefault(group, len(self.groups))
        copy = pltpu.make_async_remote_copy(
            src_ref=src, dst_ref=dst, send_sem=self.send_sems.at[g], recv_sem=self.recv_sems.at[k],
            device_id=self.targets[to], device_id_type=MESH)
        copy.start()
        return copy

    def copy(self, src, dst, group=None):
        if group is None or group not in self.local_groups:
            k = self.local_used
            self.local_used += 1
            if group is not None:
                self.local_groups[group] = k
        else:
            k = self.local_groups[group]
        copy = pltpu.make_async_copy(src, dst, self.local_sems.at[k])
        copy.start()
        return copy

    def drain(self, sent, stored):
        for group, g in self.groups.items():
            pltpu.make_async_copy(sent[group], sent[group], self.send_sems.at[g]).wait()
        for group, k in self.local_groups.items():
            pltpu.make_async_copy(stored[group], stored[group], self.local_sems.at[k]).wait()


DIAG, PARTNER, ACROSS, OWN, YZ, ACROSS_YZ = 0, 1, 2, 3, 4, 7
EVERYONE = [k for k in range(8) if k != OWN]
PARTS = 2


def spread_matrices(depth):
    row = lax.broadcasted_iota(jnp.int32, (depth, 2 * depth), 0)
    col = lax.broadcasted_iota(jnp.int32, (depth, 2 * depth), 1)
    one, zero = jnp.ones((), F32), jnp.zeros((), F32)
    return (jnp.where(col == 2 * row, one, zero).astype(BF16), jnp.where(col == 2 * row + 1, one, zero).astype(BF16))


def part_order(rows, inverse):
    i = lax.broadcasted_iota(jnp.int32, (rows, rows), 0)
    j = lax.broadcasted_iota(jnp.int32, (rows, rows), 1)
    src, dst = (j, i) if inverse else (i, j)
    run = rows // (8 * PARTS)
    piece = src // run
    place = lax.rem(piece, PARTS) * (8 * run) + (piece // PARTS) * run + lax.rem(src, run)
    return jnp.where(dst == place, jnp.ones((), F32), jnp.zeros((), F32)).astype(BF16)


class Front:
    def __init__(self, links, layer, gain_hbm, wa_hbm, wm_hbm, model_dim, outs, s):
        self.links, self.s, self.layer, self.model_dim = links, s, layer, model_dim
        self.gain_copy = links.copy(gain_hbm, s['gain_in'])
        self.qkv_out, self.zsend_out, self.zmine_out, self.h_out = outs
        self.chunks, self.cols = s['z_recv'].shape[1], s['z_recv'].shape[3]
        self.depth = s['wa'].shape[0]
        self.wa = links.copy(wa_hbm.at[layer], s['wa'])
        self.wm = links.copy(wm_hbm.at[layer], s['wm'])
        self.wa_ready, self.wm_ready = False, False
        part = self.depth // 2
        self.mine = pl.ds(pl.multiple_of(links.y * part, part), part)
        self.h_yz = {}
        self.a_core, self.a_got, self.z_core, self.early = {}, {}, {}, {}
        self.sq = {}

    def constants(self):
        lanes = self.s['u'].shape[1]
        self.gain_copy.wait()
        gain = jnp.broadcast_to(self.s['gain_in'][self.layer:self.layer + 1, :].astype(F32), (lanes, self.depth)).T
        self.s['gain'][...] = gain
        self.s['even'][...], self.s['odd'][...] = spread_matrices(self.depth)

    def squares(self, p, h_t):
        s = self.s
        s['h'][p, self.mine, :] = h_t.astype(BF16)
        s['sq_send'][p] = jnp.broadcast_to(jnp.sum(h_t * h_t, axis=0, keepdims=True), s['sq_send'].shape[1:])

    def send_h(self, p):
        s, links = self.s, self.links
        self.sq[p] = [links.push(s['sq_send'].at[p], s['sq_recv'].at[p, k], k, 'sq') for k in EVERYONE]
        self.h_yz[p] = links.push(s['h'].at[p, self.mine], s['h'].at[p, self.mine], YZ, 'h')
        links.copy(s['h'].at[p, self.mine], self.h_out.at[p], 'h')

    def normalize(self, p):
        s, links = self.s, self.links
        for c in self.sq[p]:
            c.wait_recv()
        total = s['sq_send'][p]
        for k in EVERYONE:
            total = total + s['sq_recv'][p, k]
        self.h_yz[p].wait_recv()
        h_t = s['h'][p].astype(F32)
        inv_rms = lax.rsqrt(total[:1] / self.model_dim + NORM_EPS)
        s['u'][p] = (h_t * inv_rms * s['gain'][...]).T.astype(BF16)
        shard = s['u'].shape[1] // 4
        u = jnp.concatenate([s['u'][p, pl.ds(pl.multiple_of(b * shard, shard), shard), :] for b in links.blocks], axis=0)
        s['u_rel'][p] = u
        if not self.wa_ready:
            self.wa.wait()
            self.wa_ready = True
        s['a_part'][p] = dot(u, s['wa'][...]).astype(BF16)
        self.a_core[p] = links.push(s['a_part'].at[p, pl.ds(0, 2 * shard)], s['a_core'].at[p], PARTNER, 'a_core')

    def spread(self, p):
        s = self.s
        u = s['u_rel'][p]
        gate, up = dot(u, s['even'][...]).astype(BF16), dot(u, s['odd'][...]).astype(BF16)
        shard = u.shape[0] // 4
        for k in range(4):
            s['u2'][p, 2 * k * shard:(2 * k + 1) * shard] = gate[k * shard:(k + 1) * shard]
            s['u2'][p, (2 * k + 1) * shard:(2 * k + 2) * shard] = up[k * shard:(k + 1) * shard]

    def attend_core(self, p):
        s = self.s
        half = s['a_core'].shape[1]
        self.a_core[p].wait_recv()
        s['a_sum'][p] = (s['a_part'][p, half:].astype(F32) + s['a_core'][p].astype(F32)).astype(BF16)
        shard, seqs = half // 2, s['a_got'].shape[2]
        y = self.links.y
        here, there = pl.multiple_of(y * seqs, seqs), pl.multiple_of((1 - y) * seqs, seqs)
        self.a_got[p] = [
            self.links.push(s['a_sum'].at[p, pl.ds(there, seqs)], s['a_got'].at[p, 2], ACROSS_YZ, 'a_got'),
            self.links.push(s['a_sum'].at[p, pl.ds(here, seqs)], s['a_got'].at[p, 0], ACROSS, 'a_got'),
            self.links.push(s['a_sum'].at[p, pl.ds(shard + there, seqs)], s['a_got'].at[p, 1], YZ, 'a_got')]

    def attend_ends(self, p):
        s, y = self.s, self.links.y
        shard, seqs = s['a_sum'].shape[1] // 2, s['a_got'].shape[2]
        for c in self.a_got[p]:
            c.wait_recv()
        own = s['a_sum'][p, pl.ds(shard + pl.multiple_of(y * seqs, seqs), seqs), :]
        s['a_full'][p, 0] = (own.astype(F32) + s['a_got'][p, 0].astype(F32)).astype(BF16)
        s['a_full'][p, 1] = (s['a_got'][p, 1].astype(F32) + s['a_got'][p, 2].astype(F32)).astype(BF16)
        for k, head in enumerate((y, 1 - y)):
            self.links.copy(s['a_full'].at[p, k], self.qkv_out.at[head, pl.ds(p * seqs, seqs)], 'qkv')

    def project(self, p, j):
        s = self.s
        if not self.wm_ready:
            self.wm.wait()
            self.wm_ready = True
        w = s['wm'][:, :, j * self.cols:(j + 1) * self.cols].reshape(2 * self.depth, self.cols)
        s['z_part'][p, j] = dot(s['u2'][p], w).astype(BF16)
        half = s['z_recv'].shape[2]
        self.z_core[p, j] = self.links.push(s['z_part'].at[p, j, pl.ds(0, half)], s['z_recv'].at[p, j], PARTNER, 'z')

    def combine(self, p, j):
        s, unit = self.s, p * self.chunks + j
        half = s['z_recv'].shape[2]
        shard2 = half // 2
        self.z_core[p, j].wait_recv()
        s['z_x'][unit] = (s['z_part'][p, j, half:half + shard2].astype(F32) + s['z_recv'][p, j, :shard2].astype(F32)).astype(BF16)
        if unit < EARLY:
            self.early[unit] = self.links.push(s['z_x'].at[unit], s['z_early'].at[unit], ACROSS, 'early')
        else:
            self.links.copy(s['z_x'].at[unit], self.zsend_out.at[unit - EARLY], 'z_x')
        s['z_mine'][unit] = (s['z_part'][p, j, half + shard2:].astype(F32) + s['z_recv'][p, j, shard2:].astype(F32)).astype(BF16)
        if unit >= EARLY:
            self.links.copy(s['z_mine'].at[unit], self.zmine_out.at[unit], 'z_mine')

    def finish(self):
        s = self.s
        for unit in range(EARLY):
            self.early[unit].wait_recv()
            s['z_mine'][unit] = (s['z_mine'][unit].astype(F32) + s['z_early'][unit].astype(F32)).astype(BF16)
            self.links.copy(s['z_mine'].at[unit], self.zmine_out.at[unit], 'z_mine')

    def sizes(self):
        s = self.s
        return ({'a_core': s['a_core'], 'a_got': s['a_got'], 'z': s['z_recv'], 'early': s['z_early'],
                 'sq': s['sq_recv'].at[:, pl.ds(0, len(EVERYONE))], 'h': s['h'].at[:, self.mine]},
                {'z_x': s['z_x'].at[pl.ds(EARLY, s['z_x'].shape[0] - EARLY)], 'z_mine': s['z_mine'], 'qkv': s['a_full'], 'h': s['h'].at[:, self.mine]})


class Back:
    def __init__(self, links, layer, h_hbm, o_hbm, zgot_hbm, zmine_hbm, wd_hbm, wo_hbm, s):
        self.links, self.s = links, s
        self.chunks, self.cols = s['m'].shape[1], s['m'].shape[3]
        units = PARTS * self.chunks
        self.z = []
        for first, last in ((0, 1), (1, self.chunks), (self.chunks, units)):
            run = pl.ds(first, last - first)
            self.z.append((first, links.copy(zmine_hbm.at[run], s['z_in'].at[run])))
            start = max(first, EARLY)
            if start < last:
                run = pl.ds(start - EARLY, last - start)
                self.z.append((start, links.copy(zgot_hbm.at[run], s['z_got'].at[run])))
            if first == 0:
                self.o_copy = links.copy(o_hbm, s['o_in'])
                self.h_copy = links.copy(h_hbm, s['h_in'])
        self.wd = links.copy(wd_hbm.at[layer], s['wd'])
        self.wo = links.copy(wo_hbm.at[layer], s['wo'])
        self.wo_ready, self.wd_ready = False, False
        self.across, self.partner, self.diag = {}, {}, {}
        self.o_across, self.o_partner, self.o_diag = {}, {}, {}
        self.up = {}

    def mix(self, p, j):
        s, unit = self.s, p * self.chunks + j
        while self.z and self.z[0][0] <= unit:
            self.z.pop(0)[1].wait()
        z = s['z_in'][unit].astype(F32)
        if unit >= EARLY:
            z = (z + s['z_got'][unit - EARLY].astype(F32)).astype(BF16).astype(F32)
        shard = z.shape[0] // 2
        gate, up = z[:shard], z[shard:]
        s['m'][p, j, OWN * shard:] = (gate * jax.nn.sigmoid(gate) * up).astype(BF16)

    def block(self, p, j, k):
        shard = self.s['m'].shape[2] // 4
        return self.s['m'].at[p, j, pl.ds(k * shard, shard)]

    def send(self, p, j):
        self.across[p, j] = self.links.push(self.block(p, j, OWN), self.block(p, j, ACROSS), ACROSS, 'm')

    def send_partner(self, p):
        m = self.s['m']
        shard = m.shape[2] // 4
        self.partner[p] = self.links.push(m.at[p, :, pl.ds(OWN * shard, shard)], m.at[p, :, pl.ds(PARTNER * shard, shard)], PARTNER, 'm')

    def forward(self, p, j):
        self.across[p, j].wait_recv()
        self.diag[p, j] = self.links.push(self.block(p, j, ACROSS), self.block(p, j, DIAG), PARTNER, 'm')

    def send_o_yz(self):
        y, s = self.links.y, self.s
        self.o_copy.wait()
        self.o_yz = self.links.push(s['o_in'].at[1 - y], s['o_yz'], YZ, 'o_yz')

    def o_block(self, p, k):
        shard = self.s['o'].shape[1] // 4
        return self.s['o'].at[p, pl.ds(k * shard, shard)]

    def send_o(self, p):
        y, s = self.links.y, self.s
        if p == 0:
            self.o_yz.wait_recv()
        shard = s['o'].shape[1] // 4
        seqs = shard // 2
        s['o'][p, pl.ds(OWN * shard + pl.multiple_of(y * seqs, seqs), seqs), :] = s['o_in'][y, p * seqs:(p + 1) * seqs]
        s['o'][p, pl.ds(OWN * shard + pl.multiple_of((1 - y) * seqs, seqs), seqs), :] = s['o_yz'][p * seqs:(p + 1) * seqs]
        self.o_across[p] = self.links.push(self.o_block(p, OWN), self.o_block(p, ACROSS), ACROSS, 'o')
        self.o_partner[p] = self.links.push(self.o_block(p, OWN), self.o_block(p, PARTNER), PARTNER, 'o')

    def forward_o(self, p):
        self.o_across[p].wait_recv()
        self.o_diag[p] = self.links.push(self.o_block(p, ACROSS), self.o_block(p, DIAG), PARTNER, 'o')

    def project_o(self, p):
        s = self.s
        self.o_partner[p].wait_recv()
        self.o_diag[p].wait_recv()
        if not self.wo_ready:
            self.wo.wait()
            self.wo_ready = True
        s['acc'][p] += dot(s['o'][p], s['wo'][...])

    def down(self, p, j):
        s = self.s
        if j == 0:
            self.partner[p].wait_recv()
        self.diag[p, j].wait_recv()
        if not self.wd_ready:
            self.wd.wait()
            self.wd_ready = True
        part = dot(s['m'][p, j], s['wd'][j * self.cols:(j + 1) * self.cols])
        if j == 0:
            s['acc'][p] = part
        else:
            s['acc'][p] += part

    def send_update(self, p):
        s, links = self.s, self.links
        shard = s['acc'].shape[1] // 4
        for k in range(4):
            s['update'][p, pl.ds(pl.multiple_of(links.blocks[k] * shard, shard), shard), :] = s['acc'][p, k * shard:(k + 1) * shard, :]
        s['up_part'][p] = s['update'][p].T.astype(BF16)
        part = s['up_recv'].shape[1]
        src = s['up_part'].at[p, pl.ds(pl.multiple_of((1 - links.y) * part, part), part)]
        self.up[p] = links.push(src, s['up_recv'].at[p], YZ, 'up')

    def new_h(self, p):
        s, links = self.s, self.links
        self.up[p].wait_recv()
        part = s['up_recv'].shape[1]
        own = s['up_part'][p, pl.ds(pl.multiple_of(links.y * part, part), part), :]
        return (s['h_in'][p].astype(F32) + (own.astype(F32) + s['up_recv'][p].astype(F32))).astype(BF16)

    def sizes(self):
        s = self.s
        sent = 3 * s['m'].shape[2] // 4
        return {'m': s['m'].at[:, :, pl.ds(0, sent)], 'o': s['o'].at[:, pl.ds(0, sent)], 'o_yz': s['o_yz'], 'up': s['up_recv']}

    def open(self):
        links, chunks = self.links, self.chunks
        self.mix(0, 0)
        links.meet()
        self.send(0, 0)
        self.send_o_yz()
        for j in range(1, chunks):
            self.mix(0, j)
            self.send(0, j)
            if j == 2:
                self.send_o(0)
        self.send_partner(0)
        for j in range(chunks):
            self.mix(1, j)
            self.send(1, j)
            if j == 1:
                self.send_o(1)
        self.send_partner(1)
        self.h_copy.wait()


def start_kernel(names, model_dim, h_hbm, gain_hbm, wa_hbm, wm_hbm, qkv_out, zsend_out, zmine_out, h_out, *scratch):
    s = dict(zip(names, scratch))
    links = Links(s['send'], s['recv'], s['local'], EVERYONE)
    h_copy = links.copy(h_hbm, s['h_in'])
    f = Front(links, 0, gain_hbm, wa_hbm, wm_hbm, model_dim, (qkv_out, zsend_out, zmine_out, h_out), s)
    rows = h_hbm.shape[1]
    lanes = rows // PARTS
    order = part_order(rows, False)
    h_copy.wait()
    own = dot(s['h_in'][...], order)
    for p in range(PARTS):
        f.squares(p, own[:, p * lanes:(p + 1) * lanes])
    f.constants()
    links.meet()
    for p in range(PARTS):
        f.send_h(p)
    for p in range(PARTS):
        f.normalize(p)
    f.spread(0)
    f.attend_core(0)
    f.spread(1)
    f.attend_core(1)
    finish_front(f, 0, {6: 0, 8: 1})
    links.drain(*f.sizes())


def finish_front(f, begun, exchanges):
    units = [(p, j) for p in range(PARTS) for j in range(f.chunks)]
    for n in range(begun, len(units)):
        f.project(*units[n])
        if n >= LAG:
            f.combine(*units[n - LAG])
        if n in exchanges:
            f.attend_ends(exchanges[n])
    for n in range(len(units) - LAG, len(units)):
        f.combine(*units[n])
    f.finish()


def middle_kernel(names, model_dim, h_hbm, o_hbm, gain_hbm, zmine_hbm, zgot_hbm, wd_hbm, wo_hbm, wa_hbm, wm_hbm, qkv_out, zsend_out,
                  zmine_out, h_out, *scratch):
    s = dict(zip(names, scratch))
    links = Links(s['send'], s['recv'], s['local'], EVERYONE)
    b = Back(links, 0, h_hbm, o_hbm, zgot_hbm, zmine_hbm, wd_hbm, wo_hbm, s)
    f = Front(links, 1, gain_hbm, wa_hbm, wm_hbm, model_dim, (qkv_out, zsend_out, zmine_out, h_out), s)
    b.open()
    f.constants()

    def pass_h(p):
        f.squares(p, b.new_h(p).astype(F32))
        f.send_h(p)

    first_part(b)
    second_part(b, lambda: pass_h(0))
    f.normalize(0)
    pass_h(1)
    f.spread(0)
    f.attend_core(0)
    f.project(0, 0)
    f.project(0, 1)
    f.project(0, 2)
    f.combine(0, 0)
    f.project(0, 3)
    f.combine(0, 1)
    f.project(0, 4)
    f.combine(0, 2)
    f.combine(0, 3)
    f.normalize(1)
    f.spread(1)
    f.project(1, 0)
    f.attend_core(1)
    f.combine(0, 4)
    f.attend_ends(0)
    f.project(1, 1)
    f.project(1, 2)
    f.combine(1, 0)
    f.project(1, 3)
    f.combine(1, 1)
    f.project(1, 4)
    f.combine(1, 2)
    f.combine(1, 3)
    f.attend_ends(1)
    f.combine(1, 4)
    f.finish()
    sent, stored = f.sizes()
    links.drain({**sent, **b.sizes()}, stored)


def first_part(b):
    for j in range(b.chunks):
        b.forward(0, j)
        if j == 2:
            b.forward_o(0)
        if j >= 1:
            b.down(0, j - 1)
    b.project_o(0)
    b.down(0, b.chunks - 1)
    b.send_update(0)
    b.forward(1, 0)


def second_part(b, when_updated):
    for j in range(1, b.chunks):
        b.forward(1, j)
        if j == 1:
            b.forward_o(1)
        b.down(1, j - 1)
        if j == 2:
            b.project_o(1)
        if j == b.chunks - 3:
            when_updated()
    b.down(1, b.chunks - 1)
    b.send_update(1)


def end_kernel(names, h_hbm, o_hbm, zmine_hbm, zgot_hbm, wd_hbm, wo_hbm, h_out, *scratch):
    s = dict(zip(names, scratch))
    links = Links(s['send'], s['recv'], s['local'], [PARTNER, ACROSS, YZ])
    b = Back(links, 1, h_hbm, o_hbm, zgot_hbm, zmine_hbm, wd_hbm, wo_hbm, s)
    b.open()
    first_part(b)
    h_new = []
    second_part(b, lambda: h_new.append(b.new_h(0)))
    order = part_order(h_out.shape[1], True)
    h_new.append(b.new_h(1))
    h_out[...] = dot(jnp.concatenate(h_new, axis=1), order).astype(BF16)
    links.drain(b.sizes(), {})


def attention_kernel(layer, per_step, len_hbm, qkv_hbm, k_hbm, v_hbm, *rest):
    k_out, v_out, o_hbm, kbuf, vbuf, q_scr, o_scr, qkv_ref, o_ref, len_ref, in_sem, out_sem, small_sem = rest[-13:]
    num_seqs, kv_heads, cache_len, head_dim = kbuf.shape
    slots = qkv_ref.shape[2] // head_dim
    rows = kv_heads * slots
    scale = head_dim ** -0.5

    def load(i):
        return (pltpu.make_async_copy(k_hbm.at[layer, i], kbuf.at[i], in_sem.at[0, i]),
                pltpu.make_async_copy(v_hbm.at[layer, i], vbuf.at[i], in_sem.at[1, i]))

    def store(i):
        return (pltpu.make_async_copy(kbuf.at[i], k_out.at[layer, i], out_sem.at[0, i]),
                pltpu.make_async_copy(vbuf.at[i], v_out.at[layer, i], out_sem.at[1, i]))

    qkv_copy = pltpu.make_async_copy(qkv_hbm, qkv_ref, small_sem.at[0])
    len_copy = pltpu.make_async_copy(len_hbm, len_ref, small_sem.at[1])
    qkv_copy.start()
    len_copy.start()

    @pl.loop(0, num_seqs)
    def _(i):
        for c in load(i):
            c.start()

    qkv_copy.wait()
    len_copy.wait()
    for head in range(kv_heads):
        for j in range(slots):
            q_scr[pl.ds(head * slots + j, num_seqs, stride=rows), :] = (
                qkv_ref[head, :, j * head_dim:(j + 1) * head_dim].astype(F32))

    tile_row = lax.broadcasted_iota(jnp.int32, (16, head_dim), 0)
    position = lax.broadcasted_iota(jnp.int32, (rows, cache_len), 1)

    @pl.loop(0, num_seqs // per_step)
    def _(step):
        group = [step * per_step + sub for sub in range(per_step)]
        for i in group:
            for c in load(i):
                c.wait()
            length = len_ref[i]
            base = pl.multiple_of((length // 16) * 16, 16)
            hit = tile_row == length - base
            for head in range(kv_heads):
                for buf, j in ((kbuf, slots - 2), (vbuf, slots - 1)):
                    new = q_scr[pl.ds(i * rows + head * slots + j, 1), :]
                    old = buf[i, head, pl.ds(base, 16), :].astype(F32)
                    buf[i, head, pl.ds(base, 16), :] = jnp.where(hit, new, old).astype(buf.dtype)
            for c in store(i):
                c.start()
        scores, probs = [], []
        for i in group:
            q = q_scr[pl.ds(pl.multiple_of(i * rows, rows), rows), :].astype(BF16)
            by_head = [lax.dot_general(q, kbuf[i, head], (((1,), (1,)), ((), ())), preferred_element_type=F32)
                       for head in range(kv_heads)]
            scores.append(jnp.concatenate([by_head[head][head * slots:(head + 1) * slots] for head in range(kv_heads)], axis=0))
        for i, score in zip(group, scores):
            score = jnp.where(position <= len_ref[i], score * scale, -1e30)
            e = jnp.exp(score - jnp.max(score, axis=1, keepdims=True))
            probs.append((e / jnp.sum(e, axis=1, keepdims=True)).astype(BF16))
        for i, p in zip(group, probs):
            by_head = [dot(p, vbuf[i, head]) for head in range(kv_heads)]
            o_scr[pl.ds(pl.multiple_of(i * rows, rows), rows), :] = jnp.concatenate(
                [by_head[head][head * slots:(head + 1) * slots] for head in range(kv_heads)], axis=0)

    for head in range(kv_heads):
        for j in range(slots - 2):
            o_ref[head, :, j * head_dim:(j + 1) * head_dim] = (
                o_scr[pl.ds(head * slots + j, num_seqs, stride=rows), :].astype(o_ref.dtype))
    o_copy = pltpu.make_async_copy(o_ref, o_hbm, small_sem.at[2])
    o_copy.start()

    @pl.loop(0, num_seqs)
    def _(i):
        for c in store(i):
            c.wait()

    o_copy.wait()


VMEM = pl.BlockSpec(memory_space=pltpu.VMEM)
HBM = pl.BlockSpec(memory_space=pltpu.HBM)


def attention(layer, lengths, qkv, k_cache, v_cache, outs):
    layers, num_seqs, kv_heads, cache_len, head_dim = k_cache.shape
    slots = qkv.shape[2] // head_dim
    rows = kv_heads * slots
    return pl.pallas_call(
        functools.partial(attention_kernel, layer, 2),
        out_shape=(jax.ShapeDtypeStruct(k_cache.shape, k_cache.dtype), jax.ShapeDtypeStruct(v_cache.shape, v_cache.dtype),
                   jax.ShapeDtypeStruct((kv_heads, num_seqs, (slots - 2) * head_dim), BF16)),
        in_specs=[HBM] * (4 + len(outs)),
        out_specs=(HBM, HBM, HBM),
        scratch_shapes=[pltpu.VMEM((num_seqs, kv_heads, cache_len, head_dim), BF16)] * 2
        + [pltpu.VMEM((num_seqs * rows, head_dim), F32)] * 2 + [
            pltpu.VMEM(qkv.shape, BF16), pltpu.VMEM((kv_heads, num_seqs, (slots - 2) * head_dim), BF16),
            pltpu.SMEM((num_seqs,), jnp.int32)]
        + [pltpu.SemaphoreType.DMA((2, num_seqs))] * 2 + [pltpu.SemaphoreType.DMA((3,))],
        input_output_aliases={4: 0, 5: 1} if outs else {},
        compiler_params=pltpu.CompilerParams(vmem_limit_bytes=VMEM_LIMIT),
        cost_estimate=pl.CostEstimate(flops=10 ** 10, bytes_accessed=8 * num_seqs * kv_heads * cache_len * head_dim, transcendentals=0),
        name=f'attention_{layer}',
    )(lengths, qkv, k_cache, v_cache, *outs)


def solution(mesh):
    seq_axes = ('rep', 'x', 'yz')
    hidden_spec = P('rep', ('x', 'yz'))
    cache_spec = P(None, seq_axes, None, None, None)
    in_specs = (hidden_spec, P(None, 'x'), P(None, 'x', 'yz'), P(None, 'x', None, 'yz'), P(None, 'yz', 'x'), P(None, 'yz', 'x'), cache_spec, cache_spec, P(seq_axes))
    out_specs = (hidden_spec, cache_spec, cache_spec)
    swap = [(0, 2), (2, 0), (1, 3), (3, 1)]

    def device_step(hidden, norm_gain, w_attn, w_mlp, w_out, w_down, k_cache, v_cache, lengths):
        rows, part = hidden.shape
        depth, attn_cols = w_attn.shape[1:]
        model_dim = depth * mesh.shape['x']
        mlp_cols = w_mlp.shape[3]
        out_depth = w_out.shape[1]
        cols = mlp_cols // CHUNKS
        units = CHUNKS * PARTS
        lanes = rows // PARTS
        half, shard = lanes // 2, lanes // 4
        seqs = shard // 2
        num_seqs = PARTS * seqs

        def semaphores(groups, remote, local):
            return {'send': pltpu.SemaphoreType.DMA((groups,)), 'recv': pltpu.SemaphoreType.DMA((remote,)),
                    'local': pltpu.SemaphoreType.DMA((local,))}

        front_scratch = {
            'sq_send': pltpu.VMEM((PARTS, 8, lanes), F32), 'sq_recv': pltpu.VMEM((PARTS, 8, 8, lanes), F32),
            'h': pltpu.VMEM((PARTS, depth, lanes), BF16), 'gain_in': pltpu.VMEM(norm_gain.shape, BF16), 'gain': pltpu.VMEM((depth, lanes), F32),
            'even': pltpu.VMEM((depth, 2 * depth), BF16), 'odd': pltpu.VMEM((depth, 2 * depth), BF16),
            'u': pltpu.VMEM((PARTS, lanes, depth), BF16), 'u_rel': pltpu.VMEM((PARTS, lanes, depth), BF16),
            'wa': pltpu.VMEM((depth, attn_cols), BF16), 'wm': pltpu.VMEM((depth, 2, mlp_cols), BF16),
            'a_part': pltpu.VMEM((PARTS, lanes, attn_cols), BF16), 'a_core': pltpu.VMEM((PARTS, half, attn_cols), BF16),
            'a_sum': pltpu.VMEM((PARTS, half, attn_cols), BF16), 'a_got': pltpu.VMEM((PARTS, 3, seqs, attn_cols), BF16),
            'a_full': pltpu.VMEM((PARTS, 2, seqs, attn_cols), BF16),
            'u2': pltpu.VMEM((PARTS, 2 * lanes, 2 * depth), BF16), 'z_part': pltpu.VMEM((PARTS, CHUNKS, 2 * lanes, cols), BF16),
            'z_recv': pltpu.VMEM((PARTS, CHUNKS, lanes, cols), BF16), 'z_x': pltpu.VMEM((units, half, cols), BF16),
            'z_mine': pltpu.VMEM((units, half, cols), BF16), 'z_early': pltpu.VMEM((EARLY, half, cols), BF16),
        }

        back_scratch = {
            'o_yz': pltpu.VMEM((num_seqs, out_depth), BF16), 'o': pltpu.VMEM((PARTS, lanes, out_depth), BF16),
            'm': pltpu.VMEM((PARTS, CHUNKS, lanes, cols), BF16), 'z_in': pltpu.VMEM((units, half, cols), BF16),
            'z_got': pltpu.VMEM((units - EARLY, half, cols), BF16), 'o_in': pltpu.VMEM((2, num_seqs, out_depth), BF16),
            'h_in': pltpu.VMEM((PARTS, part, lanes), BF16),
            'wd': pltpu.VMEM((mlp_cols, depth), BF16), 'wo': pltpu.VMEM((out_depth, depth), BF16),
            'acc': pltpu.VMEM((PARTS, lanes, depth), F32), 'update': pltpu.VMEM((PARTS, lanes, depth), F32),
            'up_part': pltpu.VMEM((PARTS, depth, lanes), BF16), 'up_recv': pltpu.VMEM((PARTS, part, lanes), BF16),
        }

        front_shapes = (
            jax.ShapeDtypeStruct((2, num_seqs, attn_cols), BF16), jax.ShapeDtypeStruct((units - EARLY, half, cols), BF16),
            jax.ShapeDtypeStruct((units, half, cols), BF16), jax.ShapeDtypeStruct((PARTS, part, lanes), BF16))
        front_specs = (HBM,) * 4

        def call(kernel, name, collective_id, scratch, in_specs, out_shape, out_specs, *args):
            return pl.pallas_call(
                functools.partial(kernel, tuple(scratch)), out_shape=out_shape, in_specs=list(in_specs), out_specs=out_specs,
                scratch_shapes=list(scratch.values()), name=name,
                compiler_params=pltpu.CompilerParams(collective_id=collective_id, has_side_effects=True, vmem_limit_bytes=END_VMEM_LIMIT if kernel is end_kernel else VMEM_LIMIT),
            )(*args)

        def start(names, *refs):
            start_kernel(names, model_dim, *refs)

        def middle(names, *refs):
            middle_kernel(names, model_dim, *refs)

        qkv, zsend, zmine, h_block = call(
            start, 'start', 0, {**semaphores(6, 35, 8), **front_scratch, 'h_in': pltpu.VMEM((part, rows), BF16)}, (HBM,) * 4,
            front_shapes, front_specs, hidden.T, norm_gain, w_attn, w_mlp)
        zgot = lax.ppermute(zsend, 'x', swap)
        k_new, v_new, o = attention(0, lengths, qkv, k_cache, v_cache, ())
        qkv, zsend, zmine, h_block = call(
            middle, 'middle', 1, {**semaphores(10, 66, 16), **front_scratch, **back_scratch}, (HBM,) * 9,
            front_shapes, front_specs, h_block, o, norm_gain, zmine, zgot, w_down, w_out, w_attn, w_mlp)
        zgot = lax.ppermute(zsend, 'x', swap)
        k_new, v_new, o = attention(1, lengths, qkv, k_cache, v_cache, (k_new, v_new))
        h_out = call(
            end_kernel, 'end', 2, {**semaphores(4, 31, 9), **back_scratch}, (HBM,) * 6,
            jax.ShapeDtypeStruct((part, rows), BF16), VMEM, h_block, o, zmine, zgot, w_down, w_out)
        return h_out.T, k_new, v_new

    return jax.shard_map(device_step, mesh=mesh, in_specs=in_specs, out_specs=out_specs, check_vma=False)
```

```python
import functools

import jax
import jax.numpy as jnp
from jax import lax
from jax.experimental import pallas as pl
from jax.experimental.pallas import tpu as pltpu
from jax.sharding import PartitionSpec as P

NORM_EPS = 1e-5
MESH = pl.DeviceIdType.MESH
BF16 = jnp.bfloat16
F32 = jnp.float32

CHUNKS = 5
EARLY = 1
END_VMEM_LIMIT = 56393728
VMEM_LIMIT = 67043328


def dot(a, b):
    return jnp.dot(a, b, preferred_element_type=F32)


class Links:
    def __init__(self, send_sems, recv_sems, local_sems, peers):
        self.send_sems, self.recv_sems, self.local_sems = send_sems, recv_sems, local_sems
        self.groups, self.used, self.local_groups, self.local_used = {}, 0, {}, 0
        x, y = lax.axis_index('x'), lax.axis_index('yz')
        self.x, self.y = x, y
        core = lax.rem(x, 2)
        self.along_x = (3 - x, x + 1 - 2 * core, lax.rem(x + 2, 4))
        self.blocks = self.along_x + (x,)
        self.targets = tuple({'x': p, 'yz': y} for p in self.blocks) + ({'x': x, 'yz': 1 - y},) + tuple(
            {'x': p, 'yz': 1 - y} for p in self.along_x)
        self.peers = peers
        self.barrier = pltpu.get_barrier_semaphore()
        for k in self.peers:
            pl.semaphore_signal(self.barrier, inc=1, device_id=self.targets[k], device_id_type=MESH)

    def meet(self):
        pl.semaphore_wait(self.barrier, len(self.peers))

    def push(self, src, dst, to, group):
        k = self.used
        self.used += 1
        g = self.groups.setdefault(group, len(self.groups))
        copy = pltpu.make_async_remote_copy(
            src_ref=src, dst_ref=dst, send_sem=self.send_sems.at[g], recv_sem=self.recv_sems.at[k],
            device_id=self.targets[to], device_id_type=MESH)
        copy.start()
        return copy

    def copy(self, src, dst, group=None):
        if group is None or group not in self.local_groups:
            k = self.local_used
            self.local_used += 1
            if group is not None:
                self.local_groups[group] = k
        else:
            k = self.local_groups[group]
        copy = pltpu.make_async_copy(src, dst, self.local_sems.at[k])
        copy.start()
        return copy

    def drain(self, sent, stored):
        for group, g in self.groups.items():
            pltpu.make_async_copy(sent[group], sent[group], self.send_sems.at[g]).wait()
        for group, k in self.local_groups.items():
            pltpu.make_async_copy(stored[group], stored[group], self.local_sems.at[k]).wait()


DIAG, PARTNER, ACROSS, OWN, YZ, ACROSS_YZ = 0, 1, 2, 3, 4, 7
EVERYONE = [k for k in range(8) if k != OWN]
PARTS = 2


def spread_matrices(depth):
    row = lax.broadcasted_iota(jnp.int32, (depth, 2 * depth), 0)
    col = lax.broadcasted_iota(jnp.int32, (depth, 2 * depth), 1)
    one, zero = jnp.ones((), F32), jnp.zeros((), F32)
    return (jnp.where(col == 2 * row, one, zero).astype(BF16), jnp.where(col == 2 * row + 1, one, zero).astype(BF16))


def part_order(rows, inverse):
    i = lax.broadcasted_iota(jnp.int32, (rows, rows), 0)
    j = lax.broadcasted_iota(jnp.int32, (rows, rows), 1)
    src, dst = (j, i) if inverse else (i, j)
    run = rows // (8 * PARTS)
    piece = src // run
    place = lax.rem(piece, PARTS) * (8 * run) + (piece // PARTS) * run + lax.rem(src, run)
    return jnp.where(dst == place, jnp.ones((), F32), jnp.zeros((), F32)).astype(BF16)


class Front:
    def __init__(self, links, layer, gain_hbm, wa_hbm, wm_hbm, model_dim, outs, s):
        self.links, self.s, self.layer, self.model_dim = links, s, layer, model_dim
        self.gain_copy = links.copy(gain_hbm, s['gain_in'])
        self.qkv_out, self.zsend_out, self.zmine_out, self.h_out = outs
        self.chunks, self.cols = s['z_recv'].shape[1], s['z_recv'].shape[3]
        self.depth = s['wa'].shape[0]
        self.wa = links.copy(wa_hbm.at[layer], s['wa'])
        self.wm = links.copy(wm_hbm.at[layer], s['wm'])
        self.wa_ready, self.wm_ready = False, False
        part = self.depth // 2
        self.mine = pl.ds(pl.multiple_of(links.y * part, part), part)
        self.h_yz = {}
        self.a_core, self.a_got, self.z_core, self.early = {}, {}, {}, {}
        self.sq = {}

    def constants(self):
        lanes = self.s['u'].shape[1]
        self.gain_copy.wait()
        gain = jnp.broadcast_to(self.s['gain_in'][self.layer:self.layer + 1, :].astype(F32), (lanes, self.depth)).T
        self.s['gain'][...] = gain
        if 'even' in self.s:
            self.s['even'][...], self.s['odd'][...] = spread_matrices(self.depth)

    def squares(self, p, h_t):
        s = self.s
        s['h'][p, self.mine, :] = h_t.astype(BF16)
        s['sq_send'][p] = jnp.broadcast_to(jnp.sum(h_t * h_t, axis=0, keepdims=True), s['sq_send'].shape[1:])

    def send_h(self, p):
        s, links = self.s, self.links
        self.sq[p] = [links.push(s['sq_send'].at[p], s['sq_recv'].at[p, k], k, 'sq') for k in EVERYONE]
        self.h_yz[p] = links.push(s['h'].at[p, self.mine], s['h'].at[p, self.mine], YZ, 'h')
        links.copy(s['h'].at[p, self.mine], self.h_out.at[p], 'h')

    def normalize(self, p):
        s, links = self.s, self.links
        for c in self.sq[p]:
            c.wait_recv()
        total = s['sq_send'][p]
        for k in EVERYONE:
            total = total + s['sq_recv'][p, k]
        self.h_yz[p].wait_recv()
        h_t = s['h'][p].astype(F32)
        inv_rms = lax.rsqrt(total[:1] / self.model_dim + NORM_EPS)
        s['u'][p] = (h_t * inv_rms * s['gain'][...]).T.astype(BF16)
        shard = s['u'].shape[1] // 4
        u = jnp.concatenate([s['u'][p, pl.ds(pl.multiple_of(b * shard, shard), shard), :] for b in links.blocks], axis=0)
        s['u_rel'][p] = u
        if not self.wa_ready:
            self.wa.wait()
            self.wa_ready = True
        s['a_part'][p] = dot(u, s['wa'][...]).astype(BF16)
        self.a_core[p] = links.push(s['a_part'].at[p, pl.ds(0, 2 * shard)], s['a_core'].at[p], PARTNER, 'a_core')

    def spread(self, p):
        s = self.s
        u = s['u_rel'][p]
        gate, up = dot(u, s['even'][...]).astype(BF16), dot(u, s['odd'][...]).astype(BF16)
        shard = u.shape[0] // 4
        for k in range(4):
            s['u2'][p, 2 * k * shard:(2 * k + 1) * shard] = gate[k * shard:(k + 1) * shard]
            s['u2'][p, (2 * k + 1) * shard:(2 * k + 2) * shard] = up[k * shard:(k + 1) * shard]

    def attend_core(self, p):
        s = self.s
        half = s['a_core'].shape[1]
        self.a_core[p].wait_recv()
        s['a_sum'][p] = (s['a_part'][p, half:].astype(F32) + s['a_core'][p].astype(F32)).astype(BF16)
        shard, seqs = half // 2, s['a_got'].shape[2]
        y = self.links.y
        here, there = pl.multiple_of(y * seqs, seqs), pl.multiple_of((1 - y) * seqs, seqs)
        self.a_got[p] = [
            self.links.push(s['a_sum'].at[p, pl.ds(there, seqs)], s['a_got'].at[p, 2], ACROSS_YZ, 'a_got'),
            self.links.push(s['a_sum'].at[p, pl.ds(here, seqs)], s['a_got'].at[p, 0], ACROSS, 'a_got'),
            self.links.push(s['a_sum'].at[p, pl.ds(shard + there, seqs)], s['a_got'].at[p, 1], YZ, 'a_got')]

    def attend_ends(self, p):
        s, y = self.s, self.links.y
        shard, seqs = s['a_sum'].shape[1] // 2, s['a_got'].shape[2]
        for c in self.a_got[p]:
            c.wait_recv()
        own = s['a_sum'][p, pl.ds(shard + pl.multiple_of(y * seqs, seqs), seqs), :]
        s['a_full'][p, 0] = (own.astype(F32) + s['a_got'][p, 0].astype(F32)).astype(BF16)
        s['a_full'][p, 1] = (s['a_got'][p, 1].astype(F32) + s['a_got'][p, 2].astype(F32)).astype(BF16)
        for k, head in enumerate((y, 1 - y)):
            self.links.copy(s['a_full'].at[p, k], self.qkv_out.at[head, pl.ds(p * seqs, seqs)], 'qkv')

    def project(self, p, j):
        s = self.s
        if not self.wm_ready:
            self.wm.wait()
            self.wm_ready = True
        w = s['wm'][:, :, j * self.cols:(j + 1) * self.cols].reshape(2 * self.depth, self.cols)
        s['z_part'][p, j] = dot(s['u2'][p], w).astype(BF16)
        self.push_core(p, j)

    def split_weights(self):
        s, run = self.s, 128
        i = lax.broadcasted_iota(jnp.int32, (2 * run, 2 * run), 0)
        j = lax.broadcasted_iota(jnp.int32, (2 * run, 2 * run), 1)
        place = jnp.where(i < run, 2 * i, 2 * (i - run) + 1)
        order = jnp.where(j == place, jnp.ones((), F32), jnp.zeros((), F32)).astype(BF16)
        self.wm.wait()
        for c in range(self.chunks):
            cols = slice(c * self.cols, (c + 1) * self.cols)
            for e in range(self.depth // run):
                rows = slice(e * run, (e + 1) * run)
                w = dot(order, s['wm'][rows, :, cols].reshape(2 * run, self.cols)).astype(BF16)
                s['w_split'][0, rows, cols] = w[:run]
                s['w_split'][1, rows, cols] = w[run:]

    def project_all(self, j):
        s = self.s
        lanes = s['u'].shape[1]
        shard = lanes // 4
        u = s['u_rel'][...].reshape(PARTS * lanes, self.depth)
        cols = slice(j * self.cols, (j + 1) * self.cols)
        gate, up = dot(u, s['w_split'][0, :, cols]).astype(BF16), dot(u, s['w_split'][1, :, cols]).astype(BF16)
        for p in range(PARTS):
            for k in range(4):
                rows = slice(p * lanes + k * shard, p * lanes + (k + 1) * shard)
                s['z_part'][p, j, 2 * k * shard:(2 * k + 1) * shard] = gate[rows]
                s['z_part'][p, j, (2 * k + 1) * shard:(2 * k + 2) * shard] = up[rows]
            self.push_core(p, j)

    def push_core(self, p, j):
        s = self.s
        half = s['z_recv'].shape[2]
        self.z_core[p, j] = self.links.push(s['z_part'].at[p, j, pl.ds(0, half)], s['z_recv'].at[p, j], PARTNER, 'z')

    def combine(self, p, j):
        s, unit = self.s, p * self.chunks + j
        half = s['z_recv'].shape[2]
        shard2 = half // 2
        self.z_core[p, j].wait_recv()
        s['z_x'][unit] = (s['z_part'][p, j, half:half + shard2].astype(F32) + s['z_recv'][p, j, :shard2].astype(F32)).astype(BF16)
        if unit < EARLY:
            self.early[unit] = self.links.push(s['z_x'].at[unit], s['z_early'].at[unit], ACROSS, 'early')
        else:
            self.links.copy(s['z_x'].at[unit], self.zsend_out.at[unit - EARLY], 'z_x')
        s['z_mine'][unit] = (s['z_part'][p, j, half + shard2:].astype(F32) + s['z_recv'][p, j, shard2:].astype(F32)).astype(BF16)
        if unit >= EARLY:
            self.links.copy(s['z_mine'].at[unit], self.zmine_out.at[unit], 'z_mine')

    def finish(self):
        s = self.s
        for unit in range(EARLY):
            self.early[unit].wait_recv()
            s['z_mine'][unit] = (s['z_mine'][unit].astype(F32) + s['z_early'][unit].astype(F32)).astype(BF16)
            self.links.copy(s['z_mine'].at[unit], self.zmine_out.at[unit], 'z_mine')

    def sizes(self):
        s = self.s
        return ({'a_core': s['a_core'], 'a_got': s['a_got'], 'z': s['z_recv'], 'early': s['z_early'],
                 'sq': s['sq_recv'].at[:, pl.ds(0, len(EVERYONE))], 'h': s['h'].at[:, self.mine]},
                {'z_x': s['z_x'].at[pl.ds(EARLY, s['z_x'].shape[0] - EARLY)], 'z_mine': s['z_mine'], 'qkv': s['a_full'], 'h': s['h'].at[:, self.mine]})


class Back:
    def __init__(self, links, layer, h_hbm, o_hbm, zgot_hbm, zmine_hbm, wd_hbm, wo_hbm, s):
        self.links, self.s = links, s
        self.chunks, self.cols = s['m'].shape[1], s['m'].shape[3]
        units = PARTS * self.chunks
        self.z = []
        for first, last in ((0, 1), (1, self.chunks), (self.chunks, units)):
            run = pl.ds(first, last - first)
            self.z.append((first, links.copy(zmine_hbm.at[run], s['z_in'].at[run])))
            start = max(first, EARLY)
            if start < last:
                run = pl.ds(start - EARLY, last - start)
                self.z.append((start, links.copy(zgot_hbm.at[run], s['z_got'].at[run])))
            if first == 0:
                self.o_copy = links.copy(o_hbm, s['o_in'])
                self.h_copy = links.copy(h_hbm, s['h_in'])
        self.wd = links.copy(wd_hbm.at[layer], s['wd'])
        self.wo = links.copy(wo_hbm.at[layer], s['wo'])
        self.wo_ready, self.wd_ready = False, False
        self.across, self.partner, self.diag = {}, {}, {}
        self.o_across, self.o_partner, self.o_diag = {}, {}, {}
        self.up = {}

    def mix(self, p, j):
        s, unit = self.s, p * self.chunks + j
        while self.z and self.z[0][0] <= unit:
            self.z.pop(0)[1].wait()
        z = s['z_in'][unit].astype(F32)
        if unit >= EARLY:
            z = (z + s['z_got'][unit - EARLY].astype(F32)).astype(BF16).astype(F32)
        shard = z.shape[0] // 2
        gate, up = z[:shard], z[shard:]
        s['m'][p, j, OWN * shard:] = (gate * jax.nn.sigmoid(gate) * up).astype(BF16)

    def block(self, p, j, k):
        shard = self.s['m'].shape[2] // 4
        return self.s['m'].at[p, j, pl.ds(k * shard, shard)]

    def send(self, p, j):
        self.across[p, j] = self.links.push(self.block(p, j, OWN), self.block(p, j, ACROSS), ACROSS, 'm')

    def send_partner(self, p):
        m = self.s['m']
        shard = m.shape[2] // 4
        self.partner[p] = self.links.push(m.at[p, :, pl.ds(OWN * shard, shard)], m.at[p, :, pl.ds(PARTNER * shard, shard)], PARTNER, 'm')

    def forward(self, p, j):
        self.across[p, j].wait_recv()
        self.diag[p, j] = self.links.push(self.block(p, j, ACROSS), self.block(p, j, DIAG), PARTNER, 'm')

    def send_o_yz(self):
        y, s = self.links.y, self.s
        self.o_copy.wait()
        self.o_yz = self.links.push(s['o_in'].at[1 - y], s['o_yz'], YZ, 'o_yz')

    def o_block(self, p, k):
        shard = self.s['o'].shape[1] // 4
        return self.s['o'].at[p, pl.ds(k * shard, shard)]

    def send_o(self, p):
        y, s = self.links.y, self.s
        if p == 0:
            self.o_yz.wait_recv()
        shard = s['o'].shape[1] // 4
        seqs = shard // 2
        s['o'][p, pl.ds(OWN * shard + pl.multiple_of(y * seqs, seqs), seqs), :] = s['o_in'][y, p * seqs:(p + 1) * seqs]
        s['o'][p, pl.ds(OWN * shard + pl.multiple_of((1 - y) * seqs, seqs), seqs), :] = s['o_yz'][p * seqs:(p + 1) * seqs]
        self.o_across[p] = self.links.push(self.o_block(p, OWN), self.o_block(p, ACROSS), ACROSS, 'o')
        self.o_partner[p] = self.links.push(self.o_block(p, OWN), self.o_block(p, PARTNER), PARTNER, 'o')

    def forward_o(self, p):
        self.o_across[p].wait_recv()
        self.o_diag[p] = self.links.push(self.o_block(p, ACROSS), self.o_block(p, DIAG), PARTNER, 'o')

    def project_o(self, p):
        s = self.s
        self.o_partner[p].wait_recv()
        self.o_diag[p].wait_recv()
        if not self.wo_ready:
            self.wo.wait()
            self.wo_ready = True
        s['acc'][p] += dot(s['o'][p], s['wo'][...])

    def down(self, p, j):
        s = self.s
        if j == 0:
            self.partner[p].wait_recv()
        self.diag[p, j].wait_recv()
        if not self.wd_ready:
            self.wd.wait()
            self.wd_ready = True
        part = dot(s['m'][p, j], s['wd'][j * self.cols:(j + 1) * self.cols])
        if j == 0:
            s['acc'][p] = part
        else:
            s['acc'][p] += part

    def send_update(self, p):
        s, links = self.s, self.links
        shard = s['acc'].shape[1] // 4
        for k in range(4):
            s['update'][p, pl.ds(pl.multiple_of(links.blocks[k] * shard, shard), shard), :] = s['acc'][p, k * shard:(k + 1) * shard, :]
        s['up_part'][p] = s['update'][p].T.astype(BF16)
        part = s['up_recv'].shape[1]
        src = s['up_part'].at[p, pl.ds(pl.multiple_of((1 - links.y) * part, part), part)]
        self.up[p] = links.push(src, s['up_recv'].at[p], YZ, 'up')

    def new_h(self, p):
        s, links = self.s, self.links
        self.up[p].wait_recv()
        part = s['up_recv'].shape[1]
        own = s['up_part'][p, pl.ds(pl.multiple_of(links.y * part, part), part), :]
        return (s['h_in'][p].astype(F32) + (own.astype(F32) + s['up_recv'][p].astype(F32))).astype(BF16)

    def sizes(self):
        s = self.s
        sent = 3 * s['m'].shape[2] // 4
        return {'m': s['m'].at[:, :, pl.ds(0, sent)], 'o': s['o'].at[:, pl.ds(0, sent)], 'o_yz': s['o_yz'], 'up': s['up_recv']}

    def open(self):
        links, chunks = self.links, self.chunks
        self.mix(0, 0)
        links.meet()
        self.send(0, 0)
        self.send_o_yz()
        for j in range(1, chunks):
            self.mix(0, j)
            self.send(0, j)
            if j == 2:
                self.send_o(0)
        self.send_partner(0)
        for j in range(chunks):
            self.mix(1, j)
            self.send(1, j)
            if j == 1:
                self.send_o(1)
        self.send_partner(1)
        self.h_copy.wait()


def start_kernel(names, model_dim, h_hbm, gain_hbm, wa_hbm, wm_hbm, qkv_out, zsend_out, zmine_out, h_out, *scratch):
    s = dict(zip(names, scratch))
    links = Links(s['send'], s['recv'], s['local'], EVERYONE)
    h_copy = links.copy(h_hbm, s['h_in'])
    f = Front(links, 0, gain_hbm, wa_hbm, wm_hbm, model_dim, (qkv_out, zsend_out, zmine_out, h_out), s)
    rows = h_hbm.shape[1]
    lanes = rows // PARTS
    order = part_order(rows, False)
    h_copy.wait()
    own = dot(s['h_in'][...], order)
    for p in range(PARTS):
        f.squares(p, own[:, p * lanes:(p + 1) * lanes])
    f.constants()
    links.meet()
    for p in range(PARTS):
        f.send_h(p)
    f.split_weights()
    for p in range(PARTS):
        f.normalize(p)
    f.project_all(0)
    for p in range(PARTS):
        f.attend_core(p)
    for j in range(1, f.chunks):
        f.project_all(j)
        if j == f.chunks - 1:
            f.attend_ends(0)
        for p in range(PARTS):
            f.combine(p, j - 1)
    f.attend_ends(1)
    for p in range(PARTS):
        f.combine(p, f.chunks - 1)
    f.finish()
    links.drain(*f.sizes())


def middle_kernel(names, model_dim, h_hbm, o_hbm, gain_hbm, zmine_hbm, zgot_hbm, wd_hbm, wo_hbm, wa_hbm, wm_hbm, qkv_out, zsend_out,
                  zmine_out, h_out, *scratch):
    s = dict(zip(names, scratch))
    links = Links(s['send'], s['recv'], s['local'], EVERYONE)
    b = Back(links, 0, h_hbm, o_hbm, zgot_hbm, zmine_hbm, wd_hbm, wo_hbm, s)
    f = Front(links, 1, gain_hbm, wa_hbm, wm_hbm, model_dim, (qkv_out, zsend_out, zmine_out, h_out), s)
    b.open()
    f.constants()

    def pass_h(p):
        f.squares(p, b.new_h(p).astype(F32))
        f.send_h(p)

    first_part(b)
    second_part(b, lambda: pass_h(0))
    f.normalize(0)
    pass_h(1)
    f.spread(0)
    f.attend_core(0)
    f.project(0, 0)
    f.project(0, 1)
    f.project(0, 2)
    f.combine(0, 0)
    f.project(0, 3)
    f.combine(0, 1)
    f.project(0, 4)
    f.combine(0, 2)
    f.combine(0, 3)
    f.normalize(1)
    f.spread(1)
    f.project(1, 0)
    f.attend_core(1)
    f.combine(0, 4)
    f.attend_ends(0)
    f.project(1, 1)
    f.project(1, 2)
    f.combine(1, 0)
    f.project(1, 3)
    f.combine(1, 1)
    f.project(1, 4)
    f.combine(1, 2)
    f.combine(1, 3)
    f.attend_ends(1)
    f.combine(1, 4)
    f.finish()
    sent, stored = f.sizes()
    links.drain({**sent, **b.sizes()}, stored)


def first_part(b):
    for j in range(b.chunks):
        b.forward(0, j)
        if j == 2:
            b.forward_o(0)
        if j >= 1:
            b.down(0, j - 1)
    b.project_o(0)
    b.down(0, b.chunks - 1)
    b.send_update(0)
    b.forward(1, 0)


def second_part(b, when_updated):
    for j in range(1, b.chunks):
        b.forward(1, j)
        if j == 1:
            b.forward_o(1)
        b.down(1, j - 1)
        if j == 2:
            b.project_o(1)
        if j == b.chunks - 3:
            when_updated()
    b.down(1, b.chunks - 1)
    b.send_update(1)


def end_kernel(names, h_hbm, o_hbm, zmine_hbm, zgot_hbm, wd_hbm, wo_hbm, h_out, *scratch):
    s = dict(zip(names, scratch))
    links = Links(s['send'], s['recv'], s['local'], [PARTNER, ACROSS, YZ])
    b = Back(links, 1, h_hbm, o_hbm, zgot_hbm, zmine_hbm, wd_hbm, wo_hbm, s)
    b.open()
    first_part(b)
    h_new = []
    second_part(b, lambda: h_new.append(b.new_h(0)))
    order = part_order(h_out.shape[1], True)
    h_new.append(b.new_h(1))
    h_out[...] = dot(jnp.concatenate(h_new, axis=1), order).astype(BF16)
    links.drain(b.sizes(), {})


def attention_kernel(layer, per_step, len_hbm, qkv_hbm, k_hbm, v_hbm, *rest):
    k_out, v_out, o_hbm, kbuf, vbuf, q_scr, o_scr, qkv_ref, o_ref, len_ref, in_sem, out_sem, small_sem = rest[-13:]
    num_seqs, kv_heads, cache_len, head_dim = kbuf.shape
    slots = qkv_ref.shape[2] // head_dim
    rows = kv_heads * slots
    scale = head_dim ** -0.5

    def load(i):
        return (pltpu.make_async_copy(k_hbm.at[layer, i], kbuf.at[i], in_sem.at[0, i]),
                pltpu.make_async_copy(v_hbm.at[layer, i], vbuf.at[i], in_sem.at[1, i]))

    def store(i):
        return (pltpu.make_async_copy(kbuf.at[i], k_out.at[layer, i], out_sem.at[0, i]),
                pltpu.make_async_copy(vbuf.at[i], v_out.at[layer, i], out_sem.at[1, i]))

    qkv_copy = pltpu.make_async_copy(qkv_hbm, qkv_ref, small_sem.at[0])
    len_copy = pltpu.make_async_copy(len_hbm, len_ref, small_sem.at[1])
    qkv_copy.start()
    len_copy.start()

    @pl.loop(0, num_seqs)
    def _(i):
        for c in load(i):
            c.start()

    qkv_copy.wait()
    len_copy.wait()
    for head in range(kv_heads):
        for j in range(slots):
            q_scr[pl.ds(head * slots + j, num_seqs, stride=rows), :] = (
                qkv_ref[head, :, j * head_dim:(j + 1) * head_dim].astype(F32))

    tile_row = lax.broadcasted_iota(jnp.int32, (16, head_dim), 0)
    position = lax.broadcasted_iota(jnp.int32, (rows, cache_len), 1)

    @pl.loop(0, num_seqs // per_step)
    def _(step):
        group = [step * per_step + sub for sub in range(per_step)]
        for i in group:
            for c in load(i):
                c.wait()
            length = len_ref[i]
            base = pl.multiple_of((length // 16) * 16, 16)
            hit = tile_row == length - base
            for head in range(kv_heads):
                for buf, j in ((kbuf, slots - 2), (vbuf, slots - 1)):
                    new = q_scr[pl.ds(i * rows + head * slots + j, 1), :]
                    old = buf[i, head, pl.ds(base, 16), :].astype(F32)
                    buf[i, head, pl.ds(base, 16), :] = jnp.where(hit, new, old).astype(buf.dtype)
            for c in store(i):
                c.start()
        scores, probs = [], []
        for i in group:
            q = q_scr[pl.ds(pl.multiple_of(i * rows, rows), rows), :].astype(BF16)
            by_head = [lax.dot_general(q, kbuf[i, head], (((1,), (1,)), ((), ())), preferred_element_type=F32)
                       for head in range(kv_heads)]
            scores.append(jnp.concatenate([by_head[head][head * slots:(head + 1) * slots] for head in range(kv_heads)], axis=0))
        for i, score in zip(group, scores):
            score = jnp.where(position <= len_ref[i], score * scale, -1e30)
            e = jnp.exp(score - jnp.max(score, axis=1, keepdims=True))
            probs.append((e / jnp.sum(e, axis=1, keepdims=True)).astype(BF16))
        for i, p in zip(group, probs):
            by_head = [dot(p, vbuf[i, head]) for head in range(kv_heads)]
            o_scr[pl.ds(pl.multiple_of(i * rows, rows), rows), :] = jnp.concatenate(
                [by_head[head][head * slots:(head + 1) * slots] for head in range(kv_heads)], axis=0)

    for head in range(kv_heads):
        for j in range(slots - 2):
            o_ref[head, :, j * head_dim:(j + 1) * head_dim] = (
                o_scr[pl.ds(head * slots + j, num_seqs, stride=rows), :].astype(o_ref.dtype))
    o_copy = pltpu.make_async_copy(o_ref, o_hbm, small_sem.at[2])
    o_copy.start()

    @pl.loop(0, num_seqs)
    def _(i):
        for c in store(i):
            c.wait()

    o_copy.wait()


VMEM = pl.BlockSpec(memory_space=pltpu.VMEM)
HBM = pl.BlockSpec(memory_space=pltpu.HBM)


def attention(layer, lengths, qkv, k_cache, v_cache, outs):
    layers, num_seqs, kv_heads, cache_len, head_dim = k_cache.shape
    slots = qkv.shape[2] // head_dim
    rows = kv_heads * slots
    return pl.pallas_call(
        functools.partial(attention_kernel, layer, 2),
        out_shape=(jax.ShapeDtypeStruct(k_cache.shape, k_cache.dtype), jax.ShapeDtypeStruct(v_cache.shape, v_cache.dtype),
                   jax.ShapeDtypeStruct((kv_heads, num_seqs, (slots - 2) * head_dim), BF16)),
        in_specs=[HBM] * (4 + len(outs)),
        out_specs=(HBM, HBM, HBM),
        scratch_shapes=[pltpu.VMEM((num_seqs, kv_heads, cache_len, head_dim), BF16)] * 2
        + [pltpu.VMEM((num_seqs * rows, head_dim), F32)] * 2 + [
            pltpu.VMEM(qkv.shape, BF16), pltpu.VMEM((kv_heads, num_seqs, (slots - 2) * head_dim), BF16),
            pltpu.SMEM((num_seqs,), jnp.int32)]
        + [pltpu.SemaphoreType.DMA((2, num_seqs))] * 2 + [pltpu.SemaphoreType.DMA((3,))],
        input_output_aliases={4: 0, 5: 1} if outs else {},
        compiler_params=pltpu.CompilerParams(vmem_limit_bytes=VMEM_LIMIT),
        cost_estimate=pl.CostEstimate(flops=10 ** 10, bytes_accessed=8 * num_seqs * kv_heads * cache_len * head_dim, transcendentals=0),
        name=f'attention_{layer}',
    )(lengths, qkv, k_cache, v_cache, *outs)


def solution(mesh):
    seq_axes = ('rep', 'x', 'yz')
    hidden_spec = P('rep', ('x', 'yz'))
    cache_spec = P(None, seq_axes, None, None, None)
    in_specs = (hidden_spec, P(None, 'x'), P(None, 'x', 'yz'), P(None, 'x', None, 'yz'), P(None, 'yz', 'x'), P(None, 'yz', 'x'), cache_spec, cache_spec, P(seq_axes))
    out_specs = (hidden_spec, cache_spec, cache_spec)
    swap = [(0, 2), (2, 0), (1, 3), (3, 1)]

    def device_step(hidden, norm_gain, w_attn, w_mlp, w_out, w_down, k_cache, v_cache, lengths):
        rows, part = hidden.shape
        depth, attn_cols = w_attn.shape[1:]
        model_dim = depth * mesh.shape['x']
        mlp_cols = w_mlp.shape[3]
        out_depth = w_out.shape[1]
        cols = mlp_cols // CHUNKS
        units = CHUNKS * PARTS
        lanes = rows // PARTS
        half, shard = lanes // 2, lanes // 4
        seqs = shard // 2
        num_seqs = PARTS * seqs

        def semaphores(groups, remote, local):
            return {'send': pltpu.SemaphoreType.DMA((groups,)), 'recv': pltpu.SemaphoreType.DMA((remote,)),
                    'local': pltpu.SemaphoreType.DMA((local,))}

        front_scratch = {
            'sq_send': pltpu.VMEM((PARTS, 8, lanes), F32), 'sq_recv': pltpu.VMEM((PARTS, 8, 8, lanes), F32),
            'h': pltpu.VMEM((PARTS, depth, lanes), BF16), 'gain_in': pltpu.VMEM(norm_gain.shape, BF16), 'gain': pltpu.VMEM((depth, lanes), F32),
            'u': pltpu.VMEM((PARTS, lanes, depth), BF16), 'u_rel': pltpu.VMEM((PARTS, lanes, depth), BF16),
            'wa': pltpu.VMEM((depth, attn_cols), BF16), 'wm': pltpu.VMEM((depth, 2, mlp_cols), BF16),
            'a_part': pltpu.VMEM((PARTS, lanes, attn_cols), BF16), 'a_core': pltpu.VMEM((PARTS, half, attn_cols), BF16),
            'a_sum': pltpu.VMEM((PARTS, half, attn_cols), BF16), 'a_got': pltpu.VMEM((PARTS, 3, seqs, attn_cols), BF16),
            'a_full': pltpu.VMEM((PARTS, 2, seqs, attn_cols), BF16),
            'z_part': pltpu.VMEM((PARTS, CHUNKS, 2 * lanes, cols), BF16),
            'z_recv': pltpu.VMEM((PARTS, CHUNKS, lanes, cols), BF16), 'z_x': pltpu.VMEM((units, half, cols), BF16),
            'z_mine': pltpu.VMEM((units, half, cols), BF16), 'z_early': pltpu.VMEM((EARLY, half, cols), BF16),
        }

        split_scratch = {'w_split': pltpu.VMEM((2, depth, mlp_cols), BF16)}
        spread_scratch = {
            'even': pltpu.VMEM((depth, 2 * depth), BF16), 'odd': pltpu.VMEM((depth, 2 * depth), BF16),
            'u2': pltpu.VMEM((PARTS, 2 * lanes, 2 * depth), BF16),
        }
        back_scratch = {
            'o_yz': pltpu.VMEM((num_seqs, out_depth), BF16), 'o': pltpu.VMEM((PARTS, lanes, out_depth), BF16),
            'm': pltpu.VMEM((PARTS, CHUNKS, lanes, cols), BF16), 'z_in': pltpu.VMEM((units, half, cols), BF16),
            'z_got': pltpu.VMEM((units - EARLY, half, cols), BF16), 'o_in': pltpu.VMEM((2, num_seqs, out_depth), BF16),
            'h_in': pltpu.VMEM((PARTS, part, lanes), BF16),
            'wd': pltpu.VMEM((mlp_cols, depth), BF16), 'wo': pltpu.VMEM((out_depth, depth), BF16),
            'acc': pltpu.VMEM((PARTS, lanes, depth), F32), 'update': pltpu.VMEM((PARTS, lanes, depth), F32),
            'up_part': pltpu.VMEM((PARTS, depth, lanes), BF16), 'up_recv': pltpu.VMEM((PARTS, part, lanes), BF16),
        }

        front_shapes = (
            jax.ShapeDtypeStruct((2, num_seqs, attn_cols), BF16), jax.ShapeDtypeStruct((units - EARLY, half, cols), BF16),
            jax.ShapeDtypeStruct((units, half, cols), BF16), jax.ShapeDtypeStruct((PARTS, part, lanes), BF16))
        front_specs = (HBM,) * 4

        def call(kernel, name, collective_id, scratch, in_specs, out_shape, out_specs, *args):
            return pl.pallas_call(
                functools.partial(kernel, tuple(scratch)), out_shape=out_shape, in_specs=list(in_specs), out_specs=out_specs,
                scratch_shapes=list(scratch.values()), name=name,
                compiler_params=pltpu.CompilerParams(collective_id=collective_id, has_side_effects=True, vmem_limit_bytes=END_VMEM_LIMIT if kernel is end_kernel else VMEM_LIMIT),
            )(*args)

        def start(names, *refs):
            start_kernel(names, model_dim, *refs)

        def middle(names, *refs):
            middle_kernel(names, model_dim, *refs)

        qkv, zsend, zmine, h_block = call(
            start, 'start', 0, {**semaphores(6, 35, 8), **front_scratch, **split_scratch, 'h_in': pltpu.VMEM((part, rows), BF16)}, (HBM,) * 4,
            front_shapes, front_specs, hidden.T, norm_gain, w_attn, w_mlp)
        zgot = lax.ppermute(zsend, 'x', swap)
        k_new, v_new, o = attention(0, lengths, qkv, k_cache, v_cache, ())
        qkv, zsend, zmine, h_block = call(
            middle, 'middle', 1, {**semaphores(10, 66, 16), **front_scratch, **spread_scratch, **back_scratch}, (HBM,) * 9,
            front_shapes, front_specs, h_block, o, norm_gain, zmine, zgot, w_down, w_out, w_attn, w_mlp)
        zgot = lax.ppermute(zsend, 'x', swap)
        k_new, v_new, o = attention(1, lengths, qkv, k_cache, v_cache, (k_new, v_new))
        h_out = call(
            end_kernel, 'end', 2, {**semaphores(4, 31, 9), **back_scratch}, (HBM,) * 6,
            jax.ShapeDtypeStruct((part, rows), BF16), VMEM, h_block, o, zmine, zgot, w_down, w_out)
        return h_out.T, k_new, v_new

    return jax.shard_map(device_step, mesh=mesh, in_specs=in_specs, out_specs=out_specs, check_vma=False)
```

```python
import functools

import jax
import jax.numpy as jnp
from jax import lax
from jax.experimental import pallas as pl
from jax.experimental.pallas import tpu as pltpu
from jax.sharding import PartitionSpec as P

NORM_EPS = 1e-5
MESH = pl.DeviceIdType.MESH
BF16 = jnp.bfloat16
F32 = jnp.float32

SQ_ROWS = 1
PER_COPY = 4
PER_STEP = 2
CHUNKS = 5
EARLY = (1, 2)
END_VMEM_LIMIT = 56393728
VMEM_LIMIT = 67043328


def dot(a, b):
    return jnp.dot(a, b, preferred_element_type=F32)


class Links:
    def __init__(self, send_sems, recv_sems, local_sems, peers):
        self.send_sems, self.recv_sems, self.local_sems = send_sems, recv_sems, local_sems
        self.groups, self.used, self.local_groups, self.local_used = {}, 0, {}, 0
        x, y = lax.axis_index('x'), lax.axis_index('yz')
        self.x, self.y = x, y
        core = lax.rem(x, 2)
        self.along_x = (3 - x, x + 1 - 2 * core, lax.rem(x + 2, 4))
        self.blocks = self.along_x + (x,)
        self.targets = tuple({'x': p, 'yz': y} for p in self.blocks) + ({'x': x, 'yz': 1 - y},) + tuple(
            {'x': p, 'yz': 1 - y} for p in self.along_x)
        self.peers = peers
        self.barrier = pltpu.get_barrier_semaphore()
        for k in self.peers:
            pl.semaphore_signal(self.barrier, inc=1, device_id=self.targets[k], device_id_type=MESH)

    def meet(self):
        pl.semaphore_wait(self.barrier, len(self.peers))

    def push(self, src, dst, to, group):
        k = self.used
        self.used += 1
        g = self.groups.setdefault(group, len(self.groups))
        copy = pltpu.make_async_remote_copy(
            src_ref=src, dst_ref=dst, send_sem=self.send_sems.at[g], recv_sem=self.recv_sems.at[k],
            device_id=self.targets[to], device_id_type=MESH)
        copy.start()
        return copy

    def copy(self, src, dst, group=None):
        if group is None or group not in self.local_groups:
            k = self.local_used
            self.local_used += 1
            if group is not None:
                self.local_groups[group] = k
        else:
            k = self.local_groups[group]
        copy = pltpu.make_async_copy(src, dst, self.local_sems.at[k])
        copy.start()
        return copy

    def drain(self, sent, stored):
        for group, g in self.groups.items():
            pltpu.make_async_copy(sent[group], sent[group], self.send_sems.at[g]).wait()
        for group, k in self.local_groups.items():
            pltpu.make_async_copy(stored[group], stored[group], self.local_sems.at[k]).wait()


DIAG, PARTNER, ACROSS, OWN, YZ, ACROSS_YZ = 0, 1, 2, 3, 4, 7
EVERYONE = [k for k in range(8) if k != OWN]
PARTS = 2


def part_order(rows, inverse):
    i = lax.broadcasted_iota(jnp.int32, (rows, rows), 0)
    j = lax.broadcasted_iota(jnp.int32, (rows, rows), 1)
    src, dst = (j, i) if inverse else (i, j)
    run = rows // (8 * PARTS)
    piece = src // run
    place = lax.rem(piece, PARTS) * (8 * run) + (piece // PARTS) * run + lax.rem(src, run)
    return jnp.where(dst == place, jnp.ones((), F32), jnp.zeros((), F32)).astype(BF16)


class Front:
    def __init__(self, links, layer, gain_hbm, wa_hbm, wm_hbm, model_dim, outs, s):
        self.links, self.s, self.layer, self.model_dim = links, s, layer, model_dim
        self.kept = EARLY[layer]
        self.gain_copy = links.copy(gain_hbm, s['gain_in'])
        self.qkv_out, self.zsend_out, self.zmine_out, self.h_out = outs
        self.chunks, self.cols = s['z_recv'].shape[1], s['z_recv'].shape[3]
        self.depth = s['wa'].shape[0]
        self.wa = links.copy(wa_hbm.at[layer], s['wa'])
        self.wm = links.copy(wm_hbm.at[layer], s['wm'])
        self.wa_ready = False
        part = self.depth // 2
        self.mine = pl.ds(pl.multiple_of(links.y * part, part), part)
        self.h_yz = {}
        self.a_core, self.a_got, self.z_core, self.early = {}, {}, {}, {}
        self.sq = {}

    def constants(self):
        lanes = self.s['u'].shape[1]
        self.gain_copy.wait()
        gain = jnp.broadcast_to(self.s['gain_in'][self.layer:self.layer + 1, :].astype(F32), (lanes, self.depth)).T
        self.s['gain'][...] = gain

    def squares(self, p, h_t):
        s = self.s
        s['h'][p, self.mine, :] = h_t.astype(BF16)
        s['sq_send'][p] = jnp.broadcast_to(jnp.sum(h_t * h_t, axis=0, keepdims=True), s['sq_send'].shape[1:])

    def send_h(self, p):
        s, links = self.s, self.links
        self.sq[p] = [links.push(s['sq_send'].at[p], s['sq_recv'].at[p, k], k, 'sq') for k in EVERYONE]
        self.h_yz[p] = links.push(s['h'].at[p, self.mine], s['h'].at[p, self.mine], YZ, 'h')
        links.copy(s['h'].at[p, self.mine], self.h_out.at[p], 'h')

    def normalize(self, p):
        s, links = self.s, self.links
        for c in self.sq[p]:
            c.wait_recv()
        total = s['sq_send'][p]
        for k in EVERYONE:
            total = total + s['sq_recv'][p, k]
        self.h_yz[p].wait_recv()
        h_t = s['h'][p].astype(F32)
        inv_rms = lax.rsqrt(total[:1] / self.model_dim + NORM_EPS)
        s['u'][p] = (h_t * inv_rms * s['gain'][...]).T.astype(BF16)
        shard = s['u'].shape[1] // 4
        u = jnp.concatenate([s['u'][p, pl.ds(pl.multiple_of(b * shard, shard), shard), :] for b in links.blocks], axis=0)
        s['u_rel'][p] = u
        if not self.wa_ready:
            self.wa.wait()
            self.wa_ready = True
        s['a_part'][p] = dot(u, s['wa'][...]).astype(BF16)
        self.a_core[p] = links.push(s['a_part'].at[p, pl.ds(0, 2 * shard)], s['a_core'].at[p], PARTNER, 'a_core')

    def attend_core(self, p):
        s = self.s
        half = s['a_core'].shape[1]
        self.a_core[p].wait_recv()
        s['a_sum'][p] = (s['a_part'][p, half:].astype(F32) + s['a_core'][p].astype(F32)).astype(BF16)
        shard, seqs = half // 2, s['a_got'].shape[2]
        y = self.links.y
        here, there = pl.multiple_of(y * seqs, seqs), pl.multiple_of((1 - y) * seqs, seqs)
        self.a_got[p] = [
            self.links.push(s['a_sum'].at[p, pl.ds(there, seqs)], s['a_got'].at[p, 2], ACROSS_YZ, 'a_got'),
            self.links.push(s['a_sum'].at[p, pl.ds(here, seqs)], s['a_got'].at[p, 0], ACROSS, 'a_got'),
            self.links.push(s['a_sum'].at[p, pl.ds(shard + there, seqs)], s['a_got'].at[p, 1], YZ, 'a_got')]

    def attend_ends(self, p):
        s, y = self.s, self.links.y
        shard, seqs = s['a_sum'].shape[1] // 2, s['a_got'].shape[2]
        for c in self.a_got[p]:
            c.wait_recv()
        own = s['a_sum'][p, pl.ds(shard + pl.multiple_of(y * seqs, seqs), seqs), :]
        s['a_full'][p, 0] = (own.astype(F32) + s['a_got'][p, 0].astype(F32)).astype(BF16)
        s['a_full'][p, 1] = (s['a_got'][p, 1].astype(F32) + s['a_got'][p, 2].astype(F32)).astype(BF16)
        for k, head in enumerate((y, 1 - y)):
            self.links.copy(s['a_full'].at[p, k], self.qkv_out.at[head, pl.ds(p * seqs, seqs)], 'qkv')

    def split_weights(self, c):
        s, run = self.s, 128
        i = lax.broadcasted_iota(jnp.int32, (2 * run, 2 * run), 0)
        j = lax.broadcasted_iota(jnp.int32, (2 * run, 2 * run), 1)
        place = jnp.where(i < run, 2 * i, 2 * (i - run) + 1)
        order = jnp.where(j == place, jnp.ones((), F32), jnp.zeros((), F32)).astype(BF16)
        if c == 0:
            self.wm.wait()
        cols = slice(c * self.cols, (c + 1) * self.cols)
        for e in range(self.depth // run):
            rows = slice(e * run, (e + 1) * run)
            w = dot(order, s['wm'][rows, :, cols].reshape(2 * run, self.cols)).astype(BF16)
            s['w_split'][0, rows, cols] = w[:run]
            s['w_split'][1, rows, cols] = w[run:]

    def project(self, parts, j):
        s = self.s
        lanes = s['u'].shape[1]
        shard = lanes // 4
        u = jnp.concatenate([s['u_rel'][p] for p in parts], axis=0)
        cols = slice(j * self.cols, (j + 1) * self.cols)
        gate, up = dot(u, s['w_split'][0, :, cols]).astype(BF16), dot(u, s['w_split'][1, :, cols]).astype(BF16)
        for n, p in enumerate(parts):
            for k in range(4):
                rows = slice(n * lanes + k * shard, n * lanes + (k + 1) * shard)
                s['z_part'][p, j, 2 * k * shard:(2 * k + 1) * shard] = gate[rows]
                s['z_part'][p, j, (2 * k + 1) * shard:(2 * k + 2) * shard] = up[rows]
            self.push_core(p, j)

    def push_core(self, p, j):
        s = self.s
        half = s['z_recv'].shape[2]
        self.z_core[p, j] = self.links.push(s['z_part'].at[p, j, pl.ds(0, half)], s['z_recv'].at[p, j], PARTNER, 'z')

    def combine(self, p, j):
        s, unit = self.s, p * self.chunks + j
        half = s['z_recv'].shape[2]
        shard2 = half // 2
        self.z_core[p, j].wait_recv()
        s['z_x'][unit] = (s['z_part'][p, j, half:half + shard2].astype(F32) + s['z_recv'][p, j, :shard2].astype(F32)).astype(BF16)
        if unit < self.kept:
            self.early[unit] = self.links.push(s['z_x'].at[unit], s['z_early'].at[unit], ACROSS, 'early')
        else:
            self.links.copy(s['z_x'].at[unit], self.zsend_out.at[unit - self.kept], 'z_x')
        s['z_mine'][unit] = (s['z_part'][p, j, half + shard2:].astype(F32) + s['z_recv'][p, j, shard2:].astype(F32)).astype(BF16)
        if unit >= self.kept:
            self.links.copy(s['z_mine'].at[unit], self.zmine_out.at[unit], 'z_mine')

    def finish(self):
        s = self.s
        for unit in range(self.kept):
            self.early[unit].wait_recv()
            s['z_mine'][unit] = (s['z_mine'][unit].astype(F32) + s['z_early'][unit].astype(F32)).astype(BF16)
            self.links.copy(s['z_mine'].at[unit], self.zmine_out.at[unit], 'z_mine')

    def sizes(self):
        s = self.s
        return ({'a_core': s['a_core'], 'a_got': s['a_got'], 'z': s['z_recv'], 'early': s['z_early'],
                 'sq': s['sq_recv'].at[:, pl.ds(0, len(EVERYONE))], 'h': s['h'].at[:, self.mine]},
                {'z_x': s['z_x'].at[pl.ds(self.kept, s['z_x'].shape[0] - self.kept)], 'z_mine': s['z_mine'], 'qkv': s['a_full'], 'h': s['h'].at[:, self.mine]})


class Back:
    def __init__(self, links, layer, h_hbm, o_hbm, zgot_hbm, zmine_hbm, wd_hbm, wo_hbm, s):
        self.links, self.s = links, s
        self.kept = EARLY[layer]
        self.chunks, self.cols = s['m'].shape[1], s['m'].shape[3]
        units = PARTS * self.chunks
        self.z = []
        for first, last in ((0, 1), (1, self.chunks), (self.chunks, units)):
            run = pl.ds(first, last - first)
            self.z.append((first, links.copy(zmine_hbm.at[run], s['z_in'].at[run])))
            start = max(first, self.kept)
            if start < last:
                run = pl.ds(start - self.kept, last - start)
                self.z.append((start, links.copy(zgot_hbm.at[run], s['z_got'].at[run])))
            if first == 0:
                self.o_copy = links.copy(o_hbm, s['o_in'])
                self.h_copy = links.copy(h_hbm, s['h_in'])
        self.wd = links.copy(wd_hbm.at[layer], s['wd'])
        self.wo = links.copy(wo_hbm.at[layer], s['wo'])
        self.wo_ready, self.wd_ready = False, False
        self.across, self.partner, self.diag = {}, {}, {}
        self.o_across, self.o_partner, self.o_diag = {}, {}, {}
        self.up = {}

    def mix(self, p, j):
        s, unit = self.s, p * self.chunks + j
        while self.z and self.z[0][0] <= unit:
            self.z.pop(0)[1].wait()
        z = s['z_in'][unit].astype(F32)
        if unit >= self.kept:
            z = (z + s['z_got'][unit - self.kept].astype(F32)).astype(BF16).astype(F32)
        shard = z.shape[0] // 2
        gate, up = z[:shard], z[shard:]
        s['m'][p, j, OWN * shard:] = (gate * jax.nn.sigmoid(gate) * up).astype(BF16)

    def block(self, p, j, k):
        shard = self.s['m'].shape[2] // 4
        return self.s['m'].at[p, j, pl.ds(k * shard, shard)]

    def send(self, p, j):
        self.across[p, j] = self.links.push(self.block(p, j, OWN), self.block(p, j, ACROSS), ACROSS, 'm')

    def send_partner(self, p):
        m = self.s['m']
        shard = m.shape[2] // 4
        self.partner[p] = self.links.push(m.at[p, :, pl.ds(OWN * shard, shard)], m.at[p, :, pl.ds(PARTNER * shard, shard)], PARTNER, 'm')

    def forward(self, p, j):
        self.across[p, j].wait_recv()
        self.diag[p, j] = self.links.push(self.block(p, j, ACROSS), self.block(p, j, DIAG), PARTNER, 'm')

    def send_o_yz(self):
        y, s = self.links.y, self.s
        self.o_copy.wait()
        self.o_yz = self.links.push(s['o_in'].at[1 - y], s['o_yz'], YZ, 'o_yz')

    def o_block(self, p, k):
        shard = self.s['o'].shape[1] // 4
        return self.s['o'].at[p, pl.ds(k * shard, shard)]

    def send_o(self, p):
        y, s = self.links.y, self.s
        if p == 0:
            self.o_yz.wait_recv()
        shard = s['o'].shape[1] // 4
        seqs = shard // 2
        s['o'][p, pl.ds(OWN * shard + pl.multiple_of(y * seqs, seqs), seqs), :] = s['o_in'][y, p * seqs:(p + 1) * seqs]
        s['o'][p, pl.ds(OWN * shard + pl.multiple_of((1 - y) * seqs, seqs), seqs), :] = s['o_yz'][p * seqs:(p + 1) * seqs]
        self.o_across[p] = self.links.push(self.o_block(p, OWN), self.o_block(p, ACROSS), ACROSS, 'o')
        self.o_partner[p] = self.links.push(self.o_block(p, OWN), self.o_block(p, PARTNER), PARTNER, 'o')

    def forward_o(self, p):
        self.o_across[p].wait_recv()
        self.o_diag[p] = self.links.push(self.o_block(p, ACROSS), self.o_block(p, DIAG), PARTNER, 'o')

    def project_o(self, p):
        s = self.s
        self.o_partner[p].wait_recv()
        self.o_diag[p].wait_recv()
        if not self.wo_ready:
            self.wo.wait()
            self.wo_ready = True
        s['acc'][p] += dot(s['o'][p], s['wo'][...])

    def down(self, p, j):
        s = self.s
        if j == 0:
            self.partner[p].wait_recv()
        self.diag[p, j].wait_recv()
        if not self.wd_ready:
            self.wd.wait()
            self.wd_ready = True
        part = dot(s['m'][p, j], s['wd'][j * self.cols:(j + 1) * self.cols])
        if j == 0:
            s['acc'][p] = part
        else:
            s['acc'][p] += part

    def send_update(self, p):
        s, links = self.s, self.links
        shard = s['acc'].shape[1] // 4
        for k in range(4):
            s['update'][p, pl.ds(pl.multiple_of(links.blocks[k] * shard, shard), shard), :] = s['acc'][p, k * shard:(k + 1) * shard, :]
        s['up_part'][p] = s['update'][p].T.astype(BF16)
        part = s['up_recv'].shape[1]
        src = s['up_part'].at[p, pl.ds(pl.multiple_of((1 - links.y) * part, part), part)]
        self.up[p] = links.push(src, s['up_recv'].at[p], YZ, 'up')

    def new_h(self, p):
        s, links = self.s, self.links
        self.up[p].wait_recv()
        part = s['up_recv'].shape[1]
        own = s['up_part'][p, pl.ds(pl.multiple_of(links.y * part, part), part), :]
        return (s['h_in'][p].astype(F32) + (own.astype(F32) + s['up_recv'][p].astype(F32))).astype(BF16)

    def sizes(self):
        s = self.s
        sent = 3 * s['m'].shape[2] // 4
        return {'m': s['m'].at[:, :, pl.ds(0, sent)], 'o': s['o'].at[:, pl.ds(0, sent)], 'o_yz': s['o_yz'], 'up': s['up_recv']}

    def open(self):
        links, chunks = self.links, self.chunks
        self.mix(0, 0)
        links.meet()
        self.send(0, 0)
        self.send_o_yz()
        for j in range(1, chunks):
            self.mix(0, j)
            self.send(0, j)
            if j == 2:
                self.send_o(0)
        self.send_partner(0)
        for j in range(chunks):
            self.mix(1, j)
            self.send(1, j)
            if j == 1:
                self.send_o(1)
        self.send_partner(1)
        self.h_copy.wait()


def start_kernel(names, model_dim, h_hbm, gain_hbm, wa_hbm, wm_hbm, qkv_out, zsend_out, zmine_out, h_out, *scratch):
    s = dict(zip(names, scratch))
    links = Links(s['send'], s['recv'], s['local'], EVERYONE)
    h_copy = links.copy(h_hbm, s['h_in'])
    f = Front(links, 0, gain_hbm, wa_hbm, wm_hbm, model_dim, (qkv_out, zsend_out, zmine_out, h_out), s)
    rows = h_hbm.shape[1]
    lanes = rows // PARTS
    order = part_order(rows, False)
    h_copy.wait()
    own = dot(s['h_in'][...], order)
    for p in range(PARTS):
        f.squares(p, own[:, p * lanes:(p + 1) * lanes])
    f.constants()
    links.meet()
    for p in range(PARTS):
        f.send_h(p)
    for j in range(f.chunks):
        f.split_weights(j)
    for p in range(PARTS):
        f.normalize(p)
    f.project(range(PARTS), 0)
    for p in range(PARTS):
        f.attend_core(p)
    for j in range(1, f.chunks):
        f.project(range(PARTS), j)
        if j == f.chunks - 1:
            f.attend_ends(0)
        for p in range(PARTS):
            f.combine(p, j - 1)
    f.attend_ends(1)
    for p in range(PARTS):
        f.combine(p, f.chunks - 1)
    f.finish()
    links.drain(*f.sizes())


def middle_kernel(names, model_dim, h_hbm, o_hbm, gain_hbm, zmine_hbm, zgot_hbm, wd_hbm, wo_hbm, wa_hbm, wm_hbm, qkv_out, zsend_out,
                  zmine_out, h_out, *scratch):
    s = dict(zip(names, scratch))
    links = Links(s['send'], s['recv'], s['local'], EVERYONE)
    b = Back(links, 0, h_hbm, o_hbm, zgot_hbm, zmine_hbm, wd_hbm, wo_hbm, s)
    f = Front(links, 1, gain_hbm, wa_hbm, wm_hbm, model_dim, (qkv_out, zsend_out, zmine_out, h_out), s)
    b.open()
    f.constants()

    def pass_h(p):
        f.squares(p, b.new_h(p).astype(F32))
        f.send_h(p)

    first_part(b, f.split_weights)
    second_part(b, lambda: pass_h(0))
    f.normalize(0)
    f.project([0], 0)
    f.attend_core(0)
    pass_h(1)
    f.project([0], 1)
    f.project([0], 2)
    f.combine(0, 0)
    f.project([0], 3)
    f.combine(0, 1)
    f.project([0], 4)
    f.combine(0, 2)
    f.combine(0, 3)
    f.normalize(1)
    f.project([1], 0)
    f.combine(0, 4)
    f.project([1], 1)
    f.attend_core(1)
    f.attend_ends(0)
    f.project([1], 2)
    f.combine(1, 0)
    f.project([1], 3)
    f.combine(1, 1)
    f.project([1], 4)
    f.combine(1, 2)
    f.combine(1, 3)
    f.attend_ends(1)
    f.combine(1, 4)
    f.finish()
    sent, stored = f.sizes()
    links.drain({**sent, **b.sizes()}, stored)


def first_part(b, filler):
    for j in range(b.chunks):
        b.forward(0, j)
        if filler is not None:
            filler(j)
        if j == 2:
            b.forward_o(0)
        if j >= 1:
            b.down(0, j - 1)
    b.project_o(0)
    b.down(0, b.chunks - 1)
    b.send_update(0)
    b.forward(1, 0)


def second_part(b, when_updated):
    for j in range(1, b.chunks):
        b.forward(1, j)
        if j == 1:
            b.forward_o(1)
        b.down(1, j - 1)
        if j == 2:
            b.project_o(1)
        if j == b.chunks - 3:
            when_updated()
    b.down(1, b.chunks - 1)
    b.send_update(1)


def end_kernel(names, h_hbm, o_hbm, zmine_hbm, zgot_hbm, wd_hbm, wo_hbm, h_out, *scratch):
    s = dict(zip(names, scratch))
    links = Links(s['send'], s['recv'], s['local'], [PARTNER, ACROSS, YZ])
    b = Back(links, 1, h_hbm, o_hbm, zgot_hbm, zmine_hbm, wd_hbm, wo_hbm, s)
    b.open()
    first_part(b, None)
    h_new = []
    second_part(b, lambda: h_new.append(b.new_h(0)))
    order = part_order(h_out.shape[1], True)
    h_new.append(b.new_h(1))
    h_out[...] = dot(jnp.concatenate(h_new, axis=1), order).astype(BF16)
    links.drain(b.sizes(), {})


def attention_kernel(layer, per_copy, per_step, len_hbm, qkv_hbm, k_hbm, v_hbm, *rest):
    k_out, v_out, o_hbm, kbuf, vbuf, q_scr, o_scr, qkv_ref, o_ref, len_ref, in_sem, out_sem, small_sem = rest[-13:]
    num_seqs, kv_heads, cache_len, head_dim = kbuf.shape
    slots = qkv_ref.shape[2] // head_dim
    rows = kv_heads * slots
    scale = head_dim ** -0.5

    def load(n):
        run = pl.ds(n * per_copy, per_copy)
        return (pltpu.make_async_copy(k_hbm.at[layer, run], kbuf.at[run], in_sem.at[0, n]),
                pltpu.make_async_copy(v_hbm.at[layer, run], vbuf.at[run], in_sem.at[1, n]))

    def store(n):
        run = pl.ds(n * per_copy, per_copy)
        return (pltpu.make_async_copy(kbuf.at[run], k_out.at[layer, run], out_sem.at[0, n]),
                pltpu.make_async_copy(vbuf.at[run], v_out.at[layer, run], out_sem.at[1, n]))

    qkv_copy = pltpu.make_async_copy(qkv_hbm, qkv_ref, small_sem.at[0])
    len_copy = pltpu.make_async_copy(len_hbm, len_ref, small_sem.at[1])
    qkv_copy.start()
    len_copy.start()

    @pl.loop(0, num_seqs // per_copy)
    def _(n):
        for c in load(n):
            c.start()

    qkv_copy.wait()
    len_copy.wait()
    for head in range(kv_heads):
        for j in range(slots):
            q_scr[pl.ds(head * slots + j, num_seqs, stride=rows), :] = (
                qkv_ref[head, :, j * head_dim:(j + 1) * head_dim].astype(F32))

    tile_row = lax.broadcasted_iota(jnp.int32, (16, head_dim), 0)
    position = lax.broadcasted_iota(jnp.int32, (rows, cache_len), 1)

    def patch(n):
        for c in load(n):
            c.wait()
        for sub in range(per_copy):
            i = n * per_copy + sub
            length = len_ref[i]
            base = pl.multiple_of((length // 16) * 16, 16)
            hit = tile_row == length - base
            for head in range(kv_heads):
                for buf, j in ((kbuf, slots - 2), (vbuf, slots - 1)):
                    new = q_scr[pl.ds(i * rows + head * slots + j, 1), :]
                    old = buf[i, head, pl.ds(base, 16), :].astype(F32)
                    buf[i, head, pl.ds(base, 16), :] = jnp.where(hit, new, old).astype(buf.dtype)
        for c in store(n):
            c.start()

    def attend(group):
        scores, probs = [], []
        for i in group:
            q = q_scr[pl.ds(pl.multiple_of(i * rows, rows), rows), :].astype(BF16)
            by_head = [lax.dot_general(q, kbuf[i, head], (((1,), (1,)), ((), ())), preferred_element_type=F32)
                       for head in range(kv_heads)]
            scores.append(jnp.concatenate([by_head[head][head * slots:(head + 1) * slots] for head in range(kv_heads)], axis=0))
        for i, score in zip(group, scores):
            score = jnp.where(position <= len_ref[i], score * scale, -1e30)
            e = jnp.exp(score - jnp.max(score, axis=1, keepdims=True))
            probs.append((e / jnp.sum(e, axis=1, keepdims=True)).astype(BF16))
        for i, p in zip(group, probs):
            by_head = [dot(p, vbuf[i, head]) for head in range(kv_heads)]
            o_scr[pl.ds(pl.multiple_of(i * rows, rows), rows), :] = jnp.concatenate(
                [by_head[head][head * slots:(head + 1) * slots] for head in range(kv_heads)], axis=0)

    @pl.loop(0, num_seqs // per_copy)
    def _(n):
        patch(n)
        for first in range(0, per_copy, per_step):
            attend([n * per_copy + first + sub for sub in range(per_step)])

    for head in range(kv_heads):
        for j in range(slots - 2):
            o_ref[head, :, j * head_dim:(j + 1) * head_dim] = (
                o_scr[pl.ds(head * slots + j, num_seqs, stride=rows), :].astype(o_ref.dtype))
    o_copy = pltpu.make_async_copy(o_ref, o_hbm, small_sem.at[2])
    o_copy.start()

    @pl.loop(0, num_seqs // per_copy)
    def _(n):
        for c in store(n):
            c.wait()

    o_copy.wait()


VMEM = pl.BlockSpec(memory_space=pltpu.VMEM)
HBM = pl.BlockSpec(memory_space=pltpu.HBM)


def attention(layer, lengths, qkv, k_cache, v_cache, outs):
    layers, num_seqs, kv_heads, cache_len, head_dim = k_cache.shape
    slots = qkv.shape[2] // head_dim
    rows = kv_heads * slots
    return pl.pallas_call(
        functools.partial(attention_kernel, layer, PER_COPY, PER_STEP),
        out_shape=(jax.ShapeDtypeStruct(k_cache.shape, k_cache.dtype), jax.ShapeDtypeStruct(v_cache.shape, v_cache.dtype),
                   jax.ShapeDtypeStruct((kv_heads, num_seqs, (slots - 2) * head_dim), BF16)),
        in_specs=[HBM] * (4 + len(outs)),
        out_specs=(HBM, HBM, HBM),
        scratch_shapes=[pltpu.VMEM((num_seqs, kv_heads, cache_len, head_dim), BF16)] * 2
        + [pltpu.VMEM((num_seqs * rows, head_dim), F32)] * 2 + [
            pltpu.VMEM(qkv.shape, BF16), pltpu.VMEM((kv_heads, num_seqs, (slots - 2) * head_dim), BF16),
            pltpu.SMEM((num_seqs,), jnp.int32)]
        + [pltpu.SemaphoreType.DMA((2, num_seqs // PER_COPY))] * 2 + [pltpu.SemaphoreType.DMA((3,))],
        input_output_aliases={4: 0, 5: 1} if outs else {},
        compiler_params=pltpu.CompilerParams(vmem_limit_bytes=VMEM_LIMIT),
        cost_estimate=pl.CostEstimate(flops=10 ** 10, bytes_accessed=8 * num_seqs * kv_heads * cache_len * head_dim, transcendentals=0),
        name=f'attention_{layer}',
    )(lengths, qkv, k_cache, v_cache, *outs)


def solution(mesh):
    seq_axes = ('rep', 'x', 'yz')
    hidden_spec = P('rep', ('x', 'yz'))
    cache_spec = P(None, seq_axes, None, None, None)
    in_specs = (hidden_spec, P(None, 'x'), P(None, 'x', 'yz'), P(None, 'x', None, 'yz'), P(None, 'yz', 'x'), P(None, 'yz', 'x'), cache_spec, cache_spec, P(seq_axes))
    out_specs = (hidden_spec, cache_spec, cache_spec)
    swap = [(0, 2), (2, 0), (1, 3), (3, 1)]

    def device_step(hidden, norm_gain, w_attn, w_mlp, w_out, w_down, k_cache, v_cache, lengths):
        rows, part = hidden.shape
        depth, attn_cols = w_attn.shape[1:]
        model_dim = depth * mesh.shape['x']
        mlp_cols = w_mlp.shape[3]
        out_depth = w_out.shape[1]
        cols = mlp_cols // CHUNKS
        units = CHUNKS * PARTS
        lanes = rows // PARTS
        half, shard = lanes // 2, lanes // 4
        seqs = shard // 2
        num_seqs = PARTS * seqs

        def semaphores(groups, remote, local):
            return {'send': pltpu.SemaphoreType.DMA((groups,)), 'recv': pltpu.SemaphoreType.DMA((remote,)),
                    'local': pltpu.SemaphoreType.DMA((local,))}

        def front_scratch(layer):
            return {
                'sq_send': pltpu.VMEM((PARTS, SQ_ROWS, lanes), F32), 'sq_recv': pltpu.VMEM((PARTS, 8, SQ_ROWS, lanes), F32),
                'h': pltpu.VMEM((PARTS, depth, lanes), BF16), 'gain_in': pltpu.VMEM(norm_gain.shape, BF16), 'gain': pltpu.VMEM((depth, lanes), F32),
                'u': pltpu.VMEM((PARTS, lanes, depth), BF16), 'u_rel': pltpu.VMEM((PARTS, lanes, depth), BF16),
                'wa': pltpu.VMEM((depth, attn_cols), BF16), 'wm': pltpu.VMEM((depth, 2, mlp_cols), BF16),
                'w_split': pltpu.VMEM((2, depth, mlp_cols), BF16),
                'a_part': pltpu.VMEM((PARTS, lanes, attn_cols), BF16), 'a_core': pltpu.VMEM((PARTS, half, attn_cols), BF16),
                'a_sum': pltpu.VMEM((PARTS, half, attn_cols), BF16), 'a_got': pltpu.VMEM((PARTS, 3, seqs, attn_cols), BF16),
                'a_full': pltpu.VMEM((PARTS, 2, seqs, attn_cols), BF16),
                'z_part': pltpu.VMEM((PARTS, CHUNKS, 2 * lanes, cols), BF16),
                'z_recv': pltpu.VMEM((PARTS, CHUNKS, lanes, cols), BF16), 'z_x': pltpu.VMEM((units, half, cols), BF16),
                'z_mine': pltpu.VMEM((units, half, cols), BF16), 'z_early': pltpu.VMEM((EARLY[layer], half, cols), BF16),
            }

        back_scratch = {
            'o_yz': pltpu.VMEM((num_seqs, out_depth), BF16), 'o': pltpu.VMEM((PARTS, lanes, out_depth), BF16),
            'm': pltpu.VMEM((PARTS, CHUNKS, lanes, cols), BF16), 'z_in': pltpu.VMEM((units, half, cols), BF16),
            'o_in': pltpu.VMEM((2, num_seqs, out_depth), BF16),
            'h_in': pltpu.VMEM((PARTS, part, lanes), BF16),
            'wd': pltpu.VMEM((mlp_cols, depth), BF16), 'wo': pltpu.VMEM((out_depth, depth), BF16),
            'acc': pltpu.VMEM((PARTS, lanes, depth), F32), 'update': pltpu.VMEM((PARTS, lanes, depth), F32),
            'up_part': pltpu.VMEM((PARTS, depth, lanes), BF16), 'up_recv': pltpu.VMEM((PARTS, part, lanes), BF16),
        }

        def got_scratch(layer):
            return {'z_got': pltpu.VMEM((units - EARLY[layer], half, cols), BF16)}

        def front_shapes(layer):
            return (
                jax.ShapeDtypeStruct((2, num_seqs, attn_cols), BF16), jax.ShapeDtypeStruct((units - EARLY[layer], half, cols), BF16),
                jax.ShapeDtypeStruct((units, half, cols), BF16), jax.ShapeDtypeStruct((PARTS, part, lanes), BF16))
        front_specs = (HBM,) * 4

        def call(kernel, name, collective_id, scratch, in_specs, out_shape, out_specs, *args):
            return pl.pallas_call(
                functools.partial(kernel, tuple(scratch)), out_shape=out_shape, in_specs=list(in_specs), out_specs=out_specs,
                scratch_shapes=list(scratch.values()), name=name,
                compiler_params=pltpu.CompilerParams(collective_id=collective_id, has_side_effects=True, vmem_limit_bytes=END_VMEM_LIMIT if kernel is end_kernel else VMEM_LIMIT),
            )(*args)

        def start(names, *refs):
            start_kernel(names, model_dim, *refs)

        def middle(names, *refs):
            middle_kernel(names, model_dim, *refs)

        qkv, zsend, zmine, h_block = call(
            start, 'start', 0, {**semaphores(6, 34 + EARLY[0], 8), **front_scratch(0), 'h_in': pltpu.VMEM((part, rows), BF16)}, (HBM,) * 4,
            front_shapes(0), front_specs, hidden.T, norm_gain, w_attn, w_mlp)
        zgot = lax.ppermute(zsend, 'x', swap)
        k_new, v_new, o = attention(0, lengths, qkv, k_cache, v_cache, ())
        qkv, zsend, zmine, h_block = call(
            middle, 'middle', 1, {**semaphores(10, 65 + EARLY[1], 16), **front_scratch(1), **back_scratch, **got_scratch(0)}, (HBM,) * 9,
            front_shapes(1), front_specs, h_block, o, norm_gain, zmine, zgot, w_down, w_out, w_attn, w_mlp)
        zgot = lax.ppermute(zsend, 'x', swap)
        k_new, v_new, o = attention(1, lengths, qkv, k_cache, v_cache, (k_new, v_new))
        h_out = call(
            end_kernel, 'end', 2, {**semaphores(4, 31, 9), **back_scratch, **got_scratch(1)}, (HBM,) * 6,
            jax.ShapeDtypeStruct((part, rows), BF16), VMEM, h_block, o, zmine, zgot, w_down, w_out)
        return h_out.T, k_new, v_new

    return jax.shard_map(device_step, mesh=mesh, in_specs=in_specs, out_specs=out_specs, check_vma=False)
```

```python
import functools

import jax
import jax.numpy as jnp
from jax import lax
from jax.experimental import pallas as pl
from jax.experimental.pallas import tpu as pltpu
from jax.sharding import PartitionSpec as P

NORM_EPS = 1e-5
MESH = pl.DeviceIdType.MESH
BF16 = jnp.bfloat16
F32 = jnp.float32

SQ_ROWS = 1
PER_COPY = 4
PER_STEP = 2
CHUNKS = 5
EARLY = (1, 2)
CARRY = (0, 2)
END_VMEM_LIMIT = 56393728
VMEM_LIMIT = 67043328


def dot(a, b):
    return jnp.dot(a, b, preferred_element_type=F32)


class Links:
    def __init__(self, send_sems, recv_sems, local_sems, peers):
        self.send_sems, self.recv_sems, self.local_sems = send_sems, recv_sems, local_sems
        self.groups, self.used, self.local_groups, self.local_used = {}, 0, {}, 0
        x, y = lax.axis_index('x'), lax.axis_index('yz')
        self.x, self.y = x, y
        core = lax.rem(x, 2)
        self.along_x = (3 - x, x + 1 - 2 * core, lax.rem(x + 2, 4))
        self.blocks = self.along_x + (x,)
        self.targets = tuple({'x': p, 'yz': y} for p in self.blocks) + ({'x': x, 'yz': 1 - y},) + tuple(
            {'x': p, 'yz': 1 - y} for p in self.along_x)
        self.peers = peers
        self.barrier = pltpu.get_barrier_semaphore()
        for k in self.peers:
            pl.semaphore_signal(self.barrier, inc=1, device_id=self.targets[k], device_id_type=MESH)

    def meet(self):
        pl.semaphore_wait(self.barrier, len(self.peers))

    def push(self, src, dst, to, group):
        k = self.used
        self.used += 1
        g = self.groups.setdefault(group, len(self.groups))
        copy = pltpu.make_async_remote_copy(
            src_ref=src, dst_ref=dst, send_sem=self.send_sems.at[g], recv_sem=self.recv_sems.at[k],
            device_id=self.targets[to], device_id_type=MESH)
        copy.start()
        return copy

    def copy(self, src, dst, group=None):
        if group is None or group not in self.local_groups:
            k = self.local_used
            self.local_used += 1
            if group is not None:
                self.local_groups[group] = k
        else:
            k = self.local_groups[group]
        copy = pltpu.make_async_copy(src, dst, self.local_sems.at[k])
        copy.start()
        return copy

    def drain(self, sent, stored):
        for group, g in self.groups.items():
            pltpu.make_async_copy(sent[group], sent[group], self.send_sems.at[g]).wait()
        for group, k in self.local_groups.items():
            pltpu.make_async_copy(stored[group], stored[group], self.local_sems.at[k]).wait()


DIAG, PARTNER, ACROSS, OWN, YZ, ACROSS_YZ = 0, 1, 2, 3, 4, 7
EVERYONE = [k for k in range(8) if k != OWN]
PARTS = 2


def gated(z):
    shard = z.shape[0] // 2
    gate, up = z[:shard].astype(F32), z[shard:].astype(F32)
    return (gate * jax.nn.sigmoid(gate) * up).astype(BF16)


def part_order(rows, inverse):
    i = lax.broadcasted_iota(jnp.int32, (rows, rows), 0)
    j = lax.broadcasted_iota(jnp.int32, (rows, rows), 1)
    src, dst = (j, i) if inverse else (i, j)
    run = rows // (8 * PARTS)
    piece = src // run
    place = lax.rem(piece, PARTS) * (8 * run) + (piece // PARTS) * run + lax.rem(src, run)
    return jnp.where(dst == place, jnp.ones((), F32), jnp.zeros((), F32)).astype(BF16)


class Front:
    def __init__(self, links, layer, gain_hbm, wa_hbm, wm_hbm, model_dim, outs, s):
        self.links, self.s, self.layer, self.model_dim = links, s, layer, model_dim
        self.kept, self.carry = EARLY[layer], CARRY[layer]
        self.gain_copy = links.copy(gain_hbm, s['gain_in'])
        self.qkv_out, self.zsend_out, self.zmine_out, self.h_out = outs
        self.chunks, self.cols = s['z_recv'].shape[1], s['z_recv'].shape[3]
        self.depth = s['wa'].shape[0]
        self.wa = links.copy(wa_hbm.at[layer], s['wa'])
        self.wm = links.copy(wm_hbm.at[layer], s['wm'])
        self.wa_ready = False
        part = self.depth // 2
        self.mine = pl.ds(pl.multiple_of(links.y * part, part), part)
        self.h_yz = {}
        self.a_core, self.a_got, self.z_core, self.early = {}, {}, {}, {}
        self.sq = {}

    def constants(self):
        lanes = self.s['u'].shape[1]
        self.gain_copy.wait()
        gain = jnp.broadcast_to(self.s['gain_in'][self.layer:self.layer + 1, :].astype(F32), (lanes, self.depth)).T
        self.s['gain'][...] = gain

    def squares(self, p, h_t):
        s = self.s
        s['h'][p, self.mine, :] = h_t.astype(BF16)
        s['sq_send'][p] = jnp.broadcast_to(jnp.sum(h_t * h_t, axis=0, keepdims=True), s['sq_send'].shape[1:])

    def send_h(self, p):
        s, links = self.s, self.links
        self.sq[p] = [links.push(s['sq_send'].at[p], s['sq_recv'].at[p, k], k, 'sq') for k in EVERYONE]
        self.h_yz[p] = links.push(s['h'].at[p, self.mine], s['h'].at[p, self.mine], YZ, 'h')
        links.copy(s['h'].at[p, self.mine], self.h_out.at[p], 'h')

    def normalize(self, p):
        s, links = self.s, self.links
        for c in self.sq[p]:
            c.wait_recv()
        total = s['sq_send'][p]
        for k in EVERYONE:
            total = total + s['sq_recv'][p, k]
        self.h_yz[p].wait_recv()
        h_t = s['h'][p].astype(F32)
        inv_rms = lax.rsqrt(total[:1] / self.model_dim + NORM_EPS)
        s['u'][p] = (h_t * inv_rms * s['gain'][...]).T.astype(BF16)
        shard = s['u'].shape[1] // 4
        u = jnp.concatenate([s['u'][p, pl.ds(pl.multiple_of(b * shard, shard), shard), :] for b in links.blocks], axis=0)
        s['u_rel'][p] = u
        if not self.wa_ready:
            self.wa.wait()
            self.wa_ready = True
        s['a_part'][p] = dot(u, s['wa'][...]).astype(BF16)
        self.a_core[p] = links.push(s['a_part'].at[p, pl.ds(0, 2 * shard)], s['a_core'].at[p], PARTNER, 'a_core')

    def attend_core(self, p):
        s = self.s
        half = s['a_core'].shape[1]
        self.a_core[p].wait_recv()
        s['a_sum'][p] = (s['a_part'][p, half:].astype(F32) + s['a_core'][p].astype(F32)).astype(BF16)
        shard, seqs = half // 2, s['a_got'].shape[2]
        y = self.links.y
        here, there = pl.multiple_of(y * seqs, seqs), pl.multiple_of((1 - y) * seqs, seqs)
        self.a_got[p] = [
            self.links.push(s['a_sum'].at[p, pl.ds(there, seqs)], s['a_got'].at[p, 2], ACROSS_YZ, 'a_got'),
            self.links.push(s['a_sum'].at[p, pl.ds(here, seqs)], s['a_got'].at[p, 0], ACROSS, 'a_got'),
            self.links.push(s['a_sum'].at[p, pl.ds(shard + there, seqs)], s['a_got'].at[p, 1], YZ, 'a_got')]

    def attend_ends(self, p):
        s, y = self.s, self.links.y
        shard, seqs = s['a_sum'].shape[1] // 2, s['a_got'].shape[2]
        for c in self.a_got[p]:
            c.wait_recv()
        own = s['a_sum'][p, pl.ds(shard + pl.multiple_of(y * seqs, seqs), seqs), :]
        s['a_full'][p, 0] = (own.astype(F32) + s['a_got'][p, 0].astype(F32)).astype(BF16)
        s['a_full'][p, 1] = (s['a_got'][p, 1].astype(F32) + s['a_got'][p, 2].astype(F32)).astype(BF16)
        for k, head in enumerate((y, 1 - y)):
            self.links.copy(s['a_full'].at[p, k], self.qkv_out.at[head, pl.ds(p * seqs, seqs)], 'qkv')

    def split_weights(self, c):
        s, run = self.s, 128
        i = lax.broadcasted_iota(jnp.int32, (2 * run, 2 * run), 0)
        j = lax.broadcasted_iota(jnp.int32, (2 * run, 2 * run), 1)
        place = jnp.where(i < run, 2 * i, 2 * (i - run) + 1)
        order = jnp.where(j == place, jnp.ones((), F32), jnp.zeros((), F32)).astype(BF16)
        if c == 0:
            self.wm.wait()
        cols = slice(c * self.cols, (c + 1) * self.cols)
        for e in range(self.depth // run):
            rows = slice(e * run, (e + 1) * run)
            w = dot(order, s['wm'][rows, :, cols].reshape(2 * run, self.cols)).astype(BF16)
            s['w_split'][0, rows, cols] = w[:run]
            s['w_split'][1, rows, cols] = w[run:]

    def project(self, parts, j):
        s = self.s
        lanes = s['u'].shape[1]
        shard = lanes // 4
        u = jnp.concatenate([s['u_rel'][p] for p in parts], axis=0)
        cols = slice(j * self.cols, (j + 1) * self.cols)
        gate, up = dot(u, s['w_split'][0, :, cols]).astype(BF16), dot(u, s['w_split'][1, :, cols]).astype(BF16)
        for n, p in enumerate(parts):
            for k in range(4):
                rows = slice(n * lanes + k * shard, n * lanes + (k + 1) * shard)
                s['z_part'][p, j, 2 * k * shard:(2 * k + 1) * shard] = gate[rows]
                s['z_part'][p, j, (2 * k + 1) * shard:(2 * k + 2) * shard] = up[rows]
            self.push_core(p, j)

    def push_core(self, p, j):
        s = self.s
        half = s['z_recv'].shape[2]
        self.z_core[p, j] = self.links.push(s['z_part'].at[p, j, pl.ds(0, half)], s['z_recv'].at[p, j], PARTNER, 'z')

    def combine(self, p, j):
        s, unit = self.s, p * self.chunks + j
        half = s['z_recv'].shape[2]
        shard2 = half // 2
        self.z_core[p, j].wait_recv()
        s['z_x'][unit] = (s['z_part'][p, j, half:half + shard2].astype(F32) + s['z_recv'][p, j, :shard2].astype(F32)).astype(BF16)
        if unit < self.kept:
            self.early[unit] = self.links.push(s['z_x'].at[unit], s['z_early'].at[unit], ACROSS, 'early')
        else:
            self.links.copy(s['z_x'].at[unit], self.zsend_out.at[unit - self.kept], 'z_x')
        s['z_mine'][unit] = (s['z_part'][p, j, half + shard2:].astype(F32) + s['z_recv'][p, j, shard2:].astype(F32)).astype(BF16)
        if unit >= self.kept:
            self.links.copy(s['z_mine'].at[unit], self.zmine_out.at[unit], 'z_mine')

    def take_early(self):
        s = self.s
        for unit in range(self.kept):
            self.early[unit].wait_recv()
            s['z_mine'][unit] = (s['z_mine'][unit].astype(F32) + s['z_early'][unit].astype(F32)).astype(BF16)
            self.links.copy(s['z_mine'].at[unit], self.zmine_out.at[unit], 'z_mine')
        if self.carry:
            shard = s['z_mine'].shape[1] // 2
            for unit in range(self.carry):
                s['m_early'][unit * shard:(unit + 1) * shard] = gated(s['z_mine'][unit])
            self.links.copy(s['m_early'], self.zsend_out.at[s['z_x'].shape[0] - self.kept], 'm_early')

    def sizes(self):
        s = self.s
        return ({'a_core': s['a_core'], 'a_got': s['a_got'], 'z': s['z_recv'], 'early': s['z_early'],
                 'sq': s['sq_recv'].at[:, pl.ds(0, len(EVERYONE))], 'h': s['h'].at[:, self.mine]},
                {'z_x': s['z_x'].at[pl.ds(self.kept, s['z_x'].shape[0] - self.kept)], 'z_mine': s['z_mine'], 'qkv': s['a_full'], 'h': s['h'].at[:, self.mine], 'm_early': s.get('m_early')})


class Back:
    def __init__(self, links, layer, h_hbm, o_hbm, zgot_hbm, zmine_hbm, wd_hbm, wo_hbm, s):
        self.links, self.s = links, s
        self.kept, self.carry = EARLY[layer], CARRY[layer]
        self.chunks, self.cols = s['m'].shape[1], s['m'].shape[3]
        units = PARTS * self.chunks
        shard = s['m'].shape[2] // 4
        self.z = []
        for first, last in ((0, 1), (1, self.chunks), (self.chunks, units)):
            run = pl.ds(first, last - first)
            self.z.append((first, links.copy(zmine_hbm.at[run], s['z_in'].at[run])))
            start = max(first, self.kept)
            if start < last:
                run = pl.ds(start - self.kept, last - start)
                self.z.append((start, links.copy(zgot_hbm.at[run], s['z_got'].at[run])))
            if first == 0:
                self.carried = [links.copy(zgot_hbm.at[units - self.kept, pl.ds(j * shard, shard)], self.block(0, j, ACROSS))
                                for j in range(self.carry)]
                self.o_copy = links.copy(o_hbm, s['o_in'])
                self.h_copy = links.copy(h_hbm, s['h_in'])
        self.wd = links.copy(wd_hbm.at[layer], s['wd'])
        self.wo = links.copy(wo_hbm.at[layer], s['wo'])
        self.wo_ready, self.wd_ready = False, False
        self.across, self.partner, self.diag = {}, {}, {}
        self.o_across, self.o_partner, self.o_diag = {}, {}, {}
        self.up = {}

    def mix(self, p, j):
        s, unit = self.s, p * self.chunks + j
        while self.z and self.z[0][0] <= unit:
            self.z.pop(0)[1].wait()
        z = s['z_in'][unit]
        if unit >= self.kept:
            z = (z.astype(F32) + s['z_got'][unit - self.kept].astype(F32)).astype(BF16)
        s['m'][p, j, OWN * (z.shape[0] // 2):] = gated(z)

    def block(self, p, j, k):
        shard = self.s['m'].shape[2] // 4
        return self.s['m'].at[p, j, pl.ds(k * shard, shard)]

    def send(self, p, j):
        if p > 0 or j >= self.carry:
            self.across[p, j] = self.links.push(self.block(p, j, OWN), self.block(p, j, ACROSS), ACROSS, 'm_across')

    def send_partner(self, p):
        m = self.s['m']
        shard = m.shape[2] // 4
        self.partner[p] = self.links.push(m.at[p, :, pl.ds(OWN * shard, shard)], m.at[p, :, pl.ds(PARTNER * shard, shard)], PARTNER, 'm')

    def forward(self, p, j):
        if p > 0 or j >= self.carry:
            self.across[p, j].wait_recv()
        else:
            self.carried[j].wait()
        self.diag[p, j] = self.links.push(self.block(p, j, ACROSS), self.block(p, j, DIAG), PARTNER, 'm')

    def send_o_yz(self):
        y, s = self.links.y, self.s
        self.o_copy.wait()
        self.o_yz = self.links.push(s['o_in'].at[1 - y], s['o_yz'], YZ, 'o_yz')

    def o_block(self, p, k):
        shard = self.s['o'].shape[1] // 4
        return self.s['o'].at[p, pl.ds(k * shard, shard)]

    def send_o(self, p):
        y, s = self.links.y, self.s
        if p == 0:
            self.o_yz.wait_recv()
        shard = s['o'].shape[1] // 4
        seqs = shard // 2
        s['o'][p, pl.ds(OWN * shard + pl.multiple_of(y * seqs, seqs), seqs), :] = s['o_in'][y, p * seqs:(p + 1) * seqs]
        s['o'][p, pl.ds(OWN * shard + pl.multiple_of((1 - y) * seqs, seqs), seqs), :] = s['o_yz'][p * seqs:(p + 1) * seqs]
        self.o_across[p] = self.links.push(self.o_block(p, OWN), self.o_block(p, ACROSS), ACROSS, 'o')
        self.o_partner[p] = self.links.push(self.o_block(p, OWN), self.o_block(p, PARTNER), PARTNER, 'o')

    def forward_o(self, p):
        self.o_across[p].wait_recv()
        self.o_diag[p] = self.links.push(self.o_block(p, ACROSS), self.o_block(p, DIAG), PARTNER, 'o')

    def project_o(self, p):
        s = self.s
        self.o_partner[p].wait_recv()
        self.o_diag[p].wait_recv()
        if not self.wo_ready:
            self.wo.wait()
            self.wo_ready = True
        s['acc'][p] += dot(s['o'][p], s['wo'][...])

    def down(self, p, j):
        s = self.s
        if j == 0:
            self.partner[p].wait_recv()
        self.diag[p, j].wait_recv()
        if not self.wd_ready:
            self.wd.wait()
            self.wd_ready = True
        part = dot(s['m'][p, j], s['wd'][j * self.cols:(j + 1) * self.cols])
        if j == 0:
            s['acc'][p] = part
        else:
            s['acc'][p] += part

    def send_update(self, p):
        s, links = self.s, self.links
        shard = s['acc'].shape[1] // 4
        for k in range(4):
            s['update'][p, pl.ds(pl.multiple_of(links.blocks[k] * shard, shard), shard), :] = s['acc'][p, k * shard:(k + 1) * shard, :]
        s['up_part'][p] = s['update'][p].T.astype(BF16)
        part = s['up_recv'].shape[1]
        src = s['up_part'].at[p, pl.ds(pl.multiple_of((1 - links.y) * part, part), part)]
        self.up[p] = links.push(src, s['up_recv'].at[p], YZ, 'up')

    def new_h(self, p):
        s, links = self.s, self.links
        self.up[p].wait_recv()
        part = s['up_recv'].shape[1]
        own = s['up_part'][p, pl.ds(pl.multiple_of(links.y * part, part), part), :]
        return (s['h_in'][p].astype(F32) + (own.astype(F32) + s['up_recv'][p].astype(F32))).astype(BF16)

    def sizes(self):
        s = self.s
        sent = 3 * s['m'].shape[2] // 4
        shard = sent // 3
        return {'m': s['m'].at[:, :, pl.ds(0, 2 * shard)],
                'm_across': s['m'].at[:, pl.ds(0, self.chunks - self.carry // PARTS), pl.ds(0, shard)], 'o': s['o'].at[:, pl.ds(0, sent)], 'o_yz': s['o_yz'], 'up': s['up_recv']}

    def open(self):
        links, chunks = self.links, self.chunks
        self.mix(0, 0)
        links.meet()
        self.send(0, 0)
        self.send_o_yz()
        for j in range(1, chunks):
            self.mix(0, j)
            self.send(0, j)
            if j == 2:
                self.send_o(0)
        self.send_partner(0)
        for j in range(chunks):
            self.mix(1, j)
            self.send(1, j)
            if j == 1:
                self.send_o(1)
        self.send_partner(1)
        self.h_copy.wait()


def start_kernel(names, model_dim, h_hbm, gain_hbm, wa_hbm, wm_hbm, qkv_out, zsend_out, zmine_out, h_out, *scratch):
    s = dict(zip(names, scratch))
    links = Links(s['send'], s['recv'], s['local'], EVERYONE)
    h_copy = links.copy(h_hbm, s['h_in'])
    f = Front(links, 0, gain_hbm, wa_hbm, wm_hbm, model_dim, (qkv_out, zsend_out, zmine_out, h_out), s)
    rows = h_hbm.shape[1]
    lanes = rows // PARTS
    order = part_order(rows, False)
    h_copy.wait()
    own = dot(s['h_in'][...], order)
    for p in range(PARTS):
        f.squares(p, own[:, p * lanes:(p + 1) * lanes])
    f.constants()
    links.meet()
    for p in range(PARTS):
        f.send_h(p)
    for j in range(f.chunks):
        f.split_weights(j)
    for p in range(PARTS):
        f.normalize(p)
    f.project(range(PARTS), 0)
    for p in range(PARTS):
        f.attend_core(p)
    for j in range(1, f.chunks):
        f.project(range(PARTS), j)
        if j == f.chunks - 1:
            f.attend_ends(0)
        for p in range(PARTS):
            f.combine(p, j - 1)
    f.attend_ends(1)
    for p in range(PARTS):
        f.combine(p, f.chunks - 1)
    f.take_early()
    links.drain(*f.sizes())


def middle_kernel(names, model_dim, h_hbm, o_hbm, gain_hbm, zmine_hbm, zgot_hbm, wd_hbm, wo_hbm, wa_hbm, wm_hbm, qkv_out, zsend_out,
                  zmine_out, h_out, *scratch):
    s = dict(zip(names, scratch))
    links = Links(s['send'], s['recv'], s['local'], EVERYONE)
    b = Back(links, 0, h_hbm, o_hbm, zgot_hbm, zmine_hbm, wd_hbm, wo_hbm, s)
    f = Front(links, 1, gain_hbm, wa_hbm, wm_hbm, model_dim, (qkv_out, zsend_out, zmine_out, h_out), s)
    b.open()
    f.constants()

    def pass_h(p):
        f.squares(p, b.new_h(p).astype(F32))
        f.send_h(p)

    first_part(b, f.split_weights)
    second_part(b, lambda: pass_h(0))
    f.normalize(0)
    f.project([0], 0)
    f.attend_core(0)
    pass_h(1)
    f.project([0], 1)
    f.project([0], 2)
    f.combine(0, 0)
    f.project([0], 3)
    f.combine(0, 1)
    f.project([0], 4)
    f.combine(0, 2)
    f.combine(0, 3)
    f.normalize(1)
    f.project([1], 0)
    f.combine(0, 4)
    f.project([1], 1)
    f.attend_core(1)
    f.attend_ends(0)
    f.project([1], 2)
    f.combine(1, 0)
    f.project([1], 3)
    f.combine(1, 1)
    f.project([1], 4)
    f.combine(1, 2)
    f.combine(1, 3)
    f.take_early()
    f.combine(1, 4)
    f.attend_ends(1)
    sent, stored = f.sizes()
    links.drain({**sent, **b.sizes()}, stored)


def first_part(b, filler):
    for j in range(b.chunks):
        b.forward(0, j)
        if filler is not None:
            filler(j)
        if j == 2:
            b.forward_o(0)
        if j >= 1:
            b.down(0, j - 1)
    b.project_o(0)
    b.down(0, b.chunks - 1)
    b.send_update(0)
    b.forward(1, 0)


def second_part(b, when_updated):
    for j in range(1, b.chunks):
        b.forward(1, j)
        if j == 1:
            b.forward_o(1)
        b.down(1, j - 1)
        if j == 2:
            b.project_o(1)
        if j == b.chunks - 3:
            when_updated()
    b.down(1, b.chunks - 1)
    b.send_update(1)


def end_kernel(names, h_hbm, o_hbm, zmine_hbm, zgot_hbm, wd_hbm, wo_hbm, h_out, *scratch):
    s = dict(zip(names, scratch))
    links = Links(s['send'], s['recv'], s['local'], [PARTNER, ACROSS, YZ])
    b = Back(links, 1, h_hbm, o_hbm, zgot_hbm, zmine_hbm, wd_hbm, wo_hbm, s)
    b.open()
    first_part(b, None)
    h_new = []
    second_part(b, lambda: h_new.append(b.new_h(0)))
    order = part_order(h_out.shape[1], True)
    h_new.append(b.new_h(1))
    h_out[...] = dot(jnp.concatenate(h_new, axis=1), order).astype(BF16)
    links.drain(b.sizes(), {})


def attention_kernel(layer, per_copy, per_step, len_hbm, qkv_hbm, k_hbm, v_hbm, *rest):
    k_out, v_out, o_hbm, kbuf, vbuf, q_scr, o_scr, qkv_ref, o_ref, len_ref, in_sem, out_sem, small_sem = rest[-13:]
    num_seqs, kv_heads, cache_len, head_dim = kbuf.shape
    slots = qkv_ref.shape[2] // head_dim
    rows = kv_heads * slots
    scale = head_dim ** -0.5

    def load(n):
        run = pl.ds(n * per_copy, per_copy)
        return (pltpu.make_async_copy(k_hbm.at[layer, run], kbuf.at[run], in_sem.at[0, n]),
                pltpu.make_async_copy(v_hbm.at[layer, run], vbuf.at[run], in_sem.at[1, n]))

    def store(n):
        run = pl.ds(n * per_copy, per_copy)
        return (pltpu.make_async_copy(kbuf.at[run], k_out.at[layer, run], out_sem.at[0, n]),
                pltpu.make_async_copy(vbuf.at[run], v_out.at[layer, run], out_sem.at[1, n]))

    qkv_copy = pltpu.make_async_copy(qkv_hbm, qkv_ref, small_sem.at[0])
    len_copy = pltpu.make_async_copy(len_hbm, len_ref, small_sem.at[1])
    qkv_copy.start()
    len_copy.start()

    @pl.loop(0, num_seqs // per_copy)
    def _(n):
        for c in load(n):
            c.start()

    qkv_copy.wait()
    len_copy.wait()
    for head in range(kv_heads):
        for j in range(slots):
            q_scr[pl.ds(head * slots + j, num_seqs, stride=rows), :] = (
                qkv_ref[head, :, j * head_dim:(j + 1) * head_dim].astype(F32))

    tile_row = lax.broadcasted_iota(jnp.int32, (16, head_dim), 0)
    position = lax.broadcasted_iota(jnp.int32, (rows, cache_len), 1)

    def patch(n):
        for c in load(n):
            c.wait()
        for sub in range(per_copy):
            i = n * per_copy + sub
            length = len_ref[i]
            base = pl.multiple_of((length // 16) * 16, 16)
            hit = tile_row == length - base
            for head in range(kv_heads):
                for buf, j in ((kbuf, slots - 2), (vbuf, slots - 1)):
                    new = q_scr[pl.ds(i * rows + head * slots + j, 1), :]
                    old = buf[i, head, pl.ds(base, 16), :].astype(F32)
                    buf[i, head, pl.ds(base, 16), :] = jnp.where(hit, new, old).astype(buf.dtype)
        for c in store(n):
            c.start()

    def attend(group):
        scores, probs = [], []
        for i in group:
            q = q_scr[pl.ds(pl.multiple_of(i * rows, rows), rows), :].astype(BF16)
            by_head = [lax.dot_general(q, kbuf[i, head], (((1,), (1,)), ((), ())), preferred_element_type=F32)
                       for head in range(kv_heads)]
            scores.append(jnp.concatenate([by_head[head][head * slots:(head + 1) * slots] for head in range(kv_heads)], axis=0))
        for i, score in zip(group, scores):
            score = jnp.where(position <= len_ref[i], score * scale, -1e30)
            e = jnp.exp(score - jnp.max(score, axis=1, keepdims=True))
            probs.append((e / jnp.sum(e, axis=1, keepdims=True)).astype(BF16))
        for i, p in zip(group, probs):
            by_head = [dot(p, vbuf[i, head]) for head in range(kv_heads)]
            o_scr[pl.ds(pl.multiple_of(i * rows, rows), rows), :] = jnp.concatenate(
                [by_head[head][head * slots:(head + 1) * slots] for head in range(kv_heads)], axis=0)

    @pl.loop(0, num_seqs // per_copy)
    def _(n):
        patch(n)
        for first in range(0, per_copy, per_step):
            attend([n * per_copy + first + sub for sub in range(per_step)])

    for head in range(kv_heads):
        for j in range(slots - 2):
            o_ref[head, :, j * head_dim:(j + 1) * head_dim] = (
                o_scr[pl.ds(head * slots + j, num_seqs, stride=rows), :].astype(o_ref.dtype))
    o_copy = pltpu.make_async_copy(o_ref, o_hbm, small_sem.at[2])
    o_copy.start()

    @pl.loop(0, num_seqs // per_copy)
    def _(n):
        for c in store(n):
            c.wait()

    o_copy.wait()


VMEM = pl.BlockSpec(memory_space=pltpu.VMEM)
HBM = pl.BlockSpec(memory_space=pltpu.HBM)


def attention(layer, lengths, qkv, k_cache, v_cache, outs):
    layers, num_seqs, kv_heads, cache_len, head_dim = k_cache.shape
    slots = qkv.shape[2] // head_dim
    rows = kv_heads * slots
    return pl.pallas_call(
        functools.partial(attention_kernel, layer, PER_COPY, PER_STEP),
        out_shape=(jax.ShapeDtypeStruct(k_cache.shape, k_cache.dtype), jax.ShapeDtypeStruct(v_cache.shape, v_cache.dtype),
                   jax.ShapeDtypeStruct((kv_heads, num_seqs, (slots - 2) * head_dim), BF16)),
        in_specs=[HBM] * (4 + len(outs)),
        out_specs=(HBM, HBM, HBM),
        scratch_shapes=[pltpu.VMEM((num_seqs, kv_heads, cache_len, head_dim), BF16)] * 2
        + [pltpu.VMEM((num_seqs * rows, head_dim), F32)] * 2 + [
            pltpu.VMEM(qkv.shape, BF16), pltpu.VMEM((kv_heads, num_seqs, (slots - 2) * head_dim), BF16),
            pltpu.SMEM((num_seqs,), jnp.int32)]
        + [pltpu.SemaphoreType.DMA((2, num_seqs // PER_COPY))] * 2 + [pltpu.SemaphoreType.DMA((3,))],
        input_output_aliases={4: 0, 5: 1} if outs else {},
        compiler_params=pltpu.CompilerParams(vmem_limit_bytes=VMEM_LIMIT),
        cost_estimate=pl.CostEstimate(flops=10 ** 10, bytes_accessed=8 * num_seqs * kv_heads * cache_len * head_dim, transcendentals=0),
        name=f'attention_{layer}',
    )(lengths, qkv, k_cache, v_cache, *outs)


def solution(mesh):
    seq_axes = ('rep', 'x', 'yz')
    hidden_spec = P('rep', ('x', 'yz'))
    cache_spec = P(None, seq_axes, None, None, None)
    in_specs = (hidden_spec, P(None, 'x'), P(None, 'x', 'yz'), P(None, 'x', None, 'yz'), P(None, 'yz', 'x'), P(None, 'yz', 'x'), cache_spec, cache_spec, P(seq_axes))
    out_specs = (hidden_spec, cache_spec, cache_spec)
    swap = [(0, 2), (2, 0), (1, 3), (3, 1)]

    def device_step(hidden, norm_gain, w_attn, w_mlp, w_out, w_down, k_cache, v_cache, lengths):
        rows, part = hidden.shape
        depth, attn_cols = w_attn.shape[1:]
        model_dim = depth * mesh.shape['x']
        mlp_cols = w_mlp.shape[3]
        out_depth = w_out.shape[1]
        cols = mlp_cols // CHUNKS
        units = CHUNKS * PARTS
        lanes = rows // PARTS
        half, shard = lanes // 2, lanes // 4
        seqs = shard // 2
        num_seqs = PARTS * seqs

        def semaphores(groups, remote, local):
            return {'send': pltpu.SemaphoreType.DMA((groups,)), 'recv': pltpu.SemaphoreType.DMA((remote,)),
                    'local': pltpu.SemaphoreType.DMA((local,))}

        def front_scratch(layer):
            return {
                'sq_send': pltpu.VMEM((PARTS, SQ_ROWS, lanes), F32), 'sq_recv': pltpu.VMEM((PARTS, 8, SQ_ROWS, lanes), F32),
                'h': pltpu.VMEM((PARTS, depth, lanes), BF16), 'gain_in': pltpu.VMEM(norm_gain.shape, BF16), 'gain': pltpu.VMEM((depth, lanes), F32),
                'u': pltpu.VMEM((PARTS, lanes, depth), BF16), 'u_rel': pltpu.VMEM((PARTS, lanes, depth), BF16),
                'wa': pltpu.VMEM((depth, attn_cols), BF16), 'wm': pltpu.VMEM((depth, 2, mlp_cols), BF16),
                'w_split': pltpu.VMEM((2, depth, mlp_cols), BF16),
                'a_part': pltpu.VMEM((PARTS, lanes, attn_cols), BF16), 'a_core': pltpu.VMEM((PARTS, half, attn_cols), BF16),
                'a_sum': pltpu.VMEM((PARTS, half, attn_cols), BF16), 'a_got': pltpu.VMEM((PARTS, 3, seqs, attn_cols), BF16),
                'a_full': pltpu.VMEM((PARTS, 2, seqs, attn_cols), BF16),
                'z_part': pltpu.VMEM((PARTS, CHUNKS, 2 * lanes, cols), BF16),
                'z_recv': pltpu.VMEM((PARTS, CHUNKS, lanes, cols), BF16), 'z_x': pltpu.VMEM((units, half, cols), BF16),
                'z_mine': pltpu.VMEM((units, half, cols), BF16), 'z_early': pltpu.VMEM((EARLY[layer], half, cols), BF16),
            }

        back_scratch = {
            'o_yz': pltpu.VMEM((num_seqs, out_depth), BF16), 'o': pltpu.VMEM((PARTS, lanes, out_depth), BF16),
            'm': pltpu.VMEM((PARTS, CHUNKS, lanes, cols), BF16), 'z_in': pltpu.VMEM((units, half, cols), BF16),
            'o_in': pltpu.VMEM((2, num_seqs, out_depth), BF16),
            'h_in': pltpu.VMEM((PARTS, part, lanes), BF16),
            'wd': pltpu.VMEM((mlp_cols, depth), BF16), 'wo': pltpu.VMEM((out_depth, depth), BF16),
            'acc': pltpu.VMEM((PARTS, lanes, depth), F32), 'update': pltpu.VMEM((PARTS, lanes, depth), F32),
            'up_part': pltpu.VMEM((PARTS, depth, lanes), BF16), 'up_recv': pltpu.VMEM((PARTS, part, lanes), BF16),
        }

        def got_scratch(layer):
            return {'z_got': pltpu.VMEM((units - EARLY[layer], half, cols), BF16)}

        def front_shapes(layer):
            return (
                jax.ShapeDtypeStruct((2, num_seqs, attn_cols), BF16), jax.ShapeDtypeStruct((units - EARLY[layer] + CARRY[layer] // PARTS, half, cols), BF16),
                jax.ShapeDtypeStruct((units, half, cols), BF16), jax.ShapeDtypeStruct((PARTS, part, lanes), BF16))
        front_specs = (HBM,) * 4

        def call(kernel, name, collective_id, scratch, in_specs, out_shape, out_specs, *args):
            return pl.pallas_call(
                functools.partial(kernel, tuple(scratch)), out_shape=out_shape, in_specs=list(in_specs), out_specs=out_specs,
                scratch_shapes=list(scratch.values()), name=name,
                compiler_params=pltpu.CompilerParams(collective_id=collective_id, has_side_effects=True, vmem_limit_bytes=END_VMEM_LIMIT if kernel is end_kernel else VMEM_LIMIT),
            )(*args)

        def start(names, *refs):
            start_kernel(names, model_dim, *refs)

        def middle(names, *refs):
            middle_kernel(names, model_dim, *refs)

        qkv, zsend, zmine, h_block = call(
            start, 'start', 0, {**semaphores(6, 34 + EARLY[0], 8), **front_scratch(0), 'h_in': pltpu.VMEM((part, rows), BF16)}, (HBM,) * 4,
            front_shapes(0), front_specs, hidden.T, norm_gain, w_attn, w_mlp)
        zgot = lax.ppermute(zsend, 'x', swap)
        k_new, v_new, o = attention(0, lengths, qkv, k_cache, v_cache, ())
        qkv, zsend, zmine, h_block = call(
            middle, 'middle', 1, {**semaphores(11, 65 + EARLY[1], 17), **front_scratch(1), **back_scratch, **got_scratch(0),
                       'm_early': pltpu.VMEM((half, cols), BF16)}, (HBM,) * 9,
            front_shapes(1), front_specs, h_block, o, norm_gain, zmine, zgot, w_down, w_out, w_attn, w_mlp)
        zgot = lax.ppermute(zsend, 'x', swap)
        k_new, v_new, o = attention(1, lengths, qkv, k_cache, v_cache, (k_new, v_new))
        h_out = call(
            end_kernel, 'end', 2, {**semaphores(5, 29, 11), **back_scratch, **got_scratch(1)}, (HBM,) * 6,
            jax.ShapeDtypeStruct((part, rows), BF16), VMEM, h_block, o, zmine, zgot, w_down, w_out)
        return h_out.T, k_new, v_new

    return jax.shard_map(device_step, mesh=mesh, in_specs=in_specs, out_specs=out_specs, check_vma=False)
```

```python
import functools
import types

import jax
import jax.numpy as jnp
from jax import lax
from jax.experimental import pallas as pl
from jax.experimental.pallas import tpu as pltpu
from jax.sharding import PartitionSpec as P

NORM_EPS = 1e-5
MESH = pl.DeviceIdType.MESH
BF16 = jnp.bfloat16
F32 = jnp.float32

SQ_ROWS = 1
PER_COPY = 4
PER_STEP = 2
CHUNKS = 5
EARLY = (1, 2)
CARRY = (0, 2)
END_VMEM_LIMIT = 56393728
VMEM_LIMIT = 67043328


def dot(a, b):
    return jnp.dot(a, b, preferred_element_type=F32)


class Links:
    def __init__(self, send_sems, recv_sems, local_sems, peers):
        self.send_sems, self.recv_sems, self.local_sems = send_sems, recv_sems, local_sems
        self.groups, self.used, self.local_groups, self.local_used = {}, 0, {}, 0
        x, y = lax.axis_index('x'), lax.axis_index('yz')
        self.x, self.y = x, y
        core = lax.rem(x, 2)
        self.along_x = (3 - x, x + 1 - 2 * core, lax.rem(x + 2, 4))
        self.blocks = self.along_x + (x,)
        self.targets = tuple({'x': p, 'yz': y} for p in self.blocks) + ({'x': x, 'yz': 1 - y},) + tuple(
            {'x': p, 'yz': 1 - y} for p in self.along_x)
        self.peers = peers
        self.barrier = pltpu.get_barrier_semaphore()
        for k in self.peers:
            pl.semaphore_signal(self.barrier, inc=1, device_id=self.targets[k], device_id_type=MESH)

    def meet(self):
        pl.semaphore_wait(self.barrier, len(self.peers))

    def push(self, src, dst, to, group):
        k = self.used
        self.used += 1
        g = self.groups.setdefault(group, len(self.groups))
        copy = pltpu.make_async_remote_copy(
            src_ref=src, dst_ref=dst, send_sem=self.send_sems.at[g], recv_sem=self.recv_sems.at[k],
            device_id=self.targets[to], device_id_type=MESH)
        copy.start()
        return copy

    def copy(self, src, dst, group=None):
        if group is None or group not in self.local_groups:
            k = self.local_used
            self.local_used += 1
            if group is not None:
                self.local_groups[group] = k
        else:
            k = self.local_groups[group]
        copy = pltpu.make_async_copy(src, dst, self.local_sems.at[k])
        copy.start()
        return copy

    def drain(self, sent, stored):
        for group, g in self.groups.items():
            pltpu.make_async_copy(sent[group], sent[group], self.send_sems.at[g]).wait()
        for group, k in self.local_groups.items():
            pltpu.make_async_copy(stored[group], stored[group], self.local_sems.at[k]).wait()


DIAG, PARTNER, ACROSS, OWN, YZ, ACROSS_YZ = 0, 1, 2, 3, 4, 7
EVERYONE = [k for k in range(8) if k != OWN]
PARTS = 2


def gated(z):
    shard = z.shape[0] // 2
    gate, up = z[:shard].astype(F32), z[shard:].astype(F32)
    return (gate * jax.nn.sigmoid(gate) * up).astype(BF16)


def part_order(rows, inverse):
    i = lax.broadcasted_iota(jnp.int32, (rows, rows), 0)
    j = lax.broadcasted_iota(jnp.int32, (rows, rows), 1)
    src, dst = (j, i) if inverse else (i, j)
    run = rows // (8 * PARTS)
    piece = src // run
    place = lax.rem(piece, PARTS) * (8 * run) + (piece // PARTS) * run + lax.rem(src, run)
    return jnp.where(dst == place, jnp.ones((), F32), jnp.zeros((), F32)).astype(BF16)


class Front:
    def __init__(self, links, layer, gain_hbm, wa_hbm, wm_hbm, model_dim, outs, s):
        self.links, self.s, self.layer, self.model_dim = links, s, layer, model_dim
        self.kept, self.carry = EARLY[layer], CARRY[layer]
        self.gain_copy = links.copy(gain_hbm, s.gain_in)
        self.qkv_out, self.zsend_out, self.zmine_out, self.h_out = outs
        self.chunks, self.cols = s.z_recv.shape[1], s.z_recv.shape[3]
        self.depth = s.wa.shape[0]
        self.wa = links.copy(wa_hbm.at[layer], s.wa)
        self.wm = links.copy(wm_hbm.at[layer], s.wm)
        self.wa_ready = False
        part = self.depth // 2
        self.mine = pl.ds(pl.multiple_of(links.y * part, part), part)
        self.h_yz = {}
        self.a_core, self.a_got, self.z_core, self.early = {}, {}, {}, {}
        self.sq = {}

    def constants(self):
        lanes = self.s.u.shape[1]
        self.gain_copy.wait()
        gain = jnp.broadcast_to(self.s.gain_in[self.layer:self.layer + 1, :].astype(F32), (lanes, self.depth)).T
        self.s.gain[...] = gain

    def squares(self, p, h_t):
        s = self.s
        s.h[p, self.mine, :] = h_t.astype(BF16)
        s.sq_send[p] = jnp.broadcast_to(jnp.sum(h_t * h_t, axis=0, keepdims=True), s.sq_send.shape[1:])

    def send_h(self, p):
        s, links = self.s, self.links
        self.sq[p] = [links.push(s.sq_send.at[p], s.sq_recv.at[p, k], k, 'sq') for k in EVERYONE]
        self.h_yz[p] = links.push(s.h.at[p, self.mine], s.h.at[p, self.mine], YZ, 'h')
        links.copy(s.h.at[p, self.mine], self.h_out.at[p], 'h')

    def normalize(self, p):
        s, links = self.s, self.links
        for c in self.sq[p]:
            c.wait_recv()
        total = s.sq_send[p]
        for k in EVERYONE:
            total = total + s.sq_recv[p, k]
        self.h_yz[p].wait_recv()
        h_t = s.h[p].astype(F32)
        inv_rms = lax.rsqrt(total[:1] / self.model_dim + NORM_EPS)
        s.u[p] = (h_t * inv_rms * s.gain[...]).T.astype(BF16)
        shard = s.u.shape[1] // 4
        u = jnp.concatenate([s.u[p, pl.ds(pl.multiple_of(b * shard, shard), shard), :] for b in links.blocks], axis=0)
        s.u_rel[p] = u
        if not self.wa_ready:
            self.wa.wait()
            self.wa_ready = True
        s.a_part[p] = dot(u, s.wa[...]).astype(BF16)
        self.a_core[p] = links.push(s.a_part.at[p, pl.ds(0, 2 * shard)], s.a_core.at[p], PARTNER, 'a_core')

    def attend_core(self, p):
        s = self.s
        half = s.a_core.shape[1]
        self.a_core[p].wait_recv()
        s.a_sum[p] = (s.a_part[p, half:].astype(F32) + s.a_core[p].astype(F32)).astype(BF16)
        shard, seqs = half // 2, s.a_got.shape[2]
        y = self.links.y
        here, there = pl.multiple_of(y * seqs, seqs), pl.multiple_of((1 - y) * seqs, seqs)
        self.a_got[p] = [
            self.links.push(s.a_sum.at[p, pl.ds(there, seqs)], s.a_got.at[p, 2], ACROSS_YZ, 'a_got'),
            self.links.push(s.a_sum.at[p, pl.ds(here, seqs)], s.a_got.at[p, 0], ACROSS, 'a_got'),
            self.links.push(s.a_sum.at[p, pl.ds(shard + there, seqs)], s.a_got.at[p, 1], YZ, 'a_got')]

    def attend_ends(self, p):
        s, y = self.s, self.links.y
        shard, seqs = s.a_sum.shape[1] // 2, s.a_got.shape[2]
        for c in self.a_got[p]:
            c.wait_recv()
        own = s.a_sum[p, pl.ds(shard + pl.multiple_of(y * seqs, seqs), seqs), :]
        s.a_full[p, 0] = (own.astype(F32) + s.a_got[p, 0].astype(F32)).astype(BF16)
        s.a_full[p, 1] = (s.a_got[p, 1].astype(F32) + s.a_got[p, 2].astype(F32)).astype(BF16)
        for k, head in enumerate((y, 1 - y)):
            self.links.copy(s.a_full.at[p, k], self.qkv_out.at[head, pl.ds(p * seqs, seqs)], 'qkv')

    def split_weights(self, c):
        s, run = self.s, 128
        i = lax.broadcasted_iota(jnp.int32, (2 * run, 2 * run), 0)
        j = lax.broadcasted_iota(jnp.int32, (2 * run, 2 * run), 1)
        place = jnp.where(i < run, 2 * i, 2 * (i - run) + 1)
        order = jnp.where(j == place, jnp.ones((), F32), jnp.zeros((), F32)).astype(BF16)
        if c == 0:
            self.wm.wait()
        cols = slice(c * self.cols, (c + 1) * self.cols)
        for e in range(self.depth // run):
            rows = slice(e * run, (e + 1) * run)
            w = dot(order, s.wm[rows, :, cols].reshape(2 * run, self.cols)).astype(BF16)
            s.w_split[0, rows, cols] = w[:run]
            s.w_split[1, rows, cols] = w[run:]

    def project(self, parts, j):
        s = self.s
        lanes = s.u.shape[1]
        shard = lanes // 4
        u = jnp.concatenate([s.u_rel[p] for p in parts], axis=0)
        cols = slice(j * self.cols, (j + 1) * self.cols)
        gate, up = dot(u, s.w_split[0, :, cols]).astype(BF16), dot(u, s.w_split[1, :, cols]).astype(BF16)
        for n, p in enumerate(parts):
            for k in range(4):
                rows = slice(n * lanes + k * shard, n * lanes + (k + 1) * shard)
                s.z_part[p, j, 2 * k * shard:(2 * k + 1) * shard] = gate[rows]
                s.z_part[p, j, (2 * k + 1) * shard:(2 * k + 2) * shard] = up[rows]
            self.push_core(p, j)

    def push_core(self, p, j):
        s = self.s
        half = s.z_recv.shape[2]
        self.z_core[p, j] = self.links.push(s.z_part.at[p, j, pl.ds(0, half)], s.z_recv.at[p, j], PARTNER, 'z')

    def combine(self, p, j):
        s, unit = self.s, p * self.chunks + j
        half = s.z_recv.shape[2]
        shard2 = half // 2
        self.z_core[p, j].wait_recv()
        s.z_x[unit] = (s.z_part[p, j, half:half + shard2].astype(F32) + s.z_recv[p, j, :shard2].astype(F32)).astype(BF16)
        if unit < self.kept:
            self.early[unit] = self.links.push(s.z_x.at[unit], s.z_early.at[unit], ACROSS, 'early')
        else:
            self.links.copy(s.z_x.at[unit], self.zsend_out.at[unit - self.kept], 'z_x')
        s.z_mine[unit] = (s.z_part[p, j, half + shard2:].astype(F32) + s.z_recv[p, j, shard2:].astype(F32)).astype(BF16)
        if unit >= self.kept:
            self.links.copy(s.z_mine.at[unit], self.zmine_out.at[unit], 'z_mine')

    def take_early(self):
        s = self.s
        for unit in range(self.kept):
            self.early[unit].wait_recv()
            s.z_mine[unit] = (s.z_mine[unit].astype(F32) + s.z_early[unit].astype(F32)).astype(BF16)
            self.links.copy(s.z_mine.at[unit], self.zmine_out.at[unit], 'z_mine')
        if self.carry:
            shard = s.z_mine.shape[1] // 2
            for unit in range(self.carry):
                s.m_early[unit * shard:(unit + 1) * shard] = gated(s.z_mine[unit])
            self.links.copy(s.m_early, self.zsend_out.at[s.z_x.shape[0] - self.kept], 'm_early')

    def sizes(self):
        s = self.s
        return (dict(a_core=s.a_core, a_got=s.a_got, z=s.z_recv, early=s.z_early,
                 sq=s.sq_recv.at[:, pl.ds(0, len(EVERYONE))], h=s.h.at[:, self.mine]),
                dict(z_x=s.z_x.at[pl.ds(self.kept, s.z_x.shape[0] - self.kept)], z_mine=s.z_mine, qkv=s.a_full, h=s.h.at[:, self.mine], m_early=getattr(s, 'm_early', None)))


class Back:
    def __init__(self, links, layer, h_hbm, o_hbm, zgot_hbm, zmine_hbm, wd_hbm, wo_hbm, s):
        self.links, self.s = links, s
        self.kept, self.carry = EARLY[layer], CARRY[layer]
        self.chunks, self.cols = s.m.shape[1], s.m.shape[3]
        units = PARTS * self.chunks
        shard = s.m.shape[2] // 4
        self.z = []
        for first, last in ((0, 1), (1, self.chunks), (self.chunks, units)):
            run = pl.ds(first, last - first)
            self.z.append((first, links.copy(zmine_hbm.at[run], s.z_in.at[run])))
            start = max(first, self.kept)
            if start < last:
                run = pl.ds(start - self.kept, last - start)
                self.z.append((start, links.copy(zgot_hbm.at[run], s.z_got.at[run])))
            if first == 0:
                self.carried = [links.copy(zgot_hbm.at[units - self.kept, pl.ds(j * shard, shard)], self.block(0, j, ACROSS))
                                for j in range(self.carry)]
                self.o_copy = links.copy(o_hbm, s.o_in)
                self.h_copy = links.copy(h_hbm, s.h_in)
        self.wd = links.copy(wd_hbm.at[layer], s.wd)
        self.wo = links.copy(wo_hbm.at[layer], s.wo)
        self.wo_ready, self.wd_ready = False, False
        self.across, self.partner, self.diag = {}, {}, {}
        self.o_across, self.o_partner, self.o_diag = {}, {}, {}
        self.up = {}

    def mix(self, p, j):
        s, unit = self.s, p * self.chunks + j
        while self.z and self.z[0][0] <= unit:
            self.z.pop(0)[1].wait()
        z = s.z_in[unit]
        if unit >= self.kept:
            z = (z.astype(F32) + s.z_got[unit - self.kept].astype(F32)).astype(BF16)
        s.m[p, j, OWN * (z.shape[0] // 2):] = gated(z)

    def block(self, p, j, k):
        shard = self.s.m.shape[2] // 4
        return self.s.m.at[p, j, pl.ds(k * shard, shard)]

    def send(self, p, j):
        if p > 0 or j >= self.carry:
            self.across[p, j] = self.links.push(self.block(p, j, OWN), self.block(p, j, ACROSS), ACROSS, 'm_across')

    def send_partner(self, p):
        m = self.s.m
        shard = m.shape[2] // 4
        self.partner[p] = self.links.push(m.at[p, :, pl.ds(OWN * shard, shard)], m.at[p, :, pl.ds(PARTNER * shard, shard)], PARTNER, 'm')

    def forward(self, p, j):
        if p > 0 or j >= self.carry:
            self.across[p, j].wait_recv()
        else:
            self.carried[j].wait()
        self.diag[p, j] = self.links.push(self.block(p, j, ACROSS), self.block(p, j, DIAG), PARTNER, 'm')

    def send_o_yz(self):
        y, s = self.links.y, self.s
        self.o_copy.wait()
        self.o_yz = self.links.push(s.o_in.at[1 - y], s.o_yz, YZ, 'o_yz')

    def o_block(self, p, k):
        shard = self.s.o.shape[1] // 4
        return self.s.o.at[p, pl.ds(k * shard, shard)]

    def send_o(self, p):
        y, s = self.links.y, self.s
        if p == 0:
            self.o_yz.wait_recv()
        shard = s.o.shape[1] // 4
        seqs = shard // 2
        s.o[p, pl.ds(OWN * shard + pl.multiple_of(y * seqs, seqs), seqs), :] = s.o_in[y, p * seqs:(p + 1) * seqs]
        s.o[p, pl.ds(OWN * shard + pl.multiple_of((1 - y) * seqs, seqs), seqs), :] = s.o_yz[p * seqs:(p + 1) * seqs]
        self.o_across[p] = self.links.push(self.o_block(p, OWN), self.o_block(p, ACROSS), ACROSS, 'o')
        self.o_partner[p] = self.links.push(self.o_block(p, OWN), self.o_block(p, PARTNER), PARTNER, 'o')

    def forward_o(self, p):
        self.o_across[p].wait_recv()
        self.o_diag[p] = self.links.push(self.o_block(p, ACROSS), self.o_block(p, DIAG), PARTNER, 'o')

    def project_o(self, p):
        s = self.s
        self.o_partner[p].wait_recv()
        self.o_diag[p].wait_recv()
        if not self.wo_ready:
            self.wo.wait()
            self.wo_ready = True
        s.acc[p] += dot(s.o[p], s.wo[...])

    def down(self, p, j):
        s = self.s
        if j == 0:
            self.partner[p].wait_recv()
        self.diag[p, j].wait_recv()
        if not self.wd_ready:
            self.wd.wait()
            self.wd_ready = True
        part = dot(s.m[p, j], s.wd[j * self.cols:(j + 1) * self.cols])
        if j == 0:
            s.acc[p] = part
        else:
            s.acc[p] += part

    def send_update(self, p):
        s, links = self.s, self.links
        shard = s.acc.shape[1] // 4
        for k in range(4):
            s.update[p, pl.ds(pl.multiple_of(links.blocks[k] * shard, shard), shard), :] = s.acc[p, k * shard:(k + 1) * shard, :]
        s.up_part[p] = s.update[p].T.astype(BF16)
        part = s.up_recv.shape[1]
        src = s.up_part.at[p, pl.ds(pl.multiple_of((1 - links.y) * part, part), part)]
        self.up[p] = links.push(src, s.up_recv.at[p], YZ, 'up')

    def new_h(self, p):
        s, links = self.s, self.links
        self.up[p].wait_recv()
        part = s.up_recv.shape[1]
        own = s.up_part[p, pl.ds(pl.multiple_of(links.y * part, part), part), :]
        return (s.h_in[p].astype(F32) + (own.astype(F32) + s.up_recv[p].astype(F32))).astype(BF16)

    def sizes(self):
        s = self.s
        sent = 3 * s.m.shape[2] // 4
        shard = sent // 3
        return dict(m=s.m.at[:, :, pl.ds(0, 2 * shard)],
                m_across=s.m.at[:, pl.ds(0, self.chunks - self.carry // PARTS), pl.ds(0, shard)], o=s.o.at[:, pl.ds(0, sent)], o_yz=s.o_yz, up=s.up_recv)

    def open(self):
        links, chunks = self.links, self.chunks
        self.mix(0, 0)
        links.meet()
        self.send(0, 0)
        self.send_o_yz()
        for j in range(1, chunks):
            self.mix(0, j)
            self.send(0, j)
            if j == 2:
                self.send_o(0)
        self.send_partner(0)
        for j in range(chunks):
            self.mix(1, j)
            self.send(1, j)
            if j == 1:
                self.send_o(1)
        self.send_partner(1)
        self.h_copy.wait()


def start_kernel(names, model_dim, h_hbm, gain_hbm, wa_hbm, wm_hbm, qkv_out, zsend_out, zmine_out, h_out, *scratch):
    s = types.SimpleNamespace(**dict(zip(names, scratch)))
    links = Links(s.send, s.recv, s.local, EVERYONE)
    h_copy = links.copy(h_hbm, s.h_in)
    f = Front(links, 0, gain_hbm, wa_hbm, wm_hbm, model_dim, (qkv_out, zsend_out, zmine_out, h_out), s)
    rows = h_hbm.shape[1]
    lanes = rows // PARTS
    order = part_order(rows, False)
    h_copy.wait()
    own = dot(s.h_in[...], order)
    for p in range(PARTS):
        f.squares(p, own[:, p * lanes:(p + 1) * lanes])
    f.constants()
    links.meet()
    for p in range(PARTS):
        f.send_h(p)
    for j in range(f.chunks):
        f.split_weights(j)
    for p in range(PARTS):
        f.normalize(p)
    f.project(range(PARTS), 0)
    for p in range(PARTS):
        f.attend_core(p)
    for j in range(1, f.chunks):
        f.project(range(PARTS), j)
        if j == f.chunks - 1:
            f.attend_ends(0)
        for p in range(PARTS):
            f.combine(p, j - 1)
    f.attend_ends(1)
    for p in range(PARTS):
        f.combine(p, f.chunks - 1)
    f.take_early()
    links.drain(*f.sizes())


def middle_kernel(names, model_dim, h_hbm, o_hbm, gain_hbm, zmine_hbm, zgot_hbm, wd_hbm, wo_hbm, wa_hbm, wm_hbm, qkv_out, zsend_out,
                  zmine_out, h_out, *scratch):
    s = types.SimpleNamespace(**dict(zip(names, scratch)))
    links = Links(s.send, s.recv, s.local, EVERYONE)
    b = Back(links, 0, h_hbm, o_hbm, zgot_hbm, zmine_hbm, wd_hbm, wo_hbm, s)
    f = Front(links, 1, gain_hbm, wa_hbm, wm_hbm, model_dim, (qkv_out, zsend_out, zmine_out, h_out), s)
    b.open()
    f.constants()

    def pass_h(p):
        f.squares(p, b.new_h(p).astype(F32))
        f.send_h(p)

    first_part(b, f.split_weights)
    second_part(b, lambda: pass_h(0))
    f.normalize(0)
    f.project([0], 0)
    f.attend_core(0)
    pass_h(1)
    f.project([0], 1)
    f.project([0], 2)
    f.combine(0, 0)
    f.project([0], 3)
    f.combine(0, 1)
    f.project([0], 4)
    f.combine(0, 2)
    f.combine(0, 3)
    f.normalize(1)
    f.project([1], 0)
    f.combine(0, 4)
    f.project([1], 1)
    f.attend_core(1)
    f.attend_ends(0)
    f.project([1], 2)
    f.combine(1, 0)
    f.project([1], 3)
    f.combine(1, 1)
    f.project([1], 4)
    f.combine(1, 2)
    f.combine(1, 3)
    f.take_early()
    f.combine(1, 4)
    f.attend_ends(1)
    sent, stored = f.sizes()
    links.drain(dict(**sent, **b.sizes()), stored)


def first_part(b, filler):
    for j in range(b.chunks):
        b.forward(0, j)
        if filler is not None:
            filler(j)
        if j == 2:
            b.forward_o(0)
        if j >= 1:
            b.down(0, j - 1)
    b.project_o(0)
    b.down(0, b.chunks - 1)
    b.send_update(0)
    b.forward(1, 0)


def second_part(b, when_updated):
    for j in range(1, b.chunks):
        b.forward(1, j)
        if j == 1:
            b.forward_o(1)
        b.down(1, j - 1)
        if j == 2:
            b.project_o(1)
        if j == b.chunks - 3:
            when_updated()
    b.down(1, b.chunks - 1)
    b.send_update(1)


def end_kernel(names, h_hbm, o_hbm, zmine_hbm, zgot_hbm, wd_hbm, wo_hbm, h_out, *scratch):
    s = types.SimpleNamespace(**dict(zip(names, scratch)))
    links = Links(s.send, s.recv, s.local, [PARTNER, ACROSS, YZ])
    b = Back(links, 1, h_hbm, o_hbm, zgot_hbm, zmine_hbm, wd_hbm, wo_hbm, s)
    b.open()
    first_part(b, None)
    h_new = []
    second_part(b, lambda: h_new.append(b.new_h(0)))
    order = part_order(h_out.shape[1], True)
    h_new.append(b.new_h(1))
    h_out[...] = dot(jnp.concatenate(h_new, axis=1), order).astype(BF16)
    links.drain(b.sizes(), {})


def attention_kernel(layer, per_copy, per_step, len_hbm, qkv_hbm, k_hbm, v_hbm, *rest):
    k_out, v_out, o_hbm, kbuf, vbuf, q_scr, o_scr, qkv_ref, o_ref, len_ref, in_sem, out_sem, small_sem = rest[-13:]
    num_seqs, kv_heads, cache_len, head_dim = kbuf.shape
    slots = qkv_ref.shape[2] // head_dim
    rows = kv_heads * slots
    scale = head_dim ** -0.5

    def load(n):
        run = pl.ds(n * per_copy, per_copy)
        return (pltpu.make_async_copy(k_hbm.at[layer, run], kbuf.at[run], in_sem.at[0, n]),
                pltpu.make_async_copy(v_hbm.at[layer, run], vbuf.at[run], in_sem.at[1, n]))

    def store(n):
        run = pl.ds(n * per_copy, per_copy)
        return (pltpu.make_async_copy(kbuf.at[run], k_out.at[layer, run], out_sem.at[0, n]),
                pltpu.make_async_copy(vbuf.at[run], v_out.at[layer, run], out_sem.at[1, n]))

    qkv_copy = pltpu.make_async_copy(qkv_hbm, qkv_ref, small_sem.at[0])
    len_copy = pltpu.make_async_copy(len_hbm, len_ref, small_sem.at[1])
    qkv_copy.start()
    len_copy.start()

    @pl.loop(0, num_seqs // per_copy)
    def _(n):
        for c in load(n):
            c.start()

    qkv_copy.wait()
    len_copy.wait()
    for head in range(kv_heads):
        for j in range(slots):
            q_scr[pl.ds(head * slots + j, num_seqs, stride=rows), :] = (
                qkv_ref[head, :, j * head_dim:(j + 1) * head_dim].astype(F32))

    tile_row = lax.broadcasted_iota(jnp.int32, (16, head_dim), 0)
    position = lax.broadcasted_iota(jnp.int32, (rows, cache_len), 1)

    def patch(n):
        for c in load(n):
            c.wait()
        for sub in range(per_copy):
            i = n * per_copy + sub
            length = len_ref[i]
            base = pl.multiple_of((length // 16) * 16, 16)
            hit = tile_row == length - base
            for head in range(kv_heads):
                for buf, j in ((kbuf, slots - 2), (vbuf, slots - 1)):
                    new = q_scr[pl.ds(i * rows + head * slots + j, 1), :]
                    old = buf[i, head, pl.ds(base, 16), :].astype(F32)
                    buf[i, head, pl.ds(base, 16), :] = jnp.where(hit, new, old).astype(buf.dtype)
        for c in store(n):
            c.start()

    def attend(group):
        scores, probs = [], []
        for i in group:
            q = q_scr[pl.ds(pl.multiple_of(i * rows, rows), rows), :].astype(BF16)
            by_head = [lax.dot_general(q, kbuf[i, head], (((1,), (1,)), ((), ())), preferred_element_type=F32)
                       for head in range(kv_heads)]
            scores.append(jnp.concatenate([by_head[head][head * slots:(head + 1) * slots] for head in range(kv_heads)], axis=0))
        for i, score in zip(group, scores):
            score = jnp.where(position <= len_ref[i], score * scale, -1e30)
            e = jnp.exp(score - jnp.max(score, axis=1, keepdims=True))
            probs.append((e / jnp.sum(e, axis=1, keepdims=True)).astype(BF16))
        for i, p in zip(group, probs):
            by_head = [dot(p, vbuf[i, head]) for head in range(kv_heads)]
            o_scr[pl.ds(pl.multiple_of(i * rows, rows), rows), :] = jnp.concatenate(
                [by_head[head][head * slots:(head + 1) * slots] for head in range(kv_heads)], axis=0)

    @pl.loop(0, num_seqs // per_copy)
    def _(n):
        patch(n)
        for first in range(0, per_copy, per_step):
            attend([n * per_copy + first + sub for sub in range(per_step)])

    for head in range(kv_heads):
        for j in range(slots - 2):
            o_ref[head, :, j * head_dim:(j + 1) * head_dim] = (
                o_scr[pl.ds(head * slots + j, num_seqs, stride=rows), :].astype(o_ref.dtype))
    o_copy = pltpu.make_async_copy(o_ref, o_hbm, small_sem.at[2])
    o_copy.start()

    @pl.loop(0, num_seqs // per_copy)
    def _(n):
        for c in store(n):
            c.wait()

    o_copy.wait()


VMEM = pl.BlockSpec(memory_space=pltpu.VMEM)
HBM = pl.BlockSpec(memory_space=pltpu.HBM)


def attention(layer, lengths, qkv, k_cache, v_cache, outs):
    layers, num_seqs, kv_heads, cache_len, head_dim = k_cache.shape
    slots = qkv.shape[2] // head_dim
    rows = kv_heads * slots
    return pl.pallas_call(
        functools.partial(attention_kernel, layer, PER_COPY, PER_STEP),
        out_shape=(jax.ShapeDtypeStruct(k_cache.shape, k_cache.dtype), jax.ShapeDtypeStruct(v_cache.shape, v_cache.dtype),
                   jax.ShapeDtypeStruct((kv_heads, num_seqs, (slots - 2) * head_dim), BF16)),
        in_specs=[HBM] * (4 + len(outs)),
        out_specs=(HBM, HBM, HBM),
        scratch_shapes=[pltpu.VMEM((num_seqs, kv_heads, cache_len, head_dim), BF16)] * 2
        + [pltpu.VMEM((num_seqs * rows, head_dim), F32)] * 2 + [
            pltpu.VMEM(qkv.shape, BF16), pltpu.VMEM((kv_heads, num_seqs, (slots - 2) * head_dim), BF16),
            pltpu.SMEM((num_seqs,), jnp.int32)]
        + [pltpu.SemaphoreType.DMA((2, num_seqs // PER_COPY))] * 2 + [pltpu.SemaphoreType.DMA((3,))],
        input_output_aliases={4: 0, 5: 1} if outs else {},
        compiler_params=pltpu.CompilerParams(vmem_limit_bytes=VMEM_LIMIT),
        cost_estimate=pl.CostEstimate(flops=10 ** 10, bytes_accessed=8 * num_seqs * kv_heads * cache_len * head_dim, transcendentals=0),
        name=f'attention_{layer}',
    )(lengths, qkv, k_cache, v_cache, *outs)


def solution(mesh):
    seq_axes = ('rep', 'x', 'yz')
    hidden_spec = P('rep', ('x', 'yz'))
    cache_spec = P(None, seq_axes, None, None, None)
    in_specs = (hidden_spec, P(None, 'x'), P(None, 'x', 'yz'), P(None, 'x', None, 'yz'), P(None, 'yz', 'x'), P(None, 'yz', 'x'), cache_spec, cache_spec, P(seq_axes))
    out_specs = (hidden_spec, cache_spec, cache_spec)
    swap = [(0, 2), (2, 0), (1, 3), (3, 1)]

    def device_step(hidden, norm_gain, w_attn, w_mlp, w_out, w_down, k_cache, v_cache, lengths):
        rows, part = hidden.shape
        depth, attn_cols = w_attn.shape[1:]
        model_dim = depth * mesh.shape['x']
        mlp_cols = w_mlp.shape[3]
        out_depth = w_out.shape[1]
        cols = mlp_cols // CHUNKS
        units = CHUNKS * PARTS
        lanes = rows // PARTS
        half, shard = lanes // 2, lanes // 4
        seqs = shard // 2
        num_seqs = PARTS * seqs

        def semaphores(groups, remote, local):
            return dict(send=pltpu.SemaphoreType.DMA((groups,)), recv=pltpu.SemaphoreType.DMA((remote,)),
                    local=pltpu.SemaphoreType.DMA((local,)))

        def front_scratch(layer):
            return dict(
                sq_send=pltpu.VMEM((PARTS, SQ_ROWS, lanes), F32), sq_recv=pltpu.VMEM((PARTS, 8, SQ_ROWS, lanes), F32),
                h=pltpu.VMEM((PARTS, depth, lanes), BF16), gain_in=pltpu.VMEM(norm_gain.shape, BF16), gain=pltpu.VMEM((depth, lanes), F32),
                u=pltpu.VMEM((PARTS, lanes, depth), BF16), u_rel=pltpu.VMEM((PARTS, lanes, depth), BF16),
                wa=pltpu.VMEM((depth, attn_cols), BF16), wm=pltpu.VMEM((depth, 2, mlp_cols), BF16),
                w_split=pltpu.VMEM((2, depth, mlp_cols), BF16),
                a_part=pltpu.VMEM((PARTS, lanes, attn_cols), BF16), a_core=pltpu.VMEM((PARTS, half, attn_cols), BF16),
                a_sum=pltpu.VMEM((PARTS, half, attn_cols), BF16), a_got=pltpu.VMEM((PARTS, 3, seqs, attn_cols), BF16),
                a_full=pltpu.VMEM((PARTS, 2, seqs, attn_cols), BF16),
                z_part=pltpu.VMEM((PARTS, CHUNKS, 2 * lanes, cols), BF16),
                z_recv=pltpu.VMEM((PARTS, CHUNKS, lanes, cols), BF16), z_x=pltpu.VMEM((units, half, cols), BF16),
                z_mine=pltpu.VMEM((units, half, cols), BF16), z_early=pltpu.VMEM((EARLY[layer], half, cols), BF16),
            )

        back_scratch = dict(
            o_yz=pltpu.VMEM((num_seqs, out_depth), BF16), o=pltpu.VMEM((PARTS, lanes, out_depth), BF16),
            m=pltpu.VMEM((PARTS, CHUNKS, lanes, cols), BF16), z_in=pltpu.VMEM((units, half, cols), BF16),
            o_in=pltpu.VMEM((2, num_seqs, out_depth), BF16),
            h_in=pltpu.VMEM((PARTS, part, lanes), BF16),
            wd=pltpu.VMEM((mlp_cols, depth), BF16), wo=pltpu.VMEM((out_depth, depth), BF16),
            acc=pltpu.VMEM((PARTS, lanes, depth), F32), update=pltpu.VMEM((PARTS, lanes, depth), F32),
            up_part=pltpu.VMEM((PARTS, depth, lanes), BF16), up_recv=pltpu.VMEM((PARTS, part, lanes), BF16),
        )

        def got_scratch(layer):
            return dict(z_got=pltpu.VMEM((units - EARLY[layer], half, cols), BF16))

        def front_shapes(layer):
            return (
                jax.ShapeDtypeStruct((2, num_seqs, attn_cols), BF16), jax.ShapeDtypeStruct((units - EARLY[layer] + CARRY[layer] // PARTS, half, cols), BF16),
                jax.ShapeDtypeStruct((units, half, cols), BF16), jax.ShapeDtypeStruct((PARTS, part, lanes), BF16))
        front_specs = (HBM,) * 4

        def call(kernel, name, collective_id, scratch, in_specs, out_shape, out_specs, *args):
            return pl.pallas_call(
                functools.partial(kernel, tuple(scratch)), out_shape=out_shape, in_specs=list(in_specs), out_specs=out_specs,
                scratch_shapes=list(scratch.values()), name=name,
                compiler_params=pltpu.CompilerParams(collective_id=collective_id, has_side_effects=True, vmem_limit_bytes=END_VMEM_LIMIT if kernel is end_kernel else VMEM_LIMIT),
            )(*args)

        def start(names, *refs):
            start_kernel(names, model_dim, *refs)

        def middle(names, *refs):
            middle_kernel(names, model_dim, *refs)

        qkv, zsend, zmine, h_block = call(
            start, 'start', 0, dict(**semaphores(6, 34 + EARLY[0], 8), **front_scratch(0), h_in=pltpu.VMEM((part, rows), BF16)), (HBM,) * 4,
            front_shapes(0), front_specs, hidden.T, norm_gain, w_attn, w_mlp)
        zgot = lax.ppermute(zsend, 'x', swap)
        k_new, v_new, o = attention(0, lengths, qkv, k_cache, v_cache, ())
        qkv, zsend, zmine, h_block = call(
            middle, 'middle', 1, dict(**semaphores(11, 65 + EARLY[1], 17), **front_scratch(1), **back_scratch, **got_scratch(0),
                       m_early=pltpu.VMEM((half, cols), BF16)), (HBM,) * 9,
            front_shapes(1), front_specs, h_block, o, norm_gain, zmine, zgot, w_down, w_out, w_attn, w_mlp)
        zgot = lax.ppermute(zsend, 'x', swap)
        k_new, v_new, o = attention(1, lengths, qkv, k_cache, v_cache, (k_new, v_new))
        h_out = call(
            end_kernel, 'end', 2, dict(**semaphores(5, 29, 11), **back_scratch, **got_scratch(1)), (HBM,) * 6,
            jax.ShapeDtypeStruct((part, rows), BF16), VMEM, h_block, o, zmine, zgot, w_down, w_out)
        return h_out.T, k_new, v_new

    return jax.shard_map(device_step, mesh=mesh, in_specs=in_specs, out_specs=out_specs, check_vma=False)
```

```python
import functools
import types

import jax
import jax.numpy as jnp
from jax import lax
from jax.experimental import pallas as pl
from jax.experimental.pallas import tpu as pltpu
from jax.sharding import PartitionSpec as P

NORM_EPS = 1e-5
MESH = pl.DeviceIdType.MESH
BF16 = jnp.bfloat16
F32 = jnp.float32

SQ_ROWS = 1
PER_COPY = 4
PER_STEP = 2
CHUNKS = 5
EARLY = (1, 2)
CARRY = (0, 2)
END_VMEM_LIMIT = 56393728
VMEM_LIMIT = 67043328


def dot(a, b):
    return jnp.dot(a, b, preferred_element_type=F32)


class Links:
    def __init__(self, send_sems, recv_sems, local_sems, peers):
        self.send_sems, self.recv_sems, self.local_sems = send_sems, recv_sems, local_sems
        self.groups, self.used, self.local_groups, self.local_used = {}, 0, {}, 0
        x, y = lax.axis_index('x'), lax.axis_index('yz')
        self.x, self.y = x, y
        core = lax.rem(x, 2)
        self.along_x = (3 - x, x + 1 - 2 * core, lax.rem(x + 2, 4))
        self.blocks = self.along_x + (x,)
        self.targets = tuple({'x': p, 'yz': y} for p in self.blocks) + ({'x': x, 'yz': 1 - y},) + tuple(
            {'x': p, 'yz': 1 - y} for p in self.along_x)
        self.peers = peers
        self.barrier = pltpu.get_barrier_semaphore()
        for k in self.peers:
            pl.semaphore_signal(self.barrier, inc=1, device_id=self.targets[k], device_id_type=MESH)

    def meet(self):
        pl.semaphore_wait(self.barrier, len(self.peers))

    def push(self, src, dst, to, group):
        k = self.used
        self.used += 1
        g = self.groups.setdefault(group, len(self.groups))
        copy = pltpu.make_async_remote_copy(
            src_ref=src, dst_ref=dst, send_sem=self.send_sems.at[g], recv_sem=self.recv_sems.at[k],
            device_id=self.targets[to], device_id_type=MESH)
        copy.start()
        return copy

    def copy(self, src, dst, group=None):
        if group is None or group not in self.local_groups:
            k = self.local_used
            self.local_used += 1
            if group is not None:
                self.local_groups[group] = k
        else:
            k = self.local_groups[group]
        copy = pltpu.make_async_copy(src, dst, self.local_sems.at[k])
        copy.start()
        return copy

    def drain(self, sent, stored):
        for group, g in self.groups.items():
            pltpu.make_async_copy(sent[group], sent[group], self.send_sems.at[g]).wait()
        for group, k in self.local_groups.items():
            pltpu.make_async_copy(stored[group], stored[group], self.local_sems.at[k]).wait()


DIAG, PARTNER, ACROSS, OWN, YZ, ACROSS_YZ = 0, 1, 2, 3, 4, 7
EVERYONE = [k for k in range(8) if k != OWN]
PARTS = 2


def gated(z):
    shard = z.shape[0] // 2
    gate, up = z[:shard].astype(F32), z[shard:].astype(F32)
    return (gate * jax.nn.sigmoid(gate) * up).astype(BF16)


def part_order(rows, inverse):
    i = lax.broadcasted_iota(jnp.int32, (rows, rows), 0)
    j = lax.broadcasted_iota(jnp.int32, (rows, rows), 1)
    src, dst = (j, i) if inverse else (i, j)
    run = rows // (8 * PARTS)
    piece = src // run
    place = lax.rem(piece, PARTS) * (8 * run) + (piece // PARTS) * run + lax.rem(src, run)
    return jnp.where(dst == place, jnp.ones((), F32), jnp.zeros((), F32)).astype(BF16)


class Front:
    def __init__(self, links, layer, gain_hbm, wa_hbm, wm_hbm, model_dim, outs, s):
        self.links, self.s, self.layer, self.model_dim = links, s, layer, model_dim
        self.kept, self.carry = EARLY[layer], CARRY[layer]
        self.gain_copy = links.copy(gain_hbm, s.gain_in)
        self.qkv_out, self.zsend_out, self.zmine_out, self.h_out = outs
        self.chunks, self.cols = s.z_recv.shape[1], s.z_recv.shape[3]
        self.depth = s.wa.shape[0]
        self.wa = links.copy(wa_hbm.at[layer], s.wa)
        self.wm = links.copy(wm_hbm.at[layer], s.wm)
        self.wa_ready = False
        part = self.depth // 2
        self.mine = pl.ds(pl.multiple_of(links.y * part, part), part)
        self.h_yz = {}
        self.a_core, self.a_got, self.z_core, self.early = {}, {}, {}, {}
        self.sq = {}

    def constants(self):
        lanes = self.s.u.shape[1]
        self.gain_copy.wait()
        gain = jnp.broadcast_to(self.s.gain_in[self.layer:self.layer + 1, :].astype(F32), (lanes, self.depth)).T
        self.s.gain[...] = gain

    def squares(self, p, h_t):
        s = self.s
        s.h[p, self.mine, :] = h_t.astype(BF16)
        s.sq_send[p] = jnp.broadcast_to(jnp.sum(h_t * h_t, axis=0, keepdims=True), s.sq_send.shape[1:])

    def send_h(self, p):
        s, links = self.s, self.links
        self.sq[p] = [links.push(s.sq_send.at[p], s.sq_recv.at[p, k], k, 'sq') for k in EVERYONE]
        self.h_yz[p] = links.push(s.h.at[p, self.mine], s.h.at[p, self.mine], YZ, 'h')
        links.copy(s.h.at[p, self.mine], self.h_out.at[p], 'h')

    def normalize(self, p):
        s, links = self.s, self.links
        for c in self.sq[p]:
            c.wait_recv()
        total = s.sq_send[p]
        for k in EVERYONE:
            total = total + s.sq_recv[p, k]
        self.h_yz[p].wait_recv()
        h_t = s.h[p].astype(F32)
        inv_rms = lax.rsqrt(total[:1] / self.model_dim + NORM_EPS)
        s.u[p] = (h_t * inv_rms * s.gain[...]).T.astype(BF16)
        shard = s.u.shape[1] // 4
        u = jnp.concatenate([s.u[p, pl.ds(pl.multiple_of(b * shard, shard), shard), :] for b in links.blocks], axis=0)
        s.u_rel[p] = u
        if not self.wa_ready:
            self.wa.wait()
            self.wa_ready = True
        s.a_part[p] = dot(u, s.wa[...]).astype(BF16)
        self.a_core[p] = links.push(s.a_part.at[p, pl.ds(0, 2 * shard)], s.a_core.at[p], PARTNER, 'a_core')

    def attend_core(self, p):
        s = self.s
        half = s.a_core.shape[1]
        self.a_core[p].wait_recv()
        s.a_sum[p] = (s.a_part[p, half:].astype(F32) + s.a_core[p].astype(F32)).astype(BF16)
        shard, seqs = half // 2, s.a_got.shape[2]
        y = self.links.y
        here, there = pl.multiple_of(y * seqs, seqs), pl.multiple_of((1 - y) * seqs, seqs)
        self.a_got[p] = [
            self.links.push(s.a_sum.at[p, pl.ds(there, seqs)], s.a_got.at[p, 2], ACROSS_YZ, 'a_got'),
            self.links.push(s.a_sum.at[p, pl.ds(here, seqs)], s.a_got.at[p, 0], ACROSS, 'a_got'),
            self.links.push(s.a_sum.at[p, pl.ds(shard + there, seqs)], s.a_got.at[p, 1], YZ, 'a_got')]

    def attend_ends(self, p):
        s, y = self.s, self.links.y
        shard, seqs = s.a_sum.shape[1] // 2, s.a_got.shape[2]
        for c in self.a_got[p]:
            c.wait_recv()
        own = s.a_sum[p, pl.ds(shard + pl.multiple_of(y * seqs, seqs), seqs), :]
        s.a_full[p, 0] = (own.astype(F32) + s.a_got[p, 0].astype(F32)).astype(BF16)
        s.a_full[p, 1] = (s.a_got[p, 1].astype(F32) + s.a_got[p, 2].astype(F32)).astype(BF16)
        for k, head in enumerate((y, 1 - y)):
            self.links.copy(s.a_full.at[p, k], self.qkv_out.at[head, pl.ds(p * seqs, seqs)], 'qkv')

    def split_weights(self, c):
        s, run = self.s, 128
        i = lax.broadcasted_iota(jnp.int32, (2 * run, 2 * run), 0)
        j = lax.broadcasted_iota(jnp.int32, (2 * run, 2 * run), 1)
        place = jnp.where(i < run, 2 * i, 2 * (i - run) + 1)
        order = jnp.where(j == place, jnp.ones((), F32), jnp.zeros((), F32)).astype(BF16)
        if c == 0:
            self.wm.wait()
        cols = slice(c * self.cols, (c + 1) * self.cols)
        for e in range(self.depth // run):
            rows = slice(e * run, (e + 1) * run)
            w = dot(order, s.wm[rows, :, cols].reshape(2 * run, self.cols)).astype(BF16)
            s.w_split[0, rows, cols] = w[:run]
            s.w_split[1, rows, cols] = w[run:]

    def project(self, parts, j):
        s = self.s
        lanes = s.u.shape[1]
        shard = lanes // 4
        u = jnp.concatenate([s.u_rel[p] for p in parts], axis=0)
        cols = slice(j * self.cols, (j + 1) * self.cols)
        gate, up = dot(u, s.w_split[0, :, cols]).astype(BF16), dot(u, s.w_split[1, :, cols]).astype(BF16)
        for n, p in enumerate(parts):
            for k in range(4):
                rows = slice(n * lanes + k * shard, n * lanes + (k + 1) * shard)
                s.z_part[p, j, 2 * k * shard:(2 * k + 1) * shard] = gate[rows]
                s.z_part[p, j, (2 * k + 1) * shard:(2 * k + 2) * shard] = up[rows]
            self.push_core(p, j)

    def push_core(self, p, j):
        s = self.s
        half = s.z_recv.shape[2]
        self.z_core[p, j] = self.links.push(s.z_part.at[p, j, pl.ds(0, half)], s.z_recv.at[p, j], PARTNER, 'z')

    def combine(self, p, j):
        s, unit = self.s, p * self.chunks + j
        half = s.z_recv.shape[2]
        shard2 = half // 2
        self.z_core[p, j].wait_recv()
        s.z_x[unit] = (s.z_part[p, j, half:half + shard2].astype(F32) + s.z_recv[p, j, :shard2].astype(F32)).astype(BF16)
        if unit < self.kept:
            self.early[unit] = self.links.push(s.z_x.at[unit], s.z_early.at[unit], ACROSS, 'early')
        else:
            self.links.copy(s.z_x.at[unit], self.zsend_out.at[unit - self.kept], 'z_x')
        s.z_mine[unit] = (s.z_part[p, j, half + shard2:].astype(F32) + s.z_recv[p, j, shard2:].astype(F32)).astype(BF16)
        if unit >= self.kept:
            self.links.copy(s.z_mine.at[unit], self.zmine_out.at[unit], 'z_mine')

    def take_early(self):
        s = self.s
        for unit in range(self.kept):
            self.early[unit].wait_recv()
            s.z_mine[unit] = (s.z_mine[unit].astype(F32) + s.z_early[unit].astype(F32)).astype(BF16)
            self.links.copy(s.z_mine.at[unit], self.zmine_out.at[unit], 'z_mine')
        if self.carry:
            shard = s.z_mine.shape[1] // 2
            for unit in range(self.carry):
                s.m_early[unit * shard:(unit + 1) * shard] = gated(s.z_mine[unit])
            self.links.copy(s.m_early, self.zsend_out.at[s.z_x.shape[0] - self.kept], 'm_early')

    def sizes(self):
        s = self.s
        return (dict(a_core=s.a_core, a_got=s.a_got, z=s.z_recv, early=s.z_early,
                 sq=s.sq_recv.at[:, pl.ds(0, len(EVERYONE))], h=s.h.at[:, self.mine]),
                dict(z_x=s.z_x.at[pl.ds(self.kept, s.z_x.shape[0] - self.kept)], z_mine=s.z_mine, qkv=s.a_full, h=s.h.at[:, self.mine], m_early=getattr(s, 'm_early', None)))


class Back:
    def __init__(self, links, layer, h_hbm, o_hbm, zgot_hbm, zmine_hbm, wd_hbm, wo_hbm, s):
        self.links, self.s = links, s
        self.kept, self.carry = EARLY[layer], CARRY[layer]
        self.chunks, self.cols = s.m.shape[1], s.m.shape[3]
        units = PARTS * self.chunks
        shard = s.m.shape[2] // 4
        self.z = []
        for first, last in ((0, 1), (1, self.chunks), (self.chunks, units)):
            run = pl.ds(first, last - first)
            self.z.append((first, links.copy(zmine_hbm.at[run], s.z_in.at[run])))
            start = max(first, self.kept)
            if start < last:
                run = pl.ds(start - self.kept, last - start)
                self.z.append((start, links.copy(zgot_hbm.at[run], s.z_got.at[run])))
            if first == 0:
                self.carried = [links.copy(zgot_hbm.at[units - self.kept, pl.ds(j * shard, shard)], self.block(0, j, ACROSS))
                                for j in range(self.carry)]
                self.o_copy = links.copy(o_hbm, s.o_in)
                self.h_copy = links.copy(h_hbm, s.h_in)
        self.wd = links.copy(wd_hbm.at[layer], s.wd)
        self.wo = links.copy(wo_hbm.at[layer], s.wo)
        self.wo_ready, self.wd_ready = False, False
        self.across, self.partner, self.diag = {}, {}, {}
        self.o_across, self.o_partner, self.o_diag = {}, {}, {}
        self.up = {}

    def mix(self, p, j):
        s, unit = self.s, p * self.chunks + j
        while self.z and self.z[0][0] <= unit:
            self.z.pop(0)[1].wait()
        z = s.z_in[unit]
        if unit >= self.kept:
            z = (z.astype(F32) + s.z_got[unit - self.kept].astype(F32)).astype(BF16)
        s.m[p, j, OWN * (z.shape[0] // 2):] = gated(z)

    def block(self, p, j, k):
        shard = self.s.m.shape[2] // 4
        return self.s.m.at[p, j, pl.ds(k * shard, shard)]

    def send(self, p, j):
        if p > 0 or j >= self.carry:
            self.across[p, j] = self.links.push(self.block(p, j, OWN), self.block(p, j, ACROSS), ACROSS, 'm_across')

    def send_partner(self, p):
        m = self.s.m
        shard = m.shape[2] // 4
        self.partner[p] = self.links.push(m.at[p, :, pl.ds(OWN * shard, shard)], m.at[p, :, pl.ds(PARTNER * shard, shard)], PARTNER, 'm')

    def forward(self, p, j):
        if p > 0 or j >= self.carry:
            self.across[p, j].wait_recv()
        else:
            self.carried[j].wait()
        self.diag[p, j] = self.links.push(self.block(p, j, ACROSS), self.block(p, j, DIAG), PARTNER, 'm')

    def send_o_yz(self):
        y, s = self.links.y, self.s
        self.o_copy.wait()
        self.o_yz = self.links.push(s.o_in.at[1 - y], s.o_yz, YZ, 'o_yz')

    def o_block(self, p, k):
        shard = self.s.o.shape[1] // 4
        return self.s.o.at[p, pl.ds(k * shard, shard)]

    def send_o(self, p):
        y, s = self.links.y, self.s
        if p == 0:
            self.o_yz.wait_recv()
        shard = s.o.shape[1] // 4
        seqs = shard // 2
        s.o[p, pl.ds(OWN * shard + pl.multiple_of(y * seqs, seqs), seqs), :] = s.o_in[y, p * seqs:(p + 1) * seqs]
        s.o[p, pl.ds(OWN * shard + pl.multiple_of((1 - y) * seqs, seqs), seqs), :] = s.o_yz[p * seqs:(p + 1) * seqs]
        self.o_across[p] = self.links.push(self.o_block(p, OWN), self.o_block(p, ACROSS), ACROSS, 'o')
        self.o_partner[p] = self.links.push(self.o_block(p, OWN), self.o_block(p, PARTNER), PARTNER, 'o')

    def forward_o(self, p):
        self.o_across[p].wait_recv()
        self.o_diag[p] = self.links.push(self.o_block(p, ACROSS), self.o_block(p, DIAG), PARTNER, 'o')

    def project_o(self, p):
        s = self.s
        self.o_partner[p].wait_recv()
        self.o_diag[p].wait_recv()
        if not self.wo_ready:
            self.wo.wait()
            self.wo_ready = True
        s.acc[p] += dot(s.o[p], s.wo[...])

    def down(self, p, j):
        s = self.s
        if j == 0:
            self.partner[p].wait_recv()
        self.diag[p, j].wait_recv()
        if not self.wd_ready:
            self.wd.wait()
            self.wd_ready = True
        part = dot(s.m[p, j], s.wd[j * self.cols:(j + 1) * self.cols])
        if j == 0:
            s.acc[p] = part
        else:
            s.acc[p] += part

    def send_update(self, p):
        s, links = self.s, self.links
        shard = s.acc.shape[1] // 4
        for k in range(4):
            s.update[p, pl.ds(pl.multiple_of(links.blocks[k] * shard, shard), shard), :] = s.acc[p, k * shard:(k + 1) * shard, :]
        s.up_part[p] = s.update[p].T.astype(BF16)
        part = s.up_recv.shape[1]
        src = s.up_part.at[p, pl.ds(pl.multiple_of((1 - links.y) * part, part), part)]
        self.up[p] = links.push(src, s.up_recv.at[p], YZ, 'up')

    def new_h(self, p):
        s, links = self.s, self.links
        self.up[p].wait_recv()
        part = s.up_recv.shape[1]
        own = s.up_part[p, pl.ds(pl.multiple_of(links.y * part, part), part), :]
        return (s.h_in[p].astype(F32) + (own.astype(F32) + s.up_recv[p].astype(F32))).astype(BF16)

    def sizes(self):
        s = self.s
        sent = 3 * s.m.shape[2] // 4
        shard = sent // 3
        return dict(m=s.m.at[:, :, pl.ds(0, 2 * shard)],
                m_across=s.m.at[:, pl.ds(0, self.chunks - self.carry // PARTS), pl.ds(0, shard)], o=s.o.at[:, pl.ds(0, sent)], o_yz=s.o_yz, up=s.up_recv)

    def open(self):
        links, chunks = self.links, self.chunks
        self.mix(0, 0)
        links.meet()
        self.send(0, 0)
        self.send_o_yz()
        for j in range(1, chunks):
            self.mix(0, j)
            self.send(0, j)
            if j == 2 + self.carry:
                self.send_o(0)
        self.send_partner(0)
        for j in range(chunks):
            self.mix(1, j)
            self.send(1, j)
            if j == 1:
                self.send_o(1)
        self.send_partner(1)
        self.h_copy.wait()


def start_kernel(names, model_dim, h_hbm, gain_hbm, wa_hbm, wm_hbm, qkv_out, zsend_out, zmine_out, h_out, *scratch):
    s = types.SimpleNamespace(**dict(zip(names, scratch)))
    links = Links(s.send, s.recv, s.local, EVERYONE)
    h_copy = links.copy(h_hbm, s.h_in)
    f = Front(links, 0, gain_hbm, wa_hbm, wm_hbm, model_dim, (qkv_out, zsend_out, zmine_out, h_out), s)
    rows = h_hbm.shape[1]
    lanes = rows // PARTS
    order = part_order(rows, False)
    h_copy.wait()
    own = dot(s.h_in[...], order)
    for p in range(PARTS):
        f.squares(p, own[:, p * lanes:(p + 1) * lanes])
    f.constants()
    links.meet()
    for p in range(PARTS):
        f.send_h(p)
    for j in range(f.chunks):
        f.split_weights(j)
    for p in range(PARTS):
        f.normalize(p)
    f.project(range(PARTS), 0)
    for p in range(PARTS):
        f.attend_core(p)
    for j in range(1, f.chunks):
        f.project(range(PARTS), j)
        if j == f.chunks - 1:
            f.attend_ends(0)
        for p in range(PARTS):
            f.combine(p, j - 1)
    f.attend_ends(1)
    for p in range(PARTS):
        f.combine(p, f.chunks - 1)
    f.take_early()
    links.drain(*f.sizes())


def middle_kernel(names, model_dim, h_hbm, o_hbm, gain_hbm, zmine_hbm, zgot_hbm, wd_hbm, wo_hbm, wa_hbm, wm_hbm, qkv_out, zsend_out,
                  zmine_out, h_out, *scratch):
    s = types.SimpleNamespace(**dict(zip(names, scratch)))
    links = Links(s.send, s.recv, s.local, EVERYONE)
    b = Back(links, 0, h_hbm, o_hbm, zgot_hbm, zmine_hbm, wd_hbm, wo_hbm, s)
    f = Front(links, 1, gain_hbm, wa_hbm, wm_hbm, model_dim, (qkv_out, zsend_out, zmine_out, h_out), s)
    b.open()
    f.constants()

    def pass_h(p):
        f.squares(p, b.new_h(p).astype(F32))
        f.send_h(p)

    first_part(b, f.split_weights)
    second_part(b, lambda: pass_h(0))
    f.normalize(0)
    f.project([0], 0)
    f.attend_core(0)
    pass_h(1)
    f.project([0], 1)
    f.project([0], 2)
    f.combine(0, 0)
    f.project([0], 3)
    f.combine(0, 1)
    f.project([0], 4)
    f.combine(0, 2)
    f.combine(0, 3)
    f.normalize(1)
    f.project([1], 0)
    f.combine(0, 4)
    f.project([1], 1)
    f.attend_core(1)
    f.attend_ends(0)
    f.project([1], 2)
    f.combine(1, 0)
    f.project([1], 3)
    f.combine(1, 1)
    f.project([1], 4)
    f.combine(1, 2)
    f.combine(1, 3)
    f.take_early()
    f.combine(1, 4)
    f.attend_ends(1)
    sent, stored = f.sizes()
    links.drain(dict(**sent, **b.sizes()), stored)


def first_part(b, filler):
    for j in range(b.chunks):
        b.forward(0, j)
        if filler is not None:
            filler(j)
        if j == 2 + b.carry:
            b.forward_o(0)
        if j >= 1:
            b.down(0, j - 1)
    b.project_o(0)
    b.down(0, b.chunks - 1)
    b.send_update(0)
    b.forward(1, 0)


def second_part(b, when_updated):
    for j in range(1, b.chunks):
        b.forward(1, j)
        if j == 1:
            b.forward_o(1)
        b.down(1, j - 1)
        if j == 2:
            b.project_o(1)
        if j == b.chunks - 3:
            when_updated()
    b.down(1, b.chunks - 1)
    b.send_update(1)


def end_kernel(names, h_hbm, o_hbm, zmine_hbm, zgot_hbm, wd_hbm, wo_hbm, h_out, *scratch):
    s = types.SimpleNamespace(**dict(zip(names, scratch)))
    links = Links(s.send, s.recv, s.local, [PARTNER, ACROSS, YZ])
    b = Back(links, 1, h_hbm, o_hbm, zgot_hbm, zmine_hbm, wd_hbm, wo_hbm, s)
    b.open()
    first_part(b, None)
    h_new = []
    second_part(b, lambda: h_new.append(b.new_h(0)))
    order = part_order(h_out.shape[1], True)
    h_new.append(b.new_h(1))
    h_out[...] = dot(jnp.concatenate(h_new, axis=1), order).astype(BF16)
    links.drain(b.sizes(), {})


def attention_kernel(layer, per_copy, per_step, len_hbm, qkv_hbm, k_hbm, v_hbm, *rest):
    k_out, v_out, o_hbm, kbuf, vbuf, q_scr, o_scr, qkv_ref, o_ref, len_ref, in_sem, out_sem, small_sem = rest[-13:]
    num_seqs, kv_heads, cache_len, head_dim = kbuf.shape
    slots = qkv_ref.shape[2] // head_dim
    rows = kv_heads * slots
    scale = head_dim ** -0.5

    def load(n):
        run = pl.ds(n * per_copy, per_copy)
        return (pltpu.make_async_copy(k_hbm.at[layer, run], kbuf.at[run], in_sem.at[0, n]),
                pltpu.make_async_copy(v_hbm.at[layer, run], vbuf.at[run], in_sem.at[1, n]))

    def store(n):
        run = pl.ds(n * per_copy, per_copy)
        return (pltpu.make_async_copy(kbuf.at[run], k_out.at[layer, run], out_sem.at[0, n]),
                pltpu.make_async_copy(vbuf.at[run], v_out.at[layer, run], out_sem.at[1, n]))

    qkv_copy = pltpu.make_async_copy(qkv_hbm, qkv_ref, small_sem.at[0])
    len_copy = pltpu.make_async_copy(len_hbm, len_ref, small_sem.at[1])
    qkv_copy.start()
    len_copy.start()

    @pl.loop(0, num_seqs // per_copy)
    def _(n):
        for c in load(n):
            c.start()

    qkv_copy.wait()
    len_copy.wait()
    for head in range(kv_heads):
        for j in range(slots):
            q_scr[pl.ds(head * slots + j, num_seqs, stride=rows), :] = (
                qkv_ref[head, :, j * head_dim:(j + 1) * head_dim].astype(F32))

    tile_row = lax.broadcasted_iota(jnp.int32, (16, head_dim), 0)
    position = lax.broadcasted_iota(jnp.int32, (rows, cache_len), 1)

    def patch(n):
        for c in load(n):
            c.wait()
        for sub in range(per_copy):
            i = n * per_copy + sub
            length = len_ref[i]
            base = pl.multiple_of((length // 16) * 16, 16)
            hit = tile_row == length - base
            for head in range(kv_heads):
                for buf, j in ((kbuf, slots - 2), (vbuf, slots - 1)):
                    new = q_scr[pl.ds(i * rows + head * slots + j, 1), :]
                    old = buf[i, head, pl.ds(base, 16), :].astype(F32)
                    buf[i, head, pl.ds(base, 16), :] = jnp.where(hit, new, old).astype(buf.dtype)
        for c in store(n):
            c.start()

    def attend(group):
        scores, probs = [], []
        for i in group:
            q = q_scr[pl.ds(pl.multiple_of(i * rows, rows), rows), :].astype(BF16)
            by_head = [lax.dot_general(q, kbuf[i, head], (((1,), (1,)), ((), ())), preferred_element_type=F32)
                       for head in range(kv_heads)]
            scores.append(jnp.concatenate([by_head[head][head * slots:(head + 1) * slots] for head in range(kv_heads)], axis=0))
        for i, score in zip(group, scores):
            score = jnp.where(position <= len_ref[i], score * scale, -1e30)
            e = jnp.exp(score - jnp.max(score, axis=1, keepdims=True))
            probs.append((e / jnp.sum(e, axis=1, keepdims=True)).astype(BF16))
        for i, p in zip(group, probs):
            by_head = [dot(p, vbuf[i, head]) for head in range(kv_heads)]
            o_scr[pl.ds(pl.multiple_of(i * rows, rows), rows), :] = jnp.concatenate(
                [by_head[head][head * slots:(head + 1) * slots] for head in range(kv_heads)], axis=0)

    @pl.loop(0, num_seqs // per_copy)
    def _(n):
        patch(n)
        for first in range(0, per_copy, per_step):
            attend([n * per_copy + first + sub for sub in range(per_step)])

    for head in range(kv_heads):
        for j in range(slots - 2):
            o_ref[head, :, j * head_dim:(j + 1) * head_dim] = (
                o_scr[pl.ds(head * slots + j, num_seqs, stride=rows), :].astype(o_ref.dtype))
    o_copy = pltpu.make_async_copy(o_ref, o_hbm, small_sem.at[2])
    o_copy.start()

    @pl.loop(0, num_seqs // per_copy)
    def _(n):
        for c in store(n):
            c.wait()

    o_copy.wait()


VMEM = pl.BlockSpec(memory_space=pltpu.VMEM)
HBM = pl.BlockSpec(memory_space=pltpu.HBM)


def attention(layer, lengths, qkv, k_cache, v_cache, outs):
    layers, num_seqs, kv_heads, cache_len, head_dim = k_cache.shape
    slots = qkv.shape[2] // head_dim
    rows = kv_heads * slots
    return pl.pallas_call(
        functools.partial(attention_kernel, layer, PER_COPY, PER_STEP),
        out_shape=(jax.ShapeDtypeStruct(k_cache.shape, k_cache.dtype), jax.ShapeDtypeStruct(v_cache.shape, v_cache.dtype),
                   jax.ShapeDtypeStruct((kv_heads, num_seqs, (slots - 2) * head_dim), BF16)),
        in_specs=[HBM] * (4 + len(outs)),
        out_specs=(HBM, HBM, HBM),
        scratch_shapes=[pltpu.VMEM((num_seqs, kv_heads, cache_len, head_dim), BF16)] * 2
        + [pltpu.VMEM((num_seqs * rows, head_dim), F32)] * 2 + [
            pltpu.VMEM(qkv.shape, BF16), pltpu.VMEM((kv_heads, num_seqs, (slots - 2) * head_dim), BF16),
            pltpu.SMEM((num_seqs,), jnp.int32)]
        + [pltpu.SemaphoreType.DMA((2, num_seqs // PER_COPY))] * 2 + [pltpu.SemaphoreType.DMA((3,))],
        input_output_aliases={4: 0, 5: 1} if outs else {},
        compiler_params=pltpu.CompilerParams(vmem_limit_bytes=VMEM_LIMIT),
        cost_estimate=pl.CostEstimate(flops=10 ** 10, bytes_accessed=8 * num_seqs * kv_heads * cache_len * head_dim, transcendentals=0),
        name=f'attention_{layer}',
    )(lengths, qkv, k_cache, v_cache, *outs)


def solution(mesh):
    seq_axes = ('rep', 'x', 'yz')
    hidden_spec = P('rep', ('x', 'yz'))
    cache_spec = P(None, seq_axes, None, None, None)
    in_specs = (hidden_spec, P(None, 'x'), P(None, 'x', 'yz'), P(None, 'x', None, 'yz'), P(None, 'yz', 'x'), P(None, 'yz', 'x'), cache_spec, cache_spec, P(seq_axes))
    out_specs = (hidden_spec, cache_spec, cache_spec)
    swap = [(0, 2), (2, 0), (1, 3), (3, 1)]

    def device_step(hidden, norm_gain, w_attn, w_mlp, w_out, w_down, k_cache, v_cache, lengths):
        rows, part = hidden.shape
        depth, attn_cols = w_attn.shape[1:]
        model_dim = depth * mesh.shape['x']
        mlp_cols = w_mlp.shape[3]
        out_depth = w_out.shape[1]
        cols = mlp_cols // CHUNKS
        units = CHUNKS * PARTS
        lanes = rows // PARTS
        half, shard = lanes // 2, lanes // 4
        seqs = shard // 2
        num_seqs = PARTS * seqs

        def semaphores(groups, remote, local):
            return dict(send=pltpu.SemaphoreType.DMA((groups,)), recv=pltpu.SemaphoreType.DMA((remote,)),
                    local=pltpu.SemaphoreType.DMA((local,)))

        def front_scratch(layer):
            return dict(
                sq_send=pltpu.VMEM((PARTS, SQ_ROWS, lanes), F32), sq_recv=pltpu.VMEM((PARTS, 8, SQ_ROWS, lanes), F32),
                h=pltpu.VMEM((PARTS, depth, lanes), BF16), gain_in=pltpu.VMEM(norm_gain.shape, BF16), gain=pltpu.VMEM((depth, lanes), F32),
                u=pltpu.VMEM((PARTS, lanes, depth), BF16), u_rel=pltpu.VMEM((PARTS, lanes, depth), BF16),
                wa=pltpu.VMEM((depth, attn_cols), BF16), wm=pltpu.VMEM((depth, 2, mlp_cols), BF16),
                w_split=pltpu.VMEM((2, depth, mlp_cols), BF16),
                a_part=pltpu.VMEM((PARTS, lanes, attn_cols), BF16), a_core=pltpu.VMEM((PARTS, half, attn_cols), BF16),
                a_sum=pltpu.VMEM((PARTS, half, attn_cols), BF16), a_got=pltpu.VMEM((PARTS, 3, seqs, attn_cols), BF16),
                a_full=pltpu.VMEM((PARTS, 2, seqs, attn_cols), BF16),
                z_part=pltpu.VMEM((PARTS, CHUNKS, 2 * lanes, cols), BF16),
                z_recv=pltpu.VMEM((PARTS, CHUNKS, lanes, cols), BF16), z_x=pltpu.VMEM((units, half, cols), BF16),
                z_mine=pltpu.VMEM((units, half, cols), BF16), z_early=pltpu.VMEM((EARLY[layer], half, cols), BF16),
            )

        back_scratch = dict(
            o_yz=pltpu.VMEM((num_seqs, out_depth), BF16), o=pltpu.VMEM((PARTS, lanes, out_depth), BF16),
            m=pltpu.VMEM((PARTS, CHUNKS, lanes, cols), BF16), z_in=pltpu.VMEM((units, half, cols), BF16),
            o_in=pltpu.VMEM((2, num_seqs, out_depth), BF16),
            h_in=pltpu.VMEM((PARTS, part, lanes), BF16),
            wd=pltpu.VMEM((mlp_cols, depth), BF16), wo=pltpu.VMEM((out_depth, depth), BF16),
            acc=pltpu.VMEM((PARTS, lanes, depth), F32), update=pltpu.VMEM((PARTS, lanes, depth), F32),
            up_part=pltpu.VMEM((PARTS, depth, lanes), BF16), up_recv=pltpu.VMEM((PARTS, part, lanes), BF16),
        )

        def got_scratch(layer):
            return dict(z_got=pltpu.VMEM((units - EARLY[layer], half, cols), BF16))

        def front_shapes(layer):
            return (
                jax.ShapeDtypeStruct((2, num_seqs, attn_cols), BF16), jax.ShapeDtypeStruct((units - EARLY[layer] + CARRY[layer] // PARTS, half, cols), BF16),
                jax.ShapeDtypeStruct((units, half, cols), BF16), jax.ShapeDtypeStruct((PARTS, part, lanes), BF16))
        front_specs = (HBM,) * 4

        def call(kernel, name, collective_id, scratch, in_specs, out_shape, out_specs, *args):
            return pl.pallas_call(
                functools.partial(kernel, tuple(scratch)), out_shape=out_shape, in_specs=list(in_specs), out_specs=out_specs,
                scratch_shapes=list(scratch.values()), name=name,
                compiler_params=pltpu.CompilerParams(collective_id=collective_id, has_side_effects=True, vmem_limit_bytes=END_VMEM_LIMIT if kernel is end_kernel else VMEM_LIMIT),
            )(*args)

        def start(names, *refs):
            start_kernel(names, model_dim, *refs)

        def middle(names, *refs):
            middle_kernel(names, model_dim, *refs)

        qkv, zsend, zmine, h_block = call(
            start, 'start', 0, dict(**semaphores(6, 34 + EARLY[0], 8), **front_scratch(0), h_in=pltpu.VMEM((part, rows), BF16)), (HBM,) * 4,
            front_shapes(0), front_specs, hidden.T, norm_gain, w_attn, w_mlp)
        zgot = lax.ppermute(zsend, 'x', swap)
        k_new, v_new, o = attention(0, lengths, qkv, k_cache, v_cache, ())
        qkv, zsend, zmine, h_block = call(
            middle, 'middle', 1, dict(**semaphores(11, 65 + EARLY[1], 17), **front_scratch(1), **back_scratch, **got_scratch(0),
                       m_early=pltpu.VMEM((half, cols), BF16)), (HBM,) * 9,
            front_shapes(1), front_specs, h_block, o, norm_gain, zmine, zgot, w_down, w_out, w_attn, w_mlp)
        zgot = lax.ppermute(zsend, 'x', swap)
        k_new, v_new, o = attention(1, lengths, qkv, k_cache, v_cache, (k_new, v_new))
        h_out = call(
            end_kernel, 'end', 2, dict(**semaphores(5, 29, 11), **back_scratch, **got_scratch(1)), (HBM,) * 6,
            jax.ShapeDtypeStruct((part, rows), BF16), VMEM, h_block, o, zmine, zgot, w_down, w_out)
        return h_out.T, k_new, v_new

    return jax.shard_map(device_step, mesh=mesh, in_specs=in_specs, out_specs=out_specs, check_vma=False)
```

```python
import functools
import types

import jax
import jax.numpy as jnp
from jax import lax
from jax.experimental import pallas as pl
from jax.experimental.pallas import tpu as pltpu
from jax.sharding import PartitionSpec as P

NORM_EPS = 1e-5
MESH = pl.DeviceIdType.MESH
BF16 = jnp.bfloat16
F32 = jnp.float32

SQ_ROWS = 1
PER_COPY = 4
PER_STEP = 2
CHUNKS = 5
EARLY = (1, 2)
CARRY = (0, 2)
END_VMEM_LIMIT = 56393728
VMEM_LIMIT = 67043328


def dot(a, b):
    return jnp.dot(a, b, preferred_element_type=F32)


class Links:
    def __init__(self, send_sems, recv_sems, local_sems, peers):
        self.send_sems, self.recv_sems, self.local_sems = send_sems, recv_sems, local_sems
        self.groups, self.used, self.local_groups, self.local_used = {}, 0, {}, 0
        x, y = lax.axis_index('x'), lax.axis_index('yz')
        self.x, self.y = x, y
        core = lax.rem(x, 2)
        self.along_x = (3 - x, x + 1 - 2 * core, lax.rem(x + 2, 4))
        self.blocks = self.along_x + (x,)
        self.targets = tuple({'x': p, 'yz': y} for p in self.blocks) + ({'x': x, 'yz': 1 - y},) + tuple(
            {'x': p, 'yz': 1 - y} for p in self.along_x)
        self.peers = peers
        self.barrier = pltpu.get_barrier_semaphore()
        for k in self.peers:
            pl.semaphore_signal(self.barrier, inc=1, device_id=self.targets[k], device_id_type=MESH)

    def meet(self):
        pl.semaphore_wait(self.barrier, len(self.peers))

    def slot(self):
        self.used += 1
        return self.used - 1

    def take(self, k, got):
        pltpu.make_async_copy(got, got, self.recv_sems.at[k]).wait()

    def push(self, src, dst, to, group, k=None):
        k = self.slot() if k is None else k
        g = self.groups.setdefault(group, len(self.groups))
        copy = pltpu.make_async_remote_copy(
            src_ref=src, dst_ref=dst, send_sem=self.send_sems.at[g], recv_sem=self.recv_sems.at[k],
            device_id=self.targets[to], device_id_type=MESH)
        copy.start()
        return copy

    def copy(self, src, dst, group=None):
        if group is None or group not in self.local_groups:
            k = self.local_used
            self.local_used += 1
            if group is not None:
                self.local_groups[group] = k
        else:
            k = self.local_groups[group]
        copy = pltpu.make_async_copy(src, dst, self.local_sems.at[k])
        copy.start()
        return copy

    def drain(self, sent, stored):
        for group, g in self.groups.items():
            pltpu.make_async_copy(sent[group], sent[group], self.send_sems.at[g]).wait()
        for group, k in self.local_groups.items():
            pltpu.make_async_copy(stored[group], stored[group], self.local_sems.at[k]).wait()


DIAG, PARTNER, ACROSS, OWN, YZ, ACROSS_YZ = 0, 1, 2, 3, 4, 7
EVERYONE = [k for k in range(8) if k != OWN]
PARTS = 2


def gated(z):
    shard = z.shape[0] // 2
    gate, up = z[:shard].astype(F32), z[shard:].astype(F32)
    return (gate * jax.nn.sigmoid(gate) * up).astype(BF16)


def part_order(rows, inverse):
    i = lax.broadcasted_iota(jnp.int32, (rows, rows), 0)
    j = lax.broadcasted_iota(jnp.int32, (rows, rows), 1)
    src, dst = (j, i) if inverse else (i, j)
    run = rows // (8 * PARTS)
    piece = src // run
    place = lax.rem(piece, PARTS) * (8 * run) + (piece // PARTS) * run + lax.rem(src, run)
    return jnp.where(dst == place, jnp.ones((), F32), jnp.zeros((), F32)).astype(BF16)


class Front:
    def __init__(self, links, layer, gain_hbm, wa_hbm, wm_hbm, model_dim, outs, s):
        self.links, self.s, self.layer, self.model_dim = links, s, layer, model_dim
        self.kept, self.carry = EARLY[layer], CARRY[layer]
        self.gain_copy = links.copy(gain_hbm, s.gain_in)
        self.qkv_out, self.zsend_out, self.zmine_out, self.h_out = outs
        self.chunks, self.cols = s.z_recv.shape[1], s.z_recv.shape[3]
        self.depth = s.wa.shape[0]
        self.wa = links.copy(wa_hbm.at[layer], s.wa)
        self.wm = links.copy(wm_hbm.at[layer], s.wm)
        self.wa_ready = False
        part = self.depth // 2
        self.mine = pl.ds(pl.multiple_of(links.y * part, part), part)
        self.h_yz = {}
        self.a_core, self.a_got, self.z_core, self.early = {}, {}, {}, {}
        self.sq = {}

    def constants(self):
        lanes = self.s.u.shape[1]
        self.gain_copy.wait()
        gain = jnp.broadcast_to(self.s.gain_in[self.layer:self.layer + 1, :].astype(F32), (lanes, self.depth)).T
        self.s.gain[...] = gain

    def squares(self, p, h_t):
        s = self.s
        s.h[p, self.mine, :] = h_t.astype(BF16)
        s.sq_send[p] = jnp.broadcast_to(jnp.sum(h_t * h_t, axis=0, keepdims=True), s.sq_send.shape[1:])

    def send_h(self, p):
        s, links = self.s, self.links
        self.sq[p] = links.slot()
        for k in EVERYONE:
            links.push(s.sq_send.at[p], s.sq_recv.at[p, k], k, 'sq', self.sq[p])
        self.h_yz[p] = links.push(s.h.at[p, self.mine], s.h.at[p, self.mine], YZ, 'h')
        links.copy(s.h.at[p, self.mine], self.h_out.at[p], 'h')

    def normalize(self, p):
        s, links = self.s, self.links
        links.take(self.sq[p], s.sq_recv.at[p, pl.ds(0, len(EVERYONE))])
        total = s.sq_send[p]
        for k in EVERYONE:
            total = total + s.sq_recv[p, k]
        self.h_yz[p].wait_recv()
        h_t = s.h[p].astype(F32)
        inv_rms = lax.rsqrt(total[:1] / self.model_dim + NORM_EPS)
        s.u[p] = (h_t * inv_rms * s.gain[...]).T.astype(BF16)
        shard = s.u.shape[1] // 4
        u = jnp.concatenate([s.u[p, pl.ds(pl.multiple_of(b * shard, shard), shard), :] for b in links.blocks], axis=0)
        s.u_rel[p] = u
        if not self.wa_ready:
            self.wa.wait()
            self.wa_ready = True
        s.a_part[p] = dot(u, s.wa[...]).astype(BF16)
        self.a_core[p] = links.push(s.a_part.at[p, pl.ds(0, 2 * shard)], s.a_core.at[p], PARTNER, 'a_core')

    def attend_core(self, p):
        s = self.s
        half = s.a_core.shape[1]
        self.a_core[p].wait_recv()
        s.a_sum[p] = (s.a_part[p, half:].astype(F32) + s.a_core[p].astype(F32)).astype(BF16)
        shard, seqs = half // 2, s.a_got.shape[2]
        y = self.links.y
        here, there = pl.multiple_of(y * seqs, seqs), pl.multiple_of((1 - y) * seqs, seqs)
        k = self.a_got[p] = self.links.slot()
        self.links.push(s.a_sum.at[p, pl.ds(there, seqs)], s.a_got.at[p, 2], ACROSS_YZ, 'a_got', k)
        self.links.push(s.a_sum.at[p, pl.ds(here, seqs)], s.a_got.at[p, 0], ACROSS, 'a_got', k)
        self.links.push(s.a_sum.at[p, pl.ds(shard + there, seqs)], s.a_got.at[p, 1], YZ, 'a_got', k)

    def attend_ends(self, p):
        s, y = self.s, self.links.y
        shard, seqs = s.a_sum.shape[1] // 2, s.a_got.shape[2]
        self.links.take(self.a_got[p], s.a_got.at[p])
        own = s.a_sum[p, pl.ds(shard + pl.multiple_of(y * seqs, seqs), seqs), :]
        s.a_full[p, 0] = (own.astype(F32) + s.a_got[p, 0].astype(F32)).astype(BF16)
        s.a_full[p, 1] = (s.a_got[p, 1].astype(F32) + s.a_got[p, 2].astype(F32)).astype(BF16)
        for k, head in enumerate((y, 1 - y)):
            self.links.copy(s.a_full.at[p, k], self.qkv_out.at[head, pl.ds(p * seqs, seqs)], 'qkv')

    def split_weights(self, c):
        s, run = self.s, 128
        i = lax.broadcasted_iota(jnp.int32, (2 * run, 2 * run), 0)
        j = lax.broadcasted_iota(jnp.int32, (2 * run, 2 * run), 1)
        place = jnp.where(i < run, 2 * i, 2 * (i - run) + 1)
        order = jnp.where(j == place, jnp.ones((), F32), jnp.zeros((), F32)).astype(BF16)
        if c == 0:
            self.wm.wait()
        cols = slice(c * self.cols, (c + 1) * self.cols)
        for e in range(self.depth // run):
            rows = slice(e * run, (e + 1) * run)
            w = dot(order, s.wm[rows, :, cols].reshape(2 * run, self.cols)).astype(BF16)
            s.w_split[0, rows, cols] = w[:run]
            s.w_split[1, rows, cols] = w[run:]

    def project(self, parts, j):
        s = self.s
        lanes = s.u.shape[1]
        shard = lanes // 4
        u = jnp.concatenate([s.u_rel[p] for p in parts], axis=0)
        cols = slice(j * self.cols, (j + 1) * self.cols)
        gate, up = dot(u, s.w_split[0, :, cols]).astype(BF16), dot(u, s.w_split[1, :, cols]).astype(BF16)
        for n, p in enumerate(parts):
            for k in range(4):
                rows = slice(n * lanes + k * shard, n * lanes + (k + 1) * shard)
                s.z_part[p, j, 2 * k * shard:(2 * k + 1) * shard] = gate[rows]
                s.z_part[p, j, (2 * k + 1) * shard:(2 * k + 2) * shard] = up[rows]
            self.push_core(p, j)

    def push_core(self, p, j):
        s = self.s
        half = s.z_recv.shape[2]
        self.z_core[p, j] = self.links.push(s.z_part.at[p, j, pl.ds(0, half)], s.z_recv.at[p, j], PARTNER, 'z')

    def combine(self, p, j):
        s, unit = self.s, p * self.chunks + j
        half = s.z_recv.shape[2]
        shard2 = half // 2
        self.z_core[p, j].wait_recv()
        s.z_x[unit] = (s.z_part[p, j, half:half + shard2].astype(F32) + s.z_recv[p, j, :shard2].astype(F32)).astype(BF16)
        if unit < self.kept:
            self.early[unit] = self.links.push(s.z_x.at[unit], s.z_early.at[unit], ACROSS, 'early')
        else:
            self.links.copy(s.z_x.at[unit], self.zsend_out.at[unit - self.kept], 'z_x')
        s.z_mine[unit] = (s.z_part[p, j, half + shard2:].astype(F32) + s.z_recv[p, j, shard2:].astype(F32)).astype(BF16)
        if unit >= self.kept:
            self.links.copy(s.z_mine.at[unit], self.zmine_out.at[unit], 'z_mine')

    def take_early(self):
        s = self.s
        for unit in range(self.kept):
            self.early[unit].wait_recv()
            s.z_mine[unit] = (s.z_mine[unit].astype(F32) + s.z_early[unit].astype(F32)).astype(BF16)
            self.links.copy(s.z_mine.at[unit], self.zmine_out.at[unit], 'z_mine')
        if self.carry:
            shard = s.z_mine.shape[1] // 2
            for unit in range(self.carry):
                s.m_early[unit * shard:(unit + 1) * shard] = gated(s.z_mine[unit])
            self.links.copy(s.m_early, self.zsend_out.at[s.z_x.shape[0] - self.kept], 'm_early')

    def sizes(self):
        s = self.s
        return (dict(a_core=s.a_core, a_got=s.a_got, z=s.z_recv, early=s.z_early,
                 sq=s.sq_recv.at[:, pl.ds(0, len(EVERYONE))], h=s.h.at[:, self.mine]),
                dict(z_x=s.z_x.at[pl.ds(self.kept, s.z_x.shape[0] - self.kept)], z_mine=s.z_mine, qkv=s.a_full, h=s.h.at[:, self.mine], m_early=getattr(s, 'm_early', None)))


class Back:
    def __init__(self, links, layer, h_hbm, o_hbm, zgot_hbm, zmine_hbm, wd_hbm, wo_hbm, s):
        self.links, self.s = links, s
        self.kept, self.carry = EARLY[layer], CARRY[layer]
        self.chunks, self.cols = s.m.shape[1], s.m.shape[3]
        units = PARTS * self.chunks
        shard = s.m.shape[2] // 4
        self.z = []
        for first, last in ((0, 1), (1, self.chunks), (self.chunks, units)):
            run = pl.ds(first, last - first)
            self.z.append((first, links.copy(zmine_hbm.at[run], s.z_in.at[run])))
            start = max(first, self.kept)
            if start < last:
                run = pl.ds(start - self.kept, last - start)
                self.z.append((start, links.copy(zgot_hbm.at[run], s.z_got.at[run])))
            if first == 0:
                self.carried = [links.copy(zgot_hbm.at[units - self.kept, pl.ds(j * shard, shard)], self.block(0, j, ACROSS))
                                for j in range(self.carry)]
                self.o_copy = links.copy(o_hbm, s.o_in)
                self.h_copy = links.copy(h_hbm, s.h_in)
        self.wd = links.copy(wd_hbm.at[layer], s.wd)
        self.wo = links.copy(wo_hbm.at[layer], s.wo)
        self.wo_ready, self.wd_ready = False, False
        self.across, self.partner, self.diag = {}, {}, {}
        self.o_across, self.o_partner, self.o_diag = {}, {}, {}
        self.up = {}

    def mix(self, p, j):
        s, unit = self.s, p * self.chunks + j
        while self.z and self.z[0][0] <= unit:
            self.z.pop(0)[1].wait()
        z = s.z_in[unit]
        if unit >= self.kept:
            z = (z.astype(F32) + s.z_got[unit - self.kept].astype(F32)).astype(BF16)
        s.m[p, j, OWN * (z.shape[0] // 2):] = gated(z)

    def block(self, p, j, k):
        shard = self.s.m.shape[2] // 4
        return self.s.m.at[p, j, pl.ds(k * shard, shard)]

    def send(self, p, j):
        if p > 0 or j >= self.carry:
            self.across[p, j] = self.links.push(self.block(p, j, OWN), self.block(p, j, ACROSS), ACROSS, 'm_across')

    def send_partner(self, p):
        m = self.s.m
        shard = m.shape[2] // 4
        self.partner[p] = self.links.push(m.at[p, :, pl.ds(OWN * shard, shard)], m.at[p, :, pl.ds(PARTNER * shard, shard)], PARTNER, 'm')

    def forward(self, p, j):
        if p > 0 or j >= self.carry:
            self.across[p, j].wait_recv()
        else:
            self.carried[j].wait()
        self.diag[p, j] = self.links.push(self.block(p, j, ACROSS), self.block(p, j, DIAG), PARTNER, 'm')

    def send_o_yz(self):
        y, s = self.links.y, self.s
        self.o_copy.wait()
        self.o_yz = self.links.push(s.o_in.at[1 - y], s.o_yz, YZ, 'o_yz')

    def o_block(self, p, k):
        shard = self.s.o.shape[1] // 4
        return self.s.o.at[p, pl.ds(k * shard, shard)]

    def send_o(self, p):
        y, s = self.links.y, self.s
        if p == 0:
            self.o_yz.wait_recv()
        shard = s.o.shape[1] // 4
        seqs = shard // 2
        s.o[p, pl.ds(OWN * shard + pl.multiple_of(y * seqs, seqs), seqs), :] = s.o_in[y, p * seqs:(p + 1) * seqs]
        s.o[p, pl.ds(OWN * shard + pl.multiple_of((1 - y) * seqs, seqs), seqs), :] = s.o_yz[p * seqs:(p + 1) * seqs]
        self.o_across[p] = self.links.push(self.o_block(p, OWN), self.o_block(p, ACROSS), ACROSS, 'o')
        self.o_partner[p] = self.links.push(self.o_block(p, OWN), self.o_block(p, PARTNER), PARTNER, 'o')

    def forward_o(self, p):
        self.o_across[p].wait_recv()
        self.o_diag[p] = self.links.push(self.o_block(p, ACROSS), self.o_block(p, DIAG), PARTNER, 'o')

    def project_o(self, p):
        s = self.s
        self.o_partner[p].wait_recv()
        self.o_diag[p].wait_recv()
        if not self.wo_ready:
            self.wo.wait()
            self.wo_ready = True
        s.acc[p] += dot(s.o[p], s.wo[...])

    def down(self, p, j):
        s = self.s
        if j == 0:
            self.partner[p].wait_recv()
        self.diag[p, j].wait_recv()
        if not self.wd_ready:
            self.wd.wait()
            self.wd_ready = True
        part = dot(s.m[p, j], s.wd[j * self.cols:(j + 1) * self.cols])
        if j == 0:
            s.acc[p] = part
        else:
            s.acc[p] += part

    def send_update(self, p):
        s, links = self.s, self.links
        shard = s.acc.shape[1] // 4
        for k in range(4):
            s.update[p, pl.ds(pl.multiple_of(links.blocks[k] * shard, shard), shard), :] = s.acc[p, k * shard:(k + 1) * shard, :]
        s.up_part[p] = s.update[p].T.astype(BF16)
        part = s.up_recv.shape[1]
        src = s.up_part.at[p, pl.ds(pl.multiple_of((1 - links.y) * part, part), part)]
        self.up[p] = links.push(src, s.up_recv.at[p], YZ, 'up')

    def new_h(self, p):
        s, links = self.s, self.links
        self.up[p].wait_recv()
        part = s.up_recv.shape[1]
        own = s.up_part[p, pl.ds(pl.multiple_of(links.y * part, part), part), :]
        return (s.h_in[p].astype(F32) + (own.astype(F32) + s.up_recv[p].astype(F32))).astype(BF16)

    def sizes(self):
        s = self.s
        sent = 3 * s.m.shape[2] // 4
        shard = sent // 3
        return dict(m=s.m.at[:, :, pl.ds(0, 2 * shard)],
                m_across=s.m.at[:, pl.ds(0, self.chunks - self.carry // PARTS), pl.ds(0, shard)], o=s.o.at[:, pl.ds(0, sent)], o_yz=s.o_yz, up=s.up_recv)

    def open(self):
        links, chunks = self.links, self.chunks
        for j in range(self.carry + 1):
            self.mix(0, j)
        links.meet()
        for j in range(self.carry + 1):
            self.send(0, j)
        self.send_o_yz()
        for j in range(self.carry + 1, chunks):
            self.mix(0, j)
            self.send(0, j)
            if j == 2 + self.carry:
                self.send_o(0)
        self.send_partner(0)
        for j in range(chunks):
            self.mix(1, j)
            self.send(1, j)
            if j == 1:
                self.send_o(1)
        self.send_partner(1)
        self.h_copy.wait()


def start_kernel(names, model_dim, h_hbm, gain_hbm, wa_hbm, wm_hbm, qkv_out, zsend_out, zmine_out, h_out, *scratch):
    s = types.SimpleNamespace(**dict(zip(names, scratch)))
    links = Links(s.send, s.recv, s.local, EVERYONE)
    h_copy = links.copy(h_hbm, s.h_in)
    f = Front(links, 0, gain_hbm, wa_hbm, wm_hbm, model_dim, (qkv_out, zsend_out, zmine_out, h_out), s)
    rows = h_hbm.shape[1]
    lanes = rows // PARTS
    order = part_order(rows, False)
    h_copy.wait()
    own = dot(s.h_in[...], order)
    for p in range(PARTS):
        f.squares(p, own[:, p * lanes:(p + 1) * lanes])
    f.constants()
    links.meet()
    for p in range(PARTS):
        f.send_h(p)
    for j in range(f.chunks):
        f.split_weights(j)
    for p in range(PARTS):
        f.normalize(p)
    f.project(range(PARTS), 0)
    for p in range(PARTS):
        f.attend_core(p)
    for j in range(1, f.chunks):
        f.project(range(PARTS), j)
        if j == f.chunks - 1:
            f.attend_ends(0)
        for p in range(PARTS):
            f.combine(p, j - 1)
    f.attend_ends(1)
    for p in range(PARTS):
        f.combine(p, f.chunks - 1)
    f.take_early()
    links.drain(*f.sizes())


def middle_kernel(names, model_dim, h_hbm, o_hbm, gain_hbm, zmine_hbm, zgot_hbm, wd_hbm, wo_hbm, wa_hbm, wm_hbm, qkv_out, zsend_out,
                  zmine_out, h_out, *scratch):
    s = types.SimpleNamespace(**dict(zip(names, scratch)))
    links = Links(s.send, s.recv, s.local, EVERYONE)
    b = Back(links, 0, h_hbm, o_hbm, zgot_hbm, zmine_hbm, wd_hbm, wo_hbm, s)
    f = Front(links, 1, gain_hbm, wa_hbm, wm_hbm, model_dim, (qkv_out, zsend_out, zmine_out, h_out), s)
    b.open()
    f.constants()

    def pass_h(p):
        f.squares(p, b.new_h(p).astype(F32))
        f.send_h(p)

    first_part(b, f.split_weights)
    second_part(b, lambda: pass_h(0))
    f.normalize(0)
    f.project([0], 0)
    f.attend_core(0)
    pass_h(1)
    f.project([0], 1)
    f.project([0], 2)
    f.combine(0, 0)
    f.project([0], 3)
    f.combine(0, 1)
    f.project([0], 4)
    f.combine(0, 2)
    f.combine(0, 3)
    f.normalize(1)
    f.project([1], 0)
    f.combine(0, 4)
    f.project([1], 1)
    f.attend_core(1)
    f.attend_ends(0)
    f.project([1], 2)
    f.combine(1, 0)
    f.project([1], 3)
    f.combine(1, 1)
    f.project([1], 4)
    f.combine(1, 2)
    f.combine(1, 3)
    f.take_early()
    f.combine(1, 4)
    f.attend_ends(1)
    sent, stored = f.sizes()
    links.drain(dict(**sent, **b.sizes()), stored)


def first_part(b, filler):
    for j in range(b.chunks):
        b.forward(0, j)
        if filler is not None:
            filler(j)
        if j == 2 + b.carry:
            b.forward_o(0)
        if j >= 1:
            b.down(0, j - 1)
    b.project_o(0)
    b.down(0, b.chunks - 1)
    b.send_update(0)
    b.forward(1, 0)


def second_part(b, when_updated):
    for j in range(1, b.chunks):
        b.forward(1, j)
        if j == 1:
            b.forward_o(1)
        b.down(1, j - 1)
        if j == 2:
            b.project_o(1)
        if j == b.chunks - 3:
            when_updated()
    b.down(1, b.chunks - 1)
    b.send_update(1)


def end_kernel(names, h_hbm, o_hbm, zmine_hbm, zgot_hbm, wd_hbm, wo_hbm, h_out, *scratch):
    s = types.SimpleNamespace(**dict(zip(names, scratch)))
    links = Links(s.send, s.recv, s.local, [PARTNER, ACROSS, YZ])
    b = Back(links, 1, h_hbm, o_hbm, zgot_hbm, zmine_hbm, wd_hbm, wo_hbm, s)
    b.open()
    first_part(b, None)
    h_new = []
    second_part(b, lambda: h_new.append(b.new_h(0)))
    order = part_order(h_out.shape[1], True)
    h_new.append(b.new_h(1))
    h_out[...] = dot(jnp.concatenate(h_new, axis=1), order).astype(BF16)
    links.drain(b.sizes(), {})


def attention_kernel(layer, per_copy, per_step, len_hbm, qkv_hbm, k_hbm, v_hbm, *rest):
    k_out, v_out, o_hbm, kbuf, vbuf, q_scr, o_scr, qkv_ref, o_ref, len_ref, in_sem, out_sem, small_sem = rest[-13:]
    num_seqs, kv_heads, cache_len, head_dim = kbuf.shape
    slots = qkv_ref.shape[2] // head_dim
    rows = kv_heads * slots
    scale = head_dim ** -0.5

    def load(n):
        run = pl.ds(n * per_copy, per_copy)
        return (pltpu.make_async_copy(k_hbm.at[layer, run], kbuf.at[run], in_sem.at[0, n]),
                pltpu.make_async_copy(v_hbm.at[layer, run], vbuf.at[run], in_sem.at[1, n]))

    def store(n):
        run = pl.ds(n * per_copy, per_copy)
        return (pltpu.make_async_copy(kbuf.at[run], k_out.at[layer, run], out_sem.at[0, n]),
                pltpu.make_async_copy(vbuf.at[run], v_out.at[layer, run], out_sem.at[1, n]))

    qkv_copy = pltpu.make_async_copy(qkv_hbm, qkv_ref, small_sem.at[0])
    len_copy = pltpu.make_async_copy(len_hbm, len_ref, small_sem.at[1])
    qkv_copy.start()
    len_copy.start()

    @pl.loop(0, num_seqs // per_copy)
    def _(n):
        for c in load(n):
            c.start()

    qkv_copy.wait()
    len_copy.wait()
    for head in range(kv_heads):
        for j in range(slots):
            q_scr[pl.ds(head * slots + j, num_seqs, stride=rows), :] = (
                qkv_ref[head, :, j * head_dim:(j + 1) * head_dim].astype(F32))

    tile_row = lax.broadcasted_iota(jnp.int32, (16, head_dim), 0)
    position = lax.broadcasted_iota(jnp.int32, (rows, cache_len), 1)

    def patch(n):
        for c in load(n):
            c.wait()
        for sub in range(per_copy):
            i = n * per_copy + sub
            length = len_ref[i]
            base = pl.multiple_of((length // 16) * 16, 16)
            hit = tile_row == length - base
            for head in range(kv_heads):
                for buf, j in ((kbuf, slots - 2), (vbuf, slots - 1)):
                    new = q_scr[pl.ds(i * rows + head * slots + j, 1), :]
                    old = buf[i, head, pl.ds(base, 16), :].astype(F32)
                    buf[i, head, pl.ds(base, 16), :] = jnp.where(hit, new, old).astype(buf.dtype)
        for c in store(n):
            c.start()

    def attend(group):
        scores, probs = [], []
        for i in group:
            q = q_scr[pl.ds(pl.multiple_of(i * rows, rows), rows), :].astype(BF16)
            by_head = [lax.dot_general(q, kbuf[i, head], (((1,), (1,)), ((), ())), preferred_element_type=F32)
                       for head in range(kv_heads)]
            scores.append(jnp.concatenate([by_head[head][head * slots:(head + 1) * slots] for head in range(kv_heads)], axis=0))
        for i, score in zip(group, scores):
            score = jnp.where(position <= len_ref[i], score * scale, -1e30)
            e = jnp.exp(score - jnp.max(score, axis=1, keepdims=True))
            probs.append((e / jnp.sum(e, axis=1, keepdims=True)).astype(BF16))
        for i, p in zip(group, probs):
            by_head = [dot(p, vbuf[i, head]) for head in range(kv_heads)]
            o_scr[pl.ds(pl.multiple_of(i * rows, rows), rows), :] = jnp.concatenate(
                [by_head[head][head * slots:(head + 1) * slots] for head in range(kv_heads)], axis=0)

    @pl.loop(0, num_seqs // per_copy)
    def _(n):
        patch(n)
        for first in range(0, per_copy, per_step):
            attend([n * per_copy + first + sub for sub in range(per_step)])

    for head in range(kv_heads):
        for j in range(slots - 2):
            o_ref[head, :, j * head_dim:(j + 1) * head_dim] = (
                o_scr[pl.ds(head * slots + j, num_seqs, stride=rows), :].astype(o_ref.dtype))
    o_copy = pltpu.make_async_copy(o_ref, o_hbm, small_sem.at[2])
    o_copy.start()

    @pl.loop(0, num_seqs // per_copy)
    def _(n):
        for c in store(n):
            c.wait()

    o_copy.wait()


VMEM = pl.BlockSpec(memory_space=pltpu.VMEM)
HBM = pl.BlockSpec(memory_space=pltpu.HBM)


def attention(layer, lengths, qkv, k_cache, v_cache, outs):
    layers, num_seqs, kv_heads, cache_len, head_dim = k_cache.shape
    slots = qkv.shape[2] // head_dim
    rows = kv_heads * slots
    return pl.pallas_call(
        functools.partial(attention_kernel, layer, PER_COPY, PER_STEP),
        out_shape=(jax.ShapeDtypeStruct(k_cache.shape, k_cache.dtype), jax.ShapeDtypeStruct(v_cache.shape, v_cache.dtype),
                   jax.ShapeDtypeStruct((kv_heads, num_seqs, (slots - 2) * head_dim), BF16)),
        in_specs=[HBM] * (4 + len(outs)),
        out_specs=(HBM, HBM, HBM),
        scratch_shapes=[pltpu.VMEM((num_seqs, kv_heads, cache_len, head_dim), BF16)] * 2
        + [pltpu.VMEM((num_seqs * rows, head_dim), F32)] * 2 + [
            pltpu.VMEM(qkv.shape, BF16), pltpu.VMEM((kv_heads, num_seqs, (slots - 2) * head_dim), BF16),
            pltpu.SMEM((num_seqs,), jnp.int32)]
        + [pltpu.SemaphoreType.DMA((2, num_seqs // PER_COPY))] * 2 + [pltpu.SemaphoreType.DMA((3,))],
        input_output_aliases={4: 0, 5: 1} if outs else {},
        compiler_params=pltpu.CompilerParams(vmem_limit_bytes=VMEM_LIMIT),
        cost_estimate=pl.CostEstimate(flops=10 ** 10, bytes_accessed=8 * num_seqs * kv_heads * cache_len * head_dim, transcendentals=0),
        name=f'attention_{layer}',
    )(lengths, qkv, k_cache, v_cache, *outs)


def solution(mesh):
    seq_axes = ('rep', 'x', 'yz')
    hidden_spec = P('rep', ('x', 'yz'))
    cache_spec = P(None, seq_axes, None, None, None)
    in_specs = (hidden_spec, P(None, 'x'), P(None, 'x', 'yz'), P(None, 'x', None, 'yz'), P(None, 'yz', 'x'), P(None, 'yz', 'x'), cache_spec, cache_spec, P(seq_axes))
    out_specs = (hidden_spec, cache_spec, cache_spec)
    swap = [(0, 2), (2, 0), (1, 3), (3, 1)]

    def device_step(hidden, norm_gain, w_attn, w_mlp, w_out, w_down, k_cache, v_cache, lengths):
        rows, part = hidden.shape
        depth, attn_cols = w_attn.shape[1:]
        model_dim = depth * mesh.shape['x']
        mlp_cols = w_mlp.shape[3]
        out_depth = w_out.shape[1]
        cols = mlp_cols // CHUNKS
        units = CHUNKS * PARTS
        lanes = rows // PARTS
        half, shard = lanes // 2, lanes // 4
        seqs = shard // 2
        num_seqs = PARTS * seqs

        def semaphores(groups, remote, local):
            return dict(send=pltpu.SemaphoreType.DMA((groups,)), recv=pltpu.SemaphoreType.DMA((remote,)),
                    local=pltpu.SemaphoreType.DMA((local,)))

        def front_scratch(layer):
            return dict(
                sq_send=pltpu.VMEM((PARTS, SQ_ROWS, lanes), F32), sq_recv=pltpu.VMEM((PARTS, 8, SQ_ROWS, lanes), F32),
                h=pltpu.VMEM((PARTS, depth, lanes), BF16), gain_in=pltpu.VMEM(norm_gain.shape, BF16), gain=pltpu.VMEM((depth, lanes), F32),
                u=pltpu.VMEM((PARTS, lanes, depth), BF16), u_rel=pltpu.VMEM((PARTS, lanes, depth), BF16),
                wa=pltpu.VMEM((depth, attn_cols), BF16), wm=pltpu.VMEM((depth, 2, mlp_cols), BF16),
                w_split=pltpu.VMEM((2, depth, mlp_cols), BF16),
                a_part=pltpu.VMEM((PARTS, lanes, attn_cols), BF16), a_core=pltpu.VMEM((PARTS, half, attn_cols), BF16),
                a_sum=pltpu.VMEM((PARTS, half, attn_cols), BF16), a_got=pltpu.VMEM((PARTS, 3, seqs, attn_cols), BF16),
                a_full=pltpu.VMEM((PARTS, 2, seqs, attn_cols), BF16),
                z_part=pltpu.VMEM((PARTS, CHUNKS, 2 * lanes, cols), BF16),
                z_recv=pltpu.VMEM((PARTS, CHUNKS, lanes, cols), BF16), z_x=pltpu.VMEM((units, half, cols), BF16),
                z_mine=pltpu.VMEM((units, half, cols), BF16), z_early=pltpu.VMEM((EARLY[layer], half, cols), BF16),
            )

        back_scratch = dict(
            o_yz=pltpu.VMEM((num_seqs, out_depth), BF16), o=pltpu.VMEM((PARTS, lanes, out_depth), BF16),
            m=pltpu.VMEM((PARTS, CHUNKS, lanes, cols), BF16), z_in=pltpu.VMEM((units, half, cols), BF16),
            o_in=pltpu.VMEM((2, num_seqs, out_depth), BF16),
            h_in=pltpu.VMEM((PARTS, part, lanes), BF16),
            wd=pltpu.VMEM((mlp_cols, depth), BF16), wo=pltpu.VMEM((out_depth, depth), BF16),
            acc=pltpu.VMEM((PARTS, lanes, depth), F32), update=pltpu.VMEM((PARTS, lanes, depth), F32),
            up_part=pltpu.VMEM((PARTS, depth, lanes), BF16), up_recv=pltpu.VMEM((PARTS, part, lanes), BF16),
        )

        def got_scratch(layer):
            return dict(z_got=pltpu.VMEM((units - EARLY[layer], half, cols), BF16))

        def front_shapes(layer):
            return (
                jax.ShapeDtypeStruct((2, num_seqs, attn_cols), BF16), jax.ShapeDtypeStruct((units - EARLY[layer] + CARRY[layer] // PARTS, half, cols), BF16),
                jax.ShapeDtypeStruct((units, half, cols), BF16), jax.ShapeDtypeStruct((PARTS, part, lanes), BF16))
        front_specs = (HBM,) * 4

        def call(kernel, name, collective_id, scratch, in_specs, out_shape, out_specs, *args):
            return pl.pallas_call(
                functools.partial(kernel, tuple(scratch)), out_shape=out_shape, in_specs=list(in_specs), out_specs=out_specs,
                scratch_shapes=list(scratch.values()), name=name,
                compiler_params=pltpu.CompilerParams(collective_id=collective_id, has_side_effects=True, vmem_limit_bytes=END_VMEM_LIMIT if kernel is end_kernel else VMEM_LIMIT),
            )(*args)

        def start(names, *refs):
            start_kernel(names, model_dim, *refs)

        def middle(names, *refs):
            middle_kernel(names, model_dim, *refs)

        qkv, zsend, zmine, h_block = call(
            start, 'start', 0, dict(**semaphores(6, 18 + EARLY[0], 8), **front_scratch(0), h_in=pltpu.VMEM((part, rows), BF16)), (HBM,) * 4,
            front_shapes(0), front_specs, hidden.T, norm_gain, w_attn, w_mlp)
        zgot = lax.ppermute(zsend, 'x', swap)
        k_new, v_new, o = attention(0, lengths, qkv, k_cache, v_cache, ())
        qkv, zsend, zmine, h_block = call(
            middle, 'middle', 1, dict(**semaphores(11, 49 + EARLY[1], 17), **front_scratch(1), **back_scratch, **got_scratch(0),
                       m_early=pltpu.VMEM((half, cols), BF16)), (HBM,) * 9,
            front_shapes(1), front_specs, h_block, o, norm_gain, zmine, zgot, w_down, w_out, w_attn, w_mlp)
        zgot = lax.ppermute(zsend, 'x', swap)
        k_new, v_new, o = attention(1, lengths, qkv, k_cache, v_cache, (k_new, v_new))
        h_out = call(
            end_kernel, 'end', 2, dict(**semaphores(5, 29, 11), **back_scratch, **got_scratch(1)), (HBM,) * 6,
            jax.ShapeDtypeStruct((part, rows), BF16), VMEM, h_block, o, zmine, zgot, w_down, w_out)
        return h_out.T, k_new, v_new

    return jax.shard_map(device_step, mesh=mesh, in_specs=in_specs, out_specs=out_specs, check_vma=False)
```

```python
import functools
import types

import jax
import jax.numpy as jnp
from jax import lax
from jax.experimental import pallas as pl
from jax.experimental.pallas import tpu as pltpu
from jax.sharding import PartitionSpec as P

NORM_EPS = 1e-5
MESH = pl.DeviceIdType.MESH
BF16 = jnp.bfloat16
F32 = jnp.float32

SQ_ROWS = 1
PER_COPY = 4
PER_STEP = 2
CHUNKS = 5
EARLY = (1, 2)
CARRY = (0, 2)
END_VMEM_LIMIT = 56393728
VMEM_LIMIT = 67043328


def dot(a, b):
    return jnp.dot(a, b, preferred_element_type=F32)


class Links:
    def __init__(self, send_sems, recv_sems, local_sems, peers):
        self.send_sems, self.recv_sems, self.local_sems = send_sems, recv_sems, local_sems
        self.groups, self.used, self.local_groups, self.local_used = {}, 0, {}, 0
        x, y = lax.axis_index('x'), lax.axis_index('yz')
        self.x, self.y = x, y
        core = lax.rem(x, 2)
        self.along_x = (3 - x, x + 1 - 2 * core, lax.rem(x + 2, 4))
        self.blocks = self.along_x + (x,)
        self.targets = tuple({'x': p, 'yz': y} for p in self.blocks) + ({'x': x, 'yz': 1 - y},) + tuple(
            {'x': p, 'yz': 1 - y} for p in self.along_x)
        self.peers = peers
        self.barrier = pltpu.get_barrier_semaphore()
        for k in self.peers:
            pl.semaphore_signal(self.barrier, inc=1, device_id=self.targets[k], device_id_type=MESH)

    def meet(self):
        pl.semaphore_wait(self.barrier, len(self.peers))

    def slot(self):
        self.used += 1
        return self.used - 1

    def take(self, k, got):
        pltpu.make_async_copy(got, got, self.recv_sems.at[k]).wait()

    def push(self, src, dst, to, group, k=None):
        k = self.slot() if k is None else k
        g = self.groups.setdefault(group, len(self.groups))
        copy = pltpu.make_async_remote_copy(
            src_ref=src, dst_ref=dst, send_sem=self.send_sems.at[g], recv_sem=self.recv_sems.at[k],
            device_id=self.targets[to], device_id_type=MESH)
        copy.start()
        return copy

    def copy(self, src, dst, group=None):
        if group is None or group not in self.local_groups:
            k = self.local_used
            self.local_used += 1
            if group is not None:
                self.local_groups[group] = k
        else:
            k = self.local_groups[group]
        copy = pltpu.make_async_copy(src, dst, self.local_sems.at[k])
        copy.start()
        return copy

    def drain(self, sent, stored):
        for group, g in self.groups.items():
            pltpu.make_async_copy(sent[group], sent[group], self.send_sems.at[g]).wait()
        for group, k in self.local_groups.items():
            pltpu.make_async_copy(stored[group], stored[group], self.local_sems.at[k]).wait()


DIAG, PARTNER, ACROSS, OWN, YZ, ACROSS_YZ = 0, 1, 2, 3, 4, 7
EVERYONE = [k for k in range(8) if k != OWN]
PARTS = 2


def gated(z):
    shard = z.shape[0] // 2
    gate, up = z[:shard].astype(F32), z[shard:].astype(F32)
    return (gate * jax.nn.sigmoid(gate) * up).astype(BF16)


def part_order(rows, inverse):
    i = lax.broadcasted_iota(jnp.int32, (rows, rows), 0)
    j = lax.broadcasted_iota(jnp.int32, (rows, rows), 1)
    src, dst = (j, i) if inverse else (i, j)
    run = rows // (8 * PARTS)
    piece = src // run
    place = lax.rem(piece, PARTS) * (8 * run) + (piece // PARTS) * run + lax.rem(src, run)
    return jnp.where(dst == place, jnp.ones((), F32), jnp.zeros((), F32)).astype(BF16)


class Front:
    def __init__(self, links, layer, gain_hbm, wa_hbm, wm_hbm, model_dim, outs, s):
        self.links, self.s, self.layer, self.model_dim = links, s, layer, model_dim
        self.kept, self.carry = EARLY[layer], CARRY[layer]
        self.gain_copy = links.copy(gain_hbm, s.gain_in)
        self.qkv_out, self.zsend_out, self.zmine_out, self.h_out = outs
        self.chunks, self.cols = s.z_recv.shape[1], s.z_recv.shape[3]
        self.depth = s.wa.shape[0]
        self.wa = links.copy(wa_hbm.at[layer], s.wa)
        self.wm = links.copy(wm_hbm.at[layer], s.wm)
        self.wa_ready = False
        part = self.depth // 2
        self.mine = pl.ds(pl.multiple_of(links.y * part, part), part)
        self.h_yz = {}
        self.a_core, self.a_got, self.z_core, self.early = {}, {}, {}, {}
        self.sq = {}

    def constants(self):
        lanes = self.s.u.shape[1]
        self.gain_copy.wait()
        gain = jnp.broadcast_to(self.s.gain_in[self.layer:self.layer + 1, :].astype(F32), (lanes, self.depth)).T
        self.s.gain[...] = gain

    def squares(self, p, h_t):
        s = self.s
        s.h[p, self.mine, :] = h_t.astype(BF16)
        s.sq_send[p] = jnp.broadcast_to(jnp.sum(h_t * h_t, axis=0, keepdims=True), s.sq_send.shape[1:])

    def send_h(self, p):
        s, links = self.s, self.links
        self.sq[p] = links.slot()
        for k in EVERYONE:
            links.push(s.sq_send.at[p], s.sq_recv.at[p, k], k, 'sq', self.sq[p])
        self.h_yz[p] = links.push(s.h.at[p, self.mine], s.h.at[p, self.mine], YZ, 'h')
        links.copy(s.h.at[p, self.mine], self.h_out.at[p], 'h')

    def normalize(self, p):
        s, links = self.s, self.links
        links.take(self.sq[p], s.sq_recv.at[p, pl.ds(0, len(EVERYONE))])
        total = s.sq_send[p]
        for k in EVERYONE:
            total = total + s.sq_recv[p, k]
        self.h_yz[p].wait_recv()
        h_t = s.h[p].astype(F32)
        inv_rms = lax.rsqrt(total[:1] / self.model_dim + NORM_EPS)
        s.u[p] = (h_t * inv_rms * s.gain[...]).T.astype(BF16)
        shard = s.u.shape[1] // 4
        u = jnp.concatenate([s.u[p, pl.ds(pl.multiple_of(b * shard, shard), shard), :] for b in links.blocks], axis=0)
        s.u_rel[p] = u
        if not self.wa_ready:
            self.wa.wait()
            self.wa_ready = True
        s.a_part[p] = dot(u, s.wa[...]).astype(BF16)
        self.a_core[p] = links.push(s.a_part.at[p, pl.ds(0, 2 * shard)], s.a_core.at[p], PARTNER, 'a_core')

    def attend_core(self, p):
        s = self.s
        half = s.a_core.shape[1]
        self.a_core[p].wait_recv()
        s.a_sum[p] = (s.a_part[p, half:].astype(F32) + s.a_core[p].astype(F32)).astype(BF16)
        shard, seqs = half // 2, s.a_got.shape[2]
        y = self.links.y
        here, there = pl.multiple_of(y * seqs, seqs), pl.multiple_of((1 - y) * seqs, seqs)
        k = self.a_got[p] = self.links.slot()
        self.links.push(s.a_sum.at[p, pl.ds(there, seqs)], s.a_got.at[p, 2], ACROSS_YZ, 'a_got', k)
        self.links.push(s.a_sum.at[p, pl.ds(here, seqs)], s.a_got.at[p, 0], ACROSS, 'a_got', k)
        self.links.push(s.a_sum.at[p, pl.ds(shard + there, seqs)], s.a_got.at[p, 1], YZ, 'a_got', k)

    def attend_ends(self, p):
        s, y = self.s, self.links.y
        shard, seqs = s.a_sum.shape[1] // 2, s.a_got.shape[2]
        self.links.take(self.a_got[p], s.a_got.at[p])
        own = s.a_sum[p, pl.ds(shard + pl.multiple_of(y * seqs, seqs), seqs), :]
        s.a_full[p, 0] = (own.astype(F32) + s.a_got[p, 0].astype(F32)).astype(BF16)
        s.a_full[p, 1] = (s.a_got[p, 1].astype(F32) + s.a_got[p, 2].astype(F32)).astype(BF16)
        for k, head in enumerate((y, 1 - y)):
            self.links.copy(s.a_full.at[p, k], self.qkv_out.at[head, pl.ds(p * seqs, seqs)], 'qkv')

    def split_weights(self, c):
        s, run = self.s, 128
        i = lax.broadcasted_iota(jnp.int32, (2 * run, 2 * run), 0)
        j = lax.broadcasted_iota(jnp.int32, (2 * run, 2 * run), 1)
        place = jnp.where(i < run, 2 * i, 2 * (i - run) + 1)
        order = jnp.where(j == place, jnp.ones((), F32), jnp.zeros((), F32)).astype(BF16)
        if c == 0:
            self.wm.wait()
        cols = slice(c * self.cols, (c + 1) * self.cols)
        for e in range(self.depth // run):
            rows = slice(e * run, (e + 1) * run)
            w = dot(order, s.wm[rows, :, cols].reshape(2 * run, self.cols)).astype(BF16)
            s.w_split[0, rows, cols] = w[:run]
            s.w_split[1, rows, cols] = w[run:]

    def project(self, parts, j):
        s = self.s
        lanes = s.u.shape[1]
        shard = lanes // 4
        u = jnp.concatenate([s.u_rel[p] for p in parts], axis=0)
        cols = slice(j * self.cols, (j + 1) * self.cols)
        gate, up = dot(u, s.w_split[0, :, cols]).astype(BF16), dot(u, s.w_split[1, :, cols]).astype(BF16)
        for n, p in enumerate(parts):
            for k in range(4):
                rows = slice(n * lanes + k * shard, n * lanes + (k + 1) * shard)
                s.z_part[p, j, 2 * k * shard:(2 * k + 1) * shard] = gate[rows]
                s.z_part[p, j, (2 * k + 1) * shard:(2 * k + 2) * shard] = up[rows]
            self.push_core(p, j)

    def push_core(self, p, j):
        s = self.s
        half = s.z_recv.shape[2]
        self.z_core[p, j] = self.links.push(s.z_part.at[p, j, pl.ds(0, half)], s.z_recv.at[p, j], PARTNER, 'z')

    def combine(self, p, j):
        s, unit = self.s, p * self.chunks + j
        half = s.z_recv.shape[2]
        shard2 = half // 2
        self.z_core[p, j].wait_recv()
        s.z_x[unit] = (s.z_part[p, j, half:half + shard2].astype(F32) + s.z_recv[p, j, :shard2].astype(F32)).astype(BF16)
        if unit < self.kept:
            self.early[unit] = self.links.push(s.z_x.at[unit], s.z_early.at[unit], ACROSS, 'early')
        else:
            self.links.copy(s.z_x.at[unit], self.zsend_out.at[unit - self.kept], 'z_x')
        s.z_mine[unit] = (s.z_part[p, j, half + shard2:].astype(F32) + s.z_recv[p, j, shard2:].astype(F32)).astype(BF16)
        if unit >= self.kept:
            self.links.copy(s.z_mine.at[unit], self.zmine_out.at[unit], 'z_mine')

    def take_early(self):
        s = self.s
        for unit in range(self.kept):
            self.early[unit].wait_recv()
            s.z_mine[unit] = (s.z_mine[unit].astype(F32) + s.z_early[unit].astype(F32)).astype(BF16)
            self.links.copy(s.z_mine.at[unit], self.zmine_out.at[unit], 'z_mine')
        if self.carry:
            shard = s.z_mine.shape[1] // 2
            for unit in range(self.carry):
                s.m_early[unit * shard:(unit + 1) * shard] = gated(s.z_mine[unit])
            self.links.copy(s.m_early, self.zsend_out.at[s.z_x.shape[0] - self.kept], 'm_early')

    def sizes(self):
        s = self.s
        return (dict(a_core=s.a_core, a_got=s.a_got, z=s.z_recv, early=s.z_early,
                 sq=s.sq_recv.at[:, pl.ds(0, len(EVERYONE))], h=s.h.at[:, self.mine]),
                dict(z_x=s.z_x.at[pl.ds(self.kept, s.z_x.shape[0] - self.kept)], z_mine=s.z_mine, qkv=s.a_full, h=s.h.at[:, self.mine], m_early=getattr(s, 'm_early', None)))


class Back:
    def __init__(self, links, layer, h_hbm, o_hbm, zgot_hbm, zmine_hbm, wd_hbm, wo_hbm, s):
        self.links, self.s = links, s
        self.kept, self.carry = EARLY[layer], CARRY[layer]
        self.chunks, self.cols = s.m.shape[1], s.m.shape[3]
        units = PARTS * self.chunks
        shard = s.m.shape[2] // 4
        self.z = []
        for first, last in ((0, 1), (1, self.chunks), (self.chunks, units)):
            run = pl.ds(first, last - first)
            self.z.append((first, links.copy(zmine_hbm.at[run], s.z_in.at[run])))
            start = max(first, self.kept)
            if start < last:
                run = pl.ds(start - self.kept, last - start)
                self.z.append((start, links.copy(zgot_hbm.at[run], s.z_got.at[run])))
            if first == 0:
                self.carried = [links.copy(zgot_hbm.at[units - self.kept, pl.ds(j * shard, shard)], self.block(0, j, ACROSS))
                                for j in range(self.carry)]
                self.o_copy = links.copy(o_hbm, s.o_in)
                self.h_copy = links.copy(h_hbm, s.h_in)
        self.wd = links.copy(wd_hbm.at[layer], s.wd)
        self.wo = links.copy(wo_hbm.at[layer], s.wo)
        self.wo_ready, self.wd_ready = False, False
        self.across, self.partner, self.diag = {}, {}, {}
        self.o_across, self.o_core = {}, {}
        self.up = {}

    def mix(self, p, j):
        s, unit = self.s, p * self.chunks + j
        while self.z and self.z[0][0] <= unit:
            self.z.pop(0)[1].wait()
        z = s.z_in[unit]
        if unit >= self.kept:
            z = (z.astype(F32) + s.z_got[unit - self.kept].astype(F32)).astype(BF16)
        s.m[p, j, OWN * (z.shape[0] // 2):] = gated(z)

    def block(self, p, j, k):
        shard = self.s.m.shape[2] // 4
        return self.s.m.at[p, j, pl.ds(k * shard, shard)]

    def send(self, p, j):
        if p > 0 or j >= self.carry:
            self.across[p, j] = self.links.push(self.block(p, j, OWN), self.block(p, j, ACROSS), ACROSS, 'm_across')

    def send_partner(self, p):
        m = self.s.m
        shard = m.shape[2] // 4
        self.partner[p] = self.links.push(m.at[p, :, pl.ds(OWN * shard, shard)], m.at[p, :, pl.ds(PARTNER * shard, shard)], PARTNER, 'm')

    def forward(self, p, j):
        if p > 0 or j >= self.carry:
            self.across[p, j].wait_recv()
        else:
            self.carried[j].wait()
        self.diag[p, j] = self.links.push(self.block(p, j, ACROSS), self.block(p, j, DIAG), PARTNER, 'm')

    def send_o_yz(self):
        y, s = self.links.y, self.s
        self.o_copy.wait()
        self.o_yz = self.links.push(s.o_in.at[1 - y], s.o_yz, YZ, 'o_yz')

    def o_block(self, p, k):
        shard = self.s.o.shape[1] // 4
        return self.s.o.at[p, pl.ds(k * shard, shard)]

    def send_o(self, p):
        y, s = self.links.y, self.s
        if p == 0:
            self.o_yz.wait_recv()
        shard = s.o.shape[1] // 4
        seqs = shard // 2
        s.o[p, pl.ds(OWN * shard + pl.multiple_of(y * seqs, seqs), seqs), :] = s.o_in[y, p * seqs:(p + 1) * seqs]
        s.o[p, pl.ds(OWN * shard + pl.multiple_of((1 - y) * seqs, seqs), seqs), :] = s.o_yz[p * seqs:(p + 1) * seqs]
        self.o_across[p] = self.links.push(self.o_block(p, OWN), self.o_block(p, ACROSS), ACROSS, 'o')
        self.o_core[p] = self.links.slot()
        self.links.push(self.o_block(p, OWN), self.o_block(p, PARTNER), PARTNER, 'o', self.o_core[p])

    def forward_o(self, p):
        self.o_across[p].wait_recv()
        self.links.push(self.o_block(p, ACROSS), self.o_block(p, DIAG), PARTNER, 'o', self.o_core[p])

    def project_o(self, p):
        s = self.s
        self.links.take(self.o_core[p], s.o.at[p, pl.ds(0, s.o.shape[1] // 2)])
        if not self.wo_ready:
            self.wo.wait()
            self.wo_ready = True
        s.acc[p] += dot(s.o[p], s.wo[...])

    def down(self, p, j):
        s = self.s
        if j == 0:
            self.partner[p].wait_recv()
        self.diag[p, j].wait_recv()
        if not self.wd_ready:
            self.wd.wait()
            self.wd_ready = True
        part = dot(s.m[p, j], s.wd[j * self.cols:(j + 1) * self.cols])
        if j == 0:
            s.acc[p] = part
        else:
            s.acc[p] += part

    def send_update(self, p):
        s, links = self.s, self.links
        shard = s.acc.shape[1] // 4
        for k in range(4):
            s.update[p, pl.ds(pl.multiple_of(links.blocks[k] * shard, shard), shard), :] = s.acc[p, k * shard:(k + 1) * shard, :]
        s.up_part[p] = s.update[p].T.astype(BF16)
        part = s.up_recv.shape[1]
        src = s.up_part.at[p, pl.ds(pl.multiple_of((1 - links.y) * part, part), part)]
        self.up[p] = links.push(src, s.up_recv.at[p], YZ, 'up')

    def new_h(self, p):
        s, links = self.s, self.links
        self.up[p].wait_recv()
        part = s.up_recv.shape[1]
        own = s.up_part[p, pl.ds(pl.multiple_of(links.y * part, part), part), :]
        return (s.h_in[p].astype(F32) + (own.astype(F32) + s.up_recv[p].astype(F32))).astype(BF16)

    def sizes(self):
        s = self.s
        sent = 3 * s.m.shape[2] // 4
        shard = sent // 3
        return dict(m=s.m.at[:, :, pl.ds(0, 2 * shard)],
                m_across=s.m.at[:, pl.ds(0, self.chunks - self.carry // PARTS), pl.ds(0, shard)], o=s.o.at[:, pl.ds(0, sent)], o_yz=s.o_yz, up=s.up_recv)

    def open(self):
        links, chunks = self.links, self.chunks
        for j in range(self.carry + 1):
            self.mix(0, j)
        links.meet()
        for j in range(self.carry + 1):
            self.send(0, j)
        self.send_o_yz()
        for j in range(self.carry + 1, chunks):
            self.mix(0, j)
            self.send(0, j)
            if j == 2 + self.carry:
                self.send_o(0)
        self.send_partner(0)
        for j in range(chunks):
            self.mix(1, j)
            self.send(1, j)
            if j == 1:
                self.send_o(1)
        self.send_partner(1)
        self.h_copy.wait()


def start_kernel(names, model_dim, h_hbm, gain_hbm, wa_hbm, wm_hbm, qkv_out, zsend_out, zmine_out, h_out, *scratch):
    s = types.SimpleNamespace(**dict(zip(names, scratch)))
    links = Links(s.send, s.recv, s.local, EVERYONE)
    h_copy = links.copy(h_hbm, s.h_in)
    f = Front(links, 0, gain_hbm, wa_hbm, wm_hbm, model_dim, (qkv_out, zsend_out, zmine_out, h_out), s)
    rows = h_hbm.shape[1]
    lanes = rows // PARTS
    order = part_order(rows, False)
    h_copy.wait()
    own = dot(s.h_in[...], order)
    for p in range(PARTS):
        f.squares(p, own[:, p * lanes:(p + 1) * lanes])
    f.constants()
    links.meet()
    for p in range(PARTS):
        f.send_h(p)
    for j in range(f.chunks):
        f.split_weights(j)
    for p in range(PARTS):
        f.normalize(p)
    f.project(range(PARTS), 0)
    for p in range(PARTS):
        f.attend_core(p)
    for j in range(1, f.chunks):
        f.project(range(PARTS), j)
        if j == f.chunks - 1:
            f.attend_ends(0)
        for p in range(PARTS):
            f.combine(p, j - 1)
    f.attend_ends(1)
    for p in range(PARTS):
        f.combine(p, f.chunks - 1)
    f.take_early()
    links.drain(*f.sizes())


def middle_kernel(names, model_dim, h_hbm, o_hbm, gain_hbm, zmine_hbm, zgot_hbm, wd_hbm, wo_hbm, wa_hbm, wm_hbm, qkv_out, zsend_out,
                  zmine_out, h_out, *scratch):
    s = types.SimpleNamespace(**dict(zip(names, scratch)))
    links = Links(s.send, s.recv, s.local, EVERYONE)
    b = Back(links, 0, h_hbm, o_hbm, zgot_hbm, zmine_hbm, wd_hbm, wo_hbm, s)
    f = Front(links, 1, gain_hbm, wa_hbm, wm_hbm, model_dim, (qkv_out, zsend_out, zmine_out, h_out), s)
    b.open()
    f.constants()

    def pass_h(p):
        f.squares(p, b.new_h(p).astype(F32))
        f.send_h(p)

    first_part(b, f.split_weights)
    second_part(b, lambda: pass_h(0))
    f.normalize(0)
    f.project([0], 0)
    f.attend_core(0)
    pass_h(1)
    f.project([0], 1)
    f.project([0], 2)
    f.combine(0, 0)
    f.project([0], 3)
    f.combine(0, 1)
    f.project([0], 4)
    f.combine(0, 2)
    f.combine(0, 3)
    f.normalize(1)
    f.project([1], 0)
    f.combine(0, 4)
    f.attend_core(1)
    f.project([1], 1)
    f.attend_ends(0)
    f.project([1], 2)
    f.combine(1, 0)
    f.project([1], 3)
    f.combine(1, 1)
    f.project([1], 4)
    f.combine(1, 2)
    f.combine(1, 3)
    f.take_early()
    f.combine(1, 4)
    f.attend_ends(1)
    sent, stored = f.sizes()
    links.drain(dict(**sent, **b.sizes()), stored)


def first_part(b, filler):
    for j in range(b.chunks):
        b.forward(0, j)
        if filler is not None:
            filler(j)
        if j == 2 + b.carry:
            b.forward_o(0)
        if j >= 1:
            b.down(0, j - 1)
    b.project_o(0)
    b.down(0, b.chunks - 1)
    b.send_update(0)
    b.forward(1, 0)


def second_part(b, when_updated):
    for j in range(1, b.chunks):
        b.forward(1, j)
        if j == 1:
            b.forward_o(1)
        b.down(1, j - 1)
        if j == 2:
            b.project_o(1)
        if j == b.chunks - 3:
            when_updated()
    b.down(1, b.chunks - 1)
    b.send_update(1)


def end_kernel(names, h_hbm, o_hbm, zmine_hbm, zgot_hbm, wd_hbm, wo_hbm, h_out, *scratch):
    s = types.SimpleNamespace(**dict(zip(names, scratch)))
    links = Links(s.send, s.recv, s.local, [PARTNER, ACROSS, YZ])
    b = Back(links, 1, h_hbm, o_hbm, zgot_hbm, zmine_hbm, wd_hbm, wo_hbm, s)
    b.open()
    first_part(b, None)
    h_new = []
    second_part(b, lambda: h_new.append(b.new_h(0)))
    order = part_order(h_out.shape[1], True)
    h_new.append(b.new_h(1))
    h_out[...] = dot(jnp.concatenate(h_new, axis=1), order).astype(BF16)
    links.drain(b.sizes(), {})


def attention_kernel(layer, per_copy, per_step, len_hbm, qkv_hbm, k_hbm, v_hbm, *rest):
    k_out, v_out, o_hbm, kbuf, vbuf, q_scr, o_scr, qkv_ref, o_ref, len_ref, in_sem, out_sem, small_sem = rest[-13:]
    num_seqs, kv_heads, cache_len, head_dim = kbuf.shape
    slots = qkv_ref.shape[2] // head_dim
    rows = kv_heads * slots
    scale = head_dim ** -0.5

    def load(n):
        run = pl.ds(n * per_copy, per_copy)
        return (pltpu.make_async_copy(k_hbm.at[layer, run], kbuf.at[run], in_sem.at[0, n]),
                pltpu.make_async_copy(v_hbm.at[layer, run], vbuf.at[run], in_sem.at[1, n]))

    def store(n):
        run = pl.ds(n * per_copy, per_copy)
        return (pltpu.make_async_copy(kbuf.at[run], k_out.at[layer, run], out_sem.at[0, n]),
                pltpu.make_async_copy(vbuf.at[run], v_out.at[layer, run], out_sem.at[1, n]))

    qkv_copy = pltpu.make_async_copy(qkv_hbm, qkv_ref, small_sem.at[0])
    len_copy = pltpu.make_async_copy(len_hbm, len_ref, small_sem.at[1])
    qkv_copy.start()
    len_copy.start()

    @pl.loop(0, num_seqs // per_copy)
    def _(n):
        for c in load(n):
            c.start()

    qkv_copy.wait()
    len_copy.wait()
    for head in range(kv_heads):
        for j in range(slots):
            q_scr[pl.ds(head * slots + j, num_seqs, stride=rows), :] = (
                qkv_ref[head, :, j * head_dim:(j + 1) * head_dim].astype(F32))

    tile_row = lax.broadcasted_iota(jnp.int32, (16, head_dim), 0)
    position = lax.broadcasted_iota(jnp.int32, (rows, cache_len), 1)

    def patch(n):
        for c in load(n):
            c.wait()
        for sub in range(per_copy):
            i = n * per_copy + sub
            length = len_ref[i]
            base = pl.multiple_of((length // 16) * 16, 16)
            hit = tile_row == length - base
            for head in range(kv_heads):
                for buf, j in ((kbuf, slots - 2), (vbuf, slots - 1)):
                    new = q_scr[pl.ds(i * rows + head * slots + j, 1), :]
                    old = buf[i, head, pl.ds(base, 16), :].astype(F32)
                    buf[i, head, pl.ds(base, 16), :] = jnp.where(hit, new, old).astype(buf.dtype)
        for c in store(n):
            c.start()

    def attend(group):
        scores, probs = [], []
        for i in group:
            q = q_scr[pl.ds(pl.multiple_of(i * rows, rows), rows), :].astype(BF16)
            by_head = [lax.dot_general(q, kbuf[i, head], (((1,), (1,)), ((), ())), preferred_element_type=F32)
                       for head in range(kv_heads)]
            scores.append(jnp.concatenate([by_head[head][head * slots:(head + 1) * slots] for head in range(kv_heads)], axis=0))
        for i, score in zip(group, scores):
            score = jnp.where(position <= len_ref[i], score * scale, -1e30)
            e = jnp.exp(score - jnp.max(score, axis=1, keepdims=True))
            probs.append((e / jnp.sum(e, axis=1, keepdims=True)).astype(BF16))
        for i, p in zip(group, probs):
            by_head = [dot(p, vbuf[i, head]) for head in range(kv_heads)]
            o_scr[pl.ds(pl.multiple_of(i * rows, rows), rows), :] = jnp.concatenate(
                [by_head[head][head * slots:(head + 1) * slots] for head in range(kv_heads)], axis=0)

    @pl.loop(0, num_seqs // per_copy)
    def _(n):
        patch(n)
        for first in range(0, per_copy, per_step):
            attend([n * per_copy + first + sub for sub in range(per_step)])

    for head in range(kv_heads):
        for j in range(slots - 2):
            o_ref[head, :, j * head_dim:(j + 1) * head_dim] = (
                o_scr[pl.ds(head * slots + j, num_seqs, stride=rows), :].astype(o_ref.dtype))
    o_copy = pltpu.make_async_copy(o_ref, o_hbm, small_sem.at[2])
    o_copy.start()

    @pl.loop(0, num_seqs // per_copy)
    def _(n):
        for c in store(n):
            c.wait()

    o_copy.wait()


VMEM = pl.BlockSpec(memory_space=pltpu.VMEM)
HBM = pl.BlockSpec(memory_space=pltpu.HBM)


def attention(layer, lengths, qkv, k_cache, v_cache, outs):
    layers, num_seqs, kv_heads, cache_len, head_dim = k_cache.shape
    slots = qkv.shape[2] // head_dim
    rows = kv_heads * slots
    return pl.pallas_call(
        functools.partial(attention_kernel, layer, PER_COPY, PER_STEP),
        out_shape=(jax.ShapeDtypeStruct(k_cache.shape, k_cache.dtype), jax.ShapeDtypeStruct(v_cache.shape, v_cache.dtype),
                   jax.ShapeDtypeStruct((kv_heads, num_seqs, (slots - 2) * head_dim), BF16)),
        in_specs=[HBM] * (4 + len(outs)),
        out_specs=(HBM, HBM, HBM),
        scratch_shapes=[pltpu.VMEM((num_seqs, kv_heads, cache_len, head_dim), BF16)] * 2
        + [pltpu.VMEM((num_seqs * rows, head_dim), F32)] * 2 + [
            pltpu.VMEM(qkv.shape, BF16), pltpu.VMEM((kv_heads, num_seqs, (slots - 2) * head_dim), BF16),
            pltpu.SMEM((num_seqs,), jnp.int32)]
        + [pltpu.SemaphoreType.DMA((2, num_seqs // PER_COPY))] * 2 + [pltpu.SemaphoreType.DMA((3,))],
        input_output_aliases={4: 0, 5: 1} if outs else {},
        compiler_params=pltpu.CompilerParams(vmem_limit_bytes=VMEM_LIMIT),
        cost_estimate=pl.CostEstimate(flops=10 ** 10, bytes_accessed=8 * num_seqs * kv_heads * cache_len * head_dim, transcendentals=0),
        name=f'attention_{layer}',
    )(lengths, qkv, k_cache, v_cache, *outs)


def solution(mesh):
    seq_axes = ('rep', 'x', 'yz')
    hidden_spec = P('rep', ('x', 'yz'))
    cache_spec = P(None, seq_axes, None, None, None)
    in_specs = (hidden_spec, P(None, 'x'), P(None, 'x', 'yz'), P(None, 'x', None, 'yz'), P(None, 'yz', 'x'), P(None, 'yz', 'x'), cache_spec, cache_spec, P(seq_axes))
    out_specs = (hidden_spec, cache_spec, cache_spec)
    swap = [(0, 2), (2, 0), (1, 3), (3, 1)]

    def device_step(hidden, norm_gain, w_attn, w_mlp, w_out, w_down, k_cache, v_cache, lengths):
        rows, part = hidden.shape
        depth, attn_cols = w_attn.shape[1:]
        model_dim = depth * mesh.shape['x']
        mlp_cols = w_mlp.shape[3]
        out_depth = w_out.shape[1]
        cols = mlp_cols // CHUNKS
        units = CHUNKS * PARTS
        lanes = rows // PARTS
        half, shard = lanes // 2, lanes // 4
        seqs = shard // 2
        num_seqs = PARTS * seqs

        def semaphores(groups, remote, local):
            return dict(send=pltpu.SemaphoreType.DMA((groups,)), recv=pltpu.SemaphoreType.DMA((remote,)),
                    local=pltpu.SemaphoreType.DMA((local,)))

        def front_scratch(layer):
            return dict(
                sq_send=pltpu.VMEM((PARTS, SQ_ROWS, lanes), F32), sq_recv=pltpu.VMEM((PARTS, 8, SQ_ROWS, lanes), F32),
                h=pltpu.VMEM((PARTS, depth, lanes), BF16), gain_in=pltpu.VMEM(norm_gain.shape, BF16), gain=pltpu.VMEM((depth, lanes), F32),
                u=pltpu.VMEM((PARTS, lanes, depth), BF16), u_rel=pltpu.VMEM((PARTS, lanes, depth), BF16),
                wa=pltpu.VMEM((depth, attn_cols), BF16), wm=pltpu.VMEM((depth, 2, mlp_cols), BF16),
                w_split=pltpu.VMEM((2, depth, mlp_cols), BF16),
                a_part=pltpu.VMEM((PARTS, lanes, attn_cols), BF16), a_core=pltpu.VMEM((PARTS, half, attn_cols), BF16),
                a_sum=pltpu.VMEM((PARTS, half, attn_cols), BF16), a_got=pltpu.VMEM((PARTS, 3, seqs, attn_cols), BF16),
                a_full=pltpu.VMEM((PARTS, 2, seqs, attn_cols), BF16),
                z_part=pltpu.VMEM((PARTS, CHUNKS, 2 * lanes, cols), BF16),
                z_recv=pltpu.VMEM((PARTS, CHUNKS, lanes, cols), BF16), z_x=pltpu.VMEM((units, half, cols), BF16),
                z_mine=pltpu.VMEM((units, half, cols), BF16), z_early=pltpu.VMEM((EARLY[layer], half, cols), BF16),
            )

        back_scratch = dict(
            o_yz=pltpu.VMEM((num_seqs, out_depth), BF16), o=pltpu.VMEM((PARTS, lanes, out_depth), BF16),
            m=pltpu.VMEM((PARTS, CHUNKS, lanes, cols), BF16), z_in=pltpu.VMEM((units, half, cols), BF16),
            o_in=pltpu.VMEM((2, num_seqs, out_depth), BF16),
            h_in=pltpu.VMEM((PARTS, part, lanes), BF16),
            wd=pltpu.VMEM((mlp_cols, depth), BF16), wo=pltpu.VMEM((out_depth, depth), BF16),
            acc=pltpu.VMEM((PARTS, lanes, depth), F32), update=pltpu.VMEM((PARTS, lanes, depth), F32),
            up_part=pltpu.VMEM((PARTS, depth, lanes), BF16), up_recv=pltpu.VMEM((PARTS, part, lanes), BF16),
        )

        def got_scratch(layer):
            return dict(z_got=pltpu.VMEM((units - EARLY[layer], half, cols), BF16))

        def front_shapes(layer):
            return (
                jax.ShapeDtypeStruct((2, num_seqs, attn_cols), BF16), jax.ShapeDtypeStruct((units - EARLY[layer] + CARRY[layer] // PARTS, half, cols), BF16),
                jax.ShapeDtypeStruct((units, half, cols), BF16), jax.ShapeDtypeStruct((PARTS, part, lanes), BF16))
        front_specs = (HBM,) * 4

        def call(kernel, name, collective_id, scratch, in_specs, out_shape, out_specs, *args):
            return pl.pallas_call(
                functools.partial(kernel, tuple(scratch)), out_shape=out_shape, in_specs=list(in_specs), out_specs=out_specs,
                scratch_shapes=list(scratch.values()), name=name,
                compiler_params=pltpu.CompilerParams(collective_id=collective_id, has_side_effects=True, vmem_limit_bytes=END_VMEM_LIMIT if kernel is end_kernel else VMEM_LIMIT),
            )(*args)

        def start(names, *refs):
            start_kernel(names, model_dim, *refs)

        def middle(names, *refs):
            middle_kernel(names, model_dim, *refs)

        qkv, zsend, zmine, h_block = call(
            start, 'start', 0, dict(**semaphores(6, 18 + EARLY[0], 8), **front_scratch(0), h_in=pltpu.VMEM((part, rows), BF16)), (HBM,) * 4,
            front_shapes(0), front_specs, hidden.T, norm_gain, w_attn, w_mlp)
        zgot = lax.ppermute(zsend, 'x', swap)
        k_new, v_new, o = attention(0, lengths, qkv, k_cache, v_cache, ())
        qkv, zsend, zmine, h_block = call(
            middle, 'middle', 1, dict(**semaphores(11, 47 + EARLY[1], 17), **front_scratch(1), **back_scratch, **got_scratch(0),
                       m_early=pltpu.VMEM((half, cols), BF16)), (HBM,) * 9,
            front_shapes(1), front_specs, h_block, o, norm_gain, zmine, zgot, w_down, w_out, w_attn, w_mlp)
        zgot = lax.ppermute(zsend, 'x', swap)
        k_new, v_new, o = attention(1, lengths, qkv, k_cache, v_cache, (k_new, v_new))
        h_out = call(
            end_kernel, 'end', 2, dict(**semaphores(5, 27, 11), **back_scratch, **got_scratch(1)), (HBM,) * 6,
            jax.ShapeDtypeStruct((part, rows), BF16), VMEM, h_block, o, zmine, zgot, w_down, w_out)
        return h_out.T, k_new, v_new

    return jax.shard_map(device_step, mesh=mesh, in_specs=in_specs, out_specs=out_specs, check_vma=False)
```
